32 devices in a mesh: seq: 4 (over z), fsdp: 8 (over y, x, core).
Axes of the slice: x: 2, y: 2, z: 4, core: 2. Of those that a mesh axis runs over, the one named last changes fastest.
Arguments:
- inputs: bfloat16 [8, 1024, 512], P('fsdp', 'seq'), may hold values from -6 to 6
- cotangent: bfloat16 [8, 1024, 512], P('fsdp', 'seq'), may hold values from -6 to 6
- lengths: int32 [8], P('fsdp'), may hold values from 256 to 1024, as said below
- square: float32 [4096, 512], P(('seq', 'fsdp')), may hold values from -0.25 to 0.25
- upward: float32 [4096, 512], P(('seq', 'fsdp')), may hold values from -0.25 to 0.25
- downward: float32 [4096, 512], P(('seq', 'fsdp')), may hold values from -0.125 to 0.125
- vectors: float32 [14, 512], P(None, ('seq', 'fsdp')), may hold values from 0.5 to 1.5
- kernel: float32 [31, 512], P(None, ('seq', 'fsdp')), may hold values from -1 to 1
- square_momentum: float32 [4096, 512], P(('seq', 'fsdp')), may hold values from -60 to 60
- square_variance: float32 [4096, 512], P(('seq', 'fsdp')), may hold values from 10 to 1000
- upward_momentum: float32 [4096, 512], P(('seq', 'fsdp')), may hold values from -60 to 60
- upward_variance: float32 [4096, 512], P(('seq', 'fsdp')), may hold values from 10 to 1000
- downward_momentum: float32 [4096, 512], P(('seq', 'fsdp')), may hold values from -60 to 60
- downward_variance: float32 [4096, 512], P(('seq', 'fsdp')), may hold values from 10 to 1000
- vectors_momentum: float32 [14, 512], P(None, ('seq', 'fsdp')), may hold values from -60 to 60
- vectors_variance: float32 [14, 512], P(None, ('seq', 'fsdp')), may hold values from 10 to 1000
- kernel_momentum: float32 [31, 512], P(None, ('seq', 'fsdp')), may hold values from -60 to 60
- kernel_variance: float32 [31, 512], P(None, ('seq', 'fsdp')), may hold values from 10 to 1000
Outputs:
- layer_output: bfloat16 [8, 1024, 512], P('fsdp', 'seq')
- input_grad: float32 [8, 1024, 512], P('fsdp', 'seq')
- square_grad: float32 [4096, 512], P(('seq', 'fsdp'))
- upward_grad: float32 [4096, 512], P(('seq', 'fsdp'))
- downward_grad: float32 [4096, 512], P(('seq', 'fsdp'))
- vectors_grad: float32 [14, 512], P(None, ('seq', 'fsdp'))
- kernel_grad: float32 [31, 512], P(None, ('seq', 'fsdp'))
- square_next: float32 [4096, 512], P(('seq', 'fsdp'))
- upward_next: float32 [4096, 512], P(('seq', 'fsdp'))
- downward_next: float32 [4096, 512], P(('seq', 'fsdp'))
- vectors_next: float32 [14, 512], P(None, ('seq', 'fsdp'))
- kernel_next: float32 [31, 512], P(None, ('seq', 'fsdp'))
- momentum_square: float32 [4096, 512], P(('seq', 'fsdp'))
- variance_square: float32 [4096, 512], P(('seq', 'fsdp'))
- momentum_upward: float32 [4096, 512], P(('seq', 'fsdp'))
- variance_upward: float32 [4096, 512], P(('seq', 'fsdp'))
- momentum_downward: float32 [4096, 512], P(('seq', 'fsdp'))
- variance_downward: float32 [4096, 512], P(('seq', 'fsdp'))
- momentum_vectors: float32 [14, 512], P(None, ('seq', 'fsdp'))
- variance_vectors: float32 [14, 512], P(None, ('seq', 'fsdp'))
- momentum_kernel: float32 [31, 512], P(None, ('seq', 'fsdp'))
- variance_kernel: float32 [31, 512], P(None, ('seq', 'fsdp'))
The draws below stay inside these ranges and needn't reach their ends.
Inputs may be any that keep to these rules, and one draw needn't show every extreme that they name: `lengths`: every sequence has at least 256 valid frames; some sequence has exactly 256 and some exactly 1024.
All inputs are finite; a program needn't handle non-finite values.
Results may differ from the reference program's by a relative error of at most 0.017.
Values may be sent and summed in bfloat16 or wider, within the bound.
A program may use at most 192 MiB of HBM per device.

```python
import math
import jax
import jax.numpy as jnp
from jax import lax

D = 512
H = 8
FF = 2048
KW = 31
LEN = 1024
ADAM_STEP = 4
SEQS = 8


def draw_lengths(key, part):
    first_key, second_key = jax.random.split(jax.random.fold_in(key, 7))
    drawn = jax.random.randint(first_key, (SEQS,), LEN // 4, LEN + 1)
    order = jax.random.permutation(second_key, SEQS)
    drawn = drawn.at[order[0]].set(LEN)
    drawn = drawn.at[order[1]].set(LEN // 4)
    return drawn.astype(jnp.int32)


def level_of(own_key, shape, cuts, low, largest):
    def one(axis_at, shards_of):
        heights = jax.random.uniform(jax.random.fold_in(jax.random.fold_in(own_key, 6), axis_at), (shards_of,), jnp.float32, low / len(cuts), largest / len(cuts))
        return jnp.repeat(jnp.exp(heights), shape[axis_at] // shards_of).reshape((-1,) + (1,) * (len(shape) - axis_at - 1))

    gain = one(*cuts[0])
    for cut in cuts[1:]:
        gain = gain * one(*cut)
    return gain


def noise(rng, extent, deviation, bound, cuts=(), held_as=jnp.bfloat16):
    values = deviation * jax.random.normal(rng, extent, jnp.float32)
    if cuts:
        values = values * level_of(rng, extent, cuts, -0.22, 0.18)
    return jnp.clip(values, -bound, bound).astype(held_as)


def setup_inputs(seed: int = 0) -> dict:
    key_list = jax.random.split(jax.random.key(seed), 19)
    return {
        "inputs": noise(key_list[0], (SEQS, LEN, D), 1.0, 6.0, ((0, 8), (1, 4))),
        "cotangent": noise(key_list[1], (SEQS, LEN, D), 1.0, 6.0, ((0, 8), (1, 4))),
        "lengths": draw_lengths(jax.random.fold_in(key_list[18], 71), 0),
        "square": noise(key_list[3], (8 * D, D), D ** -0.5, 0.25, ((0, 32),), jnp.float32),
        "upward": noise(key_list[4], (2 * FF, D), D ** -0.5, 0.25, ((0, 32),), jnp.float32),
        "downward": noise(key_list[5], (2 * FF, D), FF ** -0.5, 0.125, ((0, 32),), jnp.float32),
        "vectors": jnp.clip(0.5 + 1.0 * jax.random.uniform(key_list[6], (14, D), jnp.float32) ** level_of(key_list[6], (14, D), ((1, 32),), -0.2, 0.2), 0.5, 1.5),
        "kernel": noise(key_list[7], (KW, D), KW ** -0.5, 1.0, ((1, 32),), jnp.float32),
        "square_momentum": noise(key_list[8], (8 * D, D), 10.0, 60.0, ((0, 32),), jnp.float32),
        "square_variance": jnp.clip(jnp.exp(math.log(1000.0) - 4.6051702 * jax.random.uniform(key_list[9], (8 * D, D), jnp.float32) ** level_of(key_list[9], (8 * D, D), ((0, 32),), -0.2, 0.2)), 10.0, 1000.0),
        "upward_momentum": noise(key_list[10], (2 * FF, D), 10.0, 60.0, ((0, 32),), jnp.float32),
        "upward_variance": jnp.clip(jnp.exp(math.log(1000.0) - 4.6051702 * jax.random.uniform(key_list[11], (2 * FF, D), jnp.float32) ** level_of(key_list[11], (2 * FF, D), ((0, 32),), -0.2, 0.2)), 10.0, 1000.0),
        "downward_momentum": noise(key_list[12], (2 * FF, D), 10.0, 60.0, ((0, 32),), jnp.float32),
        "downward_variance": jnp.clip(jnp.exp(math.log(1000.0) - 4.6051702 * jax.random.uniform(key_list[13], (2 * FF, D), jnp.float32) ** level_of(key_list[13], (2 * FF, D), ((0, 32),), -0.2, 0.2)), 10.0, 1000.0),
        "vectors_momentum": noise(key_list[14], (14, D), 10.0, 60.0, ((1, 32),), jnp.float32),
        "vectors_variance": jnp.clip(jnp.exp(math.log(1000.0) - 4.6051702 * jax.random.uniform(key_list[15], (14, D), jnp.float32) ** level_of(key_list[15], (14, D), ((1, 32),), -0.2, 0.2)), 10.0, 1000.0),
        "kernel_momentum": noise(key_list[16], (KW, D), 10.0, 60.0, ((1, 32),), jnp.float32),
        "kernel_variance": jnp.clip(jnp.exp(math.log(1000.0) - 4.6051702 * jax.random.uniform(key_list[17], (KW, D), jnp.float32) ** level_of(key_list[17], (KW, D), ((1, 32),), -0.2, 0.2)), 10.0, 1000.0),
    }


LN_EPS = 1e-05
BN_EPS = 1e-05
BETA_ONE = 0.9
BETA_TWO = 0.98
ADAM_EPS = 1e-08
LEARN_RATE = 0.005
DECAY_RATE = 0.01

def mix(form, first_op, second_op):
    return jnp.einsum(form, first_op.astype(jnp.float32), second_op.astype(jnp.float32))

def linear(signal, weight):
    return lax.dot_general(signal, weight, (((1,), (1,)), ((), ())), preferred_element_type=jnp.float32)

def outer(first_op, second_op):
    return lax.dot_general(first_op, second_op, (((0,), (0,)), ((), ())), preferred_element_type=jnp.float32)

def layer_norm(signal, norm_gain, norm_shift):
    row_mean = lax.optimization_barrier(jnp.mean(signal, axis=-1, keepdims=True))
    centred = signal - row_mean
    row_var = lax.optimization_barrier(jnp.mean(centred * centred, axis=-1, keepdims=True))
    return centred * lax.rsqrt(row_var + LN_EPS) * norm_gain + norm_shift

def norm_back(signal, norm_gain, norm_shift, upstream):
    pullback = jax.vjp(layer_norm, signal, norm_gain, norm_shift)[1]
    return pullback(upstream)

def silu_slope(argument):
    sigma_val = jax.nn.sigmoid(argument)
    return sigma_val * (1.0 + argument * (1.0 - sigma_val))

def position_table(seq_frames, model_width):
    relative = (seq_frames - 1 - jnp.arange(2 * seq_frames - 1)).astype(jnp.float32)[:, None]
    pairs = jnp.arange(model_width // 2).astype(jnp.float32)
    frequency = jnp.exp(-math.log(10000.0) * 2.0 * pairs / model_width)
    phases = relative * frequency[None, :]
    stacked = jnp.stack([jnp.sin(phases), jnp.cos(phases)], axis=-1)
    return stacked.reshape(2 * seq_frames - 1, model_width).astype(jnp.bfloat16)

def heads_of(signal, head_size):
    return signal.reshape(signal.shape[0], signal.shape[1] // head_size, head_size)

def block_scores(query_content, query_position, key_heads, pos_heads, row_start, length, block_rows):
    seq_frames = key_heads.shape[0]
    head_size = key_heads.shape[2]
    window_len = block_rows + seq_frames - 1
    content = lax.dynamic_slice_in_dim(query_content, row_start, block_rows, 0)
    positional = lax.dynamic_slice_in_dim(query_position, row_start, block_rows, 0)
    direct = mix('rhd,khd->hrk', content, key_heads)
    window = lax.dynamic_slice_in_dim(pos_heads, seq_frames - block_rows - row_start, window_len, 0)
    pos_scores = mix('rhd,whd->hrw', positional, window)
    head_count = pos_scores.shape[0]
    flattened = pos_scores.reshape(head_count, block_rows * window_len)
    flattened = flattened[:, block_rows - 1:block_rows - 1 + block_rows * (window_len - 1)]
    shifted = flattened.reshape(head_count, block_rows, window_len - 1)[:, :, :seq_frames]
    scores = (direct + shifted) * (1.0 / math.sqrt(head_size))
    key_live = jnp.arange(seq_frames, dtype=jnp.int32) < length
    return (jnp.where(key_live[None, None, :], scores, -1e+30), window, content, positional)

def unshift(spread_in, window_len, seq_frames):
    head_count, block_rows = (spread_in.shape[0], spread_in.shape[1])
    widened = jnp.pad(spread_in, ((0, 0), (0, 0), (0, window_len - 1 - seq_frames)))
    flattened = widened.reshape(head_count, block_rows * (window_len - 1))
    flattened = jnp.pad(flattened, ((0, 0), (block_rows - 1, 1)))
    return flattened.reshape(head_count, block_rows, window_len)

def attend(query_content, query_position, key_heads, value_heads, pos_heads, length, block_rows):
    seq_frames, head_count, head_size = key_heads.shape

    def one_block(row_start):
        scores = block_scores(query_content, query_position, key_heads, pos_heads, row_start, length, block_rows)[0]
        row_max = lax.optimization_barrier(jnp.max(scores, axis=-1, keepdims=True))
        log_total = row_max + jnp.log(lax.optimization_barrier(jnp.sum(jnp.exp(scores - row_max), axis=-1, keepdims=True)))
        probability = jnp.exp(scores - log_total).astype(jnp.bfloat16)
        attended = mix('hrk,khd->rhd', probability, value_heads).astype(jnp.bfloat16)
        return (attended, log_total[..., 0])
    starts = (jnp.arange(seq_frames // block_rows) * block_rows).astype(jnp.int32)
    attended, log_totals = lax.map(one_block, starts)
    return (attended.reshape(seq_frames, head_count, head_size), log_totals)

def attend_back(query_content, query_position, key_heads, value_heads, pos_heads, length, block_rows, log_totals, grad_heads):
    seq_frames, head_count, head_size = key_heads.shape
    window_len = block_rows + seq_frames - 1

    def one_block(running, block_item):
        grad_keys, grad_values, grad_table = running
        row_start, log_total = block_item
        scores, window, content, positional = block_scores(query_content, query_position, key_heads, pos_heads, row_start, length, block_rows)
        probability = jnp.exp(scores - log_total[..., None])
        prob_bf = probability.astype(jnp.bfloat16)
        grad_here = lax.dynamic_slice_in_dim(grad_heads, row_start, block_rows, 0)
        grad_prob = mix('rhd,khd->hrk', grad_here, value_heads)
        row_delta = lax.optimization_barrier(jnp.sum(probability * grad_prob, axis=-1, keepdims=True))
        grad_score = (probability * (grad_prob - row_delta) * (1.0 / math.sqrt(head_size))).astype(jnp.bfloat16)
        grad_content = mix('hrk,khd->rhd', grad_score, key_heads)
        grad_keys = grad_keys + mix('hrk,rhd->khd', grad_score, content)
        grad_values = grad_values + mix('hrk,rhd->khd', prob_bf, grad_here)
        spread_out = unshift(grad_score, window_len, seq_frames)
        grad_position = mix('hrw,whd->rhd', spread_out, window)
        window_add = mix('hrw,rhd->whd', spread_out, positional)
        offset = seq_frames - block_rows - row_start
        current = lax.dynamic_slice_in_dim(grad_table, offset, window_len, 0)
        grad_table = lax.dynamic_update_slice_in_dim(grad_table, current + window_add, offset, 0)
        return ((grad_keys, grad_values, grad_table), (grad_content, grad_position))
    starts = (jnp.arange(seq_frames // block_rows) * block_rows).astype(jnp.int32)
    zero_keys = jnp.zeros((seq_frames, head_count, head_size), jnp.float32)
    zero_table = jnp.zeros((2 * seq_frames - 1, head_count, head_size), jnp.float32)
    (grad_keys, grad_values, grad_table), (grad_content, grad_position) = lax.scan(one_block, (zero_keys, zero_keys, zero_table), (starts, log_totals))
    grad_content = grad_content.reshape(seq_frames, head_count, head_size)
    grad_position = grad_position.reshape(seq_frames, head_count, head_size)
    return (grad_keys, grad_values, grad_table, grad_content, grad_position)

def depth_forward(glu_pad, conv_taps, frame_count):
    result = jnp.zeros((frame_count, conv_taps.shape[1]), jnp.float32)
    for tap_index in range(conv_taps.shape[0]):
        result = result + conv_taps[tap_index] * glu_pad[tap_index:tap_index + frame_count].astype(jnp.float32)
    return result

def depth_back(grad_pad, glu_pad, conv_taps, frame_count):
    rim_width = (conv_taps.shape[0] - 1) // 2
    upstream = grad_pad[rim_width:rim_width + frame_count].astype(jnp.float32)
    tap_grads = []
    grad_input = jnp.zeros((frame_count, conv_taps.shape[1]), jnp.float32)
    for tap_index in range(conv_taps.shape[0]):
        tap_grads.append(lax.optimization_barrier(jnp.sum(upstream * glu_pad[tap_index:tap_index + frame_count].astype(jnp.float32), axis=0)))
        begin = 2 * rim_width - tap_index
        grad_input = grad_input + conv_taps[tap_index] * grad_pad[begin:begin + frame_count].astype(jnp.float32)
    return (jnp.stack(tap_grads), grad_input)

def ffn_back(normed_b, hidden, active, up_rows, down_rows, upstream):
    upstream_b = upstream.astype(jnp.bfloat16)
    grad_down = outer(active, upstream_b)
    grad_active = linear(upstream_b, down_rows)
    grad_hidden = (grad_active * silu_slope(hidden)).astype(jnp.bfloat16)
    grad_up = outer(grad_hidden, normed_b)
    grad_normed = jnp.dot(grad_hidden, up_rows, preferred_element_type=jnp.float32)
    return (grad_up, grad_down, grad_normed)

def adam_step(weight, gradient, first_mom, second_mom, decay):
    first_new = BETA_ONE * first_mom + (1.0 - BETA_ONE) * gradient
    second_new = BETA_TWO * second_mom + (1.0 - BETA_TWO) * gradient * gradient
    fix_one = 1.0 - BETA_ONE ** ADAM_STEP
    fix_two = 1.0 - BETA_TWO ** ADAM_STEP
    update = first_new / fix_one / (jnp.sqrt(second_new / fix_two) + ADAM_EPS)
    return (weight - LEARN_RATE * (update + decay * weight), first_new, second_new)

def reference(inputs, cotangent, lengths, square, upward, downward, vectors, kernel, square_momentum, square_variance, upward_momentum, upward_variance, downward_momentum, downward_variance, vectors_momentum, vectors_variance, kernel_momentum, kernel_variance):
    full_sq = square.astype(jnp.bfloat16)
    full_up = upward.astype(jnp.bfloat16)
    full_down = downward.astype(jnp.bfloat16)
    small_params = lax.optimization_barrier(vectors.astype(jnp.bfloat16)).astype(jnp.float32)
    conv_taps = lax.optimization_barrier(kernel.astype(jnp.bfloat16)).astype(jnp.float32)
    rim_width = (KW - 1) // 2
    head_size = D // H
    block_rows = min(512, LEN)
    pos_table = position_table(LEN, D)
    pos_proj = linear(pos_table, full_sq[3 * D:4 * D]).astype(jnp.bfloat16)
    pos_heads = heads_of(pos_proj, head_size)

    def front(seq_in, length):
        signal = seq_in.astype(jnp.float32)
        live_mask = (jnp.arange(LEN, dtype=jnp.int32) < length).astype(jnp.float32)[:, None]
        normed1 = layer_norm(signal, small_params[0], small_params[1]).astype(jnp.bfloat16)
        hidden1 = linear(normed1, full_up[:FF])
        active1 = jax.nn.silu(hidden1).astype(jnp.bfloat16)
        resid1 = signal + 0.5 * jnp.dot(active1, full_down[:FF], preferred_element_type=jnp.float32)
        normed2 = layer_norm(resid1, small_params[2], small_params[3]).astype(jnp.bfloat16)
        qkv = linear(normed2, full_sq[:3 * D]).astype(jnp.bfloat16)
        query = qkv[:, :D].astype(jnp.float32)
        query_content = heads_of((query + small_params[10]).astype(jnp.bfloat16), head_size)
        query_position = heads_of((query + small_params[11]).astype(jnp.bfloat16), head_size)
        key_heads = heads_of(qkv[:, D:2 * D], head_size)
        value_heads = heads_of(qkv[:, 2 * D:], head_size)
        attended, log_totals = attend(query_content, query_position, key_heads, value_heads, pos_heads, length, block_rows)
        out_time = attended.reshape(LEN, D)
        resid2 = resid1 + linear(out_time, full_sq[4 * D:5 * D])
        normed3 = layer_norm(resid2, small_params[4], small_params[5]).astype(jnp.bfloat16)
        pair = linear(normed3, full_sq[5 * D:7 * D])
        lin_value, lin_gate = (pair[:, :D], pair[:, D:])
        glu = (lin_value * jax.nn.sigmoid(lin_gate) * live_mask).astype(jnp.bfloat16)
        glu_pad = jnp.pad(glu, ((rim_width, rim_width), (0, 0)))
        conv_out = depth_forward(glu_pad, conv_taps, LEN)
        return (signal, live_mask, normed1, hidden1, active1, resid1, normed2, query_content, query_position, key_heads, value_heads, log_totals, out_time, resid2, normed3, lin_value, lin_gate, glu_pad, conv_out)

    def front_short(seq_item):
        saved = front(seq_item[0], seq_item[1])
        return (saved[13], saved[18])
    resid2_all, conv_all = lax.map(front_short, (inputs, lengths))
    live_all = (jnp.arange(LEN, dtype=jnp.int32)[None, :] < lengths[:, None]).astype(jnp.float32)[..., None]
    frames = jnp.sum(live_all)
    centre = lax.optimization_barrier(jnp.sum(live_all * conv_all, axis=(0, 1))) / frames
    spread = lax.optimization_barrier(jnp.sum(live_all * (conv_all - centre) ** 2, axis=(0, 1))) / frames
    inv_std = lax.rsqrt(spread + BN_EPS)

    def tail(running, seq_item):
        resid2, conv_out, grad_y, live_mask = seq_item
        centred = conv_out - centre
        zed = centred * inv_std
        bn_val = small_params[12] * zed + small_params[13]
        swish_b = jax.nn.silu(bn_val).astype(jnp.bfloat16)
        resid3 = resid2 + linear(swish_b, full_sq[7 * D:])
        normed4 = layer_norm(resid3, small_params[6], small_params[7]).astype(jnp.bfloat16)
        hidden4 = linear(normed4, full_up[FF:])
        active4 = jax.nn.silu(hidden4).astype(jnp.bfloat16)
        resid4 = resid3 + 0.5 * jnp.dot(active4, full_down[FF:], preferred_element_type=jnp.float32)
        final = layer_norm(resid4, small_params[8], small_params[9]).astype(jnp.bfloat16)
        grad_res4, grad_gain4, grad_shift4 = norm_back(resid4, small_params[8], small_params[9], grad_y.astype(jnp.float32))
        grad_up4, grad_down4, grad_norm4 = ffn_back(normed4, hidden4, active4, full_up[FF:], full_down[FF:], 0.5 * grad_res4)
        grad_add, grad_gain3, grad_shift3 = norm_back(resid3, small_params[6], small_params[7], grad_norm4)
        grad_res3 = grad_res4 + grad_add
        grad_conv_b = grad_res3.astype(jnp.bfloat16)
        grad_point = outer(grad_conv_b, swish_b)
        grad_bn = jnp.dot(grad_conv_b, full_sq[7 * D:], preferred_element_type=jnp.float32) * silu_slope(bn_val)
        grad_zed = grad_bn * small_params[12]
        updates = (grad_up4, grad_down4, grad_point, grad_gain3, grad_shift3, grad_gain4, grad_shift4, lax.optimization_barrier(jnp.sum(grad_bn * zed, axis=0)), lax.optimization_barrier(jnp.sum(grad_bn, axis=0)), lax.optimization_barrier(jnp.sum(grad_zed, axis=0)), lax.optimization_barrier(jnp.sum(grad_zed * centred, axis=0)))
        running = tuple((old + new for old, new in zip(running, updates)))
        return (running, (final, grad_res3, grad_zed))
    zero_ff = jnp.zeros((FF, D), jnp.float32)
    zero_sq = jnp.zeros((D, D), jnp.float32)
    zero_vec = jnp.zeros((D,), jnp.float32)
    tail_init = (zero_ff, zero_ff, zero_sq) + (zero_vec,) * 8
    tail_sums, (finals, grad_res3_all, grad_zed_all) = lax.scan(tail, tail_init, (resid2_all, conv_all, cotangent, live_all))
    grad_up4, grad_down4, grad_point, grad_gain3, grad_shift3, grad_gain4, grad_shift4, grad_gamma, grad_beta, sum_one, sum_two = tail_sums

    def head_pass(running, seq_item):
        seq_in, length, grad_res3, grad_zed = seq_item
        signal, live_mask, normed1, hidden1, active1, resid1, normed2, query_content, query_position, key_heads, value_heads, log_totals, out_time, resid2, normed3, lin_value, lin_gate, glu_pad, conv_out = front(seq_in, length)
        centred = conv_out - centre
        grad_conv = inv_std * grad_zed - live_mask / frames * (inv_std * sum_one + inv_std ** 3 * sum_two * centred)
        grad_conv_b = grad_conv.astype(jnp.bfloat16)
        grad_pad = jnp.pad(grad_conv_b, ((rim_width, rim_width), (0, 0)))
        grad_taps, grad_glu = depth_back(grad_pad, glu_pad, conv_taps, LEN)
        grad_glu = grad_glu * live_mask
        gate_open = jax.nn.sigmoid(lin_gate)
        grad_pair = jnp.concatenate([grad_glu * gate_open, grad_glu * lin_value * gate_open * (1.0 - gate_open)], axis=1).astype(jnp.bfloat16)
        grad_lin = outer(grad_pair, normed3)
        grad_norm3 = jnp.dot(grad_pair, full_sq[5 * D:7 * D], preferred_element_type=jnp.float32)
        grad_add, grad_gain2, grad_shift2 = norm_back(resid2, small_params[4], small_params[5], grad_norm3)
        grad_res2 = grad_res3 + grad_add
        grad_att_b = grad_res2.astype(jnp.bfloat16)
        grad_outw = outer(grad_att_b, out_time)
        grad_out_time = jnp.dot(grad_att_b, full_sq[4 * D:5 * D], preferred_element_type=jnp.float32).astype(jnp.bfloat16)
        grad_keys, grad_values, grad_table, grad_content, grad_position = attend_back(query_content, query_position, key_heads, value_heads, pos_heads, length, block_rows, log_totals, heads_of(grad_out_time, head_size))
        grad_content = grad_content.reshape(LEN, D)
        grad_position = grad_position.reshape(LEN, D)
        grad_qkv = jnp.concatenate([(grad_content + grad_position).astype(jnp.bfloat16), grad_keys.reshape(LEN, D).astype(jnp.bfloat16), grad_values.reshape(LEN, D).astype(jnp.bfloat16)], axis=1)
        grad_inw = outer(grad_qkv, normed2)
        grad_norm2 = jnp.dot(grad_qkv, full_sq[:3 * D], preferred_element_type=jnp.float32)
        grad_pos = outer(grad_table.reshape(2 * LEN - 1, D).astype(jnp.bfloat16), pos_table)
        grad_add, grad_gain1, grad_shift1 = norm_back(resid1, small_params[2], small_params[3], grad_norm2)
        grad_res1 = grad_res2 + grad_add
        grad_up1, grad_down1, grad_norm1 = ffn_back(normed1, hidden1, active1, full_up[:FF], full_down[:FF], 0.5 * grad_res1)
        grad_add, grad_gain0, grad_shift0 = norm_back(signal, small_params[0], small_params[1], grad_norm1)
        grad_in = grad_res1 + grad_add
        updates = (grad_taps, grad_lin, grad_outw, grad_inw, grad_pos, lax.optimization_barrier(jnp.sum(grad_content, axis=0)), lax.optimization_barrier(jnp.sum(grad_position, axis=0)), grad_gain2, grad_shift2, grad_gain1, grad_shift1, grad_up1, grad_down1, grad_gain0, grad_shift0)
        running = tuple((old + new for old, new in zip(running, updates)))
        return (running, grad_in)
    head_init = (jnp.zeros((KW, D), jnp.float32), jnp.zeros((2 * D, D), jnp.float32), zero_sq, jnp.zeros((3 * D, D), jnp.float32), zero_sq) + (zero_vec,) * 6 + (zero_ff, zero_ff, zero_vec, zero_vec)
    head_sums, input_grad = lax.scan(head_pass, head_init, (inputs, lengths, grad_res3_all, grad_zed_all))
    grad_taps, grad_lin, grad_outw, grad_inw, grad_pos, grad_bias_u, grad_bias_v, grad_gain2, grad_shift2, grad_gain1, grad_shift1, grad_up1, grad_down1, grad_gain0, grad_shift0 = head_sums
    square_grad = jnp.concatenate([grad_inw, grad_pos, grad_outw, grad_lin, grad_point], axis=0)
    upward_grad = jnp.concatenate([grad_up1, grad_up4], axis=0)
    downward_grad = jnp.concatenate([grad_down1, grad_down4], axis=0)
    vectors_grad = jnp.stack([grad_gain0, grad_shift0, grad_gain1, grad_shift1, grad_gain2, grad_shift2, grad_gain3, grad_shift3, grad_gain4, grad_shift4, grad_bias_u, grad_bias_v, grad_gamma, grad_beta])
    kernel_grad = grad_taps
    square_next, momentum_square, variance_square = adam_step(square, square_grad, square_momentum, square_variance, DECAY_RATE)
    upward_next, momentum_upward, variance_upward = adam_step(upward, upward_grad, upward_momentum, upward_variance, DECAY_RATE)
    downward_next, momentum_downward, variance_downward = adam_step(downward, downward_grad, downward_momentum, downward_variance, DECAY_RATE)
    vectors_next, momentum_vectors, variance_vectors = adam_step(vectors, vectors_grad, vectors_momentum, vectors_variance, 0.0)
    kernel_next, momentum_kernel, variance_kernel = adam_step(kernel, kernel_grad, kernel_momentum, kernel_variance, DECAY_RATE)
    return (finals, input_grad, square_grad, upward_grad, downward_grad, vectors_grad, kernel_grad, square_next, upward_next, downward_next, vectors_next, kernel_next, momentum_square, variance_square, momentum_upward, variance_upward, momentum_downward, variance_downward, momentum_vectors, variance_vectors, momentum_kernel, variance_kernel)
```

```python
import math

import jax
import jax.numpy as jnp
from jax import lax
from jax.experimental import pallas as pl
from jax.experimental.pallas import tpu as pltpu
from jax.sharding import PartitionSpec as P

D = 512
H = 8
FF = 2048
ADAM_STEP = 4

LN_EPS = 1e-05
BN_EPS = 1e-05
BETA_ONE = 0.9
BETA_TWO = 0.98
ADAM_EPS = 1e-08
LEARN_RATE = 0.005
DECAY_RATE = 0.01


def padded(value, sides, width):
    for axis, dim in sides:
        count, length = (lax.axis_size(axis), value.shape[dim])
        up = [(i, (i + 1) % count) for i in range(count - 1)]
        down = [(j, i) for i, j in up]
        last = lax.slice_in_dim(value, length - width, length, axis=dim)
        initial = lax.slice_in_dim(value, 0, width, axis=dim)
        before = lax.ppermute(last, axis, up)
        after = lax.ppermute(initial, axis, down)
        value = jnp.concatenate([before, value, after], axis=dim)
    return value


def mix(form, first_op, second_op):
    return jnp.einsum(form, first_op, second_op, preferred_element_type=jnp.float32)


def linear(signal, weight):
    return lax.dot_general(
        signal, weight, (((1,), (1,)), ((), ())), preferred_element_type=jnp.float32
    )


def outer(first_op, second_op):
    return lax.dot_general(
        first_op, second_op, (((0,), (0,)), ((), ())), preferred_element_type=jnp.float32
    )


def layer_norm(signal, norm_gain, norm_shift):
    row_mean = jnp.mean(signal, axis=-1, keepdims=True)
    centred = signal - row_mean
    row_var = jnp.mean(centred * centred, axis=-1, keepdims=True)
    return centred * lax.rsqrt(row_var + LN_EPS) * norm_gain + norm_shift


def norm_back(signal, norm_gain, norm_shift, upstream):
    pullback = jax.vjp(layer_norm, signal, norm_gain, norm_shift)[1]
    return pullback(upstream)


def silu_slope(argument):
    sigma_val = jax.nn.sigmoid(argument)
    return sigma_val * (1.0 + argument * (1.0 - sigma_val))


def position_table(seq_frames, model_width):
    relative = (seq_frames - 1 - jnp.arange(2 * seq_frames - 1)).astype(jnp.float32)[:, None]
    pairs = jnp.arange(model_width // 2).astype(jnp.float32)
    frequency = jnp.exp(-math.log(10000.0) * 2.0 * pairs / model_width)
    phases = relative * frequency[None, :]
    stacked = jnp.stack([jnp.sin(phases), jnp.cos(phases)], axis=-1)
    return stacked.reshape(2 * seq_frames - 1, model_width).astype(jnp.bfloat16)


def heads_of(signal, head_size):
    return signal.reshape(signal.shape[0], signal.shape[1] // head_size, head_size)


def block_scores(
    query_content, query_position, key_heads, pos_heads, row_start, length, block_rows
):
    seq_frames = key_heads.shape[0]
    head_size = key_heads.shape[2]
    window_len = block_rows + seq_frames - 1
    content = lax.dynamic_slice_in_dim(query_content, row_start, block_rows, 0)
    positional = lax.dynamic_slice_in_dim(query_position, row_start, block_rows, 0)
    direct = mix("rhd,khd->hrk", content, key_heads)
    window = lax.dynamic_slice_in_dim(pos_heads, seq_frames - block_rows - row_start, window_len, 0)
    pos_scores = mix("rhd,whd->hrw", positional, window)
    head_count = pos_scores.shape[0]
    flattened = pos_scores.reshape(head_count, block_rows * window_len)
    flattened = flattened[:, block_rows - 1 : block_rows - 1 + block_rows * (window_len - 1)]
    shifted = flattened.reshape(head_count, block_rows, window_len - 1)[:, :, :seq_frames]
    scores = (direct + shifted) * (1.0 / math.sqrt(head_size))
    key_live = jnp.arange(seq_frames, dtype=jnp.int32) < length
    return (jnp.where(key_live[None, None, :], scores, -1e30), window, content, positional)


def unshift(spread_in, window_len, seq_frames):
    head_count, block_rows = (spread_in.shape[0], spread_in.shape[1])
    widened = jnp.pad(spread_in, ((0, 0), (0, 0), (0, window_len - 1 - seq_frames)))
    flattened = widened.reshape(head_count, block_rows * (window_len - 1))
    flattened = jnp.pad(flattened, ((0, 0), (block_rows - 1, 1)))
    return flattened.reshape(head_count, block_rows, window_len)


def attend(query_content, query_position, key_heads, value_heads, pos_heads, length, block_rows):
    seq_frames, head_count, head_size = key_heads.shape

    def one_block(row_start):
        scores = block_scores(
            query_content, query_position, key_heads, pos_heads, row_start, length, block_rows
        )[0]
        row_max = jnp.max(scores, axis=-1, keepdims=True)
        log_total = row_max + jnp.log(jnp.sum(jnp.exp(scores - row_max), axis=-1, keepdims=True))
        probability = jnp.exp(scores - log_total).astype(jnp.bfloat16)
        attended = mix("hrk,khd->rhd", probability, value_heads).astype(jnp.bfloat16)
        return (attended, log_total[..., 0])

    starts = jnp.arange(seq_frames // block_rows) * block_rows
    attended, log_totals = lax.map(one_block, starts)
    return (attended.reshape(seq_frames, head_count, head_size), log_totals)


def attend_back(
    query_content,
    query_position,
    key_heads,
    value_heads,
    pos_heads,
    length,
    block_rows,
    log_totals,
    grad_heads,
):
    seq_frames, head_count, head_size = key_heads.shape
    window_len = block_rows + seq_frames - 1

    def one_block(running, block_item):
        grad_keys, grad_values, grad_table = running
        row_start, log_total = block_item
        scores, window, content, positional = block_scores(
            query_content, query_position, key_heads, pos_heads, row_start, length, block_rows
        )
        probability = jnp.exp(scores - log_total[..., None])
        prob_bf = probability.astype(jnp.bfloat16)
        grad_here = lax.dynamic_slice_in_dim(grad_heads, row_start, block_rows, 0)
        grad_prob = mix("rhd,khd->hrk", grad_here, value_heads)
        row_delta = jnp.sum(probability * grad_prob, axis=-1, keepdims=True)
        grad_score = (probability * (grad_prob - row_delta) * (1.0 / math.sqrt(head_size))).astype(
            jnp.bfloat16
        )
        grad_content = mix("hrk,khd->rhd", grad_score, key_heads)
        grad_keys = grad_keys + mix("hrk,rhd->khd", grad_score, content)
        grad_values = grad_values + mix("hrk,rhd->khd", prob_bf, grad_here)
        spread_out = unshift(grad_score, window_len, seq_frames)
        grad_position = mix("hrw,whd->rhd", spread_out, window)
        window_add = mix("hrw,rhd->whd", spread_out, positional)
        offset = seq_frames - block_rows - row_start
        current = lax.dynamic_slice_in_dim(grad_table, offset, window_len, 0)
        grad_table = lax.dynamic_update_slice_in_dim(grad_table, current + window_add, offset, 0)
        return ((grad_keys, grad_values, grad_table), (grad_content, grad_position))

    starts = jnp.arange(seq_frames // block_rows) * block_rows
    zero_keys = jnp.zeros((seq_frames, head_count, head_size), jnp.float32)
    zero_table = jnp.zeros((2 * seq_frames - 1, head_count, head_size), jnp.float32)
    (grad_keys, grad_values, grad_table), (grad_content, grad_position) = lax.scan(
        one_block, (zero_keys, zero_keys, zero_table), (starts, log_totals)
    )
    grad_content = grad_content.reshape(seq_frames, head_count, head_size)
    grad_position = grad_position.reshape(seq_frames, head_count, head_size)
    return (grad_keys, grad_values, grad_table, grad_content, grad_position)


def depth_forward(glu_pad, conv_taps, frame_count):
    result = jnp.zeros((frame_count, conv_taps.shape[1]), jnp.float32)
    for tap_index in range(conv_taps.shape[0]):
        result = result + conv_taps[tap_index] * glu_pad[
            tap_index : tap_index + frame_count
        ].astype(jnp.float32)
    return result


def depth_back(grad_pad, glu_pad, conv_taps, frame_count):
    rim_width = (conv_taps.shape[0] - 1) // 2
    upstream = grad_pad[rim_width : rim_width + frame_count].astype(jnp.float32)
    tap_grads = []
    grad_input = jnp.zeros((frame_count, conv_taps.shape[1]), jnp.float32)
    for tap_index in range(conv_taps.shape[0]):
        tap_grads.append(
            jnp.sum(
                upstream * glu_pad[tap_index : tap_index + frame_count].astype(jnp.float32), axis=0
            )
        )
        begin = 2 * rim_width - tap_index
        grad_input = grad_input + conv_taps[tap_index] * grad_pad[
            begin : begin + frame_count
        ].astype(jnp.float32)
    return (jnp.stack(tap_grads), grad_input)


def ffn_back(normed_b, hidden, active, up_rows, down_rows, upstream):
    upstream_b = upstream.astype(jnp.bfloat16)
    grad_down = outer(active, upstream_b)
    grad_active = linear(upstream_b, down_rows)
    grad_hidden = (grad_active * silu_slope(hidden)).astype(jnp.bfloat16)
    grad_up = outer(grad_hidden, normed_b)
    grad_normed = jnp.dot(grad_hidden, up_rows, preferred_element_type=jnp.float32)
    return (grad_up, grad_down, grad_normed)


def adam_step(weight, gradient, first_mom, second_mom, decay):
    first_new = BETA_ONE * first_mom + (1.0 - BETA_ONE) * gradient
    second_new = BETA_TWO * second_mom + (1.0 - BETA_TWO) * gradient * gradient
    fix_one = 1.0 - BETA_ONE**ADAM_STEP
    fix_two = 1.0 - BETA_TWO**ADAM_STEP
    update = first_new / fix_one / (jnp.sqrt(second_new / fix_two) + ADAM_EPS)
    return (weight - LEARN_RATE * (update + decay * weight), first_new, second_new)


MESH = pl.DeviceIdType.MESH
BF = jnp.bfloat16
F32 = jnp.float32
LANES = 128


class Grid:
    def __init__(self):
        self.nz = lax.axis_size("seq")
        self.nf = lax.axis_size("fsdp")
        plane = self.nf // 2
        side = math.isqrt(plane)
        self.z = lax.axis_index("seq")
        f = lax.axis_index("fsdp")
        self.core = f % 2
        if side * side == plane:
            self.na = self.nb = side
            self.step_a = 2 + self.core * (2 * side - 2)
            self.step_b = 2 * side - self.core * (2 * side - 2)
        else:
            self.na, self.nb = plane, 1
            self.step_a, self.step_b = 2, self.nf
        self.f = f
        self.a = (f // self.step_a) % self.na
        self.b = (f // self.step_b) % self.nb
        self.plane = plane
        self.chips = plane * self.nz

    def chip(self, z, a, b):
        return z * self.plane + (a * self.step_a + b * self.step_b) // 2

    def device(self, z, a, b):
        return (z, a * self.step_a + b * self.step_b + self.core)

    def sibling(self):
        return (self.z, self.f + 1 - 2 * self.core)

    def up(self, axis):
        return self.device(self.z + (axis == "z"), self.a + (axis == "a"), self.b + (axis == "b"))

    def down(self, axis):
        return self.device(self.z - (axis == "z"), self.a - (axis == "a"), self.b - (axis == "b"))

    def place(self, axis):
        return {"z": (self.z, self.nz), "a": (self.a, self.na), "b": (self.b, self.nb)}[axis]


def greet(g):
    barrier = pltpu.get_barrier_semaphore()
    pl.semaphore_signal(barrier, inc=1, device_id=g.sibling(), device_id_type=MESH)
    total = 1
    for axis in "zab":
        p, n = g.place(axis)
        if n == 1:
            continue

        @pl.when(p < n - 1)
        def _():
            pl.semaphore_signal(barrier, inc=1, device_id=g.up(axis), device_id_type=MESH)

        @pl.when(p > 0)
        def _():
            pl.semaphore_signal(barrier, inc=1, device_id=g.down(axis), device_id_type=MESH)

        total = total + 2 - (n - 1 - p == 0) - (p == 0)
    pl.semaphore_wait(barrier, total)


def gather_kernel(ud_own, sq_own, sm_own, ud_full, sq_full, sm_full, local_sem, swap_send, swap_recv, recv_sem, sib_recv, send_sem):
    g = Grid()
    half = ud_own.shape[1]
    c = g.core
    me = g.chip(g.z, g.a, g.b)
    local = [
        pltpu.make_async_copy(ud_own.at[c], ud_full.at[c, pl.ds(me * 2 * half + c * half, half)], local_sem.at[0]),
        pltpu.make_async_copy(sq_own, sq_full.at[me, c], local_sem.at[1]),
        pltpu.make_async_copy(sm_own, sm_full.at[me, c], local_sem.at[2]),
    ]
    for copy in local:
        copy.start()
    greet(g)
    swap = pltpu.make_async_remote_copy(
        src_ref=ud_own.at[1 - c],
        dst_ref=ud_full.at[1 - c, pl.ds(me * 2 * half + c * half, half)],
        send_sem=swap_send,
        recv_sem=swap_recv,
        device_id=g.sibling(),
        device_id_type=MESH,
    )
    swap.start()

    def pieces(t):
        return (ud_full.at[c, pl.ds(t * 2 * half, 2 * half)], sq_full.at[t, c], sm_full.at[t, c])

    ways = {"z+": 0, "z-": 1, "a+": 2, "a-": 3, "b+": 4, "b-": 5, "s": 6}

    def copies(t, way):
        if way == "s":
            target = g.sibling()
        else:
            target = g.up(way[0]) if way[1] == "+" else g.down(way[0])
        arrive = sib_recv if way == "s" else recv_sem
        return [
            pltpu.make_async_remote_copy(
                src_ref=ref,
                dst_ref=ref,
                send_sem=send_sem.at[ways[way], k, t],
                recv_sem=arrive.at[k, t],
                device_id=target,
                device_id_type=MESH,
            )
            for k, ref in enumerate(pieces(t))
        ]

    def send(t, way, finish=False):
        def act():
            for copy in copies(t, way):
                if finish:
                    copy.wait_send()
                else:
                    copy.start()

        if way == "s":
            act()
            return
        p, n = g.place(way[0])
        if n == 1:
            return
        pl.when(p < n - 1 if way[1] == "+" else p > 0)(act)

    def wait(t):
        for k, ref in enumerate(pieces(t)):
            pltpu.make_async_copy(ref, ref, recv_sem.at[k, t]).wait()

    def spread(finish):
        def got(t, ways_on):
            if not finish:
                wait(t)
            for way in ways_on:
                send(t, way, finish)

        if finish:
            pass
        else:
            for copy in local:
                copy.wait()
            swap.wait_recv()
        for way in ("z+", "z-", "a+", "a-", "b+", "b-", "s"):
            send(me, way, finish)
        for k in range(1, g.nz):
            pl.when(g.z >= k)(lambda: got(g.chip(g.z - k, g.a, g.b), ("z+", "a+", "a-", "b+", "b-", "s")))
            pl.when(g.z + k < g.nz)(lambda: got(g.chip(g.z + k, g.a, g.b), ("z-", "a+", "a-", "b+", "b-", "s")))

        def column(a, b, ways_on):
            got(g.chip(g.z, a, b), ways_on)
            for k in range(1, g.nz):
                pl.when(g.z >= k)(lambda: got(g.chip(g.z - k, a, b), ways_on))
                pl.when(g.z + k < g.nz)(lambda: got(g.chip(g.z + k, a, b), ways_on))

        for k in range(1, g.na):
            pl.when(g.a >= k)(lambda: column(g.a - k, g.b, ("a+", "b+", "b-", "s")))
            pl.when(g.a + k < g.na)(lambda: column(g.a + k, g.b, ("a-", "b+", "b-", "s")))
        for kb in range(1, g.nb):

            def plane(b, ways_on):
                column(g.a, b, ways_on)
                for k in range(1, g.na):
                    pl.when(g.a >= k)(lambda: column(g.a - k, b, ways_on))
                    pl.when(g.a + k < g.na)(lambda: column(g.a + k, b, ways_on))

            pl.when(g.b >= kb)(lambda: plane(g.b - kb, ("b+", "s")))
            pl.when(g.b + kb < g.nb)(lambda: plane(g.b + kb, ("b-", "s")))

    spread(False)
    d = 1 - c

    def other(t, _):
        for k, ref in enumerate((ud_full.at[d, pl.ds(t * 2 * half, 2 * half)], sq_full.at[t, d], sm_full.at[t, d])):
            pltpu.make_async_copy(ref, ref, sib_recv.at[k, t]).wait()
        return 0

    lax.fori_loop(0, g.chips, other, 0)
    swap.wait_send()
    spread(True)


def gather_weights(ud, sq, sm):
    devices = lax.axis_size("seq") * lax.axis_size("fsdp")
    chips = devices // 2
    _, rows, width = ud.shape
    hbm = pl.BlockSpec(memory_space=pl.ANY)
    vmem = pl.BlockSpec(memory_space=pltpu.VMEM)
    dma = pltpu.SemaphoreType.DMA
    return pl.pallas_call(
        gather_kernel,
        name="gather_weights",
        out_shape=(
            jax.ShapeDtypeStruct((2, devices * rows, width), ud.dtype),
            jax.ShapeDtypeStruct((chips, 2, rows, width), sq.dtype),
            jax.ShapeDtypeStruct((chips, 2) + sm.shape, sm.dtype),
        ),
        in_specs=[vmem] * 3,
        out_specs=[hbm] * 3,
        scratch_shapes=[
            dma((3,)),
            dma,
            dma,
            dma((3, chips)),
            dma((3, chips)),
            dma((7, 3, chips)),
        ],
        compiler_params=pltpu.CompilerParams(collective_id=1, has_side_effects=True),
    )(ud, sq, sm)


def scatter_kernel(ud_in, sq_in, sm_in, ud_out, sq_out, sm_out, acc, sib, rb, ra, rz, fin, send_ud,
                   local_sem, sib_send, sib_recv, b_send, b_recv, a_send, a_recv, z_send, z_recv, fin_send, fin_recv):
    g = Grid()
    c = g.core
    d = 1 - c
    nz, na, nb = g.nz, g.na, g.nb
    ud_rows = ud_out.shape[1]
    sq_rows = sq_out.shape[0]
    sm_rows = sm_out.shape[0]
    pair = 2 * ud_rows

    def slot(z, a, b):
        return (b * na + a) * nz + z

    def block_refs(buf, n):
        return (buf.at[n, pl.ds(0, pair)], buf.at[n, pl.ds(pair, sq_rows)], buf.at[n, pl.ds(pair + sq_rows, sm_rows)])

    def chip_refs(t, col):
        return (ud_in.at[col, pl.ds(t * pair, pair)], sq_in.at[t, col], sm_in.at[t, col])

    every = [(z, a, b) for b in range(nb) for a in range(na) for z in range(nz)]
    for z, a, b in every:
        n = slot(z, a, b)
        for k, (src, dst) in enumerate(zip(chip_refs(g.chip(z, a, b), c), block_refs(acc, n))):
            pltpu.make_async_copy(src, dst, local_sem.at[k, n]).start()
    greet(g)

    def sib_copies(z, a, b):
        n = slot(z, a, b)
        if g.na == g.nb:
            t = z * g.plane + (a * g.step_b + b * g.step_a) // 2
        else:
            t = g.chip(z, a, b)
        return [
            pltpu.make_async_remote_copy(
                src_ref=src,
                dst_ref=dst,
                send_sem=sib_send.at[k, n],
                recv_sem=sib_recv.at[k, n],
                device_id=g.sibling(),
                device_id_type=MESH,
            )
            for k, (src, dst) in enumerate(zip(chip_refs(t, d), block_refs(sib, n)))
        ]

    for z, a, b in every:
        for copy in sib_copies(z, a, b):
            copy.start()

    def add(n, ref):
        acc[n] = (acc[n].astype(F32) + ref[...].astype(F32)).astype(BF)

    def ready(z, a, b):
        n = slot(z, a, b)
        for k, (src, dst) in enumerate(zip(chip_refs(0, c), block_refs(acc, n))):
            pltpu.make_async_copy(src, dst, local_sem.at[k, n]).wait()
        for k, dst in enumerate(block_refs(sib, n)):
            pltpu.make_async_copy(dst, dst, sib_recv.at[k, n]).wait()
        add(n, sib.at[n])

    def travel(axis, n, m, buf, sends, recvs, upward):
        way = 0 if upward else 1
        return pltpu.make_async_remote_copy(
            src_ref=acc.at[n],
            dst_ref=buf.at[way, m],
            send_sem=sends.at[way, m],
            recv_sem=recvs.at[way, m],
            device_id=g.up(axis) if upward else g.down(axis),
            device_id_type=MESH,
        )

    def take(n, m, buf, recvs, way):
        pltpu.make_async_copy(buf.at[way, m], buf.at[way, m], recvs.at[way, m]).wait()
        add(n, buf.at[way, m])

    stages = {"b": (rb, b_send, b_recv), "a": (ra, a_send, a_recv), "z": (rz, z_send, z_recv)}

    def line(axis, blocks, prepare, finish):
        p, n_axis = g.place(axis)
        buf, sends, recvs = stages[axis]
        for k in range(n_axis - 1, 0, -1):
            for upward in (True, False):
                q = p + k if upward else p - k
                inside = p + k < n_axis if upward else p >= k
                behind = p > 0 if upward else p < n_axis - 1
                way = 0 if upward else 1

                def act():
                    for block in blocks(q):
                        n, m = block["slot"], block["m"]
                        if finish:
                            travel(axis, n, m, buf, sends, recvs, upward).wait_send()
                        else:
                            prepare(block)
                            pl.when(behind)(lambda: take(n, m, buf, recvs, way))
                            travel(axis, n, m, buf, sends, recvs, upward).start()

                pl.when(inside)(act)

    def settle(axis, block):
        p, n_axis = g.place(axis)
        buf, _, recvs = stages[axis]
        if n_axis > 1:
            pl.when(p > 0)(lambda: take(block["slot"], block["m"], buf, recvs, 0))
            pl.when(p < n_axis - 1)(lambda: take(block["slot"], block["m"], buf, recvs, 1))

    def z_order(a, b):
        return [(z, a, b) for z in range(nz)]

    def b_blocks(q):
        out = []
        for ka in list(range(1, na)) + [0]:
            a = lax.rem(g.a + ka, na)
            for z in range(nz):
                n = slot(z, a, q)
                out.append({"slot": n, "m": n, "at": (z, a, q)})
        return out

    def a_blocks(q):
        return [{"slot": slot(z, q, g.b), "m": q * nz + z, "at": (z, q, g.b)} for z in range(nz)]

    def z_blocks(q):
        return [{"slot": slot(q, g.a, g.b), "m": q, "at": (q, g.a, g.b)}]

    def along(block, axis):
        z, a, b = block["at"]
        if axis == "b":
            return {**block, "m": block["slot"]}
        return {**block, "m": a * nz + z}

    def from_b(block):
        ready(*block["at"])
        settle("b", along(block, "b"))

    def from_a(block):
        from_b(block)
        settle("a", along(block, "a"))

    line("b", b_blocks, lambda block: ready(*block["at"]), False)
    line("a", a_blocks, from_b, False)
    line("z", z_blocks, from_a, False)
    own = z_blocks(g.z)[0]
    from_a(own)
    settle("z", own)
    n = own["slot"]
    send_ud[...] = acc[n, pl.ds(pl.multiple_of(d * ud_rows, ud_rows), ud_rows), :].astype(F32)
    last = pltpu.make_async_remote_copy(
        src_ref=send_ud,
        dst_ref=fin,
        send_sem=fin_send,
        recv_sem=fin_recv,
        device_id=g.sibling(),
        device_id_type=MESH,
    )
    last.start()
    ud_out[c] = acc[n, pl.ds(pl.multiple_of(c * ud_rows, ud_rows), ud_rows), :].astype(F32)
    sq_out[...] = acc[n, pl.ds(pair, sq_rows), :].astype(F32)
    sm_out[...] = acc[n, pl.ds(pair + sq_rows, sm_rows), :].astype(F32)
    line("b", b_blocks, None, True)
    line("a", a_blocks, None, True)
    line("z", z_blocks, None, True)
    for z, a, b in every:
        for copy in sib_copies(z, a, b):
            copy.wait_send()
    last.wait()
    ud_out[d] = fin[...]


def scatter_grads(ud, sq, sm):
    nz, nf = lax.axis_size("seq"), lax.axis_size("fsdp")
    chips = nz * nf // 2
    width = ud.shape[2]
    rows = ud.shape[1] // (2 * chips)
    r = sm.shape[2]
    total = 3 * rows + r
    plane = nf // 2
    side = math.isqrt(plane)
    na, nb = (side, side) if side * side == plane else (plane, 1)
    hbm = pl.BlockSpec(memory_space=pl.ANY)
    vmem = pl.BlockSpec(memory_space=pltpu.VMEM)
    dma = pltpu.SemaphoreType.DMA
    return pl.pallas_call(
        scatter_kernel,
        name="scatter_grads",
        out_shape=(
            jax.ShapeDtypeStruct((2, rows, width), F32),
            jax.ShapeDtypeStruct((rows, width), F32),
            jax.ShapeDtypeStruct((r, width), F32),
        ),
        in_specs=[hbm] * 3,
        out_specs=[vmem] * 3,
        scratch_shapes=[
            pltpu.VMEM((chips, total, width), BF),
            pltpu.VMEM((chips, total, width), BF),
            pltpu.VMEM((2, chips, total, width), BF),
            pltpu.VMEM((2, na * nz, total, width), BF),
            pltpu.VMEM((2, nz, total, width), BF),
            pltpu.VMEM((rows, width), F32),
            pltpu.VMEM((rows, width), F32),
            dma((3, chips)),
            dma((3, chips)),
            dma((3, chips)),
            dma((2, chips)),
            dma((2, chips)),
            dma((2, na * nz)),
            dma((2, na * nz)),
            dma((2, nz)),
            dma((2, nz)),
            dma,
            dma,
        ],
        compiler_params=pltpu.CompilerParams(collective_id=2, has_side_effects=True, vmem_limit_bytes=60000 * 1024),
    )(ud, sq, sm)


def gathered(square, upward, downward, vectors, kernel):
    share = vectors.shape[1]
    small_rows = vectors.shape[0] + kernel.shape[0]
    small = jnp.concatenate([vectors, kernel], axis=0).astype(BF).reshape(-1)
    tall = -(-small.shape[0] // (16 * LANES)) * 16
    small = jnp.pad(small, (0, tall * LANES - small.shape[0])).reshape(tall, LANES)
    matrices, squares, smalls = gather_weights(
        jnp.stack([upward, downward]).astype(BF), square.astype(BF), small
    )
    devices = smalls.shape[0] * 2
    smalls = smalls.reshape(devices, tall * LANES)[:, : small_rows * share]
    smalls = smalls.reshape(devices, small_rows, share).transpose(1, 0, 2)
    smalls = smalls.reshape(small_rows, devices * share)
    split = vectors.shape[0]
    return (
        squares.reshape(devices * square.shape[0], square.shape[1]),
        matrices[0],
        matrices[1],
        smalls[:split],
        smalls[split:],
    )


def scattered(square_full, upward_full, downward_full, vectors_full, taps_full):
    devices = lax.axis_size("seq") * lax.axis_size("fsdp")
    width = square_full.shape[1]
    small = jnp.concatenate([vectors_full, taps_full], axis=0)
    small_rows, split = small.shape[0], vectors_full.shape[0]
    share = small.shape[1] // devices
    small = small.reshape(small_rows, devices, share).transpose(1, 0, 2)
    count = small_rows * share
    tall = -(-count // (16 * width)) * 16
    small = jnp.pad(small.reshape(devices, count), ((0, 0), (0, tall * width - count)))
    matrices, squares, smalls = scatter_grads(
        jnp.stack([upward_full.astype(BF), downward_full.astype(BF)]),
        square_full.astype(BF).reshape(devices // 2, 2, -1, width),
        small.astype(BF).reshape(devices // 2, 2, tall, width),
    )
    smalls = smalls.reshape(-1)[:count].reshape(small_rows, share)
    return squares, matrices[0], matrices[1], smalls[:split], smalls[split:]


def per_device(
    inputs,
    cotangent,
    lengths,
    square,
    upward,
    downward,
    vectors,
    kernel,
    square_momentum,
    square_variance,
    upward_momentum,
    upward_variance,
    downward_momentum,
    downward_variance,
    vectors_momentum,
    vectors_variance,
    kernel_momentum,
    kernel_variance,
):
    full_sq, full_up, full_down, full_vec, full_kern = gathered(
        square, upward, downward, vectors, kernel
    )
    model_width = inputs.shape[2]
    frame_count = inputs.shape[1]
    groups = lax.axis_size("seq")
    seq_place = lax.axis_index("seq")
    seq_frames = frame_count * groups
    head_cols = model_width // groups
    col_start = seq_place * head_cols
    block_rows = min(512, seq_frames)
    rim_width = (full_kern.shape[0] - 1) // 2
    head_size = D // H
    small_params = full_vec.astype(jnp.float32)
    conv_taps = full_kern.astype(jnp.float32)
    signal = inputs[0].astype(jnp.float32)
    length = lengths[0]
    frame_index = seq_place * frame_count + jnp.arange(frame_count, dtype=jnp.int32)
    live_mask = (frame_index < length).astype(jnp.float32)[:, None]
    normed1 = layer_norm(signal, small_params[0], small_params[1]).astype(jnp.bfloat16)
    hidden1 = linear(normed1, full_up[:FF])
    active1 = jax.nn.silu(hidden1).astype(jnp.bfloat16)
    resid1 = signal + 0.5 * jnp.dot(active1, full_down[:FF], preferred_element_type=jnp.float32)
    normed2 = layer_norm(resid1, small_params[2], small_params[3]).astype(jnp.bfloat16)
    qkv = linear(normed2, full_sq[: 3 * model_width]).astype(jnp.bfloat16)
    query_time = qkv[:, :model_width]
    key_time = qkv[:, model_width : 2 * model_width]
    value_time = qkv[:, 2 * model_width :]
    query_head, key_head, value_head = (
        lax.all_to_all(query_time, "seq", split_axis=1, concat_axis=0, tiled=True),
        lax.all_to_all(key_time, "seq", split_axis=1, concat_axis=0, tiled=True),
        lax.all_to_all(value_time, "seq", split_axis=1, concat_axis=0, tiled=True),
    )
    bias_content = lax.dynamic_slice_in_dim(small_params[10], col_start, head_cols, 0)
    bias_position = lax.dynamic_slice_in_dim(small_params[11], col_start, head_cols, 0)
    query_f32 = query_head.astype(jnp.float32)
    query_content = heads_of((query_f32 + bias_content).astype(jnp.bfloat16), head_size)
    query_position = heads_of((query_f32 + bias_position).astype(jnp.bfloat16), head_size)
    key_heads = heads_of(key_head, head_size)
    value_heads = heads_of(value_head, head_size)
    pos_table = position_table(seq_frames, model_width)
    pos_weight = lax.dynamic_slice_in_dim(full_sq, 3 * model_width + col_start, head_cols, 0)
    pos_heads = heads_of(linear(pos_table, pos_weight).astype(jnp.bfloat16), head_size)
    attended, log_totals = attend(
        query_content, query_position, key_heads, value_heads, pos_heads, length, block_rows
    )
    out_time = lax.all_to_all(
        attended.reshape(seq_frames, head_cols), "seq", split_axis=0, concat_axis=1, tiled=True
    )
    resid2 = resid1 + linear(out_time, full_sq[4 * model_width : 5 * model_width])
    normed3 = layer_norm(resid2, small_params[4], small_params[5]).astype(jnp.bfloat16)
    pair = linear(normed3, full_sq[5 * model_width : 7 * model_width])
    lin_value = pair[:, :model_width]
    lin_gate = pair[:, model_width:]
    glu = (lin_value * jax.nn.sigmoid(lin_gate) * live_mask).astype(jnp.bfloat16)
    glu_pad = padded(glu, (("seq", 0),), rim_width)
    conv_out = depth_forward(glu_pad, conv_taps, frame_count)
    first_sum, frames = lax.psum(
        (jnp.sum(live_mask * conv_out, axis=0), jnp.sum(live_mask)), ("seq", "fsdp")
    )
    centre = first_sum / frames
    deviation = conv_out - centre
    spread = lax.psum(jnp.sum(live_mask * deviation * deviation, axis=0), ("seq", "fsdp")) / frames
    inv_std = lax.rsqrt(spread + BN_EPS)
    centred = conv_out - centre
    zed = centred * inv_std
    bn_val = small_params[12] * zed + small_params[13]
    swish_b = jax.nn.silu(bn_val).astype(jnp.bfloat16)
    resid3 = resid2 + linear(swish_b, full_sq[7 * model_width :])
    normed4 = layer_norm(resid3, small_params[6], small_params[7]).astype(jnp.bfloat16)
    hidden4 = linear(normed4, full_up[FF:])
    active4 = jax.nn.silu(hidden4).astype(jnp.bfloat16)
    resid4 = resid3 + 0.5 * jnp.dot(active4, full_down[FF:], preferred_element_type=jnp.float32)
    layer_output = layer_norm(resid4, small_params[8], small_params[9]).astype(jnp.bfloat16)[None]
    grad_res4, grad_gain4, grad_shift4 = norm_back(
        resid4, small_params[8], small_params[9], cotangent[0].astype(jnp.float32)
    )
    grad_up4, grad_down4, grad_norm4 = ffn_back(
        normed4, hidden4, active4, full_up[FF:], full_down[FF:], 0.5 * grad_res4
    )
    grad_add, grad_gain3, grad_shift3 = norm_back(
        resid3, small_params[6], small_params[7], grad_norm4
    )
    grad_res3 = grad_res4 + grad_add
    grad_conv_b = grad_res3.astype(jnp.bfloat16)
    grad_point = outer(grad_conv_b, swish_b)
    grad_bn = jnp.dot(
        grad_conv_b, full_sq[7 * model_width :], preferred_element_type=jnp.float32
    ) * silu_slope(bn_val)
    grad_gamma = jnp.sum(grad_bn * zed, axis=0)
    grad_beta = jnp.sum(grad_bn, axis=0)
    grad_zed = grad_bn * small_params[12]
    sum_one, sum_two = lax.psum(
        (jnp.sum(grad_zed, axis=0), jnp.sum(grad_zed * centred, axis=0)), ("seq", "fsdp")
    )
    grad_conv = inv_std * grad_zed - live_mask / frames * (
        inv_std * sum_one + inv_std**3 * sum_two * centred
    )
    grad_pad = padded(grad_conv.astype(jnp.bfloat16), (("seq", 0),), rim_width)
    grad_taps, grad_glu = depth_back(grad_pad, glu_pad, conv_taps, frame_count)
    grad_glu = grad_glu * live_mask
    gate_open = jax.nn.sigmoid(lin_gate)
    grad_pair = jnp.concatenate(
        [grad_glu * gate_open, grad_glu * lin_value * gate_open * (1.0 - gate_open)], axis=1
    ).astype(jnp.bfloat16)
    grad_lin = outer(grad_pair, normed3)
    grad_norm3 = jnp.dot(
        grad_pair, full_sq[5 * model_width : 7 * model_width], preferred_element_type=jnp.float32
    )
    grad_add, grad_gain2, grad_shift2 = norm_back(
        resid2, small_params[4], small_params[5], grad_norm3
    )
    grad_res2 = grad_res3 + grad_add
    grad_att_b = grad_res2.astype(jnp.bfloat16)
    grad_outw = outer(grad_att_b, out_time)
    grad_out_time = jnp.dot(
        grad_att_b, full_sq[4 * model_width : 5 * model_width], preferred_element_type=jnp.float32
    ).astype(jnp.bfloat16)
    grad_out_head = lax.all_to_all(grad_out_time, "seq", split_axis=1, concat_axis=0, tiled=True)
    grad_keys, grad_values, grad_table, grad_content, grad_position = attend_back(
        query_content,
        query_position,
        key_heads,
        value_heads,
        pos_heads,
        length,
        block_rows,
        log_totals,
        heads_of(grad_out_head, head_size),
    )
    grad_content = grad_content.reshape(seq_frames, head_cols)
    grad_position = grad_position.reshape(seq_frames, head_cols)
    grad_query_b = (grad_content + grad_position).astype(jnp.bfloat16)
    grad_key_b = grad_keys.reshape(seq_frames, head_cols).astype(jnp.bfloat16)
    grad_value_b = grad_values.reshape(seq_frames, head_cols).astype(jnp.bfloat16)
    grad_query_time, grad_key_time, grad_value_time = (
        lax.all_to_all(grad_query_b, "seq", split_axis=0, concat_axis=1, tiled=True),
        lax.all_to_all(grad_key_b, "seq", split_axis=0, concat_axis=1, tiled=True),
        lax.all_to_all(grad_value_b, "seq", split_axis=0, concat_axis=1, tiled=True),
    )
    grad_qkv = jnp.concatenate([grad_query_time, grad_key_time, grad_value_time], axis=1)
    grad_inw = outer(grad_qkv, normed2)
    grad_norm2 = jnp.dot(grad_qkv, full_sq[: 3 * model_width], preferred_element_type=jnp.float32)
    grad_pos_cols = outer(
        grad_table.reshape(2 * seq_frames - 1, head_cols).astype(jnp.bfloat16), pos_table
    )
    grad_pos = lax.dynamic_update_slice_in_dim(
        jnp.zeros((model_width, model_width), jnp.float32), grad_pos_cols, col_start, 0
    )
    zero_row = jnp.zeros((model_width,), jnp.float32)
    grad_bias_u = lax.dynamic_update_slice_in_dim(
        zero_row, jnp.sum(grad_content, axis=0), col_start, 0
    )
    grad_bias_v = lax.dynamic_update_slice_in_dim(
        zero_row, jnp.sum(grad_position, axis=0), col_start, 0
    )
    grad_add, grad_gain1, grad_shift1 = norm_back(
        resid1, small_params[2], small_params[3], grad_norm2
    )
    grad_res1 = grad_res2 + grad_add
    grad_up1, grad_down1, grad_norm1 = ffn_back(
        normed1, hidden1, active1, full_up[:FF], full_down[:FF], 0.5 * grad_res1
    )
    grad_add, grad_gain0, grad_shift0 = norm_back(
        signal, small_params[0], small_params[1], grad_norm1
    )
    input_grad = (grad_res1 + grad_add)[None]
    square_full = jnp.concatenate([grad_inw, grad_pos, grad_outw, grad_lin, grad_point], axis=0)
    upward_full = jnp.concatenate([grad_up1, grad_up4], axis=0)
    downward_full = jnp.concatenate([grad_down1, grad_down4], axis=0)
    vectors_full = jnp.stack(
        [
            grad_gain0,
            grad_shift0,
            grad_gain1,
            grad_shift1,
            grad_gain2,
            grad_shift2,
            grad_gain3,
            grad_shift3,
            grad_gain4,
            grad_shift4,
            grad_bias_u,
            grad_bias_v,
            grad_gamma,
            grad_beta,
        ]
    )
    square_grad, upward_grad, downward_grad, vectors_grad, kernel_grad = scattered(
        square_full, upward_full, downward_full, vectors_full, grad_taps
    )
    square_next, momentum_square, variance_square = adam_step(
        square, square_grad, square_momentum, square_variance, DECAY_RATE
    )
    upward_next, momentum_upward, variance_upward = adam_step(
        upward, upward_grad, upward_momentum, upward_variance, DECAY_RATE
    )
    downward_next, momentum_downward, variance_downward = adam_step(
        downward, downward_grad, downward_momentum, downward_variance, DECAY_RATE
    )
    vectors_next, momentum_vectors, variance_vectors = adam_step(
        vectors, vectors_grad, vectors_momentum, vectors_variance, 0.0
    )
    kernel_next, momentum_kernel, variance_kernel = adam_step(
        kernel, kernel_grad, kernel_momentum, kernel_variance, DECAY_RATE
    )
    return (
        layer_output,
        input_grad,
        square_grad,
        upward_grad,
        downward_grad,
        vectors_grad,
        kernel_grad,
        square_next,
        upward_next,
        downward_next,
        vectors_next,
        kernel_next,
        momentum_square,
        variance_square,
        momentum_upward,
        variance_upward,
        momentum_downward,
        variance_downward,
        momentum_vectors,
        variance_vectors,
        momentum_kernel,
        variance_kernel,
    )


def solution(mesh):
    return jax.shard_map(
        per_device,
        mesh=mesh,
        in_specs=(
            P("fsdp", "seq", None),
            P("fsdp", "seq", None),
            P("fsdp"),
            P(("seq", "fsdp"), None),
            P(("seq", "fsdp"), None),
            P(("seq", "fsdp"), None),
            P(None, ("seq", "fsdp")),
            P(None, ("seq", "fsdp")),
            P(("seq", "fsdp"), None),
            P(("seq", "fsdp"), None),
            P(("seq", "fsdp"), None),
            P(("seq", "fsdp"), None),
            P(("seq", "fsdp"), None),
            P(("seq", "fsdp"), None),
            P(None, ("seq", "fsdp")),
            P(None, ("seq", "fsdp")),
            P(None, ("seq", "fsdp")),
            P(None, ("seq", "fsdp")),
        ),
        out_specs=(
            P("fsdp", "seq", None),
            P("fsdp", "seq", None),
            P(("seq", "fsdp"), None),
            P(("seq", "fsdp"), None),
            P(("seq", "fsdp"), None),
            P(None, ("seq", "fsdp")),
            P(None, ("seq", "fsdp")),
            P(("seq", "fsdp"), None),
            P(("seq", "fsdp"), None),
            P(("seq", "fsdp"), None),
            P(None, ("seq", "fsdp")),
            P(None, ("seq", "fsdp")),
            P(("seq", "fsdp"), None),
            P(("seq", "fsdp"), None),
            P(("seq", "fsdp"), None),
            P(("seq", "fsdp"), None),
            P(("seq", "fsdp"), None),
            P(("seq", "fsdp"), None),
            P(None, ("seq", "fsdp")),
            P(None, ("seq", "fsdp")),
            P(None, ("seq", "fsdp")),
            P(None, ("seq", "fsdp")),
        ),
        check_vma=False,
    )
```

```python
import math

import jax
import jax.numpy as jnp
from jax import lax
from jax.experimental import pallas as pl
from jax.experimental.pallas import tpu as pltpu
from jax.sharding import PartitionSpec as P

D = 512
H = 8
FF = 2048
ADAM_STEP = 4

LN_EPS = 1e-05
BN_EPS = 1e-05
BETA_ONE = 0.9
BETA_TWO = 0.98
ADAM_EPS = 1e-08
LEARN_RATE = 0.005
DECAY_RATE = 0.01


def padded(value, sides, width):
    for axis, dim in sides:
        count, length = (lax.axis_size(axis), value.shape[dim])
        up = [(i, (i + 1) % count) for i in range(count - 1)]
        down = [(j, i) for i, j in up]
        last = lax.slice_in_dim(value, length - width, length, axis=dim)
        initial = lax.slice_in_dim(value, 0, width, axis=dim)
        before = lax.ppermute(last, axis, up)
        after = lax.ppermute(initial, axis, down)
        value = jnp.concatenate([before, value, after], axis=dim)
    return value


def mix(form, first_op, second_op):
    return jnp.einsum(form, first_op, second_op, preferred_element_type=jnp.float32)


def linear(signal, weight):
    return lax.dot_general(
        signal, weight, (((1,), (1,)), ((), ())), preferred_element_type=jnp.float32
    )


def outer(first_op, second_op):
    return lax.dot_general(
        first_op, second_op, (((0,), (0,)), ((), ())), preferred_element_type=jnp.float32
    )


def layer_norm(signal, norm_gain, norm_shift):
    row_mean = jnp.mean(signal, axis=-1, keepdims=True)
    centred = signal - row_mean
    row_var = jnp.mean(centred * centred, axis=-1, keepdims=True)
    return centred * lax.rsqrt(row_var + LN_EPS) * norm_gain + norm_shift


def norm_back(signal, norm_gain, norm_shift, upstream):
    pullback = jax.vjp(layer_norm, signal, norm_gain, norm_shift)[1]
    return pullback(upstream)


def silu_slope(argument):
    sigma_val = jax.nn.sigmoid(argument)
    return sigma_val * (1.0 + argument * (1.0 - sigma_val))


def position_table(seq_frames, model_width):
    fine = math.gcd(2 * seq_frames, 64)
    column = jnp.arange(model_width)
    frequency = jnp.exp(-math.log(10000.0) * 2.0 * (column // 2).astype(jnp.float32) / model_width)
    coarse_at = (seq_frames - 1 - fine * jnp.arange(2 * seq_frames // fine)).astype(jnp.float32)
    coarse_phase = coarse_at[:, None] * frequency[None, :]
    fine_phase = jnp.arange(fine).astype(jnp.float32)[:, None] * frequency[None, :]
    even = (column % 2 == 0)[None, :]
    sine, cosine = jnp.sin(coarse_phase), jnp.cos(coarse_phase)
    with_cosine = jnp.where(even, sine, cosine)[:, None, :]
    with_sine = jnp.where(even, -cosine, sine)[:, None, :]
    table = with_cosine * jnp.cos(fine_phase)[None] + with_sine * jnp.sin(fine_phase)[None]
    return table.reshape(2 * seq_frames, model_width).astype(jnp.bfloat16)


def depth_forward(glu_pad, conv_taps, frame_count):
    result = jnp.zeros((frame_count, conv_taps.shape[1]), jnp.float32)
    for tap_index in range(conv_taps.shape[0]):
        result = result + conv_taps[tap_index] * glu_pad[
            tap_index : tap_index + frame_count
        ].astype(jnp.float32)
    return result


def depth_back(grad_pad, glu_pad, conv_taps, frame_count):
    rim_width = (conv_taps.shape[0] - 1) // 2
    upstream = grad_pad[rim_width : rim_width + frame_count].astype(jnp.float32)
    tap_grads = []
    grad_input = jnp.zeros((frame_count, conv_taps.shape[1]), jnp.float32)
    for tap_index in range(conv_taps.shape[0]):
        tap_grads.append(
            jnp.sum(
                upstream * glu_pad[tap_index : tap_index + frame_count].astype(jnp.float32), axis=0
            )
        )
        begin = 2 * rim_width - tap_index
        grad_input = grad_input + conv_taps[tap_index] * grad_pad[
            begin : begin + frame_count
        ].astype(jnp.float32)
    return (jnp.stack(tap_grads), grad_input)


def ffn_back(normed_b, hidden, active, up_rows, down_rows, upstream):
    upstream_b = upstream.astype(jnp.bfloat16)
    grad_down = outer(active, upstream_b)
    grad_active = linear(upstream_b, down_rows)
    grad_hidden = (grad_active * silu_slope(hidden)).astype(jnp.bfloat16)
    grad_up = outer(grad_hidden, normed_b)
    grad_normed = jnp.dot(grad_hidden, up_rows, preferred_element_type=jnp.float32)
    return (grad_up, grad_down, grad_normed)


def adam_step(weight, gradient, first_mom, second_mom, decay):
    first_new = BETA_ONE * first_mom + (1.0 - BETA_ONE) * gradient
    second_new = BETA_TWO * second_mom + (1.0 - BETA_TWO) * gradient * gradient
    fix_one = 1.0 - BETA_ONE**ADAM_STEP
    fix_two = 1.0 - BETA_TWO**ADAM_STEP
    update = first_new / fix_one / (jnp.sqrt(second_new / fix_two) + ADAM_EPS)
    return (weight - LEARN_RATE * (update + decay * weight), first_new, second_new)


MESH = pl.DeviceIdType.MESH
BF = jnp.bfloat16
F32 = jnp.float32
LANES = 128


class Grid:
    def __init__(self):
        self.nz = lax.axis_size("seq")
        self.nf = lax.axis_size("fsdp")
        plane = self.nf // 2
        side = math.isqrt(plane)
        self.z = lax.axis_index("seq")
        f = lax.axis_index("fsdp")
        self.core = f % 2
        if side * side == plane:
            self.na = self.nb = side
            self.step_a = 2 + self.core * (2 * side - 2)
            self.step_b = 2 * side - self.core * (2 * side - 2)
        else:
            self.na, self.nb = plane, 1
            self.step_a, self.step_b = 2, self.nf
        self.f = f
        self.a = (f // self.step_a) % self.na
        self.b = (f // self.step_b) % self.nb
        self.plane = plane
        self.chips = plane * self.nz

    def chip(self, z, a, b):
        return z * self.plane + (a * self.step_a + b * self.step_b) // 2

    def device(self, z, a, b):
        return (z, a * self.step_a + b * self.step_b + self.core)

    def sibling(self):
        return (self.z, self.f + 1 - 2 * self.core)

    def up(self, axis):
        return self.device(self.z + (axis == "z"), self.a + (axis == "a"), self.b + (axis == "b"))

    def down(self, axis):
        return self.device(self.z - (axis == "z"), self.a - (axis == "a"), self.b - (axis == "b"))

    def place(self, axis):
        return {"z": (self.z, self.nz), "a": (self.a, self.na), "b": (self.b, self.nb)}[axis]


def greet(g):
    barrier = pltpu.get_barrier_semaphore()
    pl.semaphore_signal(barrier, inc=1, device_id=g.sibling(), device_id_type=MESH)
    total = 1
    for axis in "zab":
        p, n = g.place(axis)
        if n == 1:
            continue

        @pl.when(p < n - 1)
        def _():
            pl.semaphore_signal(barrier, inc=1, device_id=g.up(axis), device_id_type=MESH)

        @pl.when(p > 0)
        def _():
            pl.semaphore_signal(barrier, inc=1, device_id=g.down(axis), device_id_type=MESH)

        total = total + 2 - (n - 1 - p == 0) - (p == 0)
    pl.semaphore_wait(barrier, total)


def merge_moments(first_op, second_op):
    count = first_op[0:1] + second_op[0:1]
    share = second_op[0:1] / jnp.maximum(count, 1.0)
    gap = second_op[1:2] - first_op[1:2]
    mean = first_op[1:2] + gap * share
    squares = first_op[2:3] + second_op[2:3] + gap * gap * (first_op[0:1] * share)
    return jnp.concatenate([count, mean, squares, first_op[3:]], axis=0)


def meet_kernel(merge, local_ref, out_ref, buf, send_sem, recv_sem):
    g = Grid()
    barrier = pltpu.get_barrier_semaphore()
    levels = [
        (g.core, 2, lambda q: (g.z, g.f - g.core + q)),
        (g.a, g.na, lambda q: g.device(g.z, q, g.b)),
        (g.b, g.nb, lambda q: g.device(g.z, g.a, q)),
        (g.z, g.nz, lambda q: g.device(q, g.a, g.b)),
    ]
    total = 0
    for p, n, device in levels:
        for k in range(1, n):
            pl.semaphore_signal(barrier, inc=1, device_id=device(lax.rem(p + k, n)), device_id_type=MESH)
            total += 1
    pl.semaphore_wait(barrier, total)
    value = local_ref[...]
    sends = []
    for level, (p, n, device) in enumerate(levels):
        if n == 1:
            continue
        buf[level, p] = value
        for k in range(1, n):
            copy = pltpu.make_async_remote_copy(
                src_ref=buf.at[level, p],
                dst_ref=buf.at[level, p],
                send_sem=send_sem.at[level, k],
                recv_sem=recv_sem.at[level, p],
                device_id=device(lax.rem(p + k, n)),
                device_id_type=MESH,
            )
            copy.start()
            sends.append(copy)
        for k in range(1, n):
            q = lax.rem(p + k, n)
            pltpu.make_async_copy(buf.at[level, q], buf.at[level, q], recv_sem.at[level, q]).wait()
        value = buf[level, 0]
        for q in range(1, n):
            value = merge(value, buf[level, q])
    out_ref[...] = value
    for copy in sends:
        copy.wait_send()


def meet(value, merge, collective):
    nz, nf = lax.axis_size("seq"), lax.axis_size("fsdp")
    most = max(nz, nf // 2)
    vmem = pl.BlockSpec(memory_space=pltpu.VMEM)
    return pl.pallas_call(
        lambda *refs: meet_kernel(merge, *refs),
        name="meet",
        out_shape=jax.ShapeDtypeStruct(value.shape, F32),
        in_specs=[vmem],
        out_specs=vmem,
        scratch_shapes=[
            pltpu.VMEM((4, most) + value.shape, F32),
            pltpu.SemaphoreType.DMA((4, most)),
            pltpu.SemaphoreType.DMA((4, most)),
        ],
        compiler_params=pltpu.CompilerParams(collective_id=collective, has_side_effects=True),
    )(value)


NT = (((1,), (1,)), ((), ()))
TN = (((0,), (0,)), ((), ()))
NN = (((1,), (0,)), ((), ()))


def dot(first_op, second_op, dims):
    return lax.dot_general(first_op, second_op, dims, preferred_element_type=F32)


def keep_head(value, h, head_size):
    lane = lax.broadcasted_iota(jnp.int32, value.shape, 1)
    return jnp.where(lane // head_size == h, value, jnp.zeros_like(value))


def attend_kernel(head_size, len_ref, q_ref, k_ref, v_ref, pos_ref, bias_ref, o_ref, prob_ref):
    i = pl.program_id(0)
    rows, cols = q_ref.shape
    frames = k_ref.shape[0]
    width = rows + frames
    query = q_ref[...].astype(F32)
    content = (query + bias_ref[0:1, :]).astype(BF)
    positional = (query + bias_ref[1:2, :]).astype(BF)
    window = pos_ref[pl.ds(pl.multiple_of(frames - rows - i * rows, rows), width), :]
    live = lax.broadcasted_iota(jnp.int32, (rows, frames), 1) < len_ref[0]
    out = jnp.zeros((rows, cols), F32)
    for h in range(cols // head_size):
        direct = dot(keep_head(content, h, head_size), k_ref[...], NT)
        spread = dot(keep_head(positional, h, head_size), window, NT)
        shifted = pltpu.roll(spread, width - rows + 1, 1, stride=1, stride_axis=0)[:, :frames]
        score = jnp.where(live, (direct + shifted) * (1.0 / math.sqrt(head_size)), -1e30)
        top = jnp.max(score, axis=-1, keepdims=True)
        power = jnp.exp(score - top)
        prob = power * (1.0 / jnp.sum(power, axis=-1, keepdims=True))
        prob_b = prob.astype(BF)
        prob_ref[h] = prob_b
        out = out + keep_head(dot(prob_b, v_ref[...], NN), h, head_size)
    o_ref[...] = out.astype(BF)


def attend_heads(query, key, value, pos, biases, length, head_size, rows=256):
    frames, cols = query.shape
    rows = min(rows, frames)
    heads = cols // head_size
    full = lambda n: pl.BlockSpec((n, cols), lambda i: (0, 0))
    return pl.pallas_call(
        lambda *refs: attend_kernel(head_size, *refs),
        name="attend_heads",
        grid=(frames // rows,),
        in_specs=[
            pl.BlockSpec(memory_space=pltpu.SMEM),
            pl.BlockSpec((rows, cols), lambda i: (i, 0)),
            full(frames),
            full(frames),
            full(2 * frames),
            full(2),
        ],
        out_specs=[
            pl.BlockSpec((rows, cols), lambda i: (i, 0)),
            pl.BlockSpec((heads, rows, frames), lambda i: (0, i, 0)),
        ],
        out_shape=(
            jax.ShapeDtypeStruct((frames, cols), BF),
            jax.ShapeDtypeStruct((heads, frames, frames), BF),
        ),
        compiler_params=pltpu.CompilerParams(vmem_limit_bytes=48 * 1024 * 1024),
    )(length.reshape(1), query, key, value, pos, biases)


def attend_back_kernel(head_size, q_ref, k_ref, v_ref, pos_ref, bias_ref, prob_ref, go_ref,
                       gq_ref, gk_ref, gv_ref, gpos_ref, gbias_ref, gk_acc, gv_acc, gpos_acc):
    i = pl.program_id(0)
    rows, cols = q_ref.shape
    frames = k_ref.shape[0]
    width = rows + frames

    @pl.when(i == 0)
    def _():
        gk_acc[...] = jnp.zeros_like(gk_acc)
        gv_acc[...] = jnp.zeros_like(gv_acc)
        gpos_acc[...] = jnp.zeros_like(gpos_acc)
        gbias_ref[...] = jnp.zeros_like(gbias_ref)

    query = q_ref[...].astype(F32)
    content = (query + bias_ref[0:1, :]).astype(BF)
    positional = (query + bias_ref[1:2, :]).astype(BF)
    start = pl.multiple_of(frames - rows - i * rows, rows)
    window = pos_ref[pl.ds(start, width), :]
    down = lax.broadcasted_iota(jnp.int32, (rows, rows), 0)
    across = lax.broadcasted_iota(jnp.int32, (rows, rows), 1)
    turn = jnp.where(down + across == rows - 1, 1.0, 0.0).astype(BF)
    positional_turned = dot(turn, positional, NN).astype(BF)
    grad_content = jnp.zeros((rows, cols), F32)
    grad_position = jnp.zeros((rows, cols), F32)
    for h in range(cols // head_size):
        grad_out = keep_head(go_ref[...], h, head_size)
        prob_b = prob_ref[h]
        prob = prob_b.astype(F32)
        grad_prob = dot(grad_out, v_ref[...], NT)
        delta = jnp.sum(prob * grad_prob, axis=-1, keepdims=True)
        grad_score = prob * (grad_prob - delta) * (1.0 / math.sqrt(head_size))
        score_b = grad_score.astype(BF)
        grad_content = grad_content + keep_head(dot(score_b, k_ref[...], NN), h, head_size)
        gk_acc[...] += dot(keep_head(content, h, head_size), score_b, TN)
        gv_acc[...] += dot(grad_out, prob_b, TN)
        turned = dot(turn, score_b, NN)
        wide = jnp.concatenate([turned, jnp.zeros((rows, width - frames), F32)], axis=1)
        spread = pltpu.roll(wide, 0, 1, stride=1, stride_axis=0).astype(BF)
        grad_position = grad_position + keep_head(dot(spread, window, NN), h, head_size)
        gpos_acc[:, pl.ds(start, width)] += dot(keep_head(positional_turned, h, head_size), spread, TN)
    high = grad_position.astype(BF)
    low = (grad_position - high.astype(F32)).astype(BF)
    grad_position = dot(turn, high, NN) + dot(turn, low, NN)
    gq_ref[...] = (grad_content + grad_position).astype(BF)
    gbias_ref[0:1, :] += jnp.sum(grad_content, axis=0, keepdims=True)
    gbias_ref[1:2, :] += jnp.sum(grad_position, axis=0, keepdims=True)

    @pl.when(i == pl.num_programs(0) - 1)
    def _():
        gk_ref[...] = gk_acc[...].T.astype(BF)
        gv_ref[...] = gv_acc[...].T.astype(BF)
        gpos_ref[...] = gpos_acc[...].astype(BF)


def attend_heads_back(query, key, value, pos, biases, prob, grad_out, head_size, rows=256):
    frames, cols = query.shape
    rows = min(rows, frames)
    heads = cols // head_size
    full = lambda n: pl.BlockSpec((n, cols), lambda i: (0, 0))
    block = pl.BlockSpec((rows, cols), lambda i: (i, 0))
    return pl.pallas_call(
        lambda *refs: attend_back_kernel(head_size, *refs),
        name="attend_heads_back",
        grid=(frames // rows,),
        in_specs=[
            block,
            full(frames),
            full(frames),
            full(2 * frames),
            full(2),
            pl.BlockSpec((heads, rows, frames), lambda i: (0, i, 0)),
            block,
        ],
        out_specs=[
            block,
            full(frames),
            full(frames),
            pl.BlockSpec((cols, 2 * frames), lambda i: (0, 0)),
            full(2),
        ],
        out_shape=(
            jax.ShapeDtypeStruct((frames, cols), BF),
            jax.ShapeDtypeStruct((frames, cols), BF),
            jax.ShapeDtypeStruct((frames, cols), BF),
            jax.ShapeDtypeStruct((cols, 2 * frames), BF),
            jax.ShapeDtypeStruct((2, cols), F32),
        ),
        scratch_shapes=[
            pltpu.VMEM((cols, frames), F32),
            pltpu.VMEM((cols, frames), F32),
            pltpu.VMEM((cols, 2 * frames), F32),
        ],
        compiler_params=pltpu.CompilerParams(vmem_limit_bytes=48 * 1024 * 1024),
    )(query, key, value, pos, biases, prob, grad_out)

def gather_kernel(ud_own, sq_own, sm_own, ud_full, sq_full, sm_full, local_sem, swap_send, swap_recv, recv_sem, sib_recv, send_sem):
    g = Grid()
    half = ud_own.shape[1]
    c = g.core
    me = g.chip(g.z, g.a, g.b)
    local = [
        pltpu.make_async_copy(ud_own.at[c], ud_full.at[c, pl.ds(me * 2 * half + c * half, half)], local_sem.at[0]),
        pltpu.make_async_copy(sq_own, sq_full.at[me, c], local_sem.at[1]),
        pltpu.make_async_copy(sm_own, sm_full.at[me, c], local_sem.at[2]),
    ]
    for copy in local:
        copy.start()
    greet(g)
    swap = pltpu.make_async_remote_copy(
        src_ref=ud_own.at[1 - c],
        dst_ref=ud_full.at[1 - c, pl.ds(me * 2 * half + c * half, half)],
        send_sem=swap_send,
        recv_sem=swap_recv,
        device_id=g.sibling(),
        device_id_type=MESH,
    )
    swap.start()

    def pieces(t):
        return (ud_full.at[c, pl.ds(t * 2 * half, 2 * half)], sq_full.at[t, c], sm_full.at[t, c])

    ways = {"z+": 0, "z-": 1, "a+": 2, "a-": 3, "b+": 4, "b-": 5, "s": 6}

    def copies(t, way):
        if way == "s":
            target = g.sibling()
        else:
            target = g.up(way[0]) if way[1] == "+" else g.down(way[0])
        arrive = sib_recv if way == "s" else recv_sem
        return [
            pltpu.make_async_remote_copy(
                src_ref=ref,
                dst_ref=ref,
                send_sem=send_sem.at[ways[way], k, t],
                recv_sem=arrive.at[k, t],
                device_id=target,
                device_id_type=MESH,
            )
            for k, ref in enumerate(pieces(t))
        ]

    def send(t, way, finish=False):
        def act():
            for copy in copies(t, way):
                if finish:
                    copy.wait_send()
                else:
                    copy.start()

        if way == "s":
            act()
            return
        p, n = g.place(way[0])
        if n == 1:
            return
        pl.when(p < n - 1 if way[1] == "+" else p > 0)(act)

    def wait(t):
        for k, ref in enumerate(pieces(t)):
            pltpu.make_async_copy(ref, ref, recv_sem.at[k, t]).wait()

    def spread(finish):
        def got(t, ways_on):
            if not finish:
                wait(t)
            for way in ways_on:
                send(t, way, finish)

        if finish:
            pass
        else:
            for copy in local:
                copy.wait()
            swap.wait_recv()
        for way in ("z+", "z-", "a+", "a-", "b+", "b-", "s"):
            send(me, way, finish)
        for k in range(1, g.nz):
            pl.when(g.z >= k)(lambda: got(g.chip(g.z - k, g.a, g.b), ("z+", "a+", "a-", "b+", "b-", "s")))
            pl.when(g.z + k < g.nz)(lambda: got(g.chip(g.z + k, g.a, g.b), ("z-", "a+", "a-", "b+", "b-", "s")))

        def column(a, b, ways_on):
            got(g.chip(g.z, a, b), ways_on)
            for k in range(1, g.nz):
                pl.when(g.z >= k)(lambda: got(g.chip(g.z - k, a, b), ways_on))
                pl.when(g.z + k < g.nz)(lambda: got(g.chip(g.z + k, a, b), ways_on))

        for k in range(1, g.na):
            pl.when(g.a >= k)(lambda: column(g.a - k, g.b, ("a+", "b+", "b-", "s")))
            pl.when(g.a + k < g.na)(lambda: column(g.a + k, g.b, ("a-", "b+", "b-", "s")))
        for kb in range(1, g.nb):

            def plane(b, ways_on):
                column(g.a, b, ways_on)
                for k in range(1, g.na):
                    pl.when(g.a >= k)(lambda: column(g.a - k, b, ways_on))
                    pl.when(g.a + k < g.na)(lambda: column(g.a + k, b, ways_on))

            pl.when(g.b >= kb)(lambda: plane(g.b - kb, ("b+", "s")))
            pl.when(g.b + kb < g.nb)(lambda: plane(g.b + kb, ("b-", "s")))

    spread(False)
    d = 1 - c

    def other(t, _):
        for k, ref in enumerate((ud_full.at[d, pl.ds(t * 2 * half, 2 * half)], sq_full.at[t, d], sm_full.at[t, d])):
            pltpu.make_async_copy(ref, ref, sib_recv.at[k, t]).wait()
        return 0

    lax.fori_loop(0, g.chips, other, 0)
    swap.wait_send()
    spread(True)


def gather_weights(ud, sq, sm):
    devices = lax.axis_size("seq") * lax.axis_size("fsdp")
    chips = devices // 2
    _, rows, width = ud.shape
    hbm = pl.BlockSpec(memory_space=pl.ANY)
    vmem = pl.BlockSpec(memory_space=pltpu.VMEM)
    dma = pltpu.SemaphoreType.DMA
    return pl.pallas_call(
        gather_kernel,
        name="gather_weights",
        out_shape=(
            jax.ShapeDtypeStruct((2, devices * rows, width), ud.dtype),
            jax.ShapeDtypeStruct((chips, 2, rows, width), sq.dtype),
            jax.ShapeDtypeStruct((chips, 2) + sm.shape, sm.dtype),
        ),
        in_specs=[vmem] * 3,
        out_specs=[hbm] * 3,
        scratch_shapes=[
            dma((3,)),
            dma,
            dma,
            dma((3, chips)),
            dma((3, chips)),
            dma((7, 3, chips)),
        ],
        compiler_params=pltpu.CompilerParams(collective_id=1, has_side_effects=True),
    )(ud, sq, sm)


def scatter_kernel(ud_in, sq_in, sm_in, ud_out, sq_out, sm_out, acc, sib, rb, ra, rz, fin, send_ud,
                   local_sem, sib_send, sib_recv, b_send, b_recv, a_send, a_recv, z_send, z_recv, fin_send, fin_recv):
    g = Grid()
    c = g.core
    d = 1 - c
    nz, na, nb = g.nz, g.na, g.nb
    ud_rows = ud_out.shape[1]
    sq_rows = sq_out.shape[0]
    sm_rows = sm_out.shape[0]
    pair = 2 * ud_rows

    def slot(z, a, b):
        return (b * na + a) * nz + z

    def block_refs(buf, n):
        return (buf.at[n, pl.ds(0, pair)], buf.at[n, pl.ds(pair, sq_rows)], buf.at[n, pl.ds(pair + sq_rows, sm_rows)])

    def chip_refs(t, col):
        return (ud_in.at[col, pl.ds(t * pair, pair)], sq_in.at[t, col], sm_in.at[t, col])

    every = [(z, a, b) for b in range(nb) for a in range(na) for z in range(nz)]
    for z, a, b in every:
        n = slot(z, a, b)
        for k, (src, dst) in enumerate(zip(chip_refs(g.chip(z, a, b), c), block_refs(acc, n))):
            pltpu.make_async_copy(src, dst, local_sem.at[k, n]).start()
    greet(g)

    def sib_copies(z, a, b):
        n = slot(z, a, b)
        if g.na == g.nb:
            t = z * g.plane + (a * g.step_b + b * g.step_a) // 2
        else:
            t = g.chip(z, a, b)
        return [
            pltpu.make_async_remote_copy(
                src_ref=src,
                dst_ref=dst,
                send_sem=sib_send.at[k, n],
                recv_sem=sib_recv.at[k, n],
                device_id=g.sibling(),
                device_id_type=MESH,
            )
            for k, (src, dst) in enumerate(zip(chip_refs(t, d), block_refs(sib, n)))
        ]

    for z, a, b in every:
        for copy in sib_copies(z, a, b):
            copy.start()

    def add(n, ref):
        acc[n] = (acc[n].astype(F32) + ref[...].astype(F32)).astype(BF)

    def ready(z, a, b):
        n = slot(z, a, b)
        for k, (src, dst) in enumerate(zip(chip_refs(0, c), block_refs(acc, n))):
            pltpu.make_async_copy(src, dst, local_sem.at[k, n]).wait()
        for k, dst in enumerate(block_refs(sib, n)):
            pltpu.make_async_copy(dst, dst, sib_recv.at[k, n]).wait()
        add(n, sib.at[n])

    def travel(axis, n, m, buf, sends, recvs, upward):
        way = 0 if upward else 1
        return pltpu.make_async_remote_copy(
            src_ref=acc.at[n],
            dst_ref=buf.at[way, m],
            send_sem=sends.at[way, m],
            recv_sem=recvs.at[way, m],
            device_id=g.up(axis) if upward else g.down(axis),
            device_id_type=MESH,
        )

    def take(n, m, buf, recvs, way):
        pltpu.make_async_copy(buf.at[way, m], buf.at[way, m], recvs.at[way, m]).wait()
        add(n, buf.at[way, m])

    stages = {"b": (rb, b_send, b_recv), "a": (ra, a_send, a_recv), "z": (rz, z_send, z_recv)}

    def line(axis, blocks, prepare, finish):
        p, n_axis = g.place(axis)
        buf, sends, recvs = stages[axis]
        for k in range(n_axis - 1, 0, -1):
            for upward in (True, False):
                q = p + k if upward else p - k
                inside = p + k < n_axis if upward else p >= k
                behind = p > 0 if upward else p < n_axis - 1
                way = 0 if upward else 1

                def act():
                    for block in blocks(q):
                        n, m = block["slot"], block["m"]
                        if finish:
                            travel(axis, n, m, buf, sends, recvs, upward).wait_send()
                        else:
                            prepare(block)
                            pl.when(behind)(lambda: take(n, m, buf, recvs, way))
                            travel(axis, n, m, buf, sends, recvs, upward).start()

                pl.when(inside)(act)

    def settle(axis, block):
        p, n_axis = g.place(axis)
        buf, _, recvs = stages[axis]
        if n_axis > 1:
            pl.when(p > 0)(lambda: take(block["slot"], block["m"], buf, recvs, 0))
            pl.when(p < n_axis - 1)(lambda: take(block["slot"], block["m"], buf, recvs, 1))

    def z_order(a, b):
        return [(z, a, b) for z in range(nz)]

    def b_blocks(q):
        out = []
        for ka in list(range(1, na)) + [0]:
            a = lax.rem(g.a + ka, na)
            for z in range(nz):
                n = slot(z, a, q)
                out.append({"slot": n, "m": n, "at": (z, a, q)})
        return out

    def a_blocks(q):
        return [{"slot": slot(z, q, g.b), "m": q * nz + z, "at": (z, q, g.b)} for z in range(nz)]

    def z_blocks(q):
        return [{"slot": slot(q, g.a, g.b), "m": q, "at": (q, g.a, g.b)}]

    def along(block, axis):
        z, a, b = block["at"]
        if axis == "b":
            return {**block, "m": block["slot"]}
        return {**block, "m": a * nz + z}

    def from_b(block):
        ready(*block["at"])
        settle("b", along(block, "b"))

    def from_a(block):
        from_b(block)
        settle("a", along(block, "a"))

    line("b", b_blocks, lambda block: ready(*block["at"]), False)
    line("a", a_blocks, from_b, False)
    line("z", z_blocks, from_a, False)
    own = z_blocks(g.z)[0]
    from_a(own)
    settle("z", own)
    n = own["slot"]
    send_ud[...] = acc[n, pl.ds(pl.multiple_of(d * ud_rows, ud_rows), ud_rows), :].astype(F32)
    last = pltpu.make_async_remote_copy(
        src_ref=send_ud,
        dst_ref=fin,
        send_sem=fin_send,
        recv_sem=fin_recv,
        device_id=g.sibling(),
        device_id_type=MESH,
    )
    last.start()
    ud_out[c] = acc[n, pl.ds(pl.multiple_of(c * ud_rows, ud_rows), ud_rows), :].astype(F32)
    sq_out[...] = acc[n, pl.ds(pair, sq_rows), :].astype(F32)
    sm_out[...] = acc[n, pl.ds(pair + sq_rows, sm_rows), :].astype(F32)
    line("b", b_blocks, None, True)
    line("a", a_blocks, None, True)
    line("z", z_blocks, None, True)
    for z, a, b in every:
        for copy in sib_copies(z, a, b):
            copy.wait_send()
    last.wait()
    ud_out[d] = fin[...]


def scatter_grads(ud, sq, sm):
    nz, nf = lax.axis_size("seq"), lax.axis_size("fsdp")
    chips = nz * nf // 2
    width = ud.shape[2]
    rows = ud.shape[1] // (2 * chips)
    r = sm.shape[2]
    total = 3 * rows + r
    plane = nf // 2
    side = math.isqrt(plane)
    na, nb = (side, side) if side * side == plane else (plane, 1)
    hbm = pl.BlockSpec(memory_space=pl.ANY)
    vmem = pl.BlockSpec(memory_space=pltpu.VMEM)
    dma = pltpu.SemaphoreType.DMA
    return pl.pallas_call(
        scatter_kernel,
        name="scatter_grads",
        out_shape=(
            jax.ShapeDtypeStruct((2, rows, width), F32),
            jax.ShapeDtypeStruct((rows, width), F32),
            jax.ShapeDtypeStruct((r, width), F32),
        ),
        in_specs=[hbm] * 3,
        out_specs=[vmem] * 3,
        scratch_shapes=[
            pltpu.VMEM((chips, total, width), BF),
            pltpu.VMEM((chips, total, width), BF),
            pltpu.VMEM((2, chips, total, width), BF),
            pltpu.VMEM((2, na * nz, total, width), BF),
            pltpu.VMEM((2, nz, total, width), BF),
            pltpu.VMEM((rows, width), F32),
            pltpu.VMEM((rows, width), F32),
            dma((3, chips)),
            dma((3, chips)),
            dma((3, chips)),
            dma((2, chips)),
            dma((2, chips)),
            dma((2, na * nz)),
            dma((2, na * nz)),
            dma((2, nz)),
            dma((2, nz)),
            dma,
            dma,
        ],
        compiler_params=pltpu.CompilerParams(collective_id=2, has_side_effects=True, vmem_limit_bytes=60000 * 1024),
    )(ud, sq, sm)


def gathered(square, upward, downward, vectors, kernel):
    share = vectors.shape[1]
    small_rows = vectors.shape[0] + kernel.shape[0]
    small = jnp.concatenate([vectors, kernel], axis=0).astype(BF).reshape(-1)
    tall = -(-small.shape[0] // (16 * LANES)) * 16
    small = jnp.pad(small, (0, tall * LANES - small.shape[0])).reshape(tall, LANES)
    matrices, squares, smalls = gather_weights(
        jnp.stack([upward, downward]).astype(BF), square.astype(BF), small
    )
    devices = smalls.shape[0] * 2
    smalls = smalls.reshape(devices, tall * LANES)[:, : small_rows * share]
    smalls = smalls.reshape(devices, small_rows, share).transpose(1, 0, 2)
    smalls = smalls.reshape(small_rows, devices * share)
    split = vectors.shape[0]
    return (
        squares.reshape(devices * square.shape[0], square.shape[1]),
        matrices[0],
        matrices[1],
        smalls[:split],
        smalls[split:],
    )


def scattered(square_full, upward_full, downward_full, vectors_full, taps_full):
    devices = lax.axis_size("seq") * lax.axis_size("fsdp")
    width = square_full.shape[1]
    small = jnp.concatenate([vectors_full, taps_full], axis=0)
    small_rows, split = small.shape[0], vectors_full.shape[0]
    share = small.shape[1] // devices
    small = small.reshape(small_rows, devices, share).transpose(1, 0, 2)
    count = small_rows * share
    tall = -(-count // (16 * width)) * 16
    small = jnp.pad(small.reshape(devices, count), ((0, 0), (0, tall * width - count)))
    matrices, squares, smalls = scatter_grads(
        jnp.stack([upward_full.astype(BF), downward_full.astype(BF)]),
        square_full.astype(BF).reshape(devices // 2, 2, -1, width),
        small.astype(BF).reshape(devices // 2, 2, tall, width),
    )
    smalls = smalls.reshape(-1)[:count].reshape(small_rows, share)
    return squares, matrices[0], matrices[1], smalls[:split], smalls[split:]


def per_device(
    inputs,
    cotangent,
    lengths,
    square,
    upward,
    downward,
    vectors,
    kernel,
    square_momentum,
    square_variance,
    upward_momentum,
    upward_variance,
    downward_momentum,
    downward_variance,
    vectors_momentum,
    vectors_variance,
    kernel_momentum,
    kernel_variance,
):
    full_sq, full_up, full_down, full_vec, full_kern = gathered(
        square, upward, downward, vectors, kernel
    )
    model_width = inputs.shape[2]
    frame_count = inputs.shape[1]
    groups = lax.axis_size("seq")
    seq_place = lax.axis_index("seq")
    seq_frames = frame_count * groups
    head_cols = model_width // groups
    col_start = seq_place * head_cols
    rim_width = (full_kern.shape[0] - 1) // 2
    head_size = D // H
    small_params = full_vec.astype(jnp.float32)
    conv_taps = full_kern.astype(jnp.float32)
    signal = inputs[0].astype(jnp.float32)
    length = lengths[0]
    frame_index = seq_place * frame_count + jnp.arange(frame_count, dtype=jnp.int32)
    live_mask = (frame_index < length).astype(jnp.float32)[:, None]
    normed1 = layer_norm(signal, small_params[0], small_params[1]).astype(jnp.bfloat16)
    hidden1 = linear(normed1, full_up[:FF])
    active1 = jax.nn.silu(hidden1).astype(jnp.bfloat16)
    resid1 = signal + 0.5 * jnp.dot(active1, full_down[:FF], preferred_element_type=jnp.float32)
    normed2 = layer_norm(resid1, small_params[2], small_params[3]).astype(jnp.bfloat16)
    qkv = linear(normed2, full_sq[: 3 * model_width]).astype(jnp.bfloat16)
    query_time = qkv[:, :model_width]
    key_time = qkv[:, model_width : 2 * model_width]
    value_time = qkv[:, 2 * model_width :]
    query_head, key_head, value_head = (
        lax.all_to_all(query_time, "seq", split_axis=1, concat_axis=0, tiled=True),
        lax.all_to_all(key_time, "seq", split_axis=1, concat_axis=0, tiled=True),
        lax.all_to_all(value_time, "seq", split_axis=1, concat_axis=0, tiled=True),
    )
    biases = lax.dynamic_slice_in_dim(small_params[10:12], col_start, head_cols, 1)
    pos_table = position_table(seq_frames, model_width)
    pos_weight = lax.dynamic_slice_in_dim(full_sq, 3 * model_width + col_start, head_cols, 0)
    pos_heads = linear(pos_table, pos_weight).astype(jnp.bfloat16)
    attended, prob = attend_heads(
        query_head, key_head, value_head, pos_heads, biases, length, head_size
    )
    out_time = lax.all_to_all(attended, "seq", split_axis=0, concat_axis=1, tiled=True)
    resid2 = resid1 + linear(out_time, full_sq[4 * model_width : 5 * model_width])
    normed3 = layer_norm(resid2, small_params[4], small_params[5]).astype(jnp.bfloat16)
    pair = linear(normed3, full_sq[5 * model_width : 7 * model_width])
    lin_value = pair[:, :model_width]
    lin_gate = pair[:, model_width:]
    glu = (lin_value * jax.nn.sigmoid(lin_gate) * live_mask).astype(jnp.bfloat16)
    glu_pad = padded(glu, (("seq", 0),), rim_width)
    conv_out = depth_forward(glu_pad, conv_taps, frame_count)
    local_count = jnp.sum(live_mask)
    local_mean = jnp.sum(live_mask * conv_out, axis=0) / jnp.maximum(local_count, 1.0)
    local_squares = jnp.sum(live_mask * (conv_out - local_mean) ** 2, axis=0)
    moments = jnp.stack([jnp.broadcast_to(local_count, local_mean.shape), local_mean, local_squares])
    moments = meet(jnp.pad(moments, ((0, 5), (0, 0))), merge_moments, 3)
    frames, centre, spread = moments[0], moments[1], moments[2] / moments[0]
    inv_std = lax.rsqrt(spread + BN_EPS)
    centred = conv_out - centre
    zed = centred * inv_std
    bn_val = small_params[12] * zed + small_params[13]
    swish_b = jax.nn.silu(bn_val).astype(jnp.bfloat16)
    resid3 = resid2 + linear(swish_b, full_sq[7 * model_width :])
    normed4 = layer_norm(resid3, small_params[6], small_params[7]).astype(jnp.bfloat16)
    hidden4 = linear(normed4, full_up[FF:])
    active4 = jax.nn.silu(hidden4).astype(jnp.bfloat16)
    resid4 = resid3 + 0.5 * jnp.dot(active4, full_down[FF:], preferred_element_type=jnp.float32)
    layer_output = layer_norm(resid4, small_params[8], small_params[9]).astype(jnp.bfloat16)[None]
    grad_res4, grad_gain4, grad_shift4 = norm_back(
        resid4, small_params[8], small_params[9], cotangent[0].astype(jnp.float32)
    )
    grad_up4, grad_down4, grad_norm4 = ffn_back(
        normed4, hidden4, active4, full_up[FF:], full_down[FF:], 0.5 * grad_res4
    )
    grad_add, grad_gain3, grad_shift3 = norm_back(
        resid3, small_params[6], small_params[7], grad_norm4
    )
    grad_res3 = grad_res4 + grad_add
    grad_conv_b = grad_res3.astype(jnp.bfloat16)
    grad_point = outer(grad_conv_b, swish_b)
    grad_bn = jnp.dot(
        grad_conv_b, full_sq[7 * model_width :], preferred_element_type=jnp.float32
    ) * silu_slope(bn_val)
    grad_gamma = jnp.sum(grad_bn * zed, axis=0)
    grad_beta = jnp.sum(grad_bn, axis=0)
    grad_zed = grad_bn * small_params[12]
    sums = jnp.stack([jnp.sum(grad_zed, axis=0), jnp.sum(grad_zed * centred, axis=0)])
    sums = meet(jnp.pad(sums, ((0, 6), (0, 0))), lambda x, y: x + y, 4)
    sum_one, sum_two = sums[0], sums[1]
    grad_conv = inv_std * grad_zed - live_mask / frames * (
        inv_std * sum_one + inv_std**3 * sum_two * centred
    )
    grad_pad = padded(grad_conv.astype(jnp.bfloat16), (("seq", 0),), rim_width)
    grad_taps, grad_glu = depth_back(grad_pad, glu_pad, conv_taps, frame_count)
    grad_glu = grad_glu * live_mask
    gate_open = jax.nn.sigmoid(lin_gate)
    grad_pair = jnp.concatenate(
        [grad_glu * gate_open, grad_glu * lin_value * gate_open * (1.0 - gate_open)], axis=1
    ).astype(jnp.bfloat16)
    grad_lin = outer(grad_pair, normed3)
    grad_norm3 = jnp.dot(
        grad_pair, full_sq[5 * model_width : 7 * model_width], preferred_element_type=jnp.float32
    )
    grad_add, grad_gain2, grad_shift2 = norm_back(
        resid2, small_params[4], small_params[5], grad_norm3
    )
    grad_res2 = grad_res3 + grad_add
    grad_att_b = grad_res2.astype(jnp.bfloat16)
    grad_outw = outer(grad_att_b, out_time)
    grad_out_time = jnp.dot(
        grad_att_b, full_sq[4 * model_width : 5 * model_width], preferred_element_type=jnp.float32
    ).astype(jnp.bfloat16)
    grad_out_head = lax.all_to_all(grad_out_time, "seq", split_axis=1, concat_axis=0, tiled=True)
    grad_query_b, grad_key_b, grad_value_b, grad_table, grad_biases = attend_heads_back(
        query_head, key_head, value_head, pos_heads, biases, prob, grad_out_head, head_size
    )
    grad_query_time, grad_key_time, grad_value_time = (
        lax.all_to_all(grad_query_b, "seq", split_axis=0, concat_axis=1, tiled=True),
        lax.all_to_all(grad_key_b, "seq", split_axis=0, concat_axis=1, tiled=True),
        lax.all_to_all(grad_value_b, "seq", split_axis=0, concat_axis=1, tiled=True),
    )
    grad_qkv = jnp.concatenate([grad_query_time, grad_key_time, grad_value_time], axis=1)
    grad_inw = outer(grad_qkv, normed2)
    grad_norm2 = jnp.dot(grad_qkv, full_sq[: 3 * model_width], preferred_element_type=jnp.float32)
    grad_pos_cols = jnp.dot(grad_table, pos_table, preferred_element_type=jnp.float32)
    grad_pos = lax.dynamic_update_slice_in_dim(
        jnp.zeros((model_width, model_width), jnp.float32), grad_pos_cols, col_start, 0
    )
    zero_row = jnp.zeros((model_width,), jnp.float32)
    grad_bias_u = lax.dynamic_update_slice_in_dim(
        zero_row, grad_biases[0], col_start, 0
    )
    grad_bias_v = lax.dynamic_update_slice_in_dim(
        zero_row, grad_biases[1], col_start, 0
    )
    grad_add, grad_gain1, grad_shift1 = norm_back(
        resid1, small_params[2], small_params[3], grad_norm2
    )
    grad_res1 = grad_res2 + grad_add
    grad_up1, grad_down1, grad_norm1 = ffn_back(
        normed1, hidden1, active1, full_up[:FF], full_down[:FF], 0.5 * grad_res1
    )
    grad_add, grad_gain0, grad_shift0 = norm_back(
        signal, small_params[0], small_params[1], grad_norm1
    )
    input_grad = (grad_res1 + grad_add)[None]
    square_full = jnp.concatenate([grad_inw, grad_pos, grad_outw, grad_lin, grad_point], axis=0)
    upward_full = jnp.concatenate([grad_up1, grad_up4], axis=0)
    downward_full = jnp.concatenate([grad_down1, grad_down4], axis=0)
    vectors_full = jnp.stack(
        [
            grad_gain0,
            grad_shift0,
            grad_gain1,
            grad_shift1,
            grad_gain2,
            grad_shift2,
            grad_gain3,
            grad_shift3,
            grad_gain4,
            grad_shift4,
            grad_bias_u,
            grad_bias_v,
            grad_gamma,
            grad_beta,
        ]
    )
    square_grad, upward_grad, downward_grad, vectors_grad, kernel_grad = scattered(
        square_full, upward_full, downward_full, vectors_full, grad_taps
    )
    square_next, momentum_square, variance_square = adam_step(
        square, square_grad, square_momentum, square_variance, DECAY_RATE
    )
    upward_next, momentum_upward, variance_upward = adam_step(
        upward, upward_grad, upward_momentum, upward_variance, DECAY_RATE
    )
    downward_next, momentum_downward, variance_downward = adam_step(
        downward, downward_grad, downward_momentum, downward_variance, DECAY_RATE
    )
    vectors_next, momentum_vectors, variance_vectors = adam_step(
        vectors, vectors_grad, vectors_momentum, vectors_variance, 0.0
    )
    kernel_next, momentum_kernel, variance_kernel = adam_step(
        kernel, kernel_grad, kernel_momentum, kernel_variance, DECAY_RATE
    )
    return (
        layer_output,
        input_grad,
        square_grad,
        upward_grad,
        downward_grad,
        vectors_grad,
        kernel_grad,
        square_next,
        upward_next,
        downward_next,
        vectors_next,
        kernel_next,
        momentum_square,
        variance_square,
        momentum_upward,
        variance_upward,
        momentum_downward,
        variance_downward,
        momentum_vectors,
        variance_vectors,
        momentum_kernel,
        variance_kernel,
    )


def solution(mesh):
    return jax.shard_map(
        per_device,
        mesh=mesh,
        in_specs=(
            P("fsdp", "seq", None),
            P("fsdp", "seq", None),
            P("fsdp"),
            P(("seq", "fsdp"), None),
            P(("seq", "fsdp"), None),
            P(("seq", "fsdp"), None),
            P(None, ("seq", "fsdp")),
            P(None, ("seq", "fsdp")),
            P(("seq", "fsdp"), None),
            P(("seq", "fsdp"), None),
            P(("seq", "fsdp"), None),
            P(("seq", "fsdp"), None),
            P(("seq", "fsdp"), None),
            P(("seq", "fsdp"), None),
            P(None, ("seq", "fsdp")),
            P(None, ("seq", "fsdp")),
            P(None, ("seq", "fsdp")),
            P(None, ("seq", "fsdp")),
        ),
        out_specs=(
            P("fsdp", "seq", None),
            P("fsdp", "seq", None),
            P(("seq", "fsdp"), None),
            P(("seq", "fsdp"), None),
            P(("seq", "fsdp"), None),
            P(None, ("seq", "fsdp")),
            P(None, ("seq", "fsdp")),
            P(("seq", "fsdp"), None),
            P(("seq", "fsdp"), None),
            P(("seq", "fsdp"), None),
            P(None, ("seq", "fsdp")),
            P(None, ("seq", "fsdp")),
            P(("seq", "fsdp"), None),
            P(("seq", "fsdp"), None),
            P(("seq", "fsdp"), None),
            P(("seq", "fsdp"), None),
            P(("seq", "fsdp"), None),
            P(("seq", "fsdp"), None),
            P(None, ("seq", "fsdp")),
            P(None, ("seq", "fsdp")),
            P(None, ("seq", "fsdp")),
            P(None, ("seq", "fsdp")),
        ),
        check_vma=False,
    )
```

```python
import math

import jax
import jax.numpy as jnp
from jax import lax
from jax.experimental import pallas as pl
from jax.experimental.pallas import tpu as pltpu
from jax.sharding import PartitionSpec as P

D = 512
H = 8
FF = 2048
ADAM_STEP = 4

LN_EPS = 1e-05
BN_EPS = 1e-05
BETA_ONE = 0.9
BETA_TWO = 0.98
ADAM_EPS = 1e-08
LEARN_RATE = 0.005
DECAY_RATE = 0.01


def outer(first_op, second_op):
    return lax.dot_general(
        first_op, second_op, (((0,), (0,)), ((), ())), preferred_element_type=jnp.float32
    )


def layer_norm(signal, norm_gain, norm_shift):
    row_mean = jnp.mean(signal, axis=-1, keepdims=True)
    centred = signal - row_mean
    row_var = jnp.mean(centred * centred, axis=-1, keepdims=True)
    return centred * lax.rsqrt(row_var + LN_EPS) * norm_gain + norm_shift


def norm_back(signal, norm_gain, norm_shift, upstream):
    pullback = jax.vjp(layer_norm, signal, norm_gain, norm_shift)[1]
    return pullback(upstream)


def silu_slope(argument):
    sigma_val = jax.nn.sigmoid(argument)
    return sigma_val * (1.0 + argument * (1.0 - sigma_val))


def position_tables(seq_frames, model_width):
    fine = math.gcd(2 * seq_frames, 64)
    column = jnp.arange(model_width)
    frequency = jnp.exp(-math.log(10000.0) * 2.0 * (column // 2).astype(jnp.float32) / model_width)
    coarse_at = (seq_frames - 1 - fine * jnp.arange(2 * seq_frames // fine)).astype(jnp.float32)
    coarse_phase = coarse_at[:, None] * frequency[None, :]
    fine_phase = jnp.arange(fine).astype(jnp.float32)[:, None] * frequency[None, :]
    even = (column % 2 == 0)[None, :]
    sine, cosine = jnp.sin(coarse_phase), jnp.cos(coarse_phase)
    with_cosine = jnp.where(even, sine, cosine)
    with_sine = jnp.where(even, -cosine, sine)
    return jnp.stack([with_cosine, with_sine]), jnp.stack([jnp.cos(fine_phase), jnp.sin(fine_phase)])


def ffn_back(normed_b, hidden, active, up_rows, down_rows, upstream):
    upstream_b = upstream.astype(jnp.bfloat16)
    grad_down = outer(active, upstream_b)
    grad_active = lax.dot_general(upstream_b, down_rows, NT, preferred_element_type=jnp.float32)
    grad_hidden = (grad_active * silu_slope(hidden)).astype(jnp.bfloat16)
    grad_up = outer(grad_hidden, normed_b)
    grad_normed = jnp.dot(grad_hidden, up_rows, preferred_element_type=jnp.float32)
    return (grad_up, grad_down, grad_normed)


def adam_step(weight, gradient, first_mom, second_mom, decay):
    first_new = BETA_ONE * first_mom + (1.0 - BETA_ONE) * gradient
    second_new = BETA_TWO * second_mom + (1.0 - BETA_TWO) * gradient * gradient
    fix_one = 1.0 - BETA_ONE**ADAM_STEP
    fix_two = 1.0 - BETA_TWO**ADAM_STEP
    update = first_new / fix_one / (jnp.sqrt(second_new / fix_two) + ADAM_EPS)
    return (weight - LEARN_RATE * (update + decay * weight), first_new, second_new)


MESH = pl.DeviceIdType.MESH
BF = jnp.bfloat16
F32 = jnp.float32
LANES = 128


class Grid:
    def __init__(self):
        self.nz = lax.axis_size("seq")
        self.nf = lax.axis_size("fsdp")
        plane = self.nf // 2
        side = math.isqrt(plane)
        self.z = lax.axis_index("seq")
        f = lax.axis_index("fsdp")
        self.core = f % 2
        if side * side == plane:
            self.na = self.nb = side
            self.step_a = 2 + self.core * (2 * side - 2)
            self.step_b = 2 * side - self.core * (2 * side - 2)
        else:
            self.na, self.nb = plane, 1
            self.step_a, self.step_b = 2, self.nf
        self.f = f
        self.a = (f // self.step_a) % self.na
        self.b = (f // self.step_b) % self.nb
        self.plane = plane
        self.chips = plane * self.nz

    def chip(self, z, a, b):
        return z * self.plane + (a * self.step_a + b * self.step_b) // 2

    def device(self, z, a, b):
        return (z, a * self.step_a + b * self.step_b + self.core)

    def sibling(self):
        return (self.z, self.f + 1 - 2 * self.core)

    def up(self, axis):
        return self.device(self.z + (axis == "z"), self.a + (axis == "a"), self.b + (axis == "b"))

    def down(self, axis):
        return self.device(self.z - (axis == "z"), self.a - (axis == "a"), self.b - (axis == "b"))

    def line(self, axis):
        return {
            "c": (self.core, 2, lambda q: (self.z, self.f - self.core + q)),
            "a": (self.a, self.na, lambda q: self.device(self.z, q, self.b)),
            "b": (self.b, self.nb, lambda q: self.device(self.z, self.a, q)),
            "z": (self.z, self.nz, lambda q: self.device(q, self.a, self.b)),
        }[axis]

    def place(self, axis):
        return {"z": (self.z, self.nz), "a": (self.a, self.na), "b": (self.b, self.nb)}[axis]


def greet(g):
    barrier = pltpu.get_barrier_semaphore()
    pl.semaphore_signal(barrier, inc=1, device_id=g.sibling(), device_id_type=MESH)
    total = 1
    for axis in "zab":
        p, n = g.place(axis)
        if n == 1:
            continue

        @pl.when(p < n - 1)
        def _():
            pl.semaphore_signal(barrier, inc=1, device_id=g.up(axis), device_id_type=MESH)

        @pl.when(p > 0)
        def _():
            pl.semaphore_signal(barrier, inc=1, device_id=g.down(axis), device_id_type=MESH)

        total = total + 2 - (n - 1 - p == 0) - (p == 0)
    pl.semaphore_wait(barrier, total)


def merge_moments(first_op, second_op):
    count = first_op[0:1] + second_op[0:1]
    share = second_op[0:1] / jnp.maximum(count, 1.0)
    gap = second_op[1:2] - first_op[1:2]
    mean = first_op[1:2] + gap * share
    squares = first_op[2:3] + second_op[2:3] + gap * gap * (first_op[0:1] * share)
    return jnp.concatenate([count, mean, squares, first_op[3:]], axis=0)


NT = (((1,), (1,)), ((), ()))
TN = (((0,), (0,)), ((), ()))
NN = (((1,), (0,)), ((), ()))


def dot(first_op, second_op, dims):
    return lax.dot_general(first_op, second_op, dims, preferred_element_type=F32)


def keep_head(value, h, head_size):
    lane = lax.broadcasted_iota(jnp.int32, value.shape, 1)
    return jnp.where(lane // head_size == h, value, jnp.zeros_like(value))


def attend_kernel(head_size, len_ref, q_ref, k_ref, v_ref, pos_ref, bias_ref, o_ref, prob_ref):
    i = pl.program_id(0)
    rows, cols = q_ref.shape
    frames = k_ref.shape[0]
    width = rows + frames
    query = q_ref[...].astype(F32)
    content = (query + bias_ref[0:1, :]).astype(BF)
    positional = (query + bias_ref[1:2, :]).astype(BF)
    window = pos_ref[pl.ds(pl.multiple_of(frames - rows - i * rows, rows), width), :]
    live = lax.broadcasted_iota(jnp.int32, (rows, frames), 1) < len_ref[0]
    out = jnp.zeros((rows, cols), F32)
    for h in range(cols // head_size):
        direct = dot(keep_head(content, h, head_size), k_ref[...], NT)
        spread = dot(keep_head(positional, h, head_size), window, NT)
        shifted = pltpu.roll(spread, width - rows + 1, 1, stride=1, stride_axis=0)[:, :frames]
        score = jnp.where(live, (direct + shifted) * (1.0 / math.sqrt(head_size)), -1e30)
        top = jnp.max(score, axis=-1, keepdims=True)
        power = jnp.exp(score - top)
        prob = power * (1.0 / jnp.sum(power, axis=-1, keepdims=True))
        prob_b = prob.astype(BF)
        prob_ref[h] = prob_b
        out = out + keep_head(dot(prob_b, v_ref[...], NN), h, head_size)
    o_ref[...] = out.astype(BF)


def attend_heads(query, key, value, pos, biases, length, head_size, rows=256):
    frames, cols = query.shape
    rows = min(rows, frames)
    heads = cols // head_size
    full = lambda n: pl.BlockSpec((n, cols), lambda i: (0, 0))
    return pl.pallas_call(
        lambda *refs: attend_kernel(head_size, *refs),
        name="attend_heads",
        grid=(frames // rows,),
        in_specs=[
            pl.BlockSpec(memory_space=pltpu.SMEM),
            pl.BlockSpec((rows, cols), lambda i: (i, 0)),
            full(frames),
            full(frames),
            full(2 * frames),
            full(2),
        ],
        out_specs=[
            pl.BlockSpec((rows, cols), lambda i: (i, 0)),
            pl.BlockSpec((heads, rows, frames), lambda i: (0, i, 0)),
        ],
        out_shape=(
            jax.ShapeDtypeStruct((frames, cols), BF),
            jax.ShapeDtypeStruct((heads, frames, frames), BF),
        ),
        compiler_params=pltpu.CompilerParams(vmem_limit_bytes=48 * 1024 * 1024),
    )(length.reshape(1), query, key, value, pos, biases)


def attend_back_kernel(head_size, q_ref, k_ref, v_ref, pos_ref, bias_ref, prob_ref, go_ref,
                       gq_ref, gk_ref, gv_ref, gpos_ref, gbias_ref, gk_acc, gv_acc, gpos_acc):
    i = pl.program_id(0)
    rows, cols = q_ref.shape
    frames = k_ref.shape[0]
    width = rows + frames

    @pl.when(i == 0)
    def _():
        gk_acc[...] = jnp.zeros_like(gk_acc)
        gv_acc[...] = jnp.zeros_like(gv_acc)
        gpos_acc[...] = jnp.zeros_like(gpos_acc)
        gbias_ref[...] = jnp.zeros_like(gbias_ref)

    query = q_ref[...].astype(F32)
    content = (query + bias_ref[0:1, :]).astype(BF)
    positional = (query + bias_ref[1:2, :]).astype(BF)
    start = pl.multiple_of(frames - rows - i * rows, rows)
    window = pos_ref[pl.ds(start, width), :]
    down = lax.broadcasted_iota(jnp.int32, (rows, rows), 0)
    across = lax.broadcasted_iota(jnp.int32, (rows, rows), 1)
    turn = jnp.where(down + across == rows - 1, 1.0, 0.0).astype(BF)
    positional_turned = dot(turn, positional, NN).astype(BF)
    grad_content = jnp.zeros((rows, cols), F32)
    grad_position = jnp.zeros((rows, cols), F32)
    for h in range(cols // head_size):
        grad_out = keep_head(go_ref[...], h, head_size)
        prob_b = prob_ref[h]
        prob = prob_b.astype(F32)
        grad_prob = dot(grad_out, v_ref[...], NT)
        delta = jnp.sum(prob * grad_prob, axis=-1, keepdims=True)
        grad_score = prob * (grad_prob - delta) * (1.0 / math.sqrt(head_size))
        score_b = grad_score.astype(BF)
        grad_content = grad_content + keep_head(dot(score_b, k_ref[...], NN), h, head_size)
        gk_acc[...] += dot(keep_head(content, h, head_size), score_b, TN)
        gv_acc[...] += dot(grad_out, prob_b, TN)
        turned = dot(turn, score_b, NN)
        wide = jnp.concatenate([turned, jnp.zeros((rows, width - frames), F32)], axis=1)
        spread = pltpu.roll(wide, 0, 1, stride=1, stride_axis=0).astype(BF)
        grad_position = grad_position + keep_head(dot(spread, window, NN), h, head_size)
        gpos_acc[:, pl.ds(start, width)] += dot(keep_head(positional_turned, h, head_size), spread, TN)
    high = grad_position.astype(BF)
    low = (grad_position - high.astype(F32)).astype(BF)
    grad_position = dot(turn, high, NN) + dot(turn, low, NN)
    gq_ref[...] = (grad_content + grad_position).astype(BF)
    gbias_ref[0:1, :] += jnp.sum(grad_content, axis=0, keepdims=True)
    gbias_ref[1:2, :] += jnp.sum(grad_position, axis=0, keepdims=True)

    @pl.when(i == pl.num_programs(0) - 1)
    def _():
        gk_ref[...] = gk_acc[...].T.astype(BF)
        gv_ref[...] = gv_acc[...].T.astype(BF)
        gpos_ref[...] = gpos_acc[...].astype(BF)


def attend_heads_back(query, key, value, pos, biases, prob, grad_out, head_size, rows=256):
    frames, cols = query.shape
    rows = min(rows, frames)
    heads = cols // head_size
    full = lambda n: pl.BlockSpec((n, cols), lambda i: (0, 0))
    block = pl.BlockSpec((rows, cols), lambda i: (i, 0))
    return pl.pallas_call(
        lambda *refs: attend_back_kernel(head_size, *refs),
        name="attend_heads_back",
        grid=(frames // rows,),
        in_specs=[
            block,
            full(frames),
            full(frames),
            full(2 * frames),
            full(2),
            pl.BlockSpec((heads, rows, frames), lambda i: (0, i, 0)),
            block,
        ],
        out_specs=[
            block,
            full(frames),
            full(frames),
            pl.BlockSpec((cols, 2 * frames), lambda i: (0, 0)),
            full(2),
        ],
        out_shape=(
            jax.ShapeDtypeStruct((frames, cols), BF),
            jax.ShapeDtypeStruct((frames, cols), BF),
            jax.ShapeDtypeStruct((frames, cols), BF),
            jax.ShapeDtypeStruct((cols, 2 * frames), BF),
            jax.ShapeDtypeStruct((2, cols), F32),
        ),
        scratch_shapes=[
            pltpu.VMEM((cols, frames), F32),
            pltpu.VMEM((cols, frames), F32),
            pltpu.VMEM((cols, 2 * frames), F32),
        ],
        compiler_params=pltpu.CompilerParams(vmem_limit_bytes=48 * 1024 * 1024),
    )(query, key, value, pos, biases, prob, grad_out)

def normalize(value):
    mean = jnp.mean(value, axis=-1, keepdims=True)
    centred = value - mean
    spread = lax.rsqrt(jnp.mean(centred * centred, axis=-1, keepdims=True) + LN_EPS)
    return centred * spread, spread


def norm_forward(value, gains, k):
    unit, _ = normalize(value)
    return (unit * gains[2 * k : 2 * k + 1] + gains[2 * k + 1 : 2 * k + 2]).astype(BF)


def norm_backward(value, gains, k, upstream):
    unit, spread = normalize(value)
    inner = upstream * gains[2 * k : 2 * k + 1]
    along = jnp.mean(inner * unit, axis=-1, keepdims=True)
    grad = spread * (inner - jnp.mean(inner, axis=-1, keepdims=True) - unit * along)
    gain = jnp.sum(upstream * unit, axis=0, keepdims=True)
    return grad, gain, jnp.sum(upstream, axis=0, keepdims=True)


def sigmoid(value):
    return 1.0 / (1.0 + jnp.exp(-value))


def module_forward(normed, up_ref, down_ref, hidden_ref, active_ref):
    units, width = up_ref.shape
    step = min(512, units)

    def chunk(j, total):
        here = pl.ds(pl.multiple_of(j * step, step), step)
        hidden = dot(normed, up_ref[here, :], NT)
        active = (hidden * sigmoid(hidden)).astype(BF)
        hidden_ref[:, here] = hidden
        active_ref[:, here] = active
        return total + dot(active, down_ref[here, :], NN)

    return lax.fori_loop(0, units // step, chunk, jnp.zeros((normed.shape[0], width), F32))


def module_backward(upstream_b, up_ref, down_ref, hidden_ref, grad_ref):
    units, width = up_ref.shape
    step = min(512, units)

    def chunk(j, total):
        here = pl.ds(pl.multiple_of(j * step, step), step)
        hidden = hidden_ref[:, here]
        sigma = sigmoid(hidden)
        slope = sigma * (1.0 + hidden * (1.0 - sigma))
        grad = (dot(upstream_b, down_ref[here, :], NT) * slope).astype(BF)
        grad_ref[:, here] = grad
        return total + dot(grad, up_ref[here, :], NN)

    return lax.fori_loop(0, units // step, chunk, jnp.zeros((upstream_b.shape[0], width), F32))


def greet_lines(g, axes):
    barrier = pltpu.get_barrier_semaphore()
    total = 0
    for axis in axes:
        p, n, device = g.line(axis)
        for k in range(1, n):
            pl.semaphore_signal(barrier, inc=1, device_id=device(lax.rem(p + k, n)), device_id_type=MESH)
            total += 1
    pl.semaphore_wait(barrier, total)


def remote(src, dst, send, recv, device):
    return pltpu.make_async_remote_copy(
        src_ref=src, dst_ref=dst, send_sem=send, recv_sem=recv, device_id=device, device_id_type=MESH
    )


def arrived(ref, sem):
    pltpu.make_async_copy(ref, ref, sem).wait()


def front_kernel(x_ref, gains_ref, coarse_ref, fine_ref, ud_hbm, sq_hbm,
                 x1_ref, a1_ref, h1_ref, s1_ref, a2_ref, heads_ref, pos_ref,
                 up, down, wqkv, wpos, mine, load_sem, send_sem, recv_sem):
    g = Grid()
    z, nz = g.z, g.nz
    rows, width = x_ref.shape
    cols = width // nz
    units = up.shape[0]
    loads = [
        pltpu.make_async_copy(ud_hbm.at[0, pl.ds(0, units)], up, load_sem.at[0]),
        pltpu.make_async_copy(ud_hbm.at[1, pl.ds(0, units)], down, load_sem.at[1]),
        pltpu.make_async_copy(sq_hbm.at[pl.ds(0, 3 * width)], wqkv, load_sem.at[2]),
        pltpu.make_async_copy(sq_hbm.at[pl.ds(3 * width + z * cols, cols)], wpos, load_sem.at[3]),
    ]
    for load in loads:
        load.start()
    greet_lines(g, "z")
    gains = gains_ref[...]
    signal = x_ref[...].astype(F32)
    normed1 = norm_forward(signal, gains, 0)
    a1_ref[...] = normed1
    loads[0].wait()
    loads[1].wait()
    resid1 = signal + 0.5 * module_forward(normed1, up, down, h1_ref, s1_ref)
    x1_ref[...] = resid1
    normed2 = norm_forward(resid1, gains, 1)
    a2_ref[...] = normed2
    loads[2].wait()
    for k in range(3):
        out = dot(normed2, wqkv[pl.ds(k * width, width), :], NT).astype(BF)
        for q in range(nz):
            mine[q, k] = out[:, q * cols : (q + 1) * cols]
    sends = []
    for k in range(1, nz):
        q = lax.rem(z + k, nz)
        copy = remote(mine.at[q], heads_ref.at[:, pl.ds(z * rows, rows)], send_sem.at[k], recv_sem.at[z], g.device(q, g.a, g.b))
        copy.start()
        sends.append(copy)
    own = pl.ds(pl.multiple_of(z * rows, rows), rows)
    for k in range(3):
        heads_ref[k, own, :] = mine[z, k]
    loads[3].wait()
    fine = fine_ref.shape[1]
    weight = wpos[...]

    def position(i, _):
        table = coarse_ref[0, pl.ds(i, 1), :] * fine_ref[0] + coarse_ref[1, pl.ds(i, 1), :] * fine_ref[1]
        here = pl.ds(pl.multiple_of(i * fine, fine), fine)
        pos_ref[here, :] = dot(table.astype(BF), weight, NT).astype(BF)
        return 0

    lax.fori_loop(0, coarse_ref.shape[1], position, 0)
    for k in range(1, nz):
        q = lax.rem(z + k, nz)
        arrived(heads_ref.at[:, pl.ds(q * rows, rows)], recv_sem.at[q])
    for copy in sends:
        copy.wait_send()


def front(signal, gains, coarse, fine, ud_full, sq_full):
    rows, width = signal.shape
    nz = lax.axis_size("seq")
    frames, cols = rows * nz, width // nz
    units = ud_full.shape[1] // 2
    vmem = pl.BlockSpec(memory_space=pltpu.VMEM)
    hbm = pl.BlockSpec(memory_space=pl.ANY)
    shape = jax.ShapeDtypeStruct
    return pl.pallas_call(
        front_kernel,
        name="front",
        out_shape=(
            shape((rows, width), F32),
            shape((rows, width), BF),
            shape((rows, units), F32),
            shape((rows, units), BF),
            shape((rows, width), BF),
            shape((3, frames, cols), BF),
            shape((2 * frames, cols), BF),
        ),
        in_specs=[vmem, vmem, vmem, vmem, hbm, hbm],
        out_specs=[vmem] * 7,
        scratch_shapes=[
            pltpu.VMEM((units, width), BF),
            pltpu.VMEM((units, width), BF),
            pltpu.VMEM((3 * width, width), BF),
            pltpu.VMEM((cols, width), BF),
            pltpu.VMEM((nz, 3, rows, cols), BF),
            pltpu.SemaphoreType.DMA((4,)),
            pltpu.SemaphoreType.DMA((nz,)),
            pltpu.SemaphoreType.DMA((nz,)),
        ],
        compiler_params=pltpu.CompilerParams(
            collective_id=5, has_side_effects=True, vmem_limit_bytes=40 * 1024 * 1024
        ),
    )(signal, gains, coarse, fine, ud_full, sq_full)


def meet_levels(g, value, merge, buf, send_sem, recv_sem):
    sends = []
    for level, axis in enumerate("cabz"):
        p, n, device = g.line(axis)
        if n == 1:
            continue
        buf[level, p] = value
        for k in range(1, n):
            copy = remote(buf.at[level, p], buf.at[level, p], send_sem.at[level, k], recv_sem.at[level, p], device(lax.rem(p + k, n)))
            copy.start()
            sends.append(copy)
        for k in range(1, n):
            q = lax.rem(p + k, n)
            arrived(buf.at[level, q], recv_sem.at[level, q])
        value = buf[level, 0]
        for q in range(1, n):
            value = merge(value, buf[level, q])
    return value, sends


HALO = 16


def swap_edges(g, body, low, high, send_sem, recv_sem, pad):
    rows = body.shape[0]
    p, n = g.z, g.nz
    up = remote(body.at[pl.ds(rows - HALO, HALO)], low, send_sem.at[0], recv_sem.at[0], g.device(g.z + 1, g.a, g.b))
    down = remote(body.at[pl.ds(0, HALO)], high, send_sem.at[1], recv_sem.at[1], g.device(g.z - 1, g.a, g.b))
    pl.when(p < n - 1)(lambda: up.start())
    pl.when(p > 0)(lambda: down.start())
    pad[pl.ds(HALO, rows), :] = body[...].astype(F32)

    def fill(at, ref, sem, there):
        @pl.when(there)
        def _():
            arrived(ref, sem)
            pad[pl.ds(at, HALO), :] = ref[...].astype(F32)

        @pl.when(jnp.logical_not(there))
        def _():
            pad[pl.ds(at, HALO), :] = jnp.zeros((HALO, pad.shape[1]), F32)

    fill(0, low, recv_sem.at[0], p > 0)
    fill(HALO + rows, high, recv_sem.at[1], p < n - 1)

    def finish():
        pl.when(p < n - 1)(lambda: up.wait_send())
        pl.when(p > 0)(lambda: down.wait_send())

    return finish


def middle_kernel(len_ref, att_ref, x1_ref, cot_ref, gains_ref, taps_ref, ud_hbm, sq_hbm,
                  y_ref, g2_ref, go_ref, o_ref, e2_ref, a3_ref, gpair_ref, e3_ref, sw_ref, a4_ref, s4_ref, gh4_ref, e4_ref,
                  small_ref, gtaps_ref,
                  up, down, wsq, o_buf, go_buf, glu_b, gc_b, low1, high1, low2, high2, pad_glu, pad_gc, h4, c_ref,
                  buf1, buf2, load_sem, a_send, a_recv, b_send, b_recv, h_send, h_recv, m_send, m_recv):
    g = Grid()
    z, nz = g.z, g.nz
    rows, width = x1_ref.shape
    cols = width // nz
    units = up.shape[0]
    taps = taps_ref.shape[0]
    rim = (taps - 1) // 2
    loads = [
        pltpu.make_async_copy(sq_hbm.at[pl.ds(4 * width, 4 * width)], wsq, load_sem.at[0]),
        pltpu.make_async_copy(ud_hbm.at[0, pl.ds(units, units)], up, load_sem.at[1]),
        pltpu.make_async_copy(ud_hbm.at[1, pl.ds(units, units)], down, load_sem.at[2]),
    ]
    for load in loads:
        load.start()
    greet_lines(g, "cabz")
    sends = []
    for k in range(1, nz):
        q = lax.rem(z + k, nz)
        copy = remote(att_ref.at[pl.ds(q * rows, rows)], o_buf.at[z], a_send.at[k], a_recv.at[z], g.device(q, g.a, g.b))
        copy.start()
        sends.append(copy)
    o_buf[z] = att_ref[pl.ds(pl.multiple_of(z * rows, rows), rows), :]
    gains = gains_ref[...]
    frame = z * rows + lax.broadcasted_iota(jnp.int32, (rows, 1), 0)
    live = jnp.where(frame < len_ref[0], 1.0, 0.0)
    loads[0].wait()
    weight = lambda k: wsq[pl.ds((k - 4) * width, width), :]
    for k in range(1, nz):
        q = lax.rem(z + k, nz)
        arrived(o_buf.at[q], a_recv.at[q])
    out = jnp.concatenate([o_buf[q] for q in range(nz)], axis=1)
    o_ref[...] = out
    resid2 = x1_ref[...] + dot(out, weight(4), NT)
    normed3 = norm_forward(resid2, gains, 2)
    a3_ref[...] = normed3
    value = dot(normed3, weight(5), NT)
    gate = sigmoid(dot(normed3, weight(6), NT))
    glu_b[...] = (value * gate * live).astype(BF)
    done1 = swap_edges(g, glu_b, low1, high1, h_send.at[0], h_recv.at[0], pad_glu)
    for at in range(0, width, LANES):
        lanes = pl.ds(at, LANES)
        total = jnp.zeros((rows, LANES), F32)
        for m in range(taps):
            total = total + taps_ref[m : m + 1, lanes] * pad_glu[pl.ds(HALO - rim + m, rows), lanes]
        c_ref[:, lanes] = total
    conv = c_ref[...]
    count = jnp.sum(live, axis=0, keepdims=True)
    mean = jnp.sum(live * conv, axis=0, keepdims=True) / jnp.maximum(count, 1.0)
    squares = jnp.sum(live * (conv - mean) * (conv - mean), axis=0, keepdims=True)
    moments = jnp.concatenate([jnp.broadcast_to(count, mean.shape), mean, squares, jnp.zeros((5, width), F32)], axis=0)
    moments, more = meet_levels(g, moments, merge_moments, buf1, m_send.at[0], m_recv.at[0])
    sends += more
    total_frames = moments[0:1]
    inv_std = lax.rsqrt(moments[2:3] / total_frames + BN_EPS)
    centre = moments[1:2]
    centred = c_ref[...] - centre
    zed = centred * inv_std
    bn_val = gains[12:13] * zed + gains[13:14]
    swish = (bn_val * sigmoid(bn_val)).astype(BF)
    sw_ref[...] = swish
    resid3 = resid2 + dot(swish, weight(7), NT)
    normed4 = norm_forward(resid3, gains, 3)
    a4_ref[...] = normed4
    loads[1].wait()
    loads[2].wait()
    resid4 = resid3 + 0.5 * module_forward(normed4, up, down, h4, s4_ref)
    y_ref[...] = norm_forward(resid4, gains, 4)
    grad4, gain4, shift4 = norm_backward(resid4, gains, 4, cot_ref[...].astype(F32))
    half4 = (0.5 * grad4).astype(BF)
    e4_ref[...] = half4
    grad_norm, gain3, shift3 = norm_backward(resid3, gains, 3, module_backward(half4, up, down, h4, gh4_ref))
    grad3 = grad4 + grad_norm
    e3 = grad3.astype(BF)
    e3_ref[...] = e3
    sigma = sigmoid(bn_val)
    grad_bn = dot(e3, weight(7), NN) * (sigma * (1.0 + bn_val * (1.0 - sigma)))
    gamma = jnp.sum(grad_bn * zed, axis=0, keepdims=True)
    beta = jnp.sum(grad_bn, axis=0, keepdims=True)
    grad_zed = grad_bn * gains[12:13]
    sum_one = jnp.sum(grad_zed, axis=0, keepdims=True)
    sum_two = jnp.sum(grad_zed * centred, axis=0, keepdims=True)
    sums = jnp.concatenate([sum_one, sum_two, jnp.zeros((6, width), F32)], axis=0)
    sums, more = meet_levels(g, sums, lambda x, y: x + y, buf2, m_send.at[1], m_recv.at[1])
    sends += more
    offset = inv_std * sums[0:1] + inv_std * inv_std * inv_std * sums[1:2] * centred
    gc_b[...] = (inv_std * grad_zed - live / total_frames * offset).astype(BF)
    done2 = swap_edges(g, gc_b, low2, high2, h_send.at[1], h_recv.at[1], pad_gc)
    for at in range(0, width, LANES):
        lanes = pl.ds(at, LANES)
        total = jnp.zeros((rows, LANES), F32)
        upstream = pad_gc[pl.ds(HALO, rows), lanes]
        for m in range(taps):
            total = total + taps_ref[m : m + 1, lanes] * pad_gc[pl.ds(HALO + rim - m, rows), lanes]
            gtaps_ref[m : m + 1, lanes] = jnp.sum(
                upstream * pad_glu[pl.ds(HALO - rim + m, rows), lanes], axis=0, keepdims=True
            )
        c_ref[:, lanes] = total
    grad_glu = c_ref[...] * live
    gv5 = (grad_glu * gate).astype(BF)
    gv6 = (grad_glu * value * gate * (1.0 - gate)).astype(BF)
    gpair_ref[0] = gv5
    gpair_ref[1] = gv6
    grad_norm, gain2, shift2 = norm_backward(
        resid2, gains, 2, dot(gv5, weight(5), NN) + dot(gv6, weight(6), NN)
    )
    grad2 = grad3 + grad_norm
    g2_ref[...] = grad2
    e2 = grad2.astype(BF)
    e2_ref[...] = e2
    grad_out = dot(e2, weight(4), NN).astype(BF)
    for q in range(nz):
        go_buf[q] = grad_out[:, q * cols : (q + 1) * cols]
    for k in range(1, nz):
        q = lax.rem(z + k, nz)
        copy = remote(go_buf.at[q], go_ref.at[pl.ds(z * rows, rows)], b_send.at[k], b_recv.at[z], g.device(q, g.a, g.b))
        copy.start()
        sends.append(copy)
    go_ref[pl.ds(pl.multiple_of(z * rows, rows), rows), :] = go_buf[z]
    small_ref[...] = jnp.concatenate([gain2, shift2, gain3, shift3, gain4, shift4, gamma, beta], axis=0)
    for k in range(1, nz):
        q = lax.rem(z + k, nz)
        arrived(go_ref.at[pl.ds(q * rows, rows)], b_recv.at[q])
    done1()
    done2()
    for copy in sends:
        copy.wait_send()


def middle(length, attended, resid1, cotangent, gains, taps, ud_full, sq_full):
    rows, width = resid1.shape
    nz, nf = lax.axis_size("seq"), lax.axis_size("fsdp")
    frames, cols = rows * nz, width // nz
    units = ud_full.shape[1] // 2
    most = max(nz, nf // 2)
    vmem = pl.BlockSpec(memory_space=pltpu.VMEM)
    hbm = pl.BlockSpec(memory_space=pl.ANY)
    shape = jax.ShapeDtypeStruct
    dma = pltpu.SemaphoreType.DMA
    row = shape((rows, width), BF)
    return pl.pallas_call(
        middle_kernel,
        name="middle",
        out_shape=(
            row,
            shape((rows, width), F32),
            shape((frames, cols), BF),
            row,
            row,
            row,
            shape((2, rows, width), BF),
            row,
            row,
            row,
            shape((rows, units), BF),
            shape((rows, units), BF),
            row,
            shape((8, width), F32),
            shape(taps.shape, F32),
        ),
        in_specs=[pl.BlockSpec(memory_space=pltpu.SMEM)] + [vmem] * 5 + [hbm] * 2,
        out_specs=[vmem] * 15,
        scratch_shapes=[
            pltpu.VMEM((units, width), BF),
            pltpu.VMEM((units, width), BF),
            pltpu.VMEM((4 * width, width), BF),
            pltpu.VMEM((nz, rows, cols), BF),
            pltpu.VMEM((nz, rows, cols), BF),
            pltpu.VMEM((rows, width), BF),
            pltpu.VMEM((rows, width), BF),
        ]
        + [pltpu.VMEM((HALO, width), BF)] * 4
        + [
            pltpu.VMEM((rows + 2 * HALO, width), F32),
            pltpu.VMEM((rows + 2 * HALO, width), F32),
            pltpu.VMEM((rows, units), F32),
            pltpu.VMEM((rows, width), F32),
            pltpu.VMEM((4, most, 8, width), F32),
            pltpu.VMEM((4, most, 8, width), F32),
            dma((3,)),
            dma((nz,)),
            dma((nz,)),
            dma((nz,)),
            dma((nz,)),
            dma((2, 2)),
            dma((2, 2)),
            dma((2, 4, most)),
            dma((2, 4, most)),
        ],
        compiler_params=pltpu.CompilerParams(
            collective_id=6, has_side_effects=True, vmem_limit_bytes=56 * 1024 * 1024
        ),
    )(length.reshape(1), attended, resid1, cotangent, gains, taps, ud_full, sq_full)


def gather_kernel(ud_own, sq_own, sm_own, ud_full, sq_full, sm_full, local_sem, swap_send, swap_recv, recv_sem, sib_recv, send_sem):
    g = Grid()
    half = ud_own.shape[1]
    c = g.core
    me = g.chip(g.z, g.a, g.b)
    local = [
        pltpu.make_async_copy(ud_own.at[c], ud_full.at[c, pl.ds(me * 2 * half + c * half, half)], local_sem.at[0]),
        pltpu.make_async_copy(sq_own, sq_full.at[me, c], local_sem.at[1]),
        pltpu.make_async_copy(sm_own, sm_full.at[me, c], local_sem.at[2]),
    ]
    for copy in local:
        copy.start()
    greet(g)
    swap = pltpu.make_async_remote_copy(
        src_ref=ud_own.at[1 - c],
        dst_ref=ud_full.at[1 - c, pl.ds(me * 2 * half + c * half, half)],
        send_sem=swap_send,
        recv_sem=swap_recv,
        device_id=g.sibling(),
        device_id_type=MESH,
    )
    swap.start()

    def pieces(t):
        return (ud_full.at[c, pl.ds(t * 2 * half, 2 * half)], sq_full.at[t, c], sm_full.at[t, c])

    ways = {"z+": 0, "z-": 1, "a+": 2, "a-": 3, "b+": 4, "b-": 5, "s": 6}

    def copies(t, way):
        if way == "s":
            target = g.sibling()
        else:
            target = g.up(way[0]) if way[1] == "+" else g.down(way[0])
        arrive = sib_recv if way == "s" else recv_sem
        return [
            pltpu.make_async_remote_copy(
                src_ref=ref,
                dst_ref=ref,
                send_sem=send_sem.at[ways[way], k, t],
                recv_sem=arrive.at[k, t],
                device_id=target,
                device_id_type=MESH,
            )
            for k, ref in enumerate(pieces(t))
        ]

    def send(t, way, finish=False):
        def act():
            for copy in copies(t, way):
                if finish:
                    copy.wait_send()
                else:
                    copy.start()

        if way == "s":
            act()
            return
        p, n = g.place(way[0])
        if n == 1:
            return
        pl.when(p < n - 1 if way[1] == "+" else p > 0)(act)

    def wait(t):
        for k, ref in enumerate(pieces(t)):
            pltpu.make_async_copy(ref, ref, recv_sem.at[k, t]).wait()

    def spread(finish):
        def got(t, ways_on):
            if not finish:
                wait(t)
            for way in ways_on:
                send(t, way, finish)

        if finish:
            pass
        else:
            for copy in local:
                copy.wait()
            swap.wait_recv()
        for way in ("z+", "z-", "a+", "a-", "b+", "b-", "s"):
            send(me, way, finish)
        for k in range(1, g.nz):
            pl.when(g.z >= k)(lambda: got(g.chip(g.z - k, g.a, g.b), ("z+", "a+", "a-", "b+", "b-", "s")))
            pl.when(g.z + k < g.nz)(lambda: got(g.chip(g.z + k, g.a, g.b), ("z-", "a+", "a-", "b+", "b-", "s")))

        def column(a, b, ways_on):
            got(g.chip(g.z, a, b), ways_on)
            for k in range(1, g.nz):
                pl.when(g.z >= k)(lambda: got(g.chip(g.z - k, a, b), ways_on))
                pl.when(g.z + k < g.nz)(lambda: got(g.chip(g.z + k, a, b), ways_on))

        for k in range(1, g.na):
            pl.when(g.a >= k)(lambda: column(g.a - k, g.b, ("a+", "b+", "b-", "s")))
            pl.when(g.a + k < g.na)(lambda: column(g.a + k, g.b, ("a-", "b+", "b-", "s")))
        for kb in range(1, g.nb):

            def plane(b, ways_on):
                column(g.a, b, ways_on)
                for k in range(1, g.na):
                    pl.when(g.a >= k)(lambda: column(g.a - k, b, ways_on))
                    pl.when(g.a + k < g.na)(lambda: column(g.a + k, b, ways_on))

            pl.when(g.b >= kb)(lambda: plane(g.b - kb, ("b+", "s")))
            pl.when(g.b + kb < g.nb)(lambda: plane(g.b + kb, ("b-", "s")))

    spread(False)
    d = 1 - c

    def other(t, _):
        for k, ref in enumerate((ud_full.at[d, pl.ds(t * 2 * half, 2 * half)], sq_full.at[t, d], sm_full.at[t, d])):
            pltpu.make_async_copy(ref, ref, sib_recv.at[k, t]).wait()
        return 0

    lax.fori_loop(0, g.chips, other, 0)
    swap.wait_send()
    spread(True)


def gather_weights(ud, sq, sm):
    devices = lax.axis_size("seq") * lax.axis_size("fsdp")
    chips = devices // 2
    _, rows, width = ud.shape
    hbm = pl.BlockSpec(memory_space=pl.ANY)
    vmem = pl.BlockSpec(memory_space=pltpu.VMEM)
    dma = pltpu.SemaphoreType.DMA
    return pl.pallas_call(
        gather_kernel,
        name="gather_weights",
        out_shape=(
            jax.ShapeDtypeStruct((2, devices * rows, width), ud.dtype),
            jax.ShapeDtypeStruct((chips, 2, rows, width), sq.dtype),
            jax.ShapeDtypeStruct((chips, 2) + sm.shape, sm.dtype),
        ),
        in_specs=[vmem] * 3,
        out_specs=[hbm] * 3,
        scratch_shapes=[
            dma((3,)),
            dma,
            dma,
            dma((3, chips)),
            dma((3, chips)),
            dma((7, 3, chips)),
        ],
        compiler_params=pltpu.CompilerParams(collective_id=1, has_side_effects=True),
    )(ud, sq, sm)


def scatter_kernel(ud_in, sq_in, sm_in, ud_out, sq_out, sm_out, acc, sib, rb, ra, rz, fin, send_ud,
                   local_sem, sib_send, sib_recv, b_send, b_recv, a_send, a_recv, z_send, z_recv, fin_send, fin_recv):
    g = Grid()
    c = g.core
    d = 1 - c
    nz, na, nb = g.nz, g.na, g.nb
    ud_rows = ud_out.shape[1]
    sq_rows = sq_out.shape[0]
    sm_rows = sm_out.shape[0]
    pair = 2 * ud_rows

    def slot(z, a, b):
        return (b * na + a) * nz + z

    def block_refs(buf, n):
        return (buf.at[n, pl.ds(0, pair)], buf.at[n, pl.ds(pair, sq_rows)], buf.at[n, pl.ds(pair + sq_rows, sm_rows)])

    def chip_refs(t, col):
        return (ud_in.at[col, pl.ds(t * pair, pair)], sq_in.at[t, col], sm_in.at[t, col])

    every = [(z, a, b) for b in range(nb) for a in range(na) for z in range(nz)]
    for z, a, b in every:
        n = slot(z, a, b)
        for k, (src, dst) in enumerate(zip(chip_refs(g.chip(z, a, b), c), block_refs(acc, n))):
            pltpu.make_async_copy(src, dst, local_sem.at[k, n]).start()
    greet(g)

    def sib_copies(z, a, b):
        n = slot(z, a, b)
        if g.na == g.nb:
            t = z * g.plane + (a * g.step_b + b * g.step_a) // 2
        else:
            t = g.chip(z, a, b)
        return [
            pltpu.make_async_remote_copy(
                src_ref=src,
                dst_ref=dst,
                send_sem=sib_send.at[k, n],
                recv_sem=sib_recv.at[k, n],
                device_id=g.sibling(),
                device_id_type=MESH,
            )
            for k, (src, dst) in enumerate(zip(chip_refs(t, d), block_refs(sib, n)))
        ]

    for z, a, b in every:
        for copy in sib_copies(z, a, b):
            copy.start()

    def add(n, ref):
        acc[n] = (acc[n].astype(F32) + ref[...].astype(F32)).astype(BF)

    def ready(z, a, b):
        n = slot(z, a, b)
        for k, (src, dst) in enumerate(zip(chip_refs(0, c), block_refs(acc, n))):
            pltpu.make_async_copy(src, dst, local_sem.at[k, n]).wait()
        for k, dst in enumerate(block_refs(sib, n)):
            pltpu.make_async_copy(dst, dst, sib_recv.at[k, n]).wait()
        add(n, sib.at[n])

    def travel(axis, n, m, buf, sends, recvs, upward):
        way = 0 if upward else 1
        return pltpu.make_async_remote_copy(
            src_ref=acc.at[n],
            dst_ref=buf.at[way, m],
            send_sem=sends.at[way, m],
            recv_sem=recvs.at[way, m],
            device_id=g.up(axis) if upward else g.down(axis),
            device_id_type=MESH,
        )

    def take(n, m, buf, recvs, way):
        pltpu.make_async_copy(buf.at[way, m], buf.at[way, m], recvs.at[way, m]).wait()
        add(n, buf.at[way, m])

    stages = {"b": (rb, b_send, b_recv), "a": (ra, a_send, a_recv), "z": (rz, z_send, z_recv)}

    def line(axis, blocks, prepare, finish):
        p, n_axis = g.place(axis)
        buf, sends, recvs = stages[axis]
        for k in range(n_axis - 1, 0, -1):
            for upward in (True, False):
                q = p + k if upward else p - k
                inside = p + k < n_axis if upward else p >= k
                behind = p > 0 if upward else p < n_axis - 1
                way = 0 if upward else 1

                def act():
                    for block in blocks(q):
                        n, m = block["slot"], block["m"]
                        if finish:
                            travel(axis, n, m, buf, sends, recvs, upward).wait_send()
                        else:
                            prepare(block)
                            pl.when(behind)(lambda: take(n, m, buf, recvs, way))
                            travel(axis, n, m, buf, sends, recvs, upward).start()

                pl.when(inside)(act)

    def settle(axis, block):
        p, n_axis = g.place(axis)
        buf, _, recvs = stages[axis]
        if n_axis > 1:
            pl.when(p > 0)(lambda: take(block["slot"], block["m"], buf, recvs, 0))
            pl.when(p < n_axis - 1)(lambda: take(block["slot"], block["m"], buf, recvs, 1))

    def z_order(a, b):
        return [(z, a, b) for z in range(nz)]

    def b_blocks(q):
        out = []
        for ka in list(range(1, na)) + [0]:
            a = lax.rem(g.a + ka, na)
            for z in range(nz):
                n = slot(z, a, q)
                out.append({"slot": n, "m": n, "at": (z, a, q)})
        return out

    def a_blocks(q):
        return [{"slot": slot(z, q, g.b), "m": q * nz + z, "at": (z, q, g.b)} for z in range(nz)]

    def z_blocks(q):
        return [{"slot": slot(q, g.a, g.b), "m": q, "at": (q, g.a, g.b)}]

    def along(block, axis):
        z, a, b = block["at"]
        if axis == "b":
            return {**block, "m": block["slot"]}
        return {**block, "m": a * nz + z}

    def from_b(block):
        ready(*block["at"])
        settle("b", along(block, "b"))

    def from_a(block):
        from_b(block)
        settle("a", along(block, "a"))

    line("b", b_blocks, lambda block: ready(*block["at"]), False)
    line("a", a_blocks, from_b, False)
    line("z", z_blocks, from_a, False)
    own = z_blocks(g.z)[0]
    from_a(own)
    settle("z", own)
    n = own["slot"]
    send_ud[...] = acc[n, pl.ds(pl.multiple_of(d * ud_rows, ud_rows), ud_rows), :].astype(F32)
    last = pltpu.make_async_remote_copy(
        src_ref=send_ud,
        dst_ref=fin,
        send_sem=fin_send,
        recv_sem=fin_recv,
        device_id=g.sibling(),
        device_id_type=MESH,
    )
    last.start()
    ud_out[c] = acc[n, pl.ds(pl.multiple_of(c * ud_rows, ud_rows), ud_rows), :].astype(F32)
    sq_out[...] = acc[n, pl.ds(pair, sq_rows), :].astype(F32)
    sm_out[...] = acc[n, pl.ds(pair + sq_rows, sm_rows), :].astype(F32)
    line("b", b_blocks, None, True)
    line("a", a_blocks, None, True)
    line("z", z_blocks, None, True)
    for z, a, b in every:
        for copy in sib_copies(z, a, b):
            copy.wait_send()
    last.wait()
    ud_out[d] = fin[...]


def scatter_grads(ud, sq, sm):
    nz, nf = lax.axis_size("seq"), lax.axis_size("fsdp")
    chips = nz * nf // 2
    width = ud.shape[2]
    rows = ud.shape[1] // (2 * chips)
    r = sm.shape[2]
    total = 3 * rows + r
    plane = nf // 2
    side = math.isqrt(plane)
    na, nb = (side, side) if side * side == plane else (plane, 1)
    hbm = pl.BlockSpec(memory_space=pl.ANY)
    vmem = pl.BlockSpec(memory_space=pltpu.VMEM)
    dma = pltpu.SemaphoreType.DMA
    return pl.pallas_call(
        scatter_kernel,
        name="scatter_grads",
        out_shape=(
            jax.ShapeDtypeStruct((2, rows, width), F32),
            jax.ShapeDtypeStruct((rows, width), F32),
            jax.ShapeDtypeStruct((r, width), F32),
        ),
        in_specs=[hbm] * 3,
        out_specs=[vmem] * 3,
        scratch_shapes=[
            pltpu.VMEM((chips, total, width), BF),
            pltpu.VMEM((chips, total, width), BF),
            pltpu.VMEM((2, chips, total, width), BF),
            pltpu.VMEM((2, na * nz, total, width), BF),
            pltpu.VMEM((2, nz, total, width), BF),
            pltpu.VMEM((rows, width), F32),
            pltpu.VMEM((rows, width), F32),
            dma((3, chips)),
            dma((3, chips)),
            dma((3, chips)),
            dma((2, chips)),
            dma((2, chips)),
            dma((2, na * nz)),
            dma((2, na * nz)),
            dma((2, nz)),
            dma((2, nz)),
            dma,
            dma,
        ],
        compiler_params=pltpu.CompilerParams(collective_id=2, has_side_effects=True, vmem_limit_bytes=60000 * 1024),
    )(ud, sq, sm)


def gathered(square, upward, downward, vectors, kernel):
    share = vectors.shape[1]
    small_rows = vectors.shape[0] + kernel.shape[0]
    small = jnp.concatenate([vectors, kernel], axis=0).astype(BF).reshape(-1)
    tall = -(-small.shape[0] // (16 * LANES)) * 16
    small = jnp.pad(small, (0, tall * LANES - small.shape[0])).reshape(tall, LANES)
    matrices, squares, smalls = gather_weights(
        jnp.stack([upward, downward]).astype(BF), square.astype(BF), small
    )
    devices = smalls.shape[0] * 2
    smalls = smalls.reshape(devices, tall * LANES)[:, : small_rows * share]
    smalls = smalls.reshape(devices, small_rows, share).transpose(1, 0, 2)
    smalls = smalls.reshape(small_rows, devices * share)
    split = vectors.shape[0]
    return (
        matrices,
        squares.reshape(devices * square.shape[0], square.shape[1]),
        smalls[:split],
        smalls[split:],
    )


def scattered(square_full, upward_full, downward_full, vectors_full, taps_full):
    devices = lax.axis_size("seq") * lax.axis_size("fsdp")
    width = square_full.shape[1]
    small = jnp.concatenate([vectors_full, taps_full], axis=0)
    small_rows, split = small.shape[0], vectors_full.shape[0]
    share = small.shape[1] // devices
    small = small.reshape(small_rows, devices, share).transpose(1, 0, 2)
    count = small_rows * share
    tall = -(-count // (16 * width)) * 16
    small = jnp.pad(small.reshape(devices, count), ((0, 0), (0, tall * width - count)))
    matrices, squares, smalls = scatter_grads(
        jnp.stack([upward_full.astype(BF), downward_full.astype(BF)]),
        square_full.astype(BF).reshape(devices // 2, 2, -1, width),
        small.astype(BF).reshape(devices // 2, 2, tall, width),
    )
    smalls = smalls.reshape(-1)[:count].reshape(small_rows, share)
    return squares, matrices[0], matrices[1], smalls[:split], smalls[split:]


def per_device(
    inputs,
    cotangent,
    lengths,
    square,
    upward,
    downward,
    vectors,
    kernel,
    square_momentum,
    square_variance,
    upward_momentum,
    upward_variance,
    downward_momentum,
    downward_variance,
    vectors_momentum,
    vectors_variance,
    kernel_momentum,
    kernel_variance,
):
    model_width = inputs.shape[2]
    frame_count = inputs.shape[1]
    groups = lax.axis_size("seq")
    seq_place = lax.axis_index("seq")
    seq_frames = frame_count * groups
    head_cols = model_width // groups
    col_start = seq_place * head_cols
    head_size = D // H
    coarse, fine = position_tables(seq_frames, model_width)
    full_ud, full_sq, full_vec, full_kern = gathered(square, upward, downward, vectors, kernel)
    full_up, full_down = full_ud[0], full_ud[1]
    small_params = full_vec.astype(jnp.float32)
    conv_taps = full_kern.astype(jnp.float32)
    signal = inputs[0].astype(jnp.float32)
    resid1, normed1, hidden1, active1, normed2, heads, pos_heads = front(
        inputs[0], small_params, coarse, fine, full_ud, full_sq
    )
    query_head, key_head, value_head = heads[0], heads[1], heads[2]
    biases = lax.dynamic_slice_in_dim(small_params[10:12], col_start, head_cols, 1)
    attended, prob = attend_heads(
        query_head, key_head, value_head, pos_heads, biases, lengths[0], head_size
    )
    (
        layer_output, grad_res2, grad_out_head, out_time, grad_att_b, normed3, grad_pair, grad_conv_b, swish_b, normed4,
        active4, grad_hidden4, half4, small_grads, grad_taps,
    ) = middle(lengths, attended, resid1, cotangent[0], small_params, conv_taps, full_ud, full_sq)
    layer_output = layer_output[None]
    grad_gain2, grad_shift2, grad_gain3, grad_shift3, grad_gain4, grad_shift4, grad_gamma, grad_beta = (
        small_grads[k] for k in range(8)
    )
    grad_up4, grad_down4 = outer(grad_hidden4, normed4), outer(active4, half4)
    grad_point = outer(grad_conv_b, swish_b)
    grad_lin = jnp.concatenate([outer(grad_pair[0], normed3), outer(grad_pair[1], normed3)], axis=0)
    grad_outw = outer(grad_att_b, out_time)
    pos_table = (coarse[0][:, None] * fine[0][None] + coarse[1][:, None] * fine[1][None]).reshape(2 * seq_frames, model_width)
    pos_table = pos_table.astype(jnp.bfloat16)
    grad_query_b, grad_key_b, grad_value_b, grad_table, grad_biases = attend_heads_back(
        query_head, key_head, value_head, pos_heads, biases, prob, grad_out_head, head_size
    )
    grad_query_time, grad_key_time, grad_value_time = (
        lax.all_to_all(grad_query_b, "seq", split_axis=0, concat_axis=1, tiled=True),
        lax.all_to_all(grad_key_b, "seq", split_axis=0, concat_axis=1, tiled=True),
        lax.all_to_all(grad_value_b, "seq", split_axis=0, concat_axis=1, tiled=True),
    )
    grad_qkv = jnp.concatenate([grad_query_time, grad_key_time, grad_value_time], axis=1)
    grad_inw = outer(grad_qkv, normed2)
    grad_norm2 = jnp.dot(grad_qkv, full_sq[: 3 * model_width], preferred_element_type=jnp.float32)
    grad_pos_cols = jnp.dot(grad_table, pos_table, preferred_element_type=jnp.float32)
    grad_pos = lax.dynamic_update_slice_in_dim(
        jnp.zeros((model_width, model_width), jnp.float32), grad_pos_cols, col_start, 0
    )
    zero_row = jnp.zeros((model_width,), jnp.float32)
    grad_bias_u = lax.dynamic_update_slice_in_dim(
        zero_row, grad_biases[0], col_start, 0
    )
    grad_bias_v = lax.dynamic_update_slice_in_dim(
        zero_row, grad_biases[1], col_start, 0
    )
    grad_add, grad_gain1, grad_shift1 = norm_back(
        resid1, small_params[2], small_params[3], grad_norm2
    )
    grad_res1 = grad_res2 + grad_add
    grad_up1, grad_down1, grad_norm1 = ffn_back(
        normed1, hidden1, active1, full_up[:FF], full_down[:FF], 0.5 * grad_res1
    )
    grad_add, grad_gain0, grad_shift0 = norm_back(
        signal, small_params[0], small_params[1], grad_norm1
    )
    input_grad = (grad_res1 + grad_add)[None]
    square_full = jnp.concatenate([grad_inw, grad_pos, grad_outw, grad_lin, grad_point], axis=0)
    upward_full = jnp.concatenate([grad_up1, grad_up4], axis=0)
    downward_full = jnp.concatenate([grad_down1, grad_down4], axis=0)
    vectors_full = jnp.stack(
        [
            grad_gain0,
            grad_shift0,
            grad_gain1,
            grad_shift1,
            grad_gain2,
            grad_shift2,
            grad_gain3,
            grad_shift3,
            grad_gain4,
            grad_shift4,
            grad_bias_u,
            grad_bias_v,
            grad_gamma,
            grad_beta,
        ]
    )
    square_grad, upward_grad, downward_grad, vectors_grad, kernel_grad = scattered(
        square_full, upward_full, downward_full, vectors_full, grad_taps
    )
    square_next, momentum_square, variance_square = adam_step(
        square, square_grad, square_momentum, square_variance, DECAY_RATE
    )
    upward_next, momentum_upward, variance_upward = adam_step(
        upward, upward_grad, upward_momentum, upward_variance, DECAY_RATE
    )
    downward_next, momentum_downward, variance_downward = adam_step(
        downward, downward_grad, downward_momentum, downward_variance, DECAY_RATE
    )
    vectors_next, momentum_vectors, variance_vectors = adam_step(
        vectors, vectors_grad, vectors_momentum, vectors_variance, 0.0
    )
    kernel_next, momentum_kernel, variance_kernel = adam_step(
        kernel, kernel_grad, kernel_momentum, kernel_variance, DECAY_RATE
    )
    return (
        layer_output,
        input_grad,
        square_grad,
        upward_grad,
        downward_grad,
        vectors_grad,
        kernel_grad,
        square_next,
        upward_next,
        downward_next,
        vectors_next,
        kernel_next,
        momentum_square,
        variance_square,
        momentum_upward,
        variance_upward,
        momentum_downward,
        variance_downward,
        momentum_vectors,
        variance_vectors,
        momentum_kernel,
        variance_kernel,
    )


def solution(mesh):
    return jax.shard_map(
        per_device,
        mesh=mesh,
        in_specs=(
            P("fsdp", "seq", None),
            P("fsdp", "seq", None),
            P("fsdp"),
            P(("seq", "fsdp"), None),
            P(("seq", "fsdp"), None),
            P(("seq", "fsdp"), None),
            P(None, ("seq", "fsdp")),
            P(None, ("seq", "fsdp")),
            P(("seq", "fsdp"), None),
            P(("seq", "fsdp"), None),
            P(("seq", "fsdp"), None),
            P(("seq", "fsdp"), None),
            P(("seq", "fsdp"), None),
            P(("seq", "fsdp"), None),
            P(None, ("seq", "fsdp")),
            P(None, ("seq", "fsdp")),
            P(None, ("seq", "fsdp")),
            P(None, ("seq", "fsdp")),
        ),
        out_specs=(
            P("fsdp", "seq", None),
            P("fsdp", "seq", None),
            P(("seq", "fsdp"), None),
            P(("seq", "fsdp"), None),
            P(("seq", "fsdp"), None),
            P(None, ("seq", "fsdp")),
            P(None, ("seq", "fsdp")),
            P(("seq", "fsdp"), None),
            P(("seq", "fsdp"), None),
            P(("seq", "fsdp"), None),
            P(None, ("seq", "fsdp")),
            P(None, ("seq", "fsdp")),
            P(("seq", "fsdp"), None),
            P(("seq", "fsdp"), None),
            P(("seq", "fsdp"), None),
            P(("seq", "fsdp"), None),
            P(("seq", "fsdp"), None),
            P(("seq", "fsdp"), None),
            P(None, ("seq", "fsdp")),
            P(None, ("seq", "fsdp")),
            P(None, ("seq", "fsdp")),
            P(None, ("seq", "fsdp")),
        ),
        check_vma=False,
    )
```

```python
import math

import jax
import jax.numpy as jnp
from jax import lax
from jax.experimental import pallas as pl
from jax.experimental.pallas import tpu as pltpu
from jax.sharding import PartitionSpec as P

D = 512
H = 8
FF = 2048
ADAM_STEP = 4

LN_EPS = 1e-05
BN_EPS = 1e-05
BETA_ONE = 0.9
BETA_TWO = 0.98
ADAM_EPS = 1e-08
LEARN_RATE = 0.005
DECAY_RATE = 0.01


def position_tables(seq_frames, model_width):
    fine = math.gcd(2 * seq_frames, 64)
    column = jnp.arange(model_width)
    frequency = jnp.exp(-math.log(10000.0) * 2.0 * (column // 2).astype(jnp.float32) / model_width)
    coarse_at = (seq_frames - 1 - fine * jnp.arange(2 * seq_frames // fine)).astype(jnp.float32)
    coarse_phase = coarse_at[:, None] * frequency[None, :]
    fine_phase = jnp.arange(fine).astype(jnp.float32)[:, None] * frequency[None, :]
    even = (column % 2 == 0)[None, :]
    sine, cosine = jnp.sin(coarse_phase), jnp.cos(coarse_phase)
    with_cosine = jnp.where(even, sine, cosine)
    with_sine = jnp.where(even, -cosine, sine)
    return jnp.stack([with_cosine, with_sine]), jnp.stack([jnp.cos(fine_phase), jnp.sin(fine_phase)])


def adam_step(weight, gradient, first_mom, second_mom, decay):
    first_new = BETA_ONE * first_mom + (1.0 - BETA_ONE) * gradient
    second_new = BETA_TWO * second_mom + (1.0 - BETA_TWO) * gradient * gradient
    fix_one = 1.0 - BETA_ONE**ADAM_STEP
    fix_two = 1.0 - BETA_TWO**ADAM_STEP
    update = first_new / fix_one / (jnp.sqrt(second_new / fix_two) + ADAM_EPS)
    return (weight - LEARN_RATE * (update + decay * weight), first_new, second_new)


MESH = pl.DeviceIdType.MESH
BF = jnp.bfloat16
F32 = jnp.float32
LANES = 128


class Grid:
    def __init__(self):
        self.nz = lax.axis_size("seq")
        self.nf = lax.axis_size("fsdp")
        plane = self.nf // 2
        side = math.isqrt(plane)
        self.z = lax.axis_index("seq")
        f = lax.axis_index("fsdp")
        self.core = f % 2
        if side * side == plane:
            self.na = self.nb = side
            self.step_a = 2 + self.core * (2 * side - 2)
            self.step_b = 2 * side - self.core * (2 * side - 2)
        else:
            self.na, self.nb = plane, 1
            self.step_a, self.step_b = 2, self.nf
        self.f = f
        self.a = (f // self.step_a) % self.na
        self.b = (f // self.step_b) % self.nb
        self.plane = plane
        self.chips = plane * self.nz

    def chip(self, z, a, b):
        return z * self.plane + (a * self.step_a + b * self.step_b) // 2

    def device(self, z, a, b):
        return (z, a * self.step_a + b * self.step_b + self.core)

    def sibling(self):
        return (self.z, self.f + 1 - 2 * self.core)

    def up(self, axis):
        return self.device(self.z + (axis == "z"), self.a + (axis == "a"), self.b + (axis == "b"))

    def down(self, axis):
        return self.device(self.z - (axis == "z"), self.a - (axis == "a"), self.b - (axis == "b"))

    def line(self, axis):
        return {
            "c": (self.core, 2, lambda q: (self.z, self.f - self.core + q)),
            "a": (self.a, self.na, lambda q: self.device(self.z, q, self.b)),
            "b": (self.b, self.nb, lambda q: self.device(self.z, self.a, q)),
            "z": (self.z, self.nz, lambda q: self.device(q, self.a, self.b)),
        }[axis]

    def place(self, axis):
        return {"z": (self.z, self.nz), "a": (self.a, self.na), "b": (self.b, self.nb)}[axis]


def greet(g):
    barrier = pltpu.get_barrier_semaphore()
    pl.semaphore_signal(barrier, inc=1, device_id=g.sibling(), device_id_type=MESH)
    total = 1
    for axis in "zab":
        p, n = g.place(axis)
        if n == 1:
            continue

        @pl.when(p < n - 1)
        def _():
            pl.semaphore_signal(barrier, inc=1, device_id=g.up(axis), device_id_type=MESH)

        @pl.when(p > 0)
        def _():
            pl.semaphore_signal(barrier, inc=1, device_id=g.down(axis), device_id_type=MESH)

        total = total + 2 - (n - 1 - p == 0) - (p == 0)
    pl.semaphore_wait(barrier, total)


def merge_moments(first_op, second_op):
    count = first_op[0:1] + second_op[0:1]
    share = second_op[0:1] / jnp.maximum(count, 1.0)
    gap = second_op[1:2] - first_op[1:2]
    mean = first_op[1:2] + gap * share
    squares = first_op[2:3] + second_op[2:3] + gap * gap * (first_op[0:1] * share)
    return jnp.concatenate([count, mean, squares, first_op[3:]], axis=0)


NT = (((1,), (1,)), ((), ()))
TN = (((0,), (0,)), ((), ()))
NN = (((1,), (0,)), ((), ()))


def dot(first_op, second_op, dims):
    return lax.dot_general(first_op, second_op, dims, preferred_element_type=F32)


def keep_head(value, h, head_size):
    lane = lax.broadcasted_iota(jnp.int32, value.shape, 1)
    return jnp.where(lane // head_size == h, value, jnp.zeros_like(value))


def attend_kernel(head_size, len_ref, q_ref, k_ref, v_ref, pos_ref, bias_ref, o_ref, prob_ref):
    i = pl.program_id(0)
    rows, cols = q_ref.shape
    frames = k_ref.shape[0]
    width = rows + frames
    query = q_ref[...].astype(F32)
    content = (query + bias_ref[0:1, :]).astype(BF)
    positional = (query + bias_ref[1:2, :]).astype(BF)
    window = pos_ref[pl.ds(pl.multiple_of(frames - rows - i * rows, rows), width), :]
    live = lax.broadcasted_iota(jnp.int32, (rows, frames), 1) < len_ref[0]
    out = jnp.zeros((rows, cols), F32)
    for h in range(cols // head_size):
        direct = dot(keep_head(content, h, head_size), k_ref[...], NT)
        spread = dot(keep_head(positional, h, head_size), window, NT)
        shifted = pltpu.roll(spread, width - rows + 1, 1, stride=1, stride_axis=0)[:, :frames]
        score = jnp.where(live, (direct + shifted) * (1.0 / math.sqrt(head_size)), -1e30)
        top = jnp.max(score, axis=-1, keepdims=True)
        power = jnp.exp(score - top)
        prob = power * (1.0 / jnp.sum(power, axis=-1, keepdims=True))
        prob_b = prob.astype(BF)
        prob_ref[h] = prob_b
        out = out + keep_head(dot(prob_b, v_ref[...], NN), h, head_size)
    o_ref[...] = out.astype(BF)


def attend_heads(query, key, value, pos, biases, length, head_size, rows=256):
    frames, cols = query.shape
    rows = min(rows, frames)
    heads = cols // head_size
    full = lambda n: pl.BlockSpec((n, cols), lambda i: (0, 0))
    return pl.pallas_call(
        lambda *refs: attend_kernel(head_size, *refs),
        name="attend_heads",
        grid=(frames // rows,),
        in_specs=[
            pl.BlockSpec(memory_space=pltpu.SMEM),
            pl.BlockSpec((rows, cols), lambda i: (i, 0)),
            full(frames),
            full(frames),
            full(2 * frames),
            full(2),
        ],
        out_specs=[
            pl.BlockSpec((rows, cols), lambda i: (i, 0)),
            pl.BlockSpec((heads, rows, frames), lambda i: (0, i, 0)),
        ],
        out_shape=(
            jax.ShapeDtypeStruct((frames, cols), BF),
            jax.ShapeDtypeStruct((heads, frames, frames), BF),
        ),
        compiler_params=pltpu.CompilerParams(vmem_limit_bytes=48 * 1024 * 1024),
    )(length.reshape(1), query, key, value, pos, biases)


def attend_back_kernel(head_size, q_ref, k_ref, v_ref, pos_ref, bias_ref, prob_ref, go_ref,
                       gq_ref, gk_ref, gv_ref, gpos_ref, gbias_ref, gk_acc, gv_acc, gpos_acc):
    i = pl.program_id(0)
    rows, cols = q_ref.shape
    frames = k_ref.shape[0]
    width = rows + frames

    @pl.when(i == 0)
    def _():
        gk_acc[...] = jnp.zeros_like(gk_acc)
        gv_acc[...] = jnp.zeros_like(gv_acc)
        gpos_acc[...] = jnp.zeros_like(gpos_acc)
        gbias_ref[...] = jnp.zeros_like(gbias_ref)

    query = q_ref[...].astype(F32)
    content = (query + bias_ref[0:1, :]).astype(BF)
    positional = (query + bias_ref[1:2, :]).astype(BF)
    start = pl.multiple_of(frames - rows - i * rows, rows)
    window = pos_ref[pl.ds(start, width), :]
    down = lax.broadcasted_iota(jnp.int32, (rows, rows), 0)
    across = lax.broadcasted_iota(jnp.int32, (rows, rows), 1)
    turn = jnp.where(down + across == rows - 1, 1.0, 0.0).astype(BF)
    positional_turned = dot(turn, positional, NN).astype(BF)
    grad_content = jnp.zeros((rows, cols), F32)
    grad_position = jnp.zeros((rows, cols), F32)
    for h in range(cols // head_size):
        grad_out = keep_head(go_ref[...], h, head_size)
        prob_b = prob_ref[h]
        prob = prob_b.astype(F32)
        grad_prob = dot(grad_out, v_ref[...], NT)
        delta = jnp.sum(prob * grad_prob, axis=-1, keepdims=True)
        grad_score = prob * (grad_prob - delta) * (1.0 / math.sqrt(head_size))
        score_b = grad_score.astype(BF)
        grad_content = grad_content + keep_head(dot(score_b, k_ref[...], NN), h, head_size)
        gk_acc[...] += dot(keep_head(content, h, head_size), score_b, TN)
        gv_acc[...] += dot(grad_out, prob_b, TN)
        turned = dot(turn, score_b, NN)
        wide = jnp.concatenate([turned, jnp.zeros((rows, width - frames), F32)], axis=1)
        spread = pltpu.roll(wide, 0, 1, stride=1, stride_axis=0).astype(BF)
        grad_position = grad_position + keep_head(dot(spread, window, NN), h, head_size)
        gpos_acc[:, pl.ds(start, width)] += dot(keep_head(positional_turned, h, head_size), spread, TN)
    high = grad_position.astype(BF)
    low = (grad_position - high.astype(F32)).astype(BF)
    grad_position = dot(turn, high, NN) + dot(turn, low, NN)
    gq_ref[...] = (grad_content + grad_position).astype(BF)
    gbias_ref[0:1, :] += jnp.sum(grad_content, axis=0, keepdims=True)
    gbias_ref[1:2, :] += jnp.sum(grad_position, axis=0, keepdims=True)

    @pl.when(i == pl.num_programs(0) - 1)
    def _():
        gk_ref[...] = gk_acc[...].T.astype(BF)
        gv_ref[...] = gv_acc[...].T.astype(BF)
        gpos_ref[...] = gpos_acc[...].astype(BF)


def attend_heads_back(query, key, value, pos, biases, prob, grad_out, head_size, rows=256):
    frames, cols = query.shape
    rows = min(rows, frames)
    heads = cols // head_size
    full = lambda n: pl.BlockSpec((n, cols), lambda i: (0, 0))
    block = pl.BlockSpec((rows, cols), lambda i: (i, 0))
    return pl.pallas_call(
        lambda *refs: attend_back_kernel(head_size, *refs),
        name="attend_heads_back",
        grid=(frames // rows,),
        in_specs=[
            block,
            full(frames),
            full(frames),
            full(2 * frames),
            full(2),
            pl.BlockSpec((heads, rows, frames), lambda i: (0, i, 0)),
            block,
        ],
        out_specs=[
            block,
            full(frames),
            full(frames),
            pl.BlockSpec((cols, 2 * frames), lambda i: (0, 0)),
            full(2),
        ],
        out_shape=(
            jax.ShapeDtypeStruct((frames, cols), BF),
            jax.ShapeDtypeStruct((frames, cols), BF),
            jax.ShapeDtypeStruct((frames, cols), BF),
            jax.ShapeDtypeStruct((cols, 2 * frames), BF),
            jax.ShapeDtypeStruct((2, cols), F32),
        ),
        scratch_shapes=[
            pltpu.VMEM((cols, frames), F32),
            pltpu.VMEM((cols, frames), F32),
            pltpu.VMEM((cols, 2 * frames), F32),
        ],
        compiler_params=pltpu.CompilerParams(vmem_limit_bytes=48 * 1024 * 1024),
    )(query, key, value, pos, biases, prob, grad_out)

def normalize(value):
    mean = jnp.mean(value, axis=-1, keepdims=True)
    centred = value - mean
    spread = lax.rsqrt(jnp.mean(centred * centred, axis=-1, keepdims=True) + LN_EPS)
    return centred * spread, spread


def norm_forward(value, gains, k):
    unit, _ = normalize(value)
    return (unit * gains[2 * k : 2 * k + 1] + gains[2 * k + 1 : 2 * k + 2]).astype(BF)


def norm_backward(value, gains, k, upstream):
    unit, spread = normalize(value)
    inner = upstream * gains[2 * k : 2 * k + 1]
    along = jnp.mean(inner * unit, axis=-1, keepdims=True)
    grad = spread * (inner - jnp.mean(inner, axis=-1, keepdims=True) - unit * along)
    gain = jnp.sum(upstream * unit, axis=0, keepdims=True)
    return grad, gain, jnp.sum(upstream, axis=0, keepdims=True)


def sigmoid(value):
    return 1.0 / (1.0 + jnp.exp(-value))


def module_forward(normed, up_ref, down_ref, hidden_ref, active_ref):
    units, width = up_ref.shape
    step = min(512, units)

    def chunk(j, total):
        here = pl.ds(pl.multiple_of(j * step, step), step)
        hidden = dot(normed, up_ref[here, :], NT)
        active = (hidden * sigmoid(hidden)).astype(BF)
        hidden_ref[:, here] = hidden
        active_ref[:, here] = active
        return total + dot(active, down_ref[here, :], NN)

    return lax.fori_loop(0, units // step, chunk, jnp.zeros((normed.shape[0], width), F32))


def module_backward(upstream_b, up_ref, down_ref, hidden_ref, grad_ref):
    units, width = up_ref.shape
    step = min(512, units)

    def chunk(j, total):
        here = pl.ds(pl.multiple_of(j * step, step), step)
        hidden = hidden_ref[:, here]
        sigma = sigmoid(hidden)
        slope = sigma * (1.0 + hidden * (1.0 - sigma))
        grad = (dot(upstream_b, down_ref[here, :], NT) * slope).astype(BF)
        grad_ref[:, here] = grad
        return total + dot(grad, up_ref[here, :], NN)

    return lax.fori_loop(0, units // step, chunk, jnp.zeros((upstream_b.shape[0], width), F32))


def greet_lines(g, axes):
    barrier = pltpu.get_barrier_semaphore()
    total = 0
    for axis in axes:
        p, n, device = g.line(axis)
        for k in range(1, n):
            pl.semaphore_signal(barrier, inc=1, device_id=device(lax.rem(p + k, n)), device_id_type=MESH)
            total += 1
    pl.semaphore_wait(barrier, total)


def remote(src, dst, send, recv, device):
    return pltpu.make_async_remote_copy(
        src_ref=src, dst_ref=dst, send_sem=send, recv_sem=recv, device_id=device, device_id_type=MESH
    )


def arrived(ref, sem):
    pltpu.make_async_copy(ref, ref, sem).wait()


def front_kernel(x_ref, gains_ref, coarse_ref, fine_ref, ud_hbm, sq_hbm,
                 x1_ref, a1_ref, h1_ref, s1_ref, a2_ref, heads_ref, pos_ref,
                 up, down, wqkv, wpos, mine, load_sem, send_sem, recv_sem):
    g = Grid()
    z, nz = g.z, g.nz
    rows, width = x_ref.shape
    cols = width // nz
    units = up.shape[0]
    loads = [
        pltpu.make_async_copy(ud_hbm.at[0, pl.ds(0, units)], up, load_sem.at[0]),
        pltpu.make_async_copy(ud_hbm.at[1, pl.ds(0, units)], down, load_sem.at[1]),
        pltpu.make_async_copy(sq_hbm.at[pl.ds(0, 3 * width)], wqkv, load_sem.at[2]),
        pltpu.make_async_copy(sq_hbm.at[pl.ds(3 * width + z * cols, cols)], wpos, load_sem.at[3]),
    ]
    for load in loads:
        load.start()
    greet_lines(g, "z")
    gains = gains_ref[...]
    signal = x_ref[...].astype(F32)
    normed1 = norm_forward(signal, gains, 0)
    a1_ref[...] = normed1
    loads[0].wait()
    loads[1].wait()
    resid1 = signal + 0.5 * module_forward(normed1, up, down, h1_ref, s1_ref)
    x1_ref[...] = resid1
    normed2 = norm_forward(resid1, gains, 1)
    a2_ref[...] = normed2
    loads[2].wait()
    for k in range(3):
        out = dot(normed2, wqkv[pl.ds(k * width, width), :], NT).astype(BF)
        for q in range(nz):
            mine[q, k] = out[:, q * cols : (q + 1) * cols]
    sends = []
    for k in range(1, nz):
        q = lax.rem(z + k, nz)
        copy = remote(mine.at[q], heads_ref.at[:, pl.ds(z * rows, rows)], send_sem.at[k], recv_sem.at[z], g.device(q, g.a, g.b))
        copy.start()
        sends.append(copy)
    own = pl.ds(pl.multiple_of(z * rows, rows), rows)
    for k in range(3):
        heads_ref[k, own, :] = mine[z, k]
    loads[3].wait()
    fine = fine_ref.shape[1]
    weight = wpos[...]

    def position(i, _):
        table = coarse_ref[0, pl.ds(i, 1), :] * fine_ref[0] + coarse_ref[1, pl.ds(i, 1), :] * fine_ref[1]
        here = pl.ds(pl.multiple_of(i * fine, fine), fine)
        pos_ref[here, :] = dot(table.astype(BF), weight, NT).astype(BF)
        return 0

    lax.fori_loop(0, coarse_ref.shape[1], position, 0)
    for k in range(1, nz):
        q = lax.rem(z + k, nz)
        arrived(heads_ref.at[:, pl.ds(q * rows, rows)], recv_sem.at[q])
    for copy in sends:
        copy.wait_send()


def front(signal, gains, coarse, fine, ud_full, sq_full):
    rows, width = signal.shape
    nz = lax.axis_size("seq")
    frames, cols = rows * nz, width // nz
    units = ud_full.shape[1] // 2
    vmem = pl.BlockSpec(memory_space=pltpu.VMEM)
    hbm = pl.BlockSpec(memory_space=pl.ANY)
    shape = jax.ShapeDtypeStruct
    return pl.pallas_call(
        front_kernel,
        name="front",
        out_shape=(
            shape((rows, width), F32),
            shape((rows, width), BF),
            shape((rows, units), F32),
            shape((rows, units), BF),
            shape((rows, width), BF),
            shape((3, frames, cols), BF),
            shape((2 * frames, cols), BF),
        ),
        in_specs=[vmem, vmem, vmem, vmem, hbm, hbm],
        out_specs=[vmem] * 7,
        scratch_shapes=[
            pltpu.VMEM((units, width), BF),
            pltpu.VMEM((units, width), BF),
            pltpu.VMEM((3 * width, width), BF),
            pltpu.VMEM((cols, width), BF),
            pltpu.VMEM((nz, 3, rows, cols), BF),
            pltpu.SemaphoreType.DMA((4,)),
            pltpu.SemaphoreType.DMA((nz,)),
            pltpu.SemaphoreType.DMA((nz,)),
        ],
        compiler_params=pltpu.CompilerParams(
            collective_id=5, has_side_effects=True, vmem_limit_bytes=40 * 1024 * 1024
        ),
    )(signal, gains, coarse, fine, ud_full, sq_full)


def meet_levels(g, value, merge, buf, send_sem, recv_sem):
    sends = []
    for level, axis in enumerate("cabz"):
        p, n, device = g.line(axis)
        if n == 1:
            continue
        buf[level, p] = value
        for k in range(1, n):
            copy = remote(buf.at[level, p], buf.at[level, p], send_sem.at[level, k], recv_sem.at[level, p], device(lax.rem(p + k, n)))
            copy.start()
            sends.append(copy)
        for k in range(1, n):
            q = lax.rem(p + k, n)
            arrived(buf.at[level, q], recv_sem.at[level, q])
        value = buf[level, 0]
        for q in range(1, n):
            value = merge(value, buf[level, q])
    return value, sends


HALO = 16


def swap_edges(g, body, low, high, send_sem, recv_sem, pad):
    rows = body.shape[0]
    p, n = g.z, g.nz
    up = remote(body.at[pl.ds(rows - HALO, HALO)], low, send_sem.at[0], recv_sem.at[0], g.device(g.z + 1, g.a, g.b))
    down = remote(body.at[pl.ds(0, HALO)], high, send_sem.at[1], recv_sem.at[1], g.device(g.z - 1, g.a, g.b))
    pl.when(p < n - 1)(lambda: up.start())
    pl.when(p > 0)(lambda: down.start())
    pad[pl.ds(HALO, rows), :] = body[...].astype(F32)

    def fill(at, ref, sem, there):
        @pl.when(there)
        def _():
            arrived(ref, sem)
            pad[pl.ds(at, HALO), :] = ref[...].astype(F32)

        @pl.when(jnp.logical_not(there))
        def _():
            pad[pl.ds(at, HALO), :] = jnp.zeros((HALO, pad.shape[1]), F32)

    fill(0, low, recv_sem.at[0], p > 0)
    fill(HALO + rows, high, recv_sem.at[1], p < n - 1)

    def finish():
        pl.when(p < n - 1)(lambda: up.wait_send())
        pl.when(p > 0)(lambda: down.wait_send())

    return finish


def middle_kernel(len_ref, att_ref, x1_ref, cot_ref, gains_ref, taps_ref, ud_hbm, sq_hbm,
                  y_ref, g2_ref, go_ref, o_ref, e2_ref, a3_ref, gpair_ref, e3_ref, sw_ref, a4_ref, s4_ref, gh4_ref, e4_ref,
                  small_ref, gtaps_ref,
                  up, down, wsq, o_buf, go_buf, glu_b, gc_b, low1, high1, low2, high2, pad_glu, pad_gc, h4, c_ref,
                  buf1, buf2, load_sem, a_send, a_recv, b_send, b_recv, h_send, h_recv, m_send, m_recv):
    g = Grid()
    z, nz = g.z, g.nz
    rows, width = x1_ref.shape
    cols = width // nz
    units = up.shape[0]
    taps = taps_ref.shape[0]
    rim = (taps - 1) // 2
    loads = [
        pltpu.make_async_copy(sq_hbm.at[pl.ds(4 * width, 4 * width)], wsq, load_sem.at[0]),
        pltpu.make_async_copy(ud_hbm.at[0, pl.ds(units, units)], up, load_sem.at[1]),
        pltpu.make_async_copy(ud_hbm.at[1, pl.ds(units, units)], down, load_sem.at[2]),
    ]
    for load in loads:
        load.start()
    greet_lines(g, "cabz")
    sends = []
    for k in range(1, nz):
        q = lax.rem(z + k, nz)
        copy = remote(att_ref.at[pl.ds(q * rows, rows)], o_buf.at[z], a_send.at[k], a_recv.at[z], g.device(q, g.a, g.b))
        copy.start()
        sends.append(copy)
    o_buf[z] = att_ref[pl.ds(pl.multiple_of(z * rows, rows), rows), :]
    gains = gains_ref[...]
    frame = z * rows + lax.broadcasted_iota(jnp.int32, (rows, 1), 0)
    live = jnp.where(frame < len_ref[0], 1.0, 0.0)
    loads[0].wait()
    weight = lambda k: wsq[pl.ds((k - 4) * width, width), :]
    for k in range(1, nz):
        q = lax.rem(z + k, nz)
        arrived(o_buf.at[q], a_recv.at[q])
    out = jnp.concatenate([o_buf[q] for q in range(nz)], axis=1)
    o_ref[...] = out
    resid2 = x1_ref[...] + dot(out, weight(4), NT)
    normed3 = norm_forward(resid2, gains, 2)
    a3_ref[...] = normed3
    value = dot(normed3, weight(5), NT)
    gate = sigmoid(dot(normed3, weight(6), NT))
    glu_b[...] = (value * gate * live).astype(BF)
    done1 = swap_edges(g, glu_b, low1, high1, h_send.at[0], h_recv.at[0], pad_glu)
    for at in range(0, width, LANES):
        lanes = pl.ds(at, LANES)
        total = jnp.zeros((rows, LANES), F32)
        for m in range(taps):
            total = total + taps_ref[m : m + 1, lanes] * pad_glu[pl.ds(HALO - rim + m, rows), lanes]
        c_ref[:, lanes] = total
    conv = c_ref[...]
    count = jnp.sum(live, axis=0, keepdims=True)
    mean = jnp.sum(live * conv, axis=0, keepdims=True) / jnp.maximum(count, 1.0)
    squares = jnp.sum(live * (conv - mean) * (conv - mean), axis=0, keepdims=True)
    moments = jnp.concatenate([jnp.broadcast_to(count, mean.shape), mean, squares, jnp.zeros((5, width), F32)], axis=0)
    moments, more = meet_levels(g, moments, merge_moments, buf1, m_send.at[0], m_recv.at[0])
    sends += more
    total_frames = moments[0:1]
    inv_std = lax.rsqrt(moments[2:3] / total_frames + BN_EPS)
    centre = moments[1:2]
    centred = c_ref[...] - centre
    zed = centred * inv_std
    bn_val = gains[12:13] * zed + gains[13:14]
    swish = (bn_val * sigmoid(bn_val)).astype(BF)
    sw_ref[...] = swish
    resid3 = resid2 + dot(swish, weight(7), NT)
    normed4 = norm_forward(resid3, gains, 3)
    a4_ref[...] = normed4
    loads[1].wait()
    loads[2].wait()
    resid4 = resid3 + 0.5 * module_forward(normed4, up, down, h4, s4_ref)
    y_ref[...] = norm_forward(resid4, gains, 4)
    grad4, gain4, shift4 = norm_backward(resid4, gains, 4, cot_ref[...].astype(F32))
    half4 = (0.5 * grad4).astype(BF)
    e4_ref[...] = half4
    grad_norm, gain3, shift3 = norm_backward(resid3, gains, 3, module_backward(half4, up, down, h4, gh4_ref))
    grad3 = grad4 + grad_norm
    e3 = grad3.astype(BF)
    e3_ref[...] = e3
    sigma = sigmoid(bn_val)
    grad_bn = dot(e3, weight(7), NN) * (sigma * (1.0 + bn_val * (1.0 - sigma)))
    gamma = jnp.sum(grad_bn * zed, axis=0, keepdims=True)
    beta = jnp.sum(grad_bn, axis=0, keepdims=True)
    grad_zed = grad_bn * gains[12:13]
    sum_one = jnp.sum(grad_zed, axis=0, keepdims=True)
    sum_two = jnp.sum(grad_zed * centred, axis=0, keepdims=True)
    sums = jnp.concatenate([sum_one, sum_two, jnp.zeros((6, width), F32)], axis=0)
    sums, more = meet_levels(g, sums, lambda x, y: x + y, buf2, m_send.at[1], m_recv.at[1])
    sends += more
    offset = inv_std * sums[0:1] + inv_std * inv_std * inv_std * sums[1:2] * centred
    gc_b[...] = (inv_std * grad_zed - live / total_frames * offset).astype(BF)
    done2 = swap_edges(g, gc_b, low2, high2, h_send.at[1], h_recv.at[1], pad_gc)
    for at in range(0, width, LANES):
        lanes = pl.ds(at, LANES)
        total = jnp.zeros((rows, LANES), F32)
        upstream = pad_gc[pl.ds(HALO, rows), lanes]
        for m in range(taps):
            total = total + taps_ref[m : m + 1, lanes] * pad_gc[pl.ds(HALO + rim - m, rows), lanes]
            gtaps_ref[m : m + 1, lanes] = jnp.sum(
                upstream * pad_glu[pl.ds(HALO - rim + m, rows), lanes], axis=0, keepdims=True
            )
        c_ref[:, lanes] = total
    grad_glu = c_ref[...] * live
    gv5 = (grad_glu * gate).astype(BF)
    gv6 = (grad_glu * value * gate * (1.0 - gate)).astype(BF)
    gpair_ref[0] = gv5
    gpair_ref[1] = gv6
    grad_norm, gain2, shift2 = norm_backward(
        resid2, gains, 2, dot(gv5, weight(5), NN) + dot(gv6, weight(6), NN)
    )
    grad2 = grad3 + grad_norm
    g2_ref[...] = grad2
    e2 = grad2.astype(BF)
    e2_ref[...] = e2
    grad_out = dot(e2, weight(4), NN).astype(BF)
    for q in range(nz):
        go_buf[q] = grad_out[:, q * cols : (q + 1) * cols]
    for k in range(1, nz):
        q = lax.rem(z + k, nz)
        copy = remote(go_buf.at[q], go_ref.at[pl.ds(z * rows, rows)], b_send.at[k], b_recv.at[z], g.device(q, g.a, g.b))
        copy.start()
        sends.append(copy)
    go_ref[pl.ds(pl.multiple_of(z * rows, rows), rows), :] = go_buf[z]
    small_ref[...] = jnp.concatenate([gain2, shift2, gain3, shift3, gain4, shift4, gamma, beta], axis=0)
    for k in range(1, nz):
        q = lax.rem(z + k, nz)
        arrived(go_ref.at[pl.ds(q * rows, rows)], b_recv.at[q])
    done1()
    done2()
    for copy in sends:
        copy.wait_send()


def middle(length, attended, resid1, cotangent, gains, taps, ud_full, sq_full):
    rows, width = resid1.shape
    nz, nf = lax.axis_size("seq"), lax.axis_size("fsdp")
    frames, cols = rows * nz, width // nz
    units = ud_full.shape[1] // 2
    most = max(nz, nf // 2)
    vmem = pl.BlockSpec(memory_space=pltpu.VMEM)
    hbm = pl.BlockSpec(memory_space=pl.ANY)
    shape = jax.ShapeDtypeStruct
    dma = pltpu.SemaphoreType.DMA
    row = shape((rows, width), BF)
    return pl.pallas_call(
        middle_kernel,
        name="middle",
        out_shape=(
            row,
            shape((rows, width), F32),
            shape((frames, cols), BF),
            row,
            row,
            row,
            shape((2, rows, width), BF),
            row,
            row,
            row,
            shape((rows, units), BF),
            shape((rows, units), BF),
            row,
            shape((8, width), F32),
            shape(taps.shape, F32),
        ),
        in_specs=[pl.BlockSpec(memory_space=pltpu.SMEM)] + [vmem] * 5 + [hbm] * 2,
        out_specs=[vmem] * 15,
        scratch_shapes=[
            pltpu.VMEM((units, width), BF),
            pltpu.VMEM((units, width), BF),
            pltpu.VMEM((4 * width, width), BF),
            pltpu.VMEM((nz, rows, cols), BF),
            pltpu.VMEM((nz, rows, cols), BF),
            pltpu.VMEM((rows, width), BF),
            pltpu.VMEM((rows, width), BF),
        ]
        + [pltpu.VMEM((HALO, width), BF)] * 4
        + [
            pltpu.VMEM((rows + 2 * HALO, width), F32),
            pltpu.VMEM((rows + 2 * HALO, width), F32),
            pltpu.VMEM((rows, units), F32),
            pltpu.VMEM((rows, width), F32),
            pltpu.VMEM((4, most, 8, width), F32),
            pltpu.VMEM((4, most, 8, width), F32),
            dma((3,)),
            dma((nz,)),
            dma((nz,)),
            dma((nz,)),
            dma((nz,)),
            dma((2, 2)),
            dma((2, 2)),
            dma((2, 4, most)),
            dma((2, 4, most)),
        ],
        compiler_params=pltpu.CompilerParams(
            collective_id=6, has_side_effects=True, vmem_limit_bytes=56 * 1024 * 1024
        ),
    )(length.reshape(1), attended, resid1, cotangent, gains, taps, ud_full, sq_full)


def gather_kernel(ud_own, sq_own, sm_own, ud_full, sq_full, sm_full, local_sem, swap_send, swap_recv, recv_sem, sib_recv, send_sem):
    g = Grid()
    half = ud_own.shape[1]
    c = g.core
    me = g.chip(g.z, g.a, g.b)
    local = [
        pltpu.make_async_copy(ud_own.at[c], ud_full.at[c, pl.ds(me * 2 * half + c * half, half)], local_sem.at[0]),
        pltpu.make_async_copy(sq_own, sq_full.at[me, c], local_sem.at[1]),
        pltpu.make_async_copy(sm_own, sm_full.at[me, c], local_sem.at[2]),
    ]
    for copy in local:
        copy.start()
    greet(g)
    swap = pltpu.make_async_remote_copy(
        src_ref=ud_own.at[1 - c],
        dst_ref=ud_full.at[1 - c, pl.ds(me * 2 * half + c * half, half)],
        send_sem=swap_send,
        recv_sem=swap_recv,
        device_id=g.sibling(),
        device_id_type=MESH,
    )
    swap.start()

    def pieces(t):
        return (ud_full.at[c, pl.ds(t * 2 * half, 2 * half)], sq_full.at[t, c], sm_full.at[t, c])

    ways = {"z+": 0, "z-": 1, "a+": 2, "a-": 3, "b+": 4, "b-": 5, "s": 6}

    def copies(t, way):
        if way == "s":
            target = g.sibling()
        else:
            target = g.up(way[0]) if way[1] == "+" else g.down(way[0])
        arrive = sib_recv if way == "s" else recv_sem
        return [
            pltpu.make_async_remote_copy(
                src_ref=ref,
                dst_ref=ref,
                send_sem=send_sem.at[ways[way], k, t],
                recv_sem=arrive.at[k, t],
                device_id=target,
                device_id_type=MESH,
            )
            for k, ref in enumerate(pieces(t))
        ]

    def send(t, way, finish=False):
        def act():
            for copy in copies(t, way):
                if finish:
                    copy.wait_send()
                else:
                    copy.start()

        if way == "s":
            act()
            return
        p, n = g.place(way[0])
        if n == 1:
            return
        pl.when(p < n - 1 if way[1] == "+" else p > 0)(act)

    def wait(t):
        for k, ref in enumerate(pieces(t)):
            pltpu.make_async_copy(ref, ref, recv_sem.at[k, t]).wait()

    def spread(finish):
        def got(t, ways_on):
            if not finish:
                wait(t)
            for way in ways_on:
                send(t, way, finish)

        if finish:
            pass
        else:
            for copy in local:
                copy.wait()
            swap.wait_recv()
        for way in ("z+", "z-", "a+", "a-", "b+", "b-", "s"):
            send(me, way, finish)
        for k in range(1, g.nz):
            pl.when(g.z >= k)(lambda: got(g.chip(g.z - k, g.a, g.b), ("z+", "a+", "a-", "b+", "b-", "s")))
            pl.when(g.z + k < g.nz)(lambda: got(g.chip(g.z + k, g.a, g.b), ("z-", "a+", "a-", "b+", "b-", "s")))

        def column(a, b, ways_on):
            got(g.chip(g.z, a, b), ways_on)
            for k in range(1, g.nz):
                pl.when(g.z >= k)(lambda: got(g.chip(g.z - k, a, b), ways_on))
                pl.when(g.z + k < g.nz)(lambda: got(g.chip(g.z + k, a, b), ways_on))

        for k in range(1, g.na):
            pl.when(g.a >= k)(lambda: column(g.a - k, g.b, ("a+", "b+", "b-", "s")))
            pl.when(g.a + k < g.na)(lambda: column(g.a + k, g.b, ("a-", "b+", "b-", "s")))
        for kb in range(1, g.nb):

            def plane(b, ways_on):
                column(g.a, b, ways_on)
                for k in range(1, g.na):
                    pl.when(g.a >= k)(lambda: column(g.a - k, b, ways_on))
                    pl.when(g.a + k < g.na)(lambda: column(g.a + k, b, ways_on))

            pl.when(g.b >= kb)(lambda: plane(g.b - kb, ("b+", "s")))
            pl.when(g.b + kb < g.nb)(lambda: plane(g.b + kb, ("b-", "s")))

    spread(False)
    d = 1 - c

    def other(t, _):
        for k, ref in enumerate((ud_full.at[d, pl.ds(t * 2 * half, 2 * half)], sq_full.at[t, d], sm_full.at[t, d])):
            pltpu.make_async_copy(ref, ref, sib_recv.at[k, t]).wait()
        return 0

    lax.fori_loop(0, g.chips, other, 0)
    swap.wait_send()
    spread(True)


def gather_weights(ud, sq, sm):
    devices = lax.axis_size("seq") * lax.axis_size("fsdp")
    chips = devices // 2
    _, rows, width = ud.shape
    hbm = pl.BlockSpec(memory_space=pl.ANY)
    vmem = pl.BlockSpec(memory_space=pltpu.VMEM)
    dma = pltpu.SemaphoreType.DMA
    return pl.pallas_call(
        gather_kernel,
        name="gather_weights",
        out_shape=(
            jax.ShapeDtypeStruct((2, devices * rows, width), ud.dtype),
            jax.ShapeDtypeStruct((chips, 2, rows, width), sq.dtype),
            jax.ShapeDtypeStruct((chips, 2) + sm.shape, sm.dtype),
        ),
        in_specs=[vmem] * 3,
        out_specs=[hbm] * 3,
        scratch_shapes=[
            dma((3,)),
            dma,
            dma,
            dma((3, chips)),
            dma((3, chips)),
            dma((7, 3, chips)),
        ],
        compiler_params=pltpu.CompilerParams(collective_id=1, has_side_effects=True),
    )(ud, sq, sm)


class Meeting:
    def __init__(self, g, buf, send_sem, recv_sem):
        self.g, self.buf, self.send_sem, self.recv_sem = g, buf, send_sem, recv_sem
        self.sends = []

    def start(self, level, value):
        axis = "cabz"[level]
        p, n, device = self.g.line(axis)
        self.buf[level, p] = value
        for k in range(1, n):
            here = self.buf.at[level, p]
            copy = remote(here, here, self.send_sem.at[level, k], self.recv_sem.at[level, p], device(lax.rem(p + k, n)))
            copy.start()
            self.sends.append(copy)

    def total(self, level):
        p, n, _ = self.g.line("cabz"[level])
        for k in range(1, n):
            q = lax.rem(p + k, n)
            arrived(self.buf.at[level, q], self.recv_sem.at[level, q])
        value = self.buf[level, 0]
        for q in range(1, n):
            value = value + self.buf[level, q]
        return value


class Reduction:
    def __init__(self, g, gud, gsq, sib_ud, sib_sq, sib_sem, rb, ra, rz, sems):
        self.g, self.gud, self.gsq, self.sib_ud, self.sib_sq = g, gud, gsq, sib_ud, sib_sq
        self.sib_send, self.sib_recv = sib_sem
        self.bufs = {"b": rb, "a": ra, "z": rz}
        self.sems = sems
        self.sq_rows = gsq.shape[2]
        self.pair = 2 * self.sq_rows
        self.height = g.plane * self.pair

    def own(self, t):
        c = self.g.core
        return self.gud.at[c, pl.ds(pl.multiple_of(t * self.pair, self.pair), self.pair)], self.gsq.at[t, c]

    def sibling_copies(self, z):
        g = self.g
        d = 1 - g.core
        tall = pl.ds(z * self.height, self.height)
        chips = pl.ds(z * g.plane, g.plane)
        return (
            remote(self.gud.at[d, tall], self.sib_ud.at[tall], self.sib_send.at[0, z], self.sib_recv.at[0, z], g.sibling()),
            remote(self.gsq.at[chips, d], self.sib_sq.at[chips], self.sib_send.at[1, z], self.sib_recv.at[1, z], g.sibling()),
        )

    def to_sibling(self, z):
        for copy in self.sibling_copies(z):
            copy.start()

    def from_sibling(self, z):
        for copy in self.sibling_copies(z):
            copy.wait_recv()

    def add_sibling(self, t):
        ud, sq = self.own(t)
        ud[...] = ud[...] + self.sib_ud[pl.ds(pl.multiple_of(t * self.pair, self.pair), self.pair), :]
        sq[...] = sq[...] + self.sib_sq[t]

    def landing(self, axis, slot):
        buf = self.bufs[axis]
        return buf.at[slot, pl.ds(0, self.pair)], buf.at[slot, pl.ds(self.pair, self.sq_rows)]

    def slot(self, axis, upward, z, a, b):
        g = self.g
        up = 1 if upward else 0
        if axis == "b":
            return ((b + up) * g.na + a) * g.nz + z
        if axis == "a":
            return (a + up) * g.nz + z
        return z + up

    def hop(self, axis, upward, z, a, b):
        g = self.g
        slot = self.slot(axis, upward, z, a, b)
        sends, recvs = self.sems[axis]
        device = g.up(axis) if upward else g.down(axis)
        return [
            remote(src, dst, sends.at[k, slot], recvs.at[k, slot], device)
            for k, (src, dst) in enumerate(zip(self.own(g.chip(z, a, b)), self.landing(axis, slot)))
        ]

    def take(self, axis, upward, z, a, b):
        slot = self.slot(axis, upward, z, a, b)
        recvs = self.sems[axis][1]
        for k, (src, dst) in enumerate(zip(self.landing(axis, slot), self.own(self.g.chip(z, a, b)))):
            arrived(src, recvs.at[k, slot])
            dst[...] = dst[...] + src[...]

    def settle(self, axis, z, a, b):
        p, n = self.g.place(axis)
        if n > 1:
            pl.when(p > 0)(lambda: self.take(axis, True, z, a, b))
            pl.when(p < n - 1)(lambda: self.take(axis, False, z, a, b))

    def ready(self, axis, z, a, b):
        if axis == "b":
            self.add_sibling(self.g.chip(z, a, b))
        else:
            before = {"a": "b", "z": "a"}[axis]
            self.ready(before, z, a, b)
            self.settle(before, z, a, b)

    def pass_on(self, axis, upward, z, a, b, finish):
        p, n = self.g.place(axis)
        if finish:
            for copy in self.hop(axis, upward, z, a, b):
                copy.wait_send()
            return
        self.ready(axis, z, a, b)
        behind = p > 0 if upward else p < n - 1
        pl.when(behind)(lambda: self.take(axis, upward, z, a, b))
        for copy in self.hop(axis, upward, z, a, b):
            copy.start()

    def along(self, axis, planes, finish=False):
        g = self.g
        p, n = g.place(axis)
        if axis == "z":
            for q in planes:
                pl.when(p < q)(lambda: self.pass_on("z", True, q, g.a, g.b, finish))
                pl.when(p > q)(lambda: self.pass_on("z", False, q, g.a, g.b, finish))
            return
        step = planes[1] - planes[0] if len(planes) > 1 else 1
        count = len(planes)
        for k in range(n - 1, 0, -1):
            for upward in (True, False):
                q = p + k if upward else p - k

                def act():
                    if axis == "b":

                        def body(i, _):
                            a = lax.rem(g.a + 1 + i // count, g.na)
                            self.pass_on("b", upward, planes[0] + step * lax.rem(i, count), a, q, finish)
                            return 0

                        lax.fori_loop(0, g.na * count, body, 0)
                    else:

                        def body(i, _):
                            self.pass_on("a", upward, planes[0] + step * i, q, g.b, finish)
                            return 0

                        lax.fori_loop(0, count, body, 0)

                pl.when(p + k < n if upward else p >= k)(act)

    def last(self):
        g = self.g
        self.ready("z", g.z, g.a, g.b)
        self.settle("z", g.z, g.a, g.b)


def back_kernel(gq_ref, gk_ref, gv_ref, gpos_ref, gbias_ref, coarse_ref, fine_ref, gains_ref,
                x_ref, x1_ref, g2_ref, a1_ref, h1_ref, s1_ref, a2_ref,
                a4_ref, s4_ref, gh4_ref, e4_ref, o_ref, e2_ref, a3_ref, gpair_ref, e3_ref, sw_ref, some_ref, gtaps_ref,
                ud_hbm, sq_hbm,
                gx_ref, ud_out, sq_out, small_out,
                up, down, wqkv, heads, gqkv, gh1, small, gud, gsq, sib_ud, sib_sq, rb, ra, rz, sbuf, fin_send_buf, fin,
                load_sem, h_send, h_recv, sib_send, sib_recv, b_send, b_recv, a_send, a_recv, z_send, z_recv, s_send, s_recv,
                fin_send, fin_recv):
    g = Grid()
    z, nz, c = g.z, g.nz, g.core
    rows, width = x_ref.shape
    cols = width // nz
    units = up.shape[0]
    loads = [
        pltpu.make_async_copy(sq_hbm.at[pl.ds(0, 3 * width)], wqkv, load_sem.at[0]),
        pltpu.make_async_copy(ud_hbm.at[0, pl.ds(0, units)], up, load_sem.at[1]),
        pltpu.make_async_copy(ud_hbm.at[1, pl.ds(0, units)], down, load_sem.at[2]),
    ]
    for load in loads:
        load.start()
    greet_lines(g, "cabz")
    sends = []
    for k in range(1, nz):
        q = lax.rem(z + k, nz)
        for j, ref in enumerate((gq_ref, gk_ref, gv_ref)):
            copy = remote(ref.at[pl.ds(q * rows, rows)], heads.at[j, z], h_send.at[j, k], h_recv.at[j, z], g.device(q, g.a, g.b))
            copy.start()
            sends.append(copy)
    for j, ref in enumerate((gq_ref, gk_ref, gv_ref)):
        heads[j, z] = ref[pl.ds(pl.multiple_of(z * rows, rows), rows), :]
    red = Reduction(
        g, gud, gsq, sib_ud, sib_sq, (sib_send, sib_recv), rb, ra, rz,
        {"b": (b_send, b_recv), "a": (a_send, a_recv), "z": (z_send, z_recv)},
    )
    total_rows = gud.shape[1]
    sq_rows = gsq.shape[2]
    high = list(range(nz - 1, nz // 2 - 1, -1))
    low = list(range(0, nz // 2))
    part = 256

    def matrix_terms(color, left_ref, right, first_row, count):
        def body(i, _):
            here = pl.ds(pl.multiple_of(i * part, part), part)
            there = pl.ds(pl.multiple_of(first_row + i * part, part), part)
            gud[color, there, :] = dot(left_ref[:, here], right, TN).astype(BF)
            return 0

        lax.fori_loop(0, count // part, body, 0)

    per = width // sq_rows // 2

    def square_terms(block, left, right):
        sums = dot(left, right, TN).astype(BF).reshape(per, 2, sq_rows, width)
        gsq[pl.ds(block * per, per)] = sums

    matrix_terms(0, gh4_ref, a4_ref[...], units, units)
    matrix_terms(1, s4_ref, e4_ref[...], units, units)
    square_terms(7, e3_ref[...], sw_ref[...])
    square_terms(6, gpair_ref[1], a3_ref[...])
    square_terms(5, gpair_ref[0], a3_ref[...])
    square_terms(4, e2_ref[...], o_ref[...])
    for q in high:
        red.to_sibling(q)
    fine = fine_ref.shape[1]

    def position(i, total):
        table = coarse_ref[0, pl.ds(2 * i, 1), :] * fine_ref[0] + coarse_ref[1, pl.ds(2 * i, 1), :] * fine_ref[1]
        after = coarse_ref[0, pl.ds(2 * i + 1, 1), :] * fine_ref[0] + coarse_ref[1, pl.ds(2 * i + 1, 1), :] * fine_ref[1]
        both = jnp.concatenate([table, after], axis=0).astype(BF)
        return total + dot(gpos_ref[:, pl.ds(pl.multiple_of(i * 2 * fine, 2 * fine), 2 * fine)], both, NN)

    gpos = lax.fori_loop(0, coarse_ref.shape[1] // 2, position, jnp.zeros((cols, width), F32)).astype(BF)
    gsq[pl.ds(3 * per, per)] = jnp.zeros((per, 2, sq_rows, width), BF)
    pieces = cols // sq_rows
    for i in range(pieces):
        piece = z * pieces + i
        gsq[3 * per + piece // 2, piece % 2] = gpos[i * sq_rows : (i + 1) * sq_rows]
    for q in high:
        red.from_sibling(q)
    red.along("b", high)
    gains = gains_ref[...]
    loads[0].wait()
    grad_norm = jnp.zeros((rows, width), F32)
    for j in range(3):
        for k in range(1, nz):
            q = lax.rem(z + k, nz)
            arrived(heads.at[j, q], h_recv.at[j, q])
        full = jnp.concatenate([heads[j, q] for q in range(nz)], axis=1)
        gqkv[j] = full
        grad_norm = grad_norm + dot(full, wqkv[pl.ds(j * width, width), :], NN)
    resid1 = x1_ref[...]
    grad_add, gain1, shift1 = norm_backward(resid1, gains, 1, grad_norm)
    grad1 = g2_ref[...] + grad_add
    half1 = (0.5 * grad1).astype(BF)
    loads[1].wait()
    loads[2].wait()
    grad_norm = module_backward(half1, up, down, h1_ref, gh1)
    matrix_terms(0, gh1, a1_ref[...], 0, units)
    matrix_terms(1, s1_ref, half1, 0, units)
    for j in range(3):
        square_terms(j, gqkv[j], a2_ref[...])
    for q in low:
        red.to_sibling(q)
    red.along("a", high)
    grad_add, gain0, shift0 = norm_backward(x_ref[...].astype(F32), gains, 0, grad_norm)
    gx_ref[...] = grad1 + grad_add
    small[...] = jnp.zeros_like(small)
    small[0:1, :] = gain0
    small[1:2, :] = shift0
    small[2:3, :] = gain1
    small[3:4, :] = shift1
    small[4:10, :] = some_ref[0:6, :]
    small[10:12, pl.ds(pl.multiple_of(z * cols, cols), cols)] = gbias_ref[...]
    small[12:14, :] = some_ref[6:8, :]
    small[14 : 14 + gtaps_ref.shape[0], :] = gtaps_ref[...]
    meeting = Meeting(g, sbuf, s_send, s_recv)
    meeting.start(0, small[...])
    for q in low:
        red.from_sibling(q)
    red.along("b", low)
    meeting.start(1, meeting.total(0))
    red.along("z", high)
    meeting.start(2, meeting.total(1))
    red.along("a", low)
    meeting.start(3, meeting.total(2))
    red.along("z", low)
    red.last()
    me = g.chip(g.z, g.a, g.b)
    d = 1 - c
    half = ud_out.shape[1]
    at = lambda k: pl.ds(pl.multiple_of(me * 2 * half + k * half, half), half)
    fin_send_buf[...] = gud[c, at(d), :]
    swap = remote(fin_send_buf, fin, fin_send, fin_recv, g.sibling())
    swap.start()
    ud_out[c] = gud[c, at(c), :].astype(F32)
    sq_out[...] = gsq[me, c].astype(F32)
    small_out[...] = meeting.total(3)
    for planes in (high, low):
        for axis in "baz":
            red.along(axis, planes, True)
        for q in planes:
            for copy in red.sibling_copies(q):
                copy.wait_send()
    for copy in sends + meeting.sends:
        copy.wait_send()
    swap.wait()
    ud_out[d] = fin[...].astype(F32)


def back(head_grads, gpos, gbias, coarse, fine, gains, signal, resid1, grad2, first, second, squares, some, gtaps, ud_full, sq_full):
    rows, width = signal.shape
    nz, nf = lax.axis_size("seq"), lax.axis_size("fsdp")
    chips = nz * nf // 2
    plane = nf // 2
    side = math.isqrt(plane)
    na, nb = (side, side) if side * side == plane else (plane, 1)
    cols = width // nz
    units = ud_full.shape[1] // 2
    own = ud_full.shape[1] // (2 * chips)
    block = 3 * own
    most = max(nz, na, nb, 2)
    tall = -(-(14 + gtaps.shape[0]) // 8) * 8
    vmem = pl.BlockSpec(memory_space=pltpu.VMEM)
    hbm = pl.BlockSpec(memory_space=pl.ANY)
    shape = jax.ShapeDtypeStruct
    dma = pltpu.SemaphoreType.DMA
    operands = (*head_grads, gpos, gbias, coarse, fine, gains, signal, resid1, grad2, *first, *second, *squares, some, gtaps)
    slots = {"b": (nb + 1) * na * nz, "a": (na + 1) * nz, "z": nz + 1}
    return pl.pallas_call(
        back_kernel,
        name="back",
        out_shape=(
            shape((rows, width), F32),
            shape((2, own, width), F32),
            shape((own, width), F32),
            shape((tall, width), F32),
        ),
        in_specs=[vmem] * len(operands) + [hbm] * 2,
        out_specs=[vmem] * 4,
        scratch_shapes=[
            pltpu.VMEM((units, width), BF),
            pltpu.VMEM((units, width), BF),
            pltpu.VMEM((3 * width, width), BF),
            pltpu.VMEM((3, nz, rows, cols), BF),
            pltpu.VMEM((3, rows, width), BF),
            pltpu.VMEM((rows, units), BF),
            pltpu.VMEM((tall, width), F32),
            pltpu.VMEM((2, 2 * units, width), BF),
            pltpu.VMEM((chips, 2, own, width), BF),
            pltpu.VMEM((2 * units, width), BF),
            pltpu.VMEM((chips, own, width), BF),
            pltpu.VMEM((slots["b"], block, width), BF),
            pltpu.VMEM((slots["a"], block, width), BF),
            pltpu.VMEM((slots["z"], block, width), BF),
            pltpu.VMEM((4, most, tall, width), F32),
            pltpu.VMEM((own, width), BF),
            pltpu.VMEM((own, width), BF),
            dma((3,)),
            dma((3, nz)),
            dma((3, nz)),
            dma((2, nz)),
            dma((2, nz)),
            dma((2, slots["b"])),
            dma((2, slots["b"])),
            dma((2, slots["a"])),
            dma((2, slots["a"])),
            dma((2, slots["z"])),
            dma((2, slots["z"])),
            dma((4, most)),
            dma((4, most)),
            dma,
            dma,
        ],
        compiler_params=pltpu.CompilerParams(
            collective_id=7, has_side_effects=True, vmem_limit_bytes=61000 * 1024
        ),
    )(*operands, ud_full, sq_full)


def gathered(square, upward, downward, vectors, kernel):
    share = vectors.shape[1]
    small_rows = vectors.shape[0] + kernel.shape[0]
    small = jnp.concatenate([vectors, kernel], axis=0).astype(BF).reshape(-1)
    tall = -(-small.shape[0] // (16 * LANES)) * 16
    small = jnp.pad(small, (0, tall * LANES - small.shape[0])).reshape(tall, LANES)
    matrices, squares, smalls = gather_weights(
        jnp.stack([upward, downward]).astype(BF), square.astype(BF), small
    )
    devices = smalls.shape[0] * 2
    smalls = smalls.reshape(devices, tall * LANES)[:, : small_rows * share]
    smalls = smalls.reshape(devices, small_rows, share).transpose(1, 0, 2)
    smalls = smalls.reshape(small_rows, devices * share)
    split = vectors.shape[0]
    return (
        matrices,
        squares.reshape(devices * square.shape[0], square.shape[1]),
        smalls[:split],
        smalls[split:],
    )


def per_device(
    inputs,
    cotangent,
    lengths,
    square,
    upward,
    downward,
    vectors,
    kernel,
    square_momentum,
    square_variance,
    upward_momentum,
    upward_variance,
    downward_momentum,
    downward_variance,
    vectors_momentum,
    vectors_variance,
    kernel_momentum,
    kernel_variance,
):
    model_width = inputs.shape[2]
    frame_count = inputs.shape[1]
    groups = lax.axis_size("seq")
    seq_place = lax.axis_index("seq")
    seq_frames = frame_count * groups
    head_cols = model_width // groups
    col_start = seq_place * head_cols
    head_size = D // H
    coarse, fine = position_tables(seq_frames, model_width)
    full_ud, full_sq, full_vec, full_kern = gathered(square, upward, downward, vectors, kernel)
    small_params = full_vec.astype(jnp.float32)
    conv_taps = full_kern.astype(jnp.float32)
    resid1, normed1, hidden1, active1, normed2, heads, pos_heads = front(
        inputs[0], small_params, coarse, fine, full_ud, full_sq
    )
    query_head, key_head, value_head = heads[0], heads[1], heads[2]
    biases = lax.dynamic_slice_in_dim(small_params[10:12], col_start, head_cols, 1)
    attended, prob = attend_heads(
        query_head, key_head, value_head, pos_heads, biases, lengths[0], head_size
    )
    (
        layer_output, grad_res2, grad_out_head, out_time, grad_att_b, normed3, grad_pair, grad_conv_b, swish_b, normed4,
        active4, grad_hidden4, half4, small_grads, grad_taps,
    ) = middle(lengths, attended, resid1, cotangent[0], small_params, conv_taps, full_ud, full_sq)
    layer_output = layer_output[None]
    grad_query_b, grad_key_b, grad_value_b, grad_table, grad_biases = attend_heads_back(
        query_head, key_head, value_head, pos_heads, biases, prob, grad_out_head, head_size
    )
    input_grad, matrix_grads, square_grad, small_sums = back(
        (grad_query_b, grad_key_b, grad_value_b), grad_table, grad_biases, coarse, fine, small_params,
        inputs[0], resid1, grad_res2, (normed1, hidden1, active1, normed2), (normed4, active4, grad_hidden4, half4),
        (out_time, grad_att_b, normed3, grad_pair, grad_conv_b, swish_b), small_grads, grad_taps, full_ud, full_sq,
    )
    input_grad = input_grad[None]
    upward_grad, downward_grad = matrix_grads[0], matrix_grads[1]
    place = seq_place * lax.axis_size("fsdp") + lax.axis_index("fsdp")
    share = vectors.shape[1]
    small_own = lax.dynamic_slice_in_dim(small_sums, place * share, share, 1)
    vectors_grad = small_own[: vectors.shape[0]]
    kernel_grad = small_own[vectors.shape[0] : vectors.shape[0] + kernel.shape[0]]
    square_next, momentum_square, variance_square = adam_step(
        square, square_grad, square_momentum, square_variance, DECAY_RATE
    )
    upward_next, momentum_upward, variance_upward = adam_step(
        upward, upward_grad, upward_momentum, upward_variance, DECAY_RATE
    )
    downward_next, momentum_downward, variance_downward = adam_step(
        downward, downward_grad, downward_momentum, downward_variance, DECAY_RATE
    )
    vectors_next, momentum_vectors, variance_vectors = adam_step(
        vectors, vectors_grad, vectors_momentum, vectors_variance, 0.0
    )
    kernel_next, momentum_kernel, variance_kernel = adam_step(
        kernel, kernel_grad, kernel_momentum, kernel_variance, DECAY_RATE
    )
    return (
        layer_output,
        input_grad,
        square_grad,
        upward_grad,
        downward_grad,
        vectors_grad,
        kernel_grad,
        square_next,
        upward_next,
        downward_next,
        vectors_next,
        kernel_next,
        momentum_square,
        variance_square,
        momentum_upward,
        variance_upward,
        momentum_downward,
        variance_downward,
        momentum_vectors,
        variance_vectors,
        momentum_kernel,
        variance_kernel,
    )


def solution(mesh):
    return jax.shard_map(
        per_device,
        mesh=mesh,
        in_specs=(
            P("fsdp", "seq", None),
            P("fsdp", "seq", None),
            P("fsdp"),
            P(("seq", "fsdp"), None),
            P(("seq", "fsdp"), None),
            P(("seq", "fsdp"), None),
            P(None, ("seq", "fsdp")),
            P(None, ("seq", "fsdp")),
            P(("seq", "fsdp"), None),
            P(("seq", "fsdp"), None),
            P(("seq", "fsdp"), None),
            P(("seq", "fsdp"), None),
            P(("seq", "fsdp"), None),
            P(("seq", "fsdp"), None),
            P(None, ("seq", "fsdp")),
            P(None, ("seq", "fsdp")),
            P(None, ("seq", "fsdp")),
            P(None, ("seq", "fsdp")),
        ),
        out_specs=(
            P("fsdp", "seq", None),
            P("fsdp", "seq", None),
            P(("seq", "fsdp"), None),
            P(("seq", "fsdp"), None),
            P(("seq", "fsdp"), None),
            P(None, ("seq", "fsdp")),
            P(None, ("seq", "fsdp")),
            P(("seq", "fsdp"), None),
            P(("seq", "fsdp"), None),
            P(("seq", "fsdp"), None),
            P(None, ("seq", "fsdp")),
            P(None, ("seq", "fsdp")),
            P(("seq", "fsdp"), None),
            P(("seq", "fsdp"), None),
            P(("seq", "fsdp"), None),
            P(("seq", "fsdp"), None),
            P(("seq", "fsdp"), None),
            P(("seq", "fsdp"), None),
            P(None, ("seq", "fsdp")),
            P(None, ("seq", "fsdp")),
            P(None, ("seq", "fsdp")),
            P(None, ("seq", "fsdp")),
        ),
        check_vma=False,
    )
```

```python
import math

import jax
import jax.numpy as jnp
from jax import lax
from jax.experimental import pallas as pl
from jax.experimental.pallas import tpu as pltpu
from jax.sharding import PartitionSpec as P

D = 512
H = 8
FF = 2048
ADAM_STEP = 4

LN_EPS = 1e-05
BN_EPS = 1e-05
BETA_ONE = 0.9
BETA_TWO = 0.98
ADAM_EPS = 1e-08
LEARN_RATE = 0.005
DECAY_RATE = 0.01


def position_tables(seq_frames, model_width):
    fine = math.gcd(2 * seq_frames, 64)
    column = jnp.arange(model_width)
    frequency = jnp.exp(-math.log(10000.0) * 2.0 * (column // 2).astype(jnp.float32) / model_width)
    coarse_at = (seq_frames - 1 - fine * jnp.arange(2 * seq_frames // fine)).astype(jnp.float32)
    coarse_phase = coarse_at[:, None] * frequency[None, :]
    fine_phase = jnp.arange(fine).astype(jnp.float32)[:, None] * frequency[None, :]
    even = (column % 2 == 0)[None, :]
    sine, cosine = jnp.sin(coarse_phase), jnp.cos(coarse_phase)
    with_cosine = jnp.where(even, sine, cosine)
    with_sine = jnp.where(even, -cosine, sine)
    return jnp.stack([with_cosine, with_sine]), jnp.stack([jnp.cos(fine_phase), jnp.sin(fine_phase)])


def adam_step(weight, gradient, first_mom, second_mom, decay):
    first_new = BETA_ONE * first_mom + (1.0 - BETA_ONE) * gradient
    second_new = BETA_TWO * second_mom + (1.0 - BETA_TWO) * gradient * gradient
    fix_one = 1.0 - BETA_ONE**ADAM_STEP
    fix_two = 1.0 - BETA_TWO**ADAM_STEP
    update = first_new / fix_one / (jnp.sqrt(second_new / fix_two) + ADAM_EPS)
    return (weight - LEARN_RATE * (update + decay * weight), first_new, second_new)


MESH = pl.DeviceIdType.MESH
BF = jnp.bfloat16
F32 = jnp.float32
LANES = 128


class Grid:
    def __init__(self):
        self.nz = lax.axis_size("seq")
        self.nf = lax.axis_size("fsdp")
        plane = self.nf // 2
        side = math.isqrt(plane)
        self.z = lax.axis_index("seq")
        f = lax.axis_index("fsdp")
        self.core = f % 2
        if side * side == plane:
            self.na = self.nb = side
            self.step_a = 2 + self.core * (2 * side - 2)
            self.step_b = 2 * side - self.core * (2 * side - 2)
        else:
            self.na, self.nb = plane, 1
            self.step_a, self.step_b = 2, self.nf
        self.f = f
        self.a = (f // self.step_a) % self.na
        self.b = (f // self.step_b) % self.nb
        self.plane = plane
        self.chips = plane * self.nz

        self.half = self.nz // 2
        self.t = (self.z % self.half) * 2 + self.core
        self.column = f - self.core

    def time(self, q):
        return (self.z - self.z % self.half + q // 2, self.column + q % 2)

    def owner(self):
        return (self.t, self.column + self.z // self.half)

    def worker(self):
        return (self.core * self.half + self.z // 2, self.column + self.z % 2)

    def at_home(self):
        return jnp.logical_and(self.t == self.z, self.z // self.half == self.core)

    def chip(self, z, a, b):
        return z * self.plane + (a * self.step_a + b * self.step_b) // 2

    def device(self, z, a, b):
        return (z, a * self.step_a + b * self.step_b + self.core)

    def sibling(self):
        return (self.z, self.f + 1 - 2 * self.core)

    def up(self, axis):
        return self.device(self.z + (axis == "z"), self.a + (axis == "a"), self.b + (axis == "b"))

    def down(self, axis):
        return self.device(self.z - (axis == "z"), self.a - (axis == "a"), self.b - (axis == "b"))

    def line(self, axis):
        return {
            "c": (self.core, 2, lambda q: (self.z, self.f - self.core + q)),
            "a": (self.a, self.na, lambda q: self.device(self.z, q, self.b)),
            "b": (self.b, self.nb, lambda q: self.device(self.z, self.a, q)),
            "z": (self.z, self.nz, lambda q: self.device(q, self.a, self.b)),
        }[axis]

    def place(self, axis):
        return {"z": (self.z, self.nz), "a": (self.a, self.na), "b": (self.b, self.nb)}[axis]


def greet(g):
    barrier = pltpu.get_barrier_semaphore()
    pl.semaphore_signal(barrier, inc=1, device_id=g.sibling(), device_id_type=MESH)
    total = 1
    for axis in "zab":
        p, n = g.place(axis)
        if n == 1:
            continue

        @pl.when(p < n - 1)
        def _():
            pl.semaphore_signal(barrier, inc=1, device_id=g.up(axis), device_id_type=MESH)

        @pl.when(p > 0)
        def _():
            pl.semaphore_signal(barrier, inc=1, device_id=g.down(axis), device_id_type=MESH)

        total = total + 2 - (n - 1 - p == 0) - (p == 0)
    total = total + greet_mover(g, barrier, g.owner())
    pl.semaphore_wait(barrier, total)


def greet_mover(g, barrier, source):
    @pl.when(jnp.logical_not(g.at_home()))
    def _():
        pl.semaphore_signal(barrier, inc=1, device_id=source, device_id_type=MESH)

    return 1 - g.at_home().astype(jnp.int32)


def merge_moments(first_op, second_op):
    count = first_op[0:1] + second_op[0:1]
    share = second_op[0:1] / jnp.maximum(count, 1.0)
    gap = second_op[1:2] - first_op[1:2]
    mean = first_op[1:2] + gap * share
    squares = first_op[2:3] + second_op[2:3] + gap * gap * (first_op[0:1] * share)
    return jnp.concatenate([count, mean, squares, first_op[3:]], axis=0)


NT = (((1,), (1,)), ((), ()))
TN = (((0,), (0,)), ((), ()))
NN = (((1,), (0,)), ((), ()))


def dot(first_op, second_op, dims):
    return lax.dot_general(first_op, second_op, dims, preferred_element_type=F32)


def keep_head(value, h, head_size):
    lane = lax.broadcasted_iota(jnp.int32, value.shape, 1)
    return jnp.where(lane // head_size == h, value, jnp.zeros_like(value))


def attend_kernel(head_size, len_ref, q_ref, k_ref, v_ref, pos_ref, bias_ref, o_ref, prob_ref):
    i = pl.program_id(0)
    rows, cols = q_ref.shape
    frames = k_ref.shape[0]
    width = rows + frames
    query = q_ref[...].astype(F32)
    content = (query + bias_ref[0:1, :]).astype(BF)
    positional = (query + bias_ref[1:2, :]).astype(BF)
    window = pos_ref[pl.ds(pl.multiple_of(frames - rows - i * rows, rows), width), :]
    live = lax.broadcasted_iota(jnp.int32, (rows, frames), 1).astype(F32) < len_ref[0:1, 0:1]
    out = jnp.zeros((rows, cols), F32)
    for h in range(cols // head_size):
        direct = dot(keep_head(content, h, head_size), k_ref[...], NT)
        spread = dot(keep_head(positional, h, head_size), window, NT)
        shifted = pltpu.roll(spread, width - rows + 1, 1, stride=1, stride_axis=0)[:, :frames]
        score = jnp.where(live, (direct + shifted) * (1.0 / math.sqrt(head_size)), -1e30)
        top = jnp.max(score, axis=-1, keepdims=True)
        power = jnp.exp(score - top)
        prob = power * (1.0 / jnp.sum(power, axis=-1, keepdims=True))
        prob_b = prob.astype(BF)
        prob_ref[h] = prob_b
        out = out + keep_head(dot(prob_b, v_ref[...], NN), h, head_size)
    o_ref[...] = out.astype(BF)


def attend_heads(query, key, value, pos, biases, length, head_size, rows=256):
    frames, cols = query.shape
    rows = min(rows, frames)
    heads = cols // head_size
    full = lambda n: pl.BlockSpec((n, cols), lambda i: (0, 0))
    return pl.pallas_call(
        lambda *refs: attend_kernel(head_size, *refs),
        name="attend_heads",
        grid=(frames // rows,),
        in_specs=[
            pl.BlockSpec(length.shape, lambda i: (0, 0)),
            pl.BlockSpec((rows, cols), lambda i: (i, 0)),
            full(frames),
            full(frames),
            full(2 * frames),
            full(2),
        ],
        out_specs=[
            pl.BlockSpec((rows, cols), lambda i: (i, 0)),
            pl.BlockSpec((heads, rows, frames), lambda i: (0, i, 0)),
        ],
        out_shape=(
            jax.ShapeDtypeStruct((frames, cols), BF),
            jax.ShapeDtypeStruct((heads, frames, frames), BF),
        ),
        compiler_params=pltpu.CompilerParams(vmem_limit_bytes=48 * 1024 * 1024),
    )(length, query, key, value, pos, biases)


def attend_back_block(head_size, i, query_b, k_ref, v_ref, pos_ref, bias_ref, prob_ref, grad_heads, gk_acc, gv_acc, gpos_acc, gbias):
    rows, cols = query_b.shape
    frames = k_ref.shape[0]
    width = rows + frames
    query = query_b.astype(F32)
    content = (query + bias_ref[0:1, :]).astype(BF)
    positional = (query + bias_ref[1:2, :]).astype(BF)
    down = lax.broadcasted_iota(jnp.int32, (rows, rows), 0)
    across = lax.broadcasted_iota(jnp.int32, (rows, rows), 1)
    turn = jnp.where(down + across == rows - 1, 1.0, 0.0).astype(BF)
    positional_turned = dot(turn, positional, NN).astype(BF)
    here = pl.ds(frames - rows - i * rows, width)
    window = pos_ref[here, :]
    grad_content = jnp.zeros((rows, cols), F32)
    grad_position = jnp.zeros((rows, cols), F32)
    for h in range(cols // head_size):
        grad_out = keep_head(grad_heads, h, head_size)
        prob_b = prob_ref[h]
        prob = prob_b.astype(F32)
        grad_prob = dot(grad_out, v_ref[...], NT)
        delta = jnp.sum(prob * grad_prob, axis=-1, keepdims=True)
        score_b = (prob * (grad_prob - delta) * (1.0 / math.sqrt(head_size))).astype(BF)
        grad_content = grad_content + keep_head(dot(score_b, k_ref[...], NN), h, head_size)
        gk_acc[...] += dot(keep_head(content, h, head_size), score_b, TN)
        gv_acc[...] += dot(grad_out, prob_b, TN)
        wide = jnp.concatenate([dot(turn, score_b, NN), jnp.zeros((rows, width - frames), F32)], axis=1)
        spread = pltpu.roll(wide, 0, 1, stride=1, stride_axis=0).astype(BF)
        grad_position = grad_position + keep_head(dot(spread, window, NN), h, head_size)
        gpos_acc[:, here] += dot(keep_head(positional_turned, h, head_size), spread, TN)
    high = grad_position.astype(BF)
    low = (grad_position - high.astype(F32)).astype(BF)
    grad_position = dot(turn, high, NN) + dot(turn, low, NN)
    gbias[0:1, :] += jnp.sum(grad_content, axis=0, keepdims=True)
    gbias[1:2, :] += jnp.sum(grad_position, axis=0, keepdims=True)
    return (grad_content + grad_position).astype(BF)

def normalize(value):
    mean = jnp.mean(value, axis=-1, keepdims=True)
    centred = value - mean
    spread = lax.rsqrt(jnp.mean(centred * centred, axis=-1, keepdims=True) + LN_EPS)
    return centred * spread, spread


def norm_forward(value, gains, k):
    unit, _ = normalize(value)
    return (unit * gains[2 * k : 2 * k + 1] + gains[2 * k + 1 : 2 * k + 2]).astype(BF)


def norm_backward(value, gains, k, upstream):
    unit, spread = normalize(value)
    inner = upstream * gains[2 * k : 2 * k + 1]
    along = jnp.mean(inner * unit, axis=-1, keepdims=True)
    grad = spread * (inner - jnp.mean(inner, axis=-1, keepdims=True) - unit * along)
    gain = jnp.sum(upstream * unit, axis=0, keepdims=True)
    return grad, gain, jnp.sum(upstream, axis=0, keepdims=True)


def sigmoid(value):
    return 1.0 / (1.0 + jnp.exp(-value))


def module_forward(normed, up_ref, down_ref, hidden_ref, active_ref):
    units, width = up_ref.shape
    step = min(512, units)

    def chunk(j, total):
        here = pl.ds(pl.multiple_of(j * step, step), step)
        hidden = dot(normed, up_ref[here, :], NT)
        active = (hidden * sigmoid(hidden)).astype(BF)
        hidden_ref[:, here] = hidden.astype(hidden_ref.dtype)
        active_ref[:, here] = active
        return total + dot(active, down_ref[here, :], NN)

    return lax.fori_loop(0, units // step, chunk, jnp.zeros((normed.shape[0], width), F32))


def module_backward(upstream_b, up_ref, down_ref, hidden_ref, grad_ref):
    units, width = up_ref.shape
    step = min(512, units)

    def chunk(j, total):
        here = pl.ds(pl.multiple_of(j * step, step), step)
        hidden = hidden_ref[:, here].astype(F32)
        sigma = sigmoid(hidden)
        slope = sigma * (1.0 + hidden * (1.0 - sigma))
        grad = (dot(upstream_b, down_ref[here, :], NT) * slope).astype(BF)
        grad_ref[:, here] = grad
        return total + dot(grad, up_ref[here, :], NN)

    return lax.fori_loop(0, units // step, chunk, jnp.zeros((upstream_b.shape[0], width), F32))


def greet_lines(g, axes, source=None):
    barrier = pltpu.get_barrier_semaphore()
    total = g.nz - 1
    for k in range(1, g.nz):
        pl.semaphore_signal(barrier, inc=1, device_id=g.time(lax.rem(g.t + k, g.nz)), device_id_type=MESH)
    if source is not None:
        total = total + greet_mover(g, barrier, source)
    for axis in axes:
        p, n, device = g.line(axis)
        for k in range(1, n):
            pl.semaphore_signal(barrier, inc=1, device_id=device(lax.rem(p + k, n)), device_id_type=MESH)
            total += 1
    pl.semaphore_wait(barrier, total)


def remote(src, dst, send, recv, device):
    return pltpu.make_async_remote_copy(
        src_ref=src, dst_ref=dst, send_sem=send, recv_sem=recv, device_id=device, device_id_type=MESH
    )


def arrived(ref, sem):
    pltpu.make_async_copy(ref, ref, sem).wait()


def front_kernel(x_ref, gains_ref, coarse_ref, fine_ref, ud_hbm, sq_hbm,
                 x1_ref, a1_ref, h1_ref, s1_ref, a2_ref, heads_ref, pos_ref,
                 up, down, wqkv, wpos, mine, load_sem, send_sem, recv_sem):
    g = Grid()
    z, nz = g.t, g.nz
    rows, width = x_ref.shape
    cols = width // nz
    units = up.shape[0]
    loads = [
        pltpu.make_async_copy(ud_hbm.at[0, pl.ds(0, units)], up, load_sem.at[0]),
        pltpu.make_async_copy(ud_hbm.at[1, pl.ds(0, units)], down, load_sem.at[1]),
        pltpu.make_async_copy(sq_hbm.at[pl.ds(0, 3 * width)], wqkv, load_sem.at[2]),
        pltpu.make_async_copy(sq_hbm.at[pl.ds(3 * width + z * cols, cols)], wpos, load_sem.at[3]),
    ]
    for load in loads:
        load.start()
    greet_lines(g, "")
    gains = gains_ref[...]
    signal = x_ref[...].astype(F32)
    normed1 = norm_forward(signal, gains, 0)
    a1_ref[...] = normed1
    loads[0].wait()
    loads[1].wait()
    resid1 = signal + 0.5 * module_forward(normed1, up, down, h1_ref, s1_ref)
    x1_ref[...] = resid1
    normed2 = norm_forward(resid1, gains, 1)
    a2_ref[...] = normed2
    loads[2].wait()
    for k in range(3):
        out = dot(normed2, wqkv[pl.ds(k * width, width), :], NT).astype(BF)
        for q in range(nz):
            mine[q, k] = out[:, q * cols : (q + 1) * cols]
    sends = []
    for k in range(1, nz):
        q = lax.rem(z + k, nz)
        copy = remote(mine.at[q], heads_ref.at[:, pl.ds(z * rows, rows)], send_sem.at[k], recv_sem.at[z], g.time(q))
        copy.start()
        sends.append(copy)
    own = pl.ds(pl.multiple_of(z * rows, rows), rows)
    for k in range(3):
        heads_ref[k, own, :] = mine[z, k]
    loads[3].wait()
    fine = fine_ref.shape[1]
    weight = wpos[...]

    def position(i, _):
        table = coarse_ref[0, pl.ds(i, 1), :] * fine_ref[0] + coarse_ref[1, pl.ds(i, 1), :] * fine_ref[1]
        here = pl.ds(pl.multiple_of(i * fine, fine), fine)
        pos_ref[here, :] = dot(table.astype(BF), weight, NT).astype(BF)
        return 0

    lax.fori_loop(0, coarse_ref.shape[1], position, 0)
    for k in range(1, nz):
        q = lax.rem(z + k, nz)
        arrived(heads_ref.at[:, pl.ds(q * rows, rows)], recv_sem.at[q])
    for copy in sends:
        copy.wait_send()


def front(signal, gains, coarse, fine, ud_full, sq_full):
    rows, width = signal.shape
    nz = lax.axis_size("seq")
    frames, cols = rows * nz, width // nz
    units = ud_full.shape[1] // 2
    vmem = pl.BlockSpec(memory_space=pltpu.VMEM)
    hbm = pl.BlockSpec(memory_space=pl.ANY)
    shape = jax.ShapeDtypeStruct
    return pl.pallas_call(
        front_kernel,
        name="front",
        out_shape=(
            shape((rows, width), F32),
            shape((rows, width), BF),
            shape((rows, units), BF),
            shape((rows, units), BF),
            shape((rows, width), BF),
            shape((3, frames, cols), BF),
            shape((2 * frames, cols), BF),
        ),
        in_specs=[vmem, vmem, vmem, vmem, hbm, hbm],
        out_specs=[vmem] * 7,
        scratch_shapes=[
            pltpu.VMEM((units, width), BF),
            pltpu.VMEM((units, width), BF),
            pltpu.VMEM((3 * width, width), BF),
            pltpu.VMEM((cols, width), BF),
            pltpu.VMEM((nz, 3, rows, cols), BF),
            pltpu.SemaphoreType.DMA((4,)),
            pltpu.SemaphoreType.DMA((nz,)),
            pltpu.SemaphoreType.DMA((nz,)),
        ],
        compiler_params=pltpu.CompilerParams(
            collective_id=5, has_side_effects=True, vmem_limit_bytes=40 * 1024 * 1024
        ),
    )(signal, gains, coarse, fine, ud_full, sq_full)


def meet_levels(g, value, merge, buf, send_sem, recv_sem):
    sends = []
    for level, axis in enumerate("cabz"):
        p, n, device = g.line(axis)
        if n == 1:
            continue
        buf[level, p] = value
        for k in range(1, n):
            copy = remote(buf.at[level, p], buf.at[level, p], send_sem.at[level, k], recv_sem.at[level, p], device(lax.rem(p + k, n)))
            copy.start()
            sends.append(copy)
        for k in range(1, n):
            q = lax.rem(p + k, n)
            arrived(buf.at[level, q], recv_sem.at[level, q])
        value = buf[level, 0]
        for q in range(1, n):
            value = merge(value, buf[level, q])
    return value, sends


HALO = 16


def swap_edges(g, body, low, high, send_sem, recv_sem, pad):
    rows = body.shape[0]
    p, n = g.t, g.nz
    up = remote(body.at[pl.ds(rows - HALO, HALO)], low, send_sem.at[0], recv_sem.at[0], g.time(p + 1))
    down = remote(body.at[pl.ds(0, HALO)], high, send_sem.at[1], recv_sem.at[1], g.time(p - 1))
    pl.when(p < n - 1)(lambda: up.start())
    pl.when(p > 0)(lambda: down.start())
    pad[pl.ds(HALO, rows), :] = body[...].astype(F32)

    def fill(at, ref, sem, there):
        @pl.when(there)
        def _():
            arrived(ref, sem)
            pad[pl.ds(at, HALO), :] = ref[...].astype(F32)

        @pl.when(jnp.logical_not(there))
        def _():
            pad[pl.ds(at, HALO), :] = jnp.zeros((HALO, pad.shape[1]), F32)

    fill(0, low, recv_sem.at[0], p > 0)
    fill(HALO + rows, high, recv_sem.at[1], p < n - 1)

    def finish():
        pl.when(p < n - 1)(lambda: up.wait_send())
        pl.when(p > 0)(lambda: down.wait_send())

    return finish


def middle_kernel(len_ref, att_ref, x1_ref, cot_ref, gains_ref, taps_ref, ud_hbm, sq_hbm,
                  y_ref, g2_ref, go_ref, o_ref, e2_ref, a3_ref, gpair_ref, e3_ref, sw_ref, a4_ref, s4_ref, gh4_ref, e4_ref,
                  small_ref, gtaps_ref,
                  up, down, wsq, o_buf, go_buf, glu_b, gc_b, low1, high1, low2, high2, pad_glu, pad_gc, h4, c_ref, y_buf, y_sem,
                  buf1, buf2, load_sem, a_send, a_recv, b_send, b_recv, h_send, h_recv, m_send, m_recv):
    g = Grid()
    z, nz = g.t, g.nz
    rows, width = x1_ref.shape
    cols = width // nz
    units = up.shape[0]
    taps = taps_ref.shape[0]
    rim = (taps - 1) // 2
    loads = [
        pltpu.make_async_copy(sq_hbm.at[pl.ds(4 * width, 4 * width)], wsq, load_sem.at[0]),
        pltpu.make_async_copy(ud_hbm.at[0, pl.ds(units, units)], up, load_sem.at[1]),
        pltpu.make_async_copy(ud_hbm.at[1, pl.ds(units, units)], down, load_sem.at[2]),
    ]
    for load in loads:
        load.start()
    greet_lines(g, "cabz", g.worker())
    sends = []
    for k in range(1, nz):
        q = lax.rem(z + k, nz)
        copy = remote(att_ref.at[pl.ds(q * rows, rows)], o_buf.at[z], a_send.at[k], a_recv.at[z], g.time(q))
        copy.start()
        sends.append(copy)
    o_buf[z] = att_ref[pl.ds(pl.multiple_of(z * rows, rows), rows), :]
    gains = gains_ref[...]
    frame = z * rows + lax.broadcasted_iota(jnp.int32, (rows, 1), 0)
    live = jnp.where(frame.astype(F32) < len_ref[0:1, 0:1], 1.0, 0.0)
    loads[0].wait()
    weight = lambda k: wsq[pl.ds((k - 4) * width, width), :]
    for k in range(1, nz):
        q = lax.rem(z + k, nz)
        arrived(o_buf.at[q], a_recv.at[q])
    out = jnp.concatenate([o_buf[q] for q in range(nz)], axis=1)
    o_ref[...] = out
    resid2 = x1_ref[...] + dot(out, weight(4), NT)
    normed3 = norm_forward(resid2, gains, 2)
    a3_ref[...] = normed3
    value = dot(normed3, weight(5), NT)
    gate = sigmoid(dot(normed3, weight(6), NT))
    glu_b[...] = (value * gate * live).astype(BF)
    done1 = swap_edges(g, glu_b, low1, high1, h_send.at[0], h_recv.at[0], pad_glu)
    for at in range(0, width, LANES):
        lanes = pl.ds(at, LANES)
        total = jnp.zeros((rows, LANES), F32)
        for m in range(taps):
            total = total + taps_ref[m : m + 1, lanes] * pad_glu[pl.ds(HALO - rim + m, rows), lanes]
        c_ref[:, lanes] = total
    conv = c_ref[...]
    count = jnp.sum(live, axis=0, keepdims=True)
    mean = jnp.sum(live * conv, axis=0, keepdims=True) / jnp.maximum(count, 1.0)
    squares = jnp.sum(live * (conv - mean) * (conv - mean), axis=0, keepdims=True)
    moments = jnp.concatenate([jnp.broadcast_to(count, mean.shape), mean, squares, jnp.zeros((5, width), F32)], axis=0)
    moments, more = meet_levels(g, moments, merge_moments, buf1, m_send.at[0], m_recv.at[0])
    sends += more
    total_frames = moments[0:1]
    inv_std = lax.rsqrt(moments[2:3] / total_frames + BN_EPS)
    centre = moments[1:2]
    centred = c_ref[...] - centre
    zed = centred * inv_std
    bn_val = gains[12:13] * zed + gains[13:14]
    swish = (bn_val * sigmoid(bn_val)).astype(BF)
    sw_ref[...] = swish
    resid3 = resid2 + dot(swish, weight(7), NT)
    normed4 = norm_forward(resid3, gains, 3)
    a4_ref[...] = normed4
    loads[1].wait()
    loads[2].wait()
    resid4 = resid3 + 0.5 * module_forward(normed4, up, down, h4, s4_ref)
    y_buf[...] = norm_forward(resid4, gains, 4)
    away = jnp.logical_not(g.at_home())
    home = remote(y_buf, y_ref, y_sem.at[0], y_sem.at[1], g.owner())
    pl.when(away)(lambda: home.start())

    @pl.when(g.at_home())
    def _():
        y_ref[...] = y_buf[...]

    grad4, gain4, shift4 = norm_backward(resid4, gains, 4, cot_ref[...].astype(F32))
    half4 = (0.5 * grad4).astype(BF)
    e4_ref[...] = half4
    grad_norm, gain3, shift3 = norm_backward(resid3, gains, 3, module_backward(half4, up, down, h4, gh4_ref))
    grad3 = grad4 + grad_norm
    e3 = grad3.astype(BF)
    e3_ref[...] = e3
    sigma = sigmoid(bn_val)
    grad_bn = dot(e3, weight(7), NN) * (sigma * (1.0 + bn_val * (1.0 - sigma)))
    gamma = jnp.sum(grad_bn * zed, axis=0, keepdims=True)
    beta = jnp.sum(grad_bn, axis=0, keepdims=True)
    grad_zed = grad_bn * gains[12:13]
    sum_one = jnp.sum(grad_zed, axis=0, keepdims=True)
    sum_two = jnp.sum(grad_zed * centred, axis=0, keepdims=True)
    sums = jnp.concatenate([sum_one, sum_two, jnp.zeros((6, width), F32)], axis=0)
    sums, more = meet_levels(g, sums, lambda x, y: x + y, buf2, m_send.at[1], m_recv.at[1])
    sends += more
    offset = inv_std * sums[0:1] + inv_std * inv_std * inv_std * sums[1:2] * centred
    gc_b[...] = (inv_std * grad_zed - live / total_frames * offset).astype(BF)
    done2 = swap_edges(g, gc_b, low2, high2, h_send.at[1], h_recv.at[1], pad_gc)
    for at in range(0, width, LANES):
        lanes = pl.ds(at, LANES)
        total = jnp.zeros((rows, LANES), F32)
        upstream = pad_gc[pl.ds(HALO, rows), lanes]
        for m in range(taps):
            total = total + taps_ref[m : m + 1, lanes] * pad_gc[pl.ds(HALO + rim - m, rows), lanes]
            gtaps_ref[m : m + 1, lanes] = jnp.sum(
                upstream * pad_glu[pl.ds(HALO - rim + m, rows), lanes], axis=0, keepdims=True
            )
        c_ref[:, lanes] = total
    grad_glu = c_ref[...] * live
    gv5 = (grad_glu * gate).astype(BF)
    gv6 = (grad_glu * value * gate * (1.0 - gate)).astype(BF)
    gpair_ref[0] = gv5
    gpair_ref[1] = gv6
    grad_norm, gain2, shift2 = norm_backward(
        resid2, gains, 2, dot(gv5, weight(5), NN) + dot(gv6, weight(6), NN)
    )
    grad2 = grad3 + grad_norm
    g2_ref[...] = grad2
    e2 = grad2.astype(BF)
    e2_ref[...] = e2
    grad_out = dot(e2, weight(4), NN).astype(BF)
    for q in range(nz):
        go_buf[q] = grad_out[:, q * cols : (q + 1) * cols]
    for k in range(1, nz):
        q = lax.rem(z + k, nz)
        copy = remote(go_buf.at[q], go_ref.at[pl.ds(z * rows, rows)], b_send.at[k], b_recv.at[z], g.time(q))
        copy.start()
        sends.append(copy)
    go_ref[pl.ds(pl.multiple_of(z * rows, rows), rows), :] = go_buf[z]
    small_ref[...] = jnp.concatenate([gain2, shift2, gain3, shift3, gain4, shift4, gamma, beta], axis=0)
    for k in range(1, nz):
        q = lax.rem(z + k, nz)
        arrived(go_ref.at[pl.ds(q * rows, rows)], b_recv.at[q])
    pl.when(away)(lambda: home.wait())
    done1()
    done2()
    for copy in sends:
        copy.wait_send()


def middle(length, attended, resid1, cotangent, gains, taps, ud_full, sq_full):
    rows, width = resid1.shape
    nz, nf = lax.axis_size("seq"), lax.axis_size("fsdp")
    frames, cols = rows * nz, width // nz
    units = ud_full.shape[1] // 2
    most = max(nz, nf // 2)
    vmem = pl.BlockSpec(memory_space=pltpu.VMEM)
    hbm = pl.BlockSpec(memory_space=pl.ANY)
    shape = jax.ShapeDtypeStruct
    dma = pltpu.SemaphoreType.DMA
    row = shape((rows, width), BF)
    return pl.pallas_call(
        middle_kernel,
        name="middle",
        out_shape=(
            row,
            shape((rows, width), F32),
            shape((frames, cols), BF),
            row,
            row,
            row,
            shape((2, rows, width), BF),
            row,
            row,
            row,
            shape((rows, units), BF),
            shape((rows, units), BF),
            row,
            shape((8, width), F32),
            shape(taps.shape, F32),
        ),
        in_specs=[vmem] * 6 + [hbm] * 2,
        out_specs=[vmem] * 15,
        scratch_shapes=[
            pltpu.VMEM((units, width), BF),
            pltpu.VMEM((units, width), BF),
            pltpu.VMEM((4 * width, width), BF),
            pltpu.VMEM((nz, rows, cols), BF),
            pltpu.VMEM((nz, rows, cols), BF),
            pltpu.VMEM((rows, width), BF),
            pltpu.VMEM((rows, width), BF),
        ]
        + [pltpu.VMEM((HALO, width), BF)] * 4
        + [
            pltpu.VMEM((rows + 2 * HALO, width), F32),
            pltpu.VMEM((rows + 2 * HALO, width), F32),
            pltpu.VMEM((rows, units), F32),
            pltpu.VMEM((rows, width), F32),
            pltpu.VMEM((rows, width), BF),
            dma((2,)),
            pltpu.VMEM((4, most, 8, width), F32),
            pltpu.VMEM((4, most, 8, width), F32),
            dma((3,)),
            dma((nz,)),
            dma((nz,)),
            dma((nz,)),
            dma((nz,)),
            dma((2, 2)),
            dma((2, 2)),
            dma((2, 4, most)),
            dma((2, 4, most)),
        ],
        compiler_params=pltpu.CompilerParams(
            collective_id=6, has_side_effects=True, vmem_limit_bytes=56 * 1024 * 1024
        ),
    )(length, attended, resid1, cotangent, gains, taps, ud_full, sq_full)


def gather_kernel(ud_own, sq_own, sm_own, x_in, cot_in, len_in, ud_full, sq_full, sm_full, x_out, cot_out, len_out, move_send, move_recv, local_sem, swap_send, swap_recv, recv_sem, sib_recv, send_sem):
    g = Grid()
    half = ud_own.shape[1]
    c = g.core
    me = g.chip(g.z, g.a, g.b)
    local = [
        pltpu.make_async_copy(ud_own.at[c], ud_full.at[c, pl.ds(me * 2 * half + c * half, half)], local_sem.at[0]),
        pltpu.make_async_copy(sq_own, sq_full.at[me, c], local_sem.at[1]),
        pltpu.make_async_copy(sm_own, sm_full.at[me, c], local_sem.at[2]),
    ]
    for copy in local:
        copy.start()
    greet(g)
    moves = [
        remote(src, dst, move_send.at[k], move_recv.at[k], g.worker())
        for k, (src, dst) in enumerate(((x_in, x_out), (len_in, len_out), (cot_in, cot_out)))
    ]

    @pl.when(jnp.logical_not(g.at_home()))
    def _():
        for copy in moves:
            copy.start()

    @pl.when(g.at_home())
    def _():
        x_out[...] = x_in[...]
        len_out[...] = len_in[...]
        cot_out[...] = cot_in[...]

    swap = pltpu.make_async_remote_copy(
        src_ref=ud_own.at[1 - c],
        dst_ref=ud_full.at[1 - c, pl.ds(me * 2 * half + c * half, half)],
        send_sem=swap_send,
        recv_sem=swap_recv,
        device_id=g.sibling(),
        device_id_type=MESH,
    )
    swap.start()

    def pieces(t):
        return (ud_full.at[c, pl.ds(t * 2 * half, 2 * half)], sq_full.at[t, c], sm_full.at[t, c])

    ways = {"z+": 0, "z-": 1, "a+": 2, "a-": 3, "b+": 4, "b-": 5, "s": 6}

    def copies(t, way):
        if way == "s":
            target = g.sibling()
        else:
            target = g.up(way[0]) if way[1] == "+" else g.down(way[0])
        arrive = sib_recv if way == "s" else recv_sem
        return [
            pltpu.make_async_remote_copy(
                src_ref=ref,
                dst_ref=ref,
                send_sem=send_sem.at[ways[way], k, t],
                recv_sem=arrive.at[k, t],
                device_id=target,
                device_id_type=MESH,
            )
            for k, ref in enumerate(pieces(t))
        ]

    def send(t, way, finish=False):
        def act():
            for copy in copies(t, way):
                if finish:
                    copy.wait_send()
                else:
                    copy.start()

        if way == "s":
            act()
            return
        p, n = g.place(way[0])
        if n == 1:
            return
        pl.when(p < n - 1 if way[1] == "+" else p > 0)(act)

    def wait(t):
        for k, ref in enumerate(pieces(t)):
            pltpu.make_async_copy(ref, ref, recv_sem.at[k, t]).wait()

    def spread(finish):
        def got(t, ways_on):
            if not finish:
                wait(t)
            for way in ways_on:
                send(t, way, finish)

        if finish:
            pass
        else:
            for copy in local:
                copy.wait()
            swap.wait_recv()
        for way in ("z+", "z-", "a+", "a-", "b+", "b-", "s"):
            send(me, way, finish)
        for k in range(1, g.nz):
            pl.when(g.z >= k)(lambda: got(g.chip(g.z - k, g.a, g.b), ("z+", "a+", "a-", "b+", "b-", "s")))
            pl.when(g.z + k < g.nz)(lambda: got(g.chip(g.z + k, g.a, g.b), ("z-", "a+", "a-", "b+", "b-", "s")))

        def column(a, b, ways_on):
            got(g.chip(g.z, a, b), ways_on)
            for k in range(1, g.nz):
                pl.when(g.z >= k)(lambda: got(g.chip(g.z - k, a, b), ways_on))
                pl.when(g.z + k < g.nz)(lambda: got(g.chip(g.z + k, a, b), ways_on))

        for k in range(1, g.na):
            pl.when(g.a >= k)(lambda: column(g.a - k, g.b, ("a+", "b+", "b-", "s")))
            pl.when(g.a + k < g.na)(lambda: column(g.a + k, g.b, ("a-", "b+", "b-", "s")))
        for kb in range(1, g.nb):

            def plane(b, ways_on):
                column(g.a, b, ways_on)
                for k in range(1, g.na):
                    pl.when(g.a >= k)(lambda: column(g.a - k, b, ways_on))
                    pl.when(g.a + k < g.na)(lambda: column(g.a + k, b, ways_on))

            pl.when(g.b >= kb)(lambda: plane(g.b - kb, ("b+", "s")))
            pl.when(g.b + kb < g.nb)(lambda: plane(g.b + kb, ("b-", "s")))

    spread(False)
    d = 1 - c

    def other(t, _):
        for k, ref in enumerate((ud_full.at[d, pl.ds(t * 2 * half, 2 * half)], sq_full.at[t, d], sm_full.at[t, d])):
            pltpu.make_async_copy(ref, ref, sib_recv.at[k, t]).wait()
        return 0

    lax.fori_loop(0, g.chips, other, 0)
    swap.wait_send()
    spread(True)

    @pl.when(jnp.logical_not(g.at_home()))
    def _():
        for copy in moves:
            copy.wait()


def gather_weights(ud, sq, sm, signal, cotangent, length):
    devices = lax.axis_size("seq") * lax.axis_size("fsdp")
    chips = devices // 2
    _, rows, width = ud.shape
    hbm = pl.BlockSpec(memory_space=pl.ANY)
    vmem = pl.BlockSpec(memory_space=pltpu.VMEM)
    dma = pltpu.SemaphoreType.DMA
    return pl.pallas_call(
        gather_kernel,
        name="gather_weights",
        out_shape=(
            jax.ShapeDtypeStruct((2, devices * rows, width), ud.dtype),
            jax.ShapeDtypeStruct((chips, 2, rows, width), sq.dtype),
            jax.ShapeDtypeStruct((chips, 2) + sm.shape, sm.dtype),
            jax.ShapeDtypeStruct(signal.shape, signal.dtype),
            jax.ShapeDtypeStruct(cotangent.shape, cotangent.dtype),
            jax.ShapeDtypeStruct(length.shape, length.dtype),
        ),
        in_specs=[vmem] * 6,
        out_specs=[hbm] * 3 + [vmem] * 3,
        scratch_shapes=[
            dma((3,)),
            dma((3,)),
            dma((3,)),
            dma,
            dma,
            dma((3, chips)),
            dma((3, chips)),
            dma((7, 3, chips)),
        ],
        compiler_params=pltpu.CompilerParams(collective_id=1, has_side_effects=True),
    )(ud, sq, sm, signal, cotangent, length)


class Meeting:
    def __init__(self, g, buf, send_sem, recv_sem):
        self.g, self.buf, self.send_sem, self.recv_sem = g, buf, send_sem, recv_sem
        self.sends = []

    def start(self, level, value):
        axis = "cabz"[level]
        p, n, device = self.g.line(axis)
        self.buf[level, p] = value
        for k in range(1, n):
            here = self.buf.at[level, p]
            copy = remote(here, here, self.send_sem.at[level, k], self.recv_sem.at[level, p], device(lax.rem(p + k, n)))
            copy.start()
            self.sends.append(copy)

    def total(self, level):
        p, n, _ = self.g.line("cabz"[level])
        for k in range(1, n):
            q = lax.rem(p + k, n)
            arrived(self.buf.at[level, q], self.recv_sem.at[level, q])
        value = self.buf[level, 0]
        for q in range(1, n):
            value = value + self.buf[level, q]
        return value


class Reduction:
    def __init__(self, g, gud, gsq, sib_ud, sib_sq, sib_sem, rb, ra, rz, sems):
        self.g, self.gud, self.gsq, self.sib_ud, self.sib_sq = g, gud, gsq, sib_ud, sib_sq
        self.sib_send, self.sib_recv = sib_sem
        self.bufs = {"b": rb, "a": ra, "z": rz}
        self.sems = sems
        self.sq_rows = gsq.shape[2]
        self.pair = 2 * self.sq_rows
        self.height = g.plane * self.pair

    def rows(self, t, part):
        return pl.ds(pl.multiple_of(t * self.pair + (part - 1) * self.sq_rows, self.sq_rows), self.sq_rows)

    def own(self, t, part):
        c = self.g.core
        return self.gsq.at[t, c] if part == 0 else self.gud.at[c, self.rows(t, part)]

    def sibling_copy(self, z, kind):
        g = self.g
        d = 1 - g.core
        if kind == 0:
            chips = pl.ds(z * g.plane, g.plane)
            src, dst = self.gsq.at[chips, d], self.sib_sq.at[chips]
        else:
            tall = pl.ds(z * self.height, self.height)
            src, dst = self.gud.at[d, tall], self.sib_ud.at[tall]
        return remote(src, dst, self.sib_send.at[kind, z], self.sib_recv.at[kind, z], g.sibling())

    def to_sibling(self, planes, kind):
        for z in planes:
            self.sibling_copy(z, kind).start()

    def from_sibling(self, planes, kind):
        for z in planes:
            self.sibling_copy(z, kind).wait_recv()

    def add_sibling(self, t, part):
        ref = self.own(t, part)
        ref[...] = ref[...] + (self.sib_sq[t] if part == 0 else self.sib_ud[self.rows(t, part), :])

    def landing(self, axis, slot, part):
        return self.bufs[axis].at[slot, pl.ds(part * self.sq_rows, self.sq_rows)]

    def slot(self, axis, upward, z, a, b, there):
        g = self.g
        p, n = g.place(axis)
        q = {"z": z, "a": a, "b": b}[axis]
        if there:
            p = p + 1 if upward else p - 1
        if upward:
            q = q + 1 - n * (p == n - 1)
        return {"b": (q * g.na + a) * g.nz + z, "a": q * g.nz + z, "z": q}[axis]

    def hop(self, axis, upward, z, a, b, part):
        g = self.g
        slot = self.slot(axis, upward, z, a, b, True)
        sends, recvs = self.sems[axis]
        device = g.up(axis) if upward else g.down(axis)
        src, dst = self.own(g.chip(z, a, b), part), self.landing(axis, slot, part)
        return remote(src, dst, sends.at[1 if upward else 0, part, slot], recvs.at[part, slot], device)

    def take(self, axis, upward, z, a, b, part):
        slot = self.slot(axis, upward, z, a, b, False)
        src, dst = self.landing(axis, slot, part), self.own(self.g.chip(z, a, b), part)
        arrived(src, self.sems[axis][1].at[part, slot])
        dst[...] = dst[...] + src[...]

    def settle(self, axis, z, a, b, part):
        p, n = self.g.place(axis)
        if n > 1:
            pl.when(p > 0)(lambda: self.take(axis, True, z, a, b, part))
            pl.when(p < n - 1)(lambda: self.take(axis, False, z, a, b, part))

    def ready(self, axis, z, a, b, part):
        if axis == "b":
            self.add_sibling(self.g.chip(z, a, b), part)
        else:
            before = {"a": "b", "z": "a"}[axis]
            self.ready(before, z, a, b, part)
            self.settle(before, z, a, b, part)

    def pass_on(self, axis, upward, z, a, b, part, finish):
        p, n = self.g.place(axis)
        if finish:
            self.hop(axis, upward, z, a, b, part).wait_send()
            return
        self.ready(axis, z, a, b, part)
        behind = p > 0 if upward else p < n - 1
        pl.when(behind)(lambda: self.take(axis, upward, z, a, b, part))
        self.hop(axis, upward, z, a, b, part).start()

    def along(self, axis, planes, part, finish=False):
        g = self.g
        p, n = g.place(axis)
        if axis == "z":
            for q in planes:
                pl.when(p < q)(lambda: self.pass_on("z", True, q, g.a, g.b, part, finish))
                pl.when(p > q)(lambda: self.pass_on("z", False, q, g.a, g.b, part, finish))
            return
        step = planes[1] - planes[0] if len(planes) > 1 else 1
        count = len(planes)
        for k in range(n - 1, 0, -1):
            for upward in (True, False):
                q = p + k if upward else p - k

                def act():
                    def body(i, _):
                        plane = planes[0] + step * lax.rem(i, count)
                        if axis == "b":
                            a = lax.rem(g.a + 1 + i // count, g.na)
                            self.pass_on("b", upward, plane, a, q, part, finish)
                        else:
                            self.pass_on("a", upward, plane, q, g.b, part, finish)
                        return 0

                    lax.fori_loop(0, (g.na if axis == "b" else 1) * count, body, 0)

                pl.when(p + k < n if upward else p >= k)(act)

    def last(self, part):
        g = self.g
        self.ready("z", g.z, g.a, g.b, part)
        self.settle("z", g.z, g.a, g.b, part)


def back_kernel(head_size, qkv_ref, pos_ref, bias_ref, go_ref, coarse_ref, fine_ref, gains_ref,
                x_ref, x1_ref, g2_ref, a1_ref, h1_ref, s1_ref, a2_ref,
                a4_ref, s4_ref, gh4_ref, e4_ref, o_ref, e2_ref, a3_ref, gpair_ref, e3_ref, sw_ref, some_ref, gtaps_ref,
                prob_hbm, ud_hbm, sq_hbm,
                gx_ref, ud_out, sq_out, small_out,
                prob_buf, gk_acc, gv_acc, gpos_acc, gbias, grads, prob_sem, wqkv, heads, gqkv, gh1, small, gud, gsq, sib_ud, sib_sq, rb, ra, rz, sbuf, fin_send_buf, fin, gx_buf, gx_in, gx_sem,
                load_sem, h_send, h_recv, sib_send, sib_recv, b_send, b_recv, a_send, a_recv, z_send, z_recv, s_send, s_recv,
                fin_send, fin_recv):
    g = Grid()
    z, nz, c = g.t, g.nz, g.core
    rows, width = x_ref.shape
    cols = width // nz
    units = h1_ref.shape[1]
    frames = qkv_ref.shape[1]
    up, down = gud.at[0, pl.ds(0, units)], gud.at[1, pl.ds(0, units)]
    loads = [
        pltpu.make_async_copy(sq_hbm.at[pl.ds(0, 3 * width)], wqkv, load_sem.at[0]),
        pltpu.make_async_copy(ud_hbm.at[0, pl.ds(0, units)], up, load_sem.at[1]),
        pltpu.make_async_copy(ud_hbm.at[1, pl.ds(0, units)], down, load_sem.at[2]),
    ]

    def probabilities(i):
        return pltpu.make_async_copy(prob_hbm.at[:, pl.ds(i * rows, rows)], prob_buf.at[i % 2], prob_sem.at[i % 2])

    probabilities(0).start()
    for load in loads:
        load.start()
    greet_lines(g, "cabz", g.worker())
    sends = []
    red = Reduction(
        g, gud, gsq, sib_ud, sib_sq, (sib_send, sib_recv), rb, ra, rz,
        {"b": (b_send, b_recv), "a": (a_send, a_recv), "z": (z_send, z_recv)},
    )
    total_rows = gud.shape[1]
    sq_rows = gsq.shape[2]
    high = list(range(nz - 1, nz // 2 - 1, -1))
    low = list(range(0, nz // 2))
    part = 256

    def matrix_terms(color, left_ref, right, first_row, count):
        def body(i, _):
            here = pl.ds(pl.multiple_of(i * part, part), part)
            there = pl.ds(pl.multiple_of(first_row + i * part, part), part)
            gud[color, there, :] = dot(left_ref[:, here], right, TN).astype(BF)
            return 0

        lax.fori_loop(0, count // part, body, 0)

    per = width // sq_rows // 2

    def square_terms(block, left, right):
        sums = dot(left, right, TN).astype(BF).reshape(per, 2, sq_rows, width)
        gsq[pl.ds(block * per, per)] = sums

    square_terms(7, e3_ref[...], sw_ref[...])
    square_terms(6, gpair_ref[1], a3_ref[...])
    square_terms(5, gpair_ref[0], a3_ref[...])
    square_terms(4, e2_ref[...], o_ref[...])
    red.to_sibling(high, 0)
    matrix_terms(0, gh4_ref, a4_ref[...], units, units)
    matrix_terms(1, s4_ref, e4_ref[...], units, units)
    red.to_sibling(high, 1)
    gk_acc[...] = jnp.zeros_like(gk_acc)
    gv_acc[...] = jnp.zeros_like(gv_acc)
    gpos_acc[...] = jnp.zeros_like(gpos_acc)
    gbias[...] = jnp.zeros_like(gbias)
    to_time = lambda j, q, k: remote(grads.at[j, q], heads.at[j, z], h_send.at[j, k], h_recv.at[j, z], g.time(q))
    for i in range(nz):
        if i + 1 < nz:
            probabilities(i + 1).start()
        probabilities(i).wait()
        here = pl.ds(i * rows, rows)
        grads[0, i] = attend_back_block(
            head_size, i, qkv_ref[0, here, :], qkv_ref.at[1], qkv_ref.at[2], pos_ref, bias_ref, prob_buf.at[i % 2],
            go_ref[here, :], gk_acc, gv_acc, gpos_acc, gbias,
        )
        if i == 0:
            red.from_sibling(high, 0)
            red.along("b", high, 0)
        if i == 1:
            red.from_sibling(high, 1)
            red.along("b", high, 1)
            red.along("b", high, 2)
    grads_k = gk_acc[...].T.astype(BF)
    grads_v = gv_acc[...].T.astype(BF)
    for q in range(nz):
        grads[1, q] = grads_k[q * rows : (q + 1) * rows]
        grads[2, q] = grads_v[q * rows : (q + 1) * rows]
    for k in range(1, nz):
        q = lax.rem(z + k, nz)
        for j in range(3):
            copy = to_time(j, q, k)
            copy.start()
            sends.append(copy)
    for j in range(3):
        heads[j, z] = grads[j, z]
    red.along("a", high, 0)
    fine = fine_ref.shape[1]

    def position(i, total):
        table = coarse_ref[0, pl.ds(2 * i, 1), :] * fine_ref[0] + coarse_ref[1, pl.ds(2 * i, 1), :] * fine_ref[1]
        after = coarse_ref[0, pl.ds(2 * i + 1, 1), :] * fine_ref[0] + coarse_ref[1, pl.ds(2 * i + 1, 1), :] * fine_ref[1]
        both = jnp.concatenate([table, after], axis=0).astype(BF)
        return total + dot(gpos_acc[:, pl.ds(pl.multiple_of(i * 2 * fine, 2 * fine), 2 * fine)].astype(BF), both, NN)

    gpos = lax.fori_loop(0, coarse_ref.shape[1] // 2, position, jnp.zeros((cols, width), F32)).astype(BF)
    gsq[pl.ds(3 * per, per)] = jnp.zeros((per, 2, sq_rows, width), BF)
    pieces = cols // sq_rows
    for i in range(pieces):
        piece = z * pieces + i
        gsq[3 * per + piece // 2, piece % 2] = gpos[i * sq_rows : (i + 1) * sq_rows]
    gains = gains_ref[...]
    loads[0].wait()
    grad_norm = jnp.zeros((rows, width), F32)
    for j in range(3):
        for k in range(1, nz):
            q = lax.rem(z + k, nz)
            arrived(heads.at[j, q], h_recv.at[j, q])
        full = jnp.concatenate([heads[j, q] for q in range(nz)], axis=1)
        gqkv[j] = full
        grad_norm = grad_norm + dot(full, wqkv[pl.ds(j * width, width), :], NN)
    for j in range(3):
        square_terms(j, gqkv[j], a2_ref[...])
    red.to_sibling(low, 0)
    resid1 = x1_ref[...]
    grad_add, gain1, shift1 = norm_backward(resid1, gains, 1, grad_norm)
    grad1 = g2_ref[...] + grad_add
    half1 = (0.5 * grad1).astype(BF)
    loads[1].wait()
    loads[2].wait()
    red.along("a", high, 1)
    grad_norm = module_backward(half1, up, down, h1_ref, gh1)
    red.from_sibling(low, 0)
    red.along("b", low, 0)
    matrix_terms(0, gh1, a1_ref[...], 0, units)
    matrix_terms(1, s1_ref, half1, 0, units)
    red.to_sibling(low, 1)
    red.along("a", high, 2)
    grad_add, gain0, shift0 = norm_backward(x_ref[...].astype(F32), gains, 0, grad_norm)
    away = jnp.logical_not(g.at_home())
    gx_buf[...] = (grad1 + grad_add).astype(BF)
    home = remote(gx_buf, gx_in, gx_sem.at[0], gx_sem.at[1], g.owner())
    pl.when(away)(lambda: home.start())
    small[...] = jnp.zeros_like(small)
    small[0:1, :] = gain0
    small[1:2, :] = shift0
    small[2:3, :] = gain1
    small[3:4, :] = shift1
    small[4:10, :] = some_ref[0:6, :]
    small[10:12, pl.ds(pl.multiple_of(z * cols, cols), cols)] = gbias[...]
    small[12:14, :] = some_ref[6:8, :]
    small[14 : 14 + gtaps_ref.shape[0], :] = gtaps_ref[...]
    meeting = Meeting(g, sbuf, s_send, s_recv)
    meeting.start(0, small[...])
    red.from_sibling(low, 1)
    red.along("b", low, 1)
    red.along("b", low, 2)
    red.along("a", low, 0)
    meeting.start(1, meeting.total(0))
    red.along("z", high, 0)
    red.along("z", high, 1)
    red.along("a", low, 1)
    red.along("z", low, 0)
    meeting.start(2, meeting.total(1))
    red.along("z", high, 2)
    red.along("a", low, 2)
    red.along("z", low, 1)
    meeting.start(3, meeting.total(2))
    red.along("z", low, 2)
    for part in range(3):
        red.last(part)
    me = g.chip(g.z, g.a, g.b)
    d = 1 - c
    half = ud_out.shape[1]
    at = lambda k: pl.ds(pl.multiple_of(me * 2 * half + k * half, half), half)
    fin_send_buf[...] = gud[c, at(d), :]
    swap = remote(fin_send_buf, fin, fin_send, fin_recv, g.sibling())
    swap.start()
    ud_out[c] = gud[c, at(c), :].astype(F32)
    sq_out[...] = gsq[me, c].astype(F32)
    small_out[...] = meeting.total(3)
    for planes in (high, low):
        for part in range(3):
            for axis in "baz":
                red.along(axis, planes, part, True)
        for kind in range(2):
            for q in planes:
                red.sibling_copy(q, kind).wait_send()
    for copy in sends + meeting.sends:
        copy.wait_send()

    @pl.when(away)
    def _():
        home.wait()
        gx_ref[...] = gx_in[...].astype(F32)

    @pl.when(g.at_home())
    def _():
        gx_ref[...] = gx_buf[...].astype(F32)

    swap.wait()
    ud_out[d] = fin[...].astype(F32)


def back(qkv, pos, biases, grad_out, prob, head_size, coarse, fine, gains, signal, resid1, grad2, first, second, squares, some, gtaps, ud_full, sq_full):
    rows, width = signal.shape
    nz, nf = lax.axis_size("seq"), lax.axis_size("fsdp")
    chips = nz * nf // 2
    plane = nf // 2
    side = math.isqrt(plane)
    na, nb = (side, side) if side * side == plane else (plane, 1)
    cols = width // nz
    units = ud_full.shape[1] // 2
    own = ud_full.shape[1] // (2 * chips)
    block = 3 * own
    most = max(nz, na, nb, 2)
    tall = -(-(14 + gtaps.shape[0]) // 8) * 8
    vmem = pl.BlockSpec(memory_space=pltpu.VMEM)
    hbm = pl.BlockSpec(memory_space=pl.ANY)
    shape = jax.ShapeDtypeStruct
    dma = pltpu.SemaphoreType.DMA
    frames = rows * nz
    heads = cols // head_size
    operands = (qkv, pos, biases, grad_out, coarse, fine, gains, signal, resid1, grad2, *first, *second, *squares, some, gtaps)
    places = lambda n: n + 1 if n > 2 else 1
    slots = {"b": places(nb) * na * nz, "a": places(na) * nz, "z": places(nz)}
    return pl.pallas_call(
        lambda *refs: back_kernel(head_size, *refs),
        name="back",
        out_shape=(
            shape((rows, width), F32),
            shape((2, own, width), F32),
            shape((own, width), F32),
            shape((tall, width), F32),
        ),
        in_specs=[vmem] * len(operands) + [hbm] * 3,
        out_specs=[vmem] * 4,
        scratch_shapes=[
            pltpu.VMEM((2, heads, rows, frames), BF),
            pltpu.VMEM((cols, frames), F32),
            pltpu.VMEM((cols, frames), F32),
            pltpu.VMEM((cols, 2 * frames), F32),
            pltpu.VMEM((2, cols), F32),
            pltpu.VMEM((3, nz, rows, cols), BF),
            dma((2,)),
            pltpu.VMEM((3 * width, width), BF),
            pltpu.VMEM((3, nz, rows, cols), BF),
            pltpu.VMEM((3, rows, width), BF),
            pltpu.VMEM((rows, units), BF),
            pltpu.VMEM((tall, width), F32),
            pltpu.VMEM((2, 2 * units, width), BF),
            pltpu.VMEM((chips, 2, own, width), BF),
            pltpu.VMEM((2 * units, width), BF),
            pltpu.VMEM((chips, own, width), BF),
            pltpu.VMEM((slots["b"], block, width), BF),
            pltpu.VMEM((slots["a"], block, width), BF),
            pltpu.VMEM((slots["z"], block, width), BF),
            pltpu.VMEM((4, most, tall, width), F32),
            pltpu.VMEM((own, width), BF),
            pltpu.VMEM((own, width), BF),
            pltpu.VMEM((rows, width), BF),
            pltpu.VMEM((rows, width), BF),
            dma((2,)),
            dma((3,)),
            dma((3, nz)),
            dma((3, nz)),
            dma((2, nz)),
            dma((2, nz)),
            dma((2, 3, slots["b"])),
            dma((3, slots["b"])),
            dma((2, 3, slots["a"])),
            dma((3, slots["a"])),
            dma((2, 3, slots["z"])),
            dma((3, slots["z"])),
            dma((4, most)),
            dma((4, most)),
            dma,
            dma,
        ],
        compiler_params=pltpu.CompilerParams(
            collective_id=7, has_side_effects=True, vmem_limit_bytes=61000 * 1024
        ),
    )(*operands, prob, ud_full, sq_full)


def gathered(square, upward, downward, vectors, kernel, signal, cotangent, lengths):
    share = vectors.shape[1]
    small_rows = vectors.shape[0] + kernel.shape[0]
    small = jnp.concatenate([vectors, kernel], axis=0).astype(BF).reshape(-1)
    tall = -(-small.shape[0] // (16 * LANES)) * 16
    small = jnp.pad(small, (0, tall * LANES - small.shape[0])).reshape(tall, LANES)
    length = jnp.broadcast_to(lengths.astype(F32)[:, None], (8, LANES))
    matrices, squares, smalls, signal, cotangent, length = gather_weights(
        jnp.stack([upward, downward]).astype(BF), square.astype(BF), small, signal, cotangent, length
    )
    devices = smalls.shape[0] * 2
    smalls = smalls.reshape(devices, tall * LANES)[:, : small_rows * share]
    smalls = smalls.reshape(devices, small_rows, share).transpose(1, 0, 2)
    smalls = smalls.reshape(small_rows, devices * share)
    split = vectors.shape[0]
    return (
        matrices,
        squares.reshape(devices * square.shape[0], square.shape[1]),
        smalls[:split],
        smalls[split:],
        signal,
        cotangent,
        length,
    )


def per_device(
    inputs,
    cotangent,
    lengths,
    square,
    upward,
    downward,
    vectors,
    kernel,
    square_momentum,
    square_variance,
    upward_momentum,
    upward_variance,
    downward_momentum,
    downward_variance,
    vectors_momentum,
    vectors_variance,
    kernel_momentum,
    kernel_variance,
):
    model_width = inputs.shape[2]
    frame_count = inputs.shape[1]
    groups = lax.axis_size("seq")
    seq_place = lax.axis_index("seq")
    seq_frames = frame_count * groups
    head_cols = model_width // groups
    slice_place = seq_place % (groups // 2) * 2 + lax.axis_index("fsdp") % 2
    col_start = slice_place * head_cols
    head_size = D // H
    coarse, fine = position_tables(seq_frames, model_width)
    full_ud, full_sq, full_vec, full_kern, signal, cotangent_here, length = gathered(
        square, upward, downward, vectors, kernel, inputs[0], cotangent[0], lengths
    )
    small_params = full_vec.astype(jnp.float32)
    conv_taps = full_kern.astype(jnp.float32)
    resid1, normed1, hidden1, active1, normed2, heads, pos_heads = front(
        signal, small_params, coarse, fine, full_ud, full_sq
    )
    query_head, key_head, value_head = heads[0], heads[1], heads[2]
    biases = lax.dynamic_slice_in_dim(small_params[10:12], col_start, head_cols, 1)
    attended, prob = attend_heads(
        query_head, key_head, value_head, pos_heads, biases, length, head_size
    )
    (
        layer_output, grad_res2, grad_out_head, out_time, grad_att_b, normed3, grad_pair, grad_conv_b, swish_b, normed4,
        active4, grad_hidden4, half4, small_grads, grad_taps,
    ) = middle(length, attended, resid1, cotangent_here, small_params, conv_taps, full_ud, full_sq)
    layer_output = layer_output[None]
    input_grad, matrix_grads, square_grad, small_sums = back(
        heads, pos_heads, biases, grad_out_head, prob, head_size, coarse, fine, small_params,
        signal, resid1, grad_res2, (normed1, hidden1, active1, normed2), (normed4, active4, grad_hidden4, half4),
        (out_time, grad_att_b, normed3, grad_pair, grad_conv_b, swish_b), small_grads, grad_taps, full_ud, full_sq,
    )
    input_grad = input_grad[None]
    upward_grad, downward_grad = matrix_grads[0], matrix_grads[1]
    place = seq_place * lax.axis_size("fsdp") + lax.axis_index("fsdp")
    share = vectors.shape[1]
    small_own = lax.dynamic_slice_in_dim(small_sums, place * share, share, 1)
    vectors_grad = small_own[: vectors.shape[0]]
    kernel_grad = small_own[vectors.shape[0] : vectors.shape[0] + kernel.shape[0]]
    square_next, momentum_square, variance_square = adam_step(
        square, square_grad, square_momentum, square_variance, DECAY_RATE
    )
    upward_next, momentum_upward, variance_upward = adam_step(
        upward, upward_grad, upward_momentum, upward_variance, DECAY_RATE
    )
    downward_next, momentum_downward, variance_downward = adam_step(
        downward, downward_grad, downward_momentum, downward_variance, DECAY_RATE
    )
    vectors_next, momentum_vectors, variance_vectors = adam_step(
        vectors, vectors_grad, vectors_momentum, vectors_variance, 0.0
    )
    kernel_next, momentum_kernel, variance_kernel = adam_step(
        kernel, kernel_grad, kernel_momentum, kernel_variance, DECAY_RATE
    )
    return (
        layer_output,
        input_grad,
        square_grad,
        upward_grad,
        downward_grad,
        vectors_grad,
        kernel_grad,
        square_next,
        upward_next,
        downward_next,
        vectors_next,
        kernel_next,
        momentum_square,
        variance_square,
        momentum_upward,
        variance_upward,
        momentum_downward,
        variance_downward,
        momentum_vectors,
        variance_vectors,
        momentum_kernel,
        variance_kernel,
    )


def solution(mesh):
    return jax.shard_map(
        per_device,
        mesh=mesh,
        in_specs=(
            P("fsdp", "seq", None),
            P("fsdp", "seq", None),
            P("fsdp"),
            P(("seq", "fsdp"), None),
            P(("seq", "fsdp"), None),
            P(("seq", "fsdp"), None),
            P(None, ("seq", "fsdp")),
            P(None, ("seq", "fsdp")),
            P(("seq", "fsdp"), None),
            P(("seq", "fsdp"), None),
            P(("seq", "fsdp"), None),
            P(("seq", "fsdp"), None),
            P(("seq", "fsdp"), None),
            P(("seq", "fsdp"), None),
            P(None, ("seq", "fsdp")),
            P(None, ("seq", "fsdp")),
            P(None, ("seq", "fsdp")),
            P(None, ("seq", "fsdp")),
        ),
        out_specs=(
            P("fsdp", "seq", None),
            P("fsdp", "seq", None),
            P(("seq", "fsdp"), None),
            P(("seq", "fsdp"), None),
            P(("seq", "fsdp"), None),
            P(None, ("seq", "fsdp")),
            P(None, ("seq", "fsdp")),
            P(("seq", "fsdp"), None),
            P(("seq", "fsdp"), None),
            P(("seq", "fsdp"), None),
            P(None, ("seq", "fsdp")),
            P(None, ("seq", "fsdp")),
            P(("seq", "fsdp"), None),
            P(("seq", "fsdp"), None),
            P(("seq", "fsdp"), None),
            P(("seq", "fsdp"), None),
            P(("seq", "fsdp"), None),
            P(("seq", "fsdp"), None),
            P(None, ("seq", "fsdp")),
            P(None, ("seq", "fsdp")),
            P(None, ("seq", "fsdp")),
            P(None, ("seq", "fsdp")),
        ),
        check_vma=False,
    )
```

```python
import math

import jax
import jax.numpy as jnp
from jax import lax
from jax.experimental import pallas as pl
from jax.experimental.pallas import tpu as pltpu
from jax.sharding import PartitionSpec as P

D = 512
H = 8
FF = 2048
ADAM_STEP = 4

LN_EPS = 1e-05
BN_EPS = 1e-05
BETA_ONE = 0.9
BETA_TWO = 0.98
ADAM_EPS = 1e-08
LEARN_RATE = 0.005
DECAY_RATE = 0.01


def position_tables(seq_frames, model_width):
    fine = math.gcd(2 * seq_frames, 64)
    column = jnp.arange(model_width)
    frequency = jnp.exp(-math.log(10000.0) * 2.0 * (column // 2).astype(jnp.float32) / model_width)
    coarse_at = (seq_frames - 1 - fine * jnp.arange(2 * seq_frames // fine)).astype(jnp.float32)
    coarse_phase = coarse_at[:, None] * frequency[None, :]
    fine_phase = jnp.arange(fine).astype(jnp.float32)[:, None] * frequency[None, :]
    even = (column % 2 == 0)[None, :]
    sine, cosine = jnp.sin(coarse_phase), jnp.cos(coarse_phase)
    with_cosine = jnp.where(even, sine, cosine)
    with_sine = jnp.where(even, -cosine, sine)
    return jnp.stack([with_cosine, with_sine]), jnp.stack([jnp.cos(fine_phase), jnp.sin(fine_phase)])


def adam_step(weight, gradient, first_mom, second_mom, decay):
    first_new = BETA_ONE * first_mom + (1.0 - BETA_ONE) * gradient
    second_new = BETA_TWO * second_mom + (1.0 - BETA_TWO) * gradient * gradient
    fix_one = 1.0 - BETA_ONE**ADAM_STEP
    fix_two = 1.0 - BETA_TWO**ADAM_STEP
    update = first_new / fix_one / (jnp.sqrt(second_new / fix_two) + ADAM_EPS)
    return (weight - LEARN_RATE * (update + decay * weight), first_new, second_new)


MESH = pl.DeviceIdType.MESH
BF = jnp.bfloat16
F32 = jnp.float32
LANES = 128


class Grid:
    def __init__(self):
        self.nz = lax.axis_size("seq")
        self.nf = lax.axis_size("fsdp")
        plane = self.nf // 2
        side = math.isqrt(plane)
        self.z = lax.axis_index("seq")
        f = lax.axis_index("fsdp")
        self.core = f % 2
        if side * side == plane:
            self.na = self.nb = side
            self.step_a = 2 + self.core * (2 * side - 2)
            self.step_b = 2 * side - self.core * (2 * side - 2)
        else:
            self.na, self.nb = plane, 1
            self.step_a, self.step_b = 2, self.nf
        self.f = f
        self.a = (f // self.step_a) % self.na
        self.b = (f // self.step_b) % self.nb
        self.plane = plane
        self.chips = plane * self.nz

        self.half = self.nz // 2
        self.t = (self.z % self.half) * 2 + self.core
        self.column = f - self.core

    def time(self, q):
        return (self.z - self.z % self.half + q // 2, self.column + q % 2)

    def owner(self):
        return (self.t, self.column + self.z // self.half)

    def worker(self):
        return (self.core * self.half + self.z // 2, self.column + self.z % 2)

    def at_home(self):
        return jnp.logical_and(self.t == self.z, self.z // self.half == self.core)

    def chip(self, z, a, b):
        return z * self.plane + (a * self.step_a + b * self.step_b) // 2

    def device(self, z, a, b):
        return (z, a * self.step_a + b * self.step_b + self.core)

    def sibling(self):
        return (self.z, self.f + 1 - 2 * self.core)

    def up(self, axis):
        return self.device(self.z + (axis == "z"), self.a + (axis == "a"), self.b + (axis == "b"))

    def down(self, axis):
        return self.device(self.z - (axis == "z"), self.a - (axis == "a"), self.b - (axis == "b"))

    def line(self, axis):
        return {
            "c": (self.core, 2, lambda q: (self.z, self.f - self.core + q)),
            "a": (self.a, self.na, lambda q: self.device(self.z, q, self.b)),
            "b": (self.b, self.nb, lambda q: self.device(self.z, self.a, q)),
            "z": (self.z, self.nz, lambda q: self.device(q, self.a, self.b)),
        }[axis]

    def place(self, axis):
        return {"z": (self.z, self.nz), "a": (self.a, self.na), "b": (self.b, self.nb)}[axis]


def greet_mover(g, barrier, source):
    @pl.when(jnp.logical_not(g.at_home()))
    def _():
        pl.semaphore_signal(barrier, inc=1, device_id=source, device_id_type=MESH)

    return 1 - g.at_home().astype(jnp.int32)


def merge_moments(first_op, second_op):
    count = first_op[0:1] + second_op[0:1]
    share = second_op[0:1] / jnp.maximum(count, 1.0)
    gap = second_op[1:2] - first_op[1:2]
    mean = first_op[1:2] + gap * share
    squares = first_op[2:3] + second_op[2:3] + gap * gap * (first_op[0:1] * share)
    return jnp.concatenate([count, mean, squares, first_op[3:]], axis=0)


NT = (((1,), (1,)), ((), ()))
TN = (((0,), (0,)), ((), ()))
NN = (((1,), (0,)), ((), ()))


def dot(first_op, second_op, dims):
    return lax.dot_general(first_op, second_op, dims, preferred_element_type=F32)


def keep_head(value, h, head_size):
    lane = lax.broadcasted_iota(jnp.int32, value.shape, 1)
    return jnp.where(lane // head_size == h, value, jnp.zeros_like(value))


def attend_block(head_size, i, query_b, k_ref, v_ref, pos_ref, bias, len_ref, prob_ref):
    rows, cols = query_b.shape
    frames = k_ref.shape[0]
    width = rows + frames
    query = query_b.astype(F32)
    content = (query + bias[0:1, :]).astype(BF)
    positional = (query + bias[1:2, :]).astype(BF)
    window = pos_ref[pl.ds(pl.multiple_of(frames - rows - i * rows, rows), width), :]
    live = lax.broadcasted_iota(jnp.int32, (rows, frames), 1).astype(F32) < len_ref[0:1, 0:1]
    out = jnp.zeros((rows, cols), F32)
    for h in range(cols // head_size):
        direct = dot(keep_head(content, h, head_size), k_ref[...], NT)
        spread = dot(keep_head(positional, h, head_size), window, NT)
        shifted = pltpu.roll(spread, width - rows + 1, 1, stride=1, stride_axis=0)[:, :frames]
        score = jnp.where(live, (direct + shifted) * (1.0 / math.sqrt(head_size)), -1e30)
        top = jnp.max(score, axis=-1, keepdims=True)
        power = jnp.exp(score - top)
        prob_b = (power * (1.0 / jnp.sum(power, axis=-1, keepdims=True))).astype(BF)
        prob_ref[h] = prob_b
        out = out + keep_head(dot(prob_b, v_ref[...], NN), h, head_size)
    return out.astype(BF)


def attend_back_block(head_size, i, query_b, k_ref, v_ref, pos_ref, bias, prob_ref, grad_heads, gk_acc, gv_acc, gpos_acc, gbias):
    rows, cols = query_b.shape
    frames = k_ref.shape[0]
    width = rows + frames
    query = query_b.astype(F32)
    content = (query + bias[0:1, :]).astype(BF)
    positional = (query + bias[1:2, :]).astype(BF)
    down = lax.broadcasted_iota(jnp.int32, (rows, rows), 0)
    across = lax.broadcasted_iota(jnp.int32, (rows, rows), 1)
    turn = jnp.where(down + across == rows - 1, 1.0, 0.0).astype(BF)
    positional_turned = dot(turn, positional, NN).astype(BF)
    here = pl.ds(pl.multiple_of(frames - rows - i * rows, rows), width)
    window = pos_ref[here, :]
    grad_content = jnp.zeros((rows, cols), F32)
    grad_position = jnp.zeros((rows, cols), F32)
    for h in range(cols // head_size):
        grad_out = keep_head(grad_heads, h, head_size)
        prob_b = prob_ref[h]
        prob = prob_b.astype(F32)
        grad_prob = dot(grad_out, v_ref[...], NT)
        delta = jnp.sum(prob * grad_prob, axis=-1, keepdims=True)
        score_b = (prob * (grad_prob - delta) * (1.0 / math.sqrt(head_size))).astype(BF)
        grad_content = grad_content + keep_head(dot(score_b, k_ref[...], NN), h, head_size)
        gk_acc[...] += dot(keep_head(content, h, head_size), score_b, TN)
        gv_acc[...] += dot(grad_out, prob_b, TN)
        wide = jnp.concatenate([dot(turn, score_b, NN), jnp.zeros((rows, width - frames), F32)], axis=1)
        spread = pltpu.roll(wide, 0, 1, stride=1, stride_axis=0).astype(BF)
        grad_position = grad_position + keep_head(dot(spread, window, NN), h, head_size)
        gpos_acc[:, here] += dot(keep_head(positional_turned, h, head_size), spread, TN)
    high = grad_position.astype(BF)
    low = (grad_position - high.astype(F32)).astype(BF)
    grad_position = dot(turn, high, NN) + dot(turn, low, NN)
    gbias[0:1, :] += jnp.sum(grad_content, axis=0, keepdims=True)
    gbias[1:2, :] += jnp.sum(grad_position, axis=0, keepdims=True)
    return (grad_content + grad_position).astype(BF)

def normalize(value):
    mean = jnp.mean(value, axis=-1, keepdims=True)
    centred = value - mean
    spread = lax.rsqrt(jnp.mean(centred * centred, axis=-1, keepdims=True) + LN_EPS)
    return centred * spread, spread


def norm_forward(value, gains, k):
    unit, _ = normalize(value)
    return (unit * gains[2 * k : 2 * k + 1] + gains[2 * k + 1 : 2 * k + 2]).astype(BF)


def norm_backward(value, gains, k, upstream):
    unit, spread = normalize(value)
    inner = upstream * gains[2 * k : 2 * k + 1]
    along = jnp.mean(inner * unit, axis=-1, keepdims=True)
    grad = spread * (inner - jnp.mean(inner, axis=-1, keepdims=True) - unit * along)
    gain = jnp.sum(upstream * unit, axis=0, keepdims=True)
    return grad, gain, jnp.sum(upstream, axis=0, keepdims=True)


def sigmoid(value):
    return 1.0 / (1.0 + jnp.exp(-value))


def module_forward(normed, up_ref, down_ref, hidden_ref, active_ref):
    units, width = up_ref.shape
    step = min(512, units)

    def chunk(j, total):
        here = pl.ds(pl.multiple_of(j * step, step), step)
        hidden = dot(normed, up_ref[here, :], NT)
        active = (hidden * sigmoid(hidden)).astype(BF)
        hidden_ref[:, here] = hidden.astype(hidden_ref.dtype)
        active_ref[:, here] = active
        return total + dot(active, down_ref[here, :], NN)

    return lax.fori_loop(0, units // step, chunk, jnp.zeros((normed.shape[0], width), F32))


def module_backward(upstream_b, up_ref, down_ref, hidden_ref, grad_ref):
    units, width = up_ref.shape
    step = min(512, units)

    def chunk(j, total):
        here = pl.ds(pl.multiple_of(j * step, step), step)
        hidden = hidden_ref[:, here].astype(F32)
        sigma = sigmoid(hidden)
        slope = sigma * (1.0 + hidden * (1.0 - sigma))
        grad = (dot(upstream_b, down_ref[here, :], NT) * slope).astype(BF)
        grad_ref[:, here] = grad
        return total + dot(grad, up_ref[here, :], NN)

    return lax.fori_loop(0, units // step, chunk, jnp.zeros((upstream_b.shape[0], width), F32))


def greet_lines(g, axes, source=None):
    barrier = pltpu.get_barrier_semaphore()
    total = g.nz - 1
    for k in range(1, g.nz):
        pl.semaphore_signal(barrier, inc=1, device_id=g.time(lax.rem(g.t + k, g.nz)), device_id_type=MESH)
    if source is not None:
        total = total + greet_mover(g, barrier, source)
    for axis in axes:
        p, n, device = g.line(axis)
        for k in range(1, n):
            pl.semaphore_signal(barrier, inc=1, device_id=device(lax.rem(p + k, n)), device_id_type=MESH)
            total += 1
    pl.semaphore_wait(barrier, total)


def remote(src, dst, send, recv, device):
    return pltpu.make_async_remote_copy(
        src_ref=src, dst_ref=dst, send_sem=send, recv_sem=recv, device_id=device, device_id_type=MESH
    )


def arrived(ref, sem):
    pltpu.make_async_copy(ref, ref, sem).wait()


def meet_levels(g, value, merge, buf, send_sem, recv_sem):
    sends = []
    for level, axis in enumerate("cabz"):
        p, n, device = g.line(axis)
        if n == 1:
            continue
        buf[level, p] = value
        for k in range(1, n):
            copy = remote(buf.at[level, p], buf.at[level, p], send_sem.at[level, k], recv_sem.at[level, p], device(lax.rem(p + k, n)))
            copy.start()
            sends.append(copy)
        for k in range(1, n):
            q = lax.rem(p + k, n)
            arrived(buf.at[level, q], recv_sem.at[level, q])
        value = buf[level, 0]
        for q in range(1, n):
            value = merge(value, buf[level, q])
    return value, sends


HALO = 16


def swap_edges(g, body, low, high, send_sem, recv_sem, pad):
    rows = body.shape[0]
    p, n = g.t, g.nz
    up = remote(body.at[pl.ds(rows - HALO, HALO)], low, send_sem.at[0], recv_sem.at[0], g.time(p + 1))
    down = remote(body.at[pl.ds(0, HALO)], high, send_sem.at[1], recv_sem.at[1], g.time(p - 1))
    pl.when(p < n - 1)(lambda: up.start())
    pl.when(p > 0)(lambda: down.start())
    pad[pl.ds(HALO, rows), :] = body[...].astype(F32)

    def fill(at, ref, sem, there):
        @pl.when(there)
        def _():
            arrived(ref, sem)
            pad[pl.ds(at, HALO), :] = ref[...].astype(F32)

        @pl.when(jnp.logical_not(there))
        def _():
            pad[pl.ds(at, HALO), :] = jnp.zeros((HALO, pad.shape[1]), F32)

    fill(0, low, recv_sem.at[0], p > 0)
    fill(HALO + rows, high, recv_sem.at[1], p < n - 1)

    def finish():
        pl.when(p < n - 1)(lambda: up.wait_send())
        pl.when(p > 0)(lambda: down.wait_send())

    return finish


def middle_kernel(taps, len_ref, att_ref, x1_ref, cot_ref, gains_ref, ud_hbm, sq_hbm,
                  y_ref, g2_ref, go_ref, o_ref, e2_ref, a3_ref, gpair_ref, e3_ref, sw_ref, a4_ref, s4_ref, gh4_ref, e4_ref,
                  small_ref, gtaps_ref,
                  up, down, wsq, o_buf, go_buf, glu_b, gc_b, low1, high1, low2, high2, pad_glu, pad_gc, h4, c_ref, y_buf, y_sem,
                  buf1, buf2, load_sem, a_send, a_recv, b_send, b_recv, h_send, h_recv, m_send, m_recv):
    g = Grid()
    z, nz = g.t, g.nz
    rows, width = x1_ref.shape
    cols = width // nz
    units = up.shape[0]
    rim = (taps - 1) // 2
    loads = [
        pltpu.make_async_copy(sq_hbm.at[pl.ds(4 * width, 4 * width)], wsq, load_sem.at[0]),
        pltpu.make_async_copy(ud_hbm.at[0, pl.ds(units, units)], up, load_sem.at[1]),
        pltpu.make_async_copy(ud_hbm.at[1, pl.ds(units, units)], down, load_sem.at[2]),
    ]
    for load in loads:
        load.start()
    greet_lines(g, "cabz", g.worker())
    sends = []
    for k in range(1, nz):
        q = lax.rem(z + k, nz)
        copy = remote(att_ref.at[pl.ds(q * rows, rows)], o_buf.at[z], a_send.at[k], a_recv.at[z], g.time(q))
        copy.start()
        sends.append(copy)
    o_buf[z] = att_ref[pl.ds(pl.multiple_of(z * rows, rows), rows), :]
    gains = gains_ref[...]
    frame = z * rows + lax.broadcasted_iota(jnp.int32, (rows, 1), 0)
    live = jnp.where(frame.astype(F32) < len_ref[0:1, 0:1], 1.0, 0.0)
    loads[0].wait()
    weight = lambda k: wsq[pl.ds((k - 4) * width, width), :]
    for k in range(1, nz):
        q = lax.rem(z + k, nz)
        arrived(o_buf.at[q], a_recv.at[q])
    out = jnp.concatenate([o_buf[q] for q in range(nz)], axis=1)
    o_ref[...] = out
    resid2 = x1_ref[...] + dot(out, weight(4), NT)
    normed3 = norm_forward(resid2, gains, 2)
    a3_ref[...] = normed3
    value = dot(normed3, weight(5), NT)
    gate = sigmoid(dot(normed3, weight(6), NT))
    glu_b[...] = (value * gate * live).astype(BF)
    done1 = swap_edges(g, glu_b, low1, high1, h_send.at[0], h_recv.at[0], pad_glu)
    for at in range(0, width, LANES):
        lanes = pl.ds(at, LANES)
        total = jnp.zeros((rows, LANES), F32)
        for m in range(taps):
            total = total + gains_ref[14 + m : 15 + m, lanes] * pad_glu[pl.ds(HALO - rim + m, rows), lanes]
        c_ref[:, lanes] = total
    conv = c_ref[...]
    count = jnp.sum(live, axis=0, keepdims=True)
    mean = jnp.sum(live * conv, axis=0, keepdims=True) / jnp.maximum(count, 1.0)
    squares = jnp.sum(live * (conv - mean) * (conv - mean), axis=0, keepdims=True)
    moments = jnp.concatenate([jnp.broadcast_to(count, mean.shape), mean, squares, jnp.zeros((5, width), F32)], axis=0)
    moments, more = meet_levels(g, moments, merge_moments, buf1, m_send.at[0], m_recv.at[0])
    sends += more
    total_frames = moments[0:1]
    inv_std = lax.rsqrt(moments[2:3] / total_frames + BN_EPS)
    centre = moments[1:2]
    centred = c_ref[...] - centre
    zed = centred * inv_std
    bn_val = gains[12:13] * zed + gains[13:14]
    swish = (bn_val * sigmoid(bn_val)).astype(BF)
    sw_ref[...] = swish
    resid3 = resid2 + dot(swish, weight(7), NT)
    normed4 = norm_forward(resid3, gains, 3)
    a4_ref[...] = normed4
    loads[1].wait()
    loads[2].wait()
    resid4 = resid3 + 0.5 * module_forward(normed4, up, down, h4, s4_ref)
    y_buf[...] = norm_forward(resid4, gains, 4)
    away = jnp.logical_not(g.at_home())
    home = remote(y_buf, y_ref, y_sem.at[0], y_sem.at[1], g.owner())
    pl.when(away)(lambda: home.start())

    @pl.when(g.at_home())
    def _():
        y_ref[...] = y_buf[...]

    grad4, gain4, shift4 = norm_backward(resid4, gains, 4, cot_ref[...].astype(F32))
    half4 = (0.5 * grad4).astype(BF)
    e4_ref[...] = half4
    grad_norm, gain3, shift3 = norm_backward(resid3, gains, 3, module_backward(half4, up, down, h4, gh4_ref))
    grad3 = grad4 + grad_norm
    e3 = grad3.astype(BF)
    e3_ref[...] = e3
    sigma = sigmoid(bn_val)
    grad_bn = dot(e3, weight(7), NN) * (sigma * (1.0 + bn_val * (1.0 - sigma)))
    gamma = jnp.sum(grad_bn * zed, axis=0, keepdims=True)
    beta = jnp.sum(grad_bn, axis=0, keepdims=True)
    grad_zed = grad_bn * gains[12:13]
    sum_one = jnp.sum(grad_zed, axis=0, keepdims=True)
    sum_two = jnp.sum(grad_zed * centred, axis=0, keepdims=True)
    sums = jnp.concatenate([sum_one, sum_two, jnp.zeros((6, width), F32)], axis=0)
    sums, more = meet_levels(g, sums, lambda x, y: x + y, buf2, m_send.at[1], m_recv.at[1])
    sends += more
    offset = inv_std * sums[0:1] + inv_std * inv_std * inv_std * sums[1:2] * centred
    gc_b[...] = (inv_std * grad_zed - live / total_frames * offset).astype(BF)
    done2 = swap_edges(g, gc_b, low2, high2, h_send.at[1], h_recv.at[1], pad_gc)
    for at in range(0, width, LANES):
        lanes = pl.ds(at, LANES)
        total = jnp.zeros((rows, LANES), F32)
        upstream = pad_gc[pl.ds(HALO, rows), lanes]
        for m in range(taps):
            total = total + gains_ref[14 + m : 15 + m, lanes] * pad_gc[pl.ds(HALO + rim - m, rows), lanes]
            gtaps_ref[m : m + 1, lanes] = jnp.sum(
                upstream * pad_glu[pl.ds(HALO - rim + m, rows), lanes], axis=0, keepdims=True
            )
        c_ref[:, lanes] = total
    grad_glu = c_ref[...] * live
    gv5 = (grad_glu * gate).astype(BF)
    gv6 = (grad_glu * value * gate * (1.0 - gate)).astype(BF)
    gpair_ref[0] = gv5
    gpair_ref[1] = gv6
    grad_norm, gain2, shift2 = norm_backward(
        resid2, gains, 2, dot(gv5, weight(5), NN) + dot(gv6, weight(6), NN)
    )
    grad2 = grad3 + grad_norm
    g2_ref[...] = grad2
    e2 = grad2.astype(BF)
    e2_ref[...] = e2
    grad_out = dot(e2, weight(4), NN).astype(BF)
    for q in range(nz):
        go_buf[q] = grad_out[:, q * cols : (q + 1) * cols]
    for k in range(1, nz):
        q = lax.rem(z + k, nz)
        copy = remote(go_buf.at[q], go_ref.at[pl.ds(z * rows, rows)], b_send.at[k], b_recv.at[z], g.time(q))
        copy.start()
        sends.append(copy)
    go_ref[pl.ds(pl.multiple_of(z * rows, rows), rows), :] = go_buf[z]
    small_ref[...] = jnp.concatenate([gain2, shift2, gain3, shift3, gain4, shift4, gamma, beta], axis=0)
    for k in range(1, nz):
        q = lax.rem(z + k, nz)
        arrived(go_ref.at[pl.ds(q * rows, rows)], b_recv.at[q])
    pl.when(away)(lambda: home.wait())
    done1()
    done2()
    for copy in sends:
        copy.wait_send()


def middle(length, attended, resid1, cotangent, gains, taps, ud_full, sq_full):
    rows, width = resid1.shape
    nz, nf = lax.axis_size("seq"), lax.axis_size("fsdp")
    frames, cols = rows * nz, width // nz
    units = ud_full.shape[1] // 2
    most = max(nz, nf // 2)
    vmem = pl.BlockSpec(memory_space=pltpu.VMEM)
    hbm = pl.BlockSpec(memory_space=pl.ANY)
    shape = jax.ShapeDtypeStruct
    dma = pltpu.SemaphoreType.DMA
    row = shape((rows, width), BF)
    return pl.pallas_call(
        lambda *refs: middle_kernel(taps, *refs),
        name="middle",
        out_shape=(
            row,
            shape((rows, width), F32),
            shape((frames, cols), BF),
            row,
            row,
            row,
            shape((2, rows, width), BF),
            row,
            row,
            row,
            shape((rows, units), BF),
            shape((rows, units), BF),
            row,
            shape((8, width), F32),
            shape((taps, width), F32),
        ),
        in_specs=[vmem] * 5 + [hbm] * 2,
        out_specs=[vmem] * 15,
        scratch_shapes=[
            pltpu.VMEM((units, width), BF),
            pltpu.VMEM((units, width), BF),
            pltpu.VMEM((4 * width, width), BF),
            pltpu.VMEM((nz, rows, cols), BF),
            pltpu.VMEM((nz, rows, cols), BF),
            pltpu.VMEM((rows, width), BF),
            pltpu.VMEM((rows, width), BF),
        ]
        + [pltpu.VMEM((HALO, width), BF)] * 4
        + [
            pltpu.VMEM((rows + 2 * HALO, width), F32),
            pltpu.VMEM((rows + 2 * HALO, width), F32),
            pltpu.VMEM((rows, units), F32),
            pltpu.VMEM((rows, width), F32),
            pltpu.VMEM((rows, width), BF),
            dma((2,)),
            pltpu.VMEM((4, most, 8, width), F32),
            pltpu.VMEM((4, most, 8, width), F32),
            dma((3,)),
            dma((nz,)),
            dma((nz,)),
            dma((nz,)),
            dma((nz,)),
            dma((2, 2)),
            dma((2, 2)),
            dma((2, 4, most)),
            dma((2, 4, most)),
        ],
        compiler_params=pltpu.CompilerParams(
            collective_id=6, has_side_effects=True, vmem_limit_bytes=56 * 1024 * 1024
        ),
    )(length, attended, resid1, cotangent, gains, ud_full, sq_full)


class Meeting:
    def __init__(self, g, buf, send_sem, recv_sem):
        self.g, self.buf, self.send_sem, self.recv_sem = g, buf, send_sem, recv_sem
        self.sends = []

    def start(self, level, value):
        axis = "cabz"[level]
        p, n, device = self.g.line(axis)
        self.buf[level, p] = value
        for k in range(1, n):
            here = self.buf.at[level, p]
            copy = remote(here, here, self.send_sem.at[level, k], self.recv_sem.at[level, p], device(lax.rem(p + k, n)))
            copy.start()
            self.sends.append(copy)

    def total(self, level):
        p, n, _ = self.g.line("cabz"[level])
        for k in range(1, n):
            q = lax.rem(p + k, n)
            arrived(self.buf.at[level, q], self.recv_sem.at[level, q])
        value = self.buf[level, 0]
        for q in range(1, n):
            value = value + self.buf[level, q]
        return value


class Reduction:
    def __init__(self, g, gud, gsq, sib_ud, sib_sq, sib_sem, rb, ra, rz, sems):
        self.g, self.gud, self.gsq, self.sib_ud, self.sib_sq = g, gud, gsq, sib_ud, sib_sq
        self.sib_send, self.sib_recv = sib_sem
        self.bufs = {"b": rb, "a": ra, "z": rz}
        self.sems = sems
        self.sq_rows = gsq.shape[2]
        self.pair = 2 * self.sq_rows
        self.height = g.plane * self.pair

    def rows(self, t, part):
        return pl.ds(pl.multiple_of(t * self.pair + (part - 1) * self.sq_rows, self.sq_rows), self.sq_rows)

    def own(self, t, part):
        c = self.g.core
        return self.gsq.at[t, c] if part == 0 else self.gud.at[c, self.rows(t, part)]

    def sibling_copy(self, z, kind):
        g = self.g
        d = 1 - g.core
        if kind == 0:
            chips = pl.ds(z * g.plane, g.plane)
            src, dst = self.gsq.at[chips, d], self.sib_sq.at[chips]
        else:
            tall = pl.ds(z * self.height, self.height)
            src, dst = self.gud.at[d, tall], self.sib_ud.at[tall]
        return remote(src, dst, self.sib_send.at[kind, z], self.sib_recv.at[kind, z], g.sibling())

    def to_sibling(self, planes, kind):
        for z in planes:
            self.sibling_copy(z, kind).start()

    def from_sibling(self, planes, kind):
        for z in planes:
            self.sibling_copy(z, kind).wait_recv()

    def add_sibling(self, t, part):
        ref = self.own(t, part)
        ref[...] = ref[...] + (self.sib_sq[t] if part == 0 else self.sib_ud[self.rows(t, part), :])

    def landing(self, axis, slot, part):
        return self.bufs[axis].at[slot, pl.ds(part * self.sq_rows, self.sq_rows)]

    def slot(self, axis, upward, z, a, b, there):
        g = self.g
        p, n = g.place(axis)
        q = {"z": z, "a": a, "b": b}[axis]
        if there:
            p = p + 1 if upward else p - 1
        if upward:
            q = q + 1 - n * (p == n - 1)
        return {"b": (q * g.na + a) * g.nz + z, "a": q * g.nz + z, "z": q}[axis]

    def hop(self, axis, upward, z, a, b, part):
        g = self.g
        slot = self.slot(axis, upward, z, a, b, True)
        sends, recvs = self.sems[axis]
        device = g.up(axis) if upward else g.down(axis)
        src, dst = self.own(g.chip(z, a, b), part), self.landing(axis, slot, part)
        return remote(src, dst, sends.at[1 if upward else 0, part, slot], recvs.at[part, slot], device)

    def take(self, axis, upward, z, a, b, part):
        slot = self.slot(axis, upward, z, a, b, False)
        src, dst = self.landing(axis, slot, part), self.own(self.g.chip(z, a, b), part)
        arrived(src, self.sems[axis][1].at[part, slot])
        dst[...] = dst[...] + src[...]

    def settle(self, axis, z, a, b, part):
        p, n = self.g.place(axis)
        if n > 1:
            pl.when(p > 0)(lambda: self.take(axis, True, z, a, b, part))
            pl.when(p < n - 1)(lambda: self.take(axis, False, z, a, b, part))

    def ready(self, axis, z, a, b, part):
        if axis == "b":
            self.add_sibling(self.g.chip(z, a, b), part)
        else:
            before = {"a": "b", "z": "a"}[axis]
            self.ready(before, z, a, b, part)
            self.settle(before, z, a, b, part)

    def pass_on(self, axis, upward, z, a, b, part, finish):
        p, n = self.g.place(axis)
        if finish:
            self.hop(axis, upward, z, a, b, part).wait_send()
            return
        self.ready(axis, z, a, b, part)
        behind = p > 0 if upward else p < n - 1
        pl.when(behind)(lambda: self.take(axis, upward, z, a, b, part))
        self.hop(axis, upward, z, a, b, part).start()

    def along(self, axis, planes, part, finish=False):
        g = self.g
        p, n = g.place(axis)
        if axis == "z":
            for q in planes:
                pl.when(p < q)(lambda: self.pass_on("z", True, q, g.a, g.b, part, finish))
                pl.when(p > q)(lambda: self.pass_on("z", False, q, g.a, g.b, part, finish))
            return
        step = planes[1] - planes[0] if len(planes) > 1 else 1
        count = len(planes)
        for k in range(n - 1, 0, -1):
            for upward in (True, False):
                q = p + k if upward else p - k

                def act():
                    def body(i, _):
                        plane = planes[0] + step * lax.rem(i, count)
                        if axis == "b":
                            a = lax.rem(g.a + 1 + i // count, g.na)
                            self.pass_on("b", upward, plane, a, q, part, finish)
                        else:
                            self.pass_on("a", upward, plane, q, g.b, part, finish)
                        return 0

                    lax.fori_loop(0, (g.na if axis == "b" else 1) * count, body, 0)

                pl.when(p + k < n if upward else p >= k)(act)

    def last(self, part):
        g = self.g
        self.ready("z", g.z, g.a, g.b, part)
        self.settle("z", g.z, g.a, g.b, part)


def back_kernel(head_size, qkv_ref, pos_ref, go_ref, coarse_ref, fine_ref, gains_ref,
                x_ref, x1_ref, g2_ref, a1_ref, h1_ref, s1_ref, a2_ref,
                a4_ref, s4_ref, gh4_ref, e4_ref, o_ref, e2_ref, a3_ref, gpair_ref, e3_ref, sw_ref, some_ref, gtaps_ref,
                prob_hbm, ud_hbm, sq_hbm,
                gx_ref, ud_out, sq_out, small_out,
                prob_buf, gk_acc, gv_acc, gpos_acc, gbias, grads, prob_sem, wqkv, heads, gqkv, gh1, small, gud, gsq, sib_ud, sib_sq, rb, ra, rz, sbuf, fin_send_buf, fin, gx_buf, gx_in, gx_sem,
                load_sem, h_send, h_recv, sib_send, sib_recv, b_send, b_recv, a_send, a_recv, z_send, z_recv, s_send, s_recv,
                fin_send, fin_recv):
    g = Grid()
    z, nz, c = g.t, g.nz, g.core
    rows, width = x_ref.shape
    cols = width // nz
    units = h1_ref.shape[1]
    frames = qkv_ref.shape[1]
    up, down = gud.at[0, pl.ds(0, units)], gud.at[1, pl.ds(0, units)]
    loads = [
        pltpu.make_async_copy(sq_hbm.at[pl.ds(0, 3 * width)], wqkv, load_sem.at[0]),
        pltpu.make_async_copy(ud_hbm.at[0, pl.ds(0, units)], up, load_sem.at[1]),
        pltpu.make_async_copy(ud_hbm.at[1, pl.ds(0, units)], down, load_sem.at[2]),
    ]

    def probabilities(i):
        return pltpu.make_async_copy(prob_hbm.at[:, pl.ds(i * rows, rows)], prob_buf.at[i % 2], prob_sem.at[i % 2])

    probabilities(0).start()
    for load in loads:
        load.start()
    greet_lines(g, "cabz", g.worker())
    sends = []
    red = Reduction(
        g, gud, gsq, sib_ud, sib_sq, (sib_send, sib_recv), rb, ra, rz,
        {"b": (b_send, b_recv), "a": (a_send, a_recv), "z": (z_send, z_recv)},
    )
    total_rows = gud.shape[1]
    sq_rows = gsq.shape[2]
    high = list(range(nz - 1, nz // 2 - 1, -1))
    low = list(range(0, nz // 2))
    part = 256

    def matrix_terms(color, left_ref, right, first_row, count):
        def body(i, _):
            here = pl.ds(pl.multiple_of(i * part, part), part)
            there = pl.ds(pl.multiple_of(first_row + i * part, part), part)
            gud[color, there, :] = dot(left_ref[:, here], right, TN).astype(BF)
            return 0

        lax.fori_loop(0, count // part, body, 0)

    per = width // sq_rows // 2

    def square_terms(block, left, right):
        sums = dot(left, right, TN).astype(BF).reshape(per, 2, sq_rows, width)
        gsq[pl.ds(block * per, per)] = sums

    square_terms(7, e3_ref[...], sw_ref[...])
    square_terms(6, gpair_ref[1], a3_ref[...])
    square_terms(5, gpair_ref[0], a3_ref[...])
    square_terms(4, e2_ref[...], o_ref[...])
    red.to_sibling(high, 0)
    matrix_terms(0, gh4_ref, a4_ref[...], units, units)
    matrix_terms(1, s4_ref, e4_ref[...], units, units)
    red.to_sibling(high, 1)
    gk_acc[...] = jnp.zeros_like(gk_acc)
    gv_acc[...] = jnp.zeros_like(gv_acc)
    gpos_acc[...] = jnp.zeros_like(gpos_acc)
    gbias[...] = jnp.zeros_like(gbias)
    to_time = lambda j, q, k: remote(grads.at[j, q], heads.at[j, z], h_send.at[j, k], h_recv.at[j, z], g.time(q))
    bias = gains_ref[10:12, pl.ds(pl.multiple_of(z * cols, cols), cols)]

    def attend(i, _):
        pl.when(i + 1 < nz)(lambda: probabilities(i + 1).start())
        probabilities(i).wait()
        here = pl.ds(pl.multiple_of(i * rows, rows), rows)
        grads[0, i] = attend_back_block(
            head_size, i, qkv_ref[0, here, :], qkv_ref.at[1], qkv_ref.at[2], pos_ref, bias, prob_buf.at[i % 2],
            go_ref[here, :], gk_acc, gv_acc, gpos_acc, gbias,
        )

        @pl.when(i == 0)
        def _():
            red.from_sibling(high, 0)
            red.along("b", high, 0)

        @pl.when(i == 1)
        def _():
            red.from_sibling(high, 1)
            red.along("b", high, 1)
            red.along("b", high, 2)

        return 0

    lax.fori_loop(0, nz, attend, 0)
    grads_k = gk_acc[...].T.astype(BF)
    grads_v = gv_acc[...].T.astype(BF)
    for q in range(nz):
        grads[1, q] = grads_k[q * rows : (q + 1) * rows]
        grads[2, q] = grads_v[q * rows : (q + 1) * rows]
    for k in range(1, nz):
        q = lax.rem(z + k, nz)
        for j in range(3):
            copy = to_time(j, q, k)
            copy.start()
            sends.append(copy)
    for j in range(3):
        heads[j, z] = grads[j, z]
    red.along("a", high, 0)
    fine = fine_ref.shape[1]

    def position(i, total):
        table = coarse_ref[0, pl.ds(2 * i, 1), :] * fine_ref[0] + coarse_ref[1, pl.ds(2 * i, 1), :] * fine_ref[1]
        after = coarse_ref[0, pl.ds(2 * i + 1, 1), :] * fine_ref[0] + coarse_ref[1, pl.ds(2 * i + 1, 1), :] * fine_ref[1]
        both = jnp.concatenate([table, after], axis=0).astype(BF)
        return total + dot(gpos_acc[:, pl.ds(pl.multiple_of(i * 2 * fine, 2 * fine), 2 * fine)].astype(BF), both, NN)

    gpos = lax.fori_loop(0, coarse_ref.shape[1] // 2, position, jnp.zeros((cols, width), F32)).astype(BF)
    gsq[pl.ds(3 * per, per)] = jnp.zeros((per, 2, sq_rows, width), BF)
    pieces = cols // sq_rows
    for i in range(pieces):
        piece = z * pieces + i
        gsq[3 * per + piece // 2, piece % 2] = gpos[i * sq_rows : (i + 1) * sq_rows]
    gains = gains_ref[...]
    loads[0].wait()
    grad_norm = jnp.zeros((rows, width), F32)
    for j in range(3):
        for k in range(1, nz):
            q = lax.rem(z + k, nz)
            arrived(heads.at[j, q], h_recv.at[j, q])
        full = jnp.concatenate([heads[j, q] for q in range(nz)], axis=1)
        gqkv[j] = full
        grad_norm = grad_norm + dot(full, wqkv[pl.ds(j * width, width), :], NN)
    for j in range(3):
        square_terms(j, gqkv[j], a2_ref[...])
    red.to_sibling(low, 0)
    resid1 = x1_ref[...]
    grad_add, gain1, shift1 = norm_backward(resid1, gains, 1, grad_norm)
    grad1 = g2_ref[...] + grad_add
    half1 = (0.5 * grad1).astype(BF)
    loads[1].wait()
    loads[2].wait()
    red.along("a", high, 1)
    grad_norm = module_backward(half1, up, down, h1_ref, gh1)
    red.from_sibling(low, 0)
    red.along("b", low, 0)
    matrix_terms(0, gh1, a1_ref[...], 0, units)
    matrix_terms(1, s1_ref, half1, 0, units)
    red.to_sibling(low, 1)
    red.along("a", high, 2)
    grad_add, gain0, shift0 = norm_backward(x_ref[...].astype(F32), gains, 0, grad_norm)
    away = jnp.logical_not(g.at_home())
    gx_buf[...] = (grad1 + grad_add).astype(BF)
    home = remote(gx_buf, gx_in, gx_sem.at[0], gx_sem.at[1], g.owner())
    pl.when(away)(lambda: home.start())
    small[...] = jnp.zeros_like(small)
    small[0:1, :] = gain0
    small[1:2, :] = shift0
    small[2:3, :] = gain1
    small[3:4, :] = shift1
    small[4:10, :] = some_ref[0:6, :]
    small[10:12, pl.ds(pl.multiple_of(z * cols, cols), cols)] = gbias[...]
    small[12:14, :] = some_ref[6:8, :]
    small[14 : 14 + gtaps_ref.shape[0], :] = gtaps_ref[...]
    meeting = Meeting(g, sbuf, s_send, s_recv)
    meeting.start(0, small[...])
    red.from_sibling(low, 1)
    red.along("b", low, 1)
    red.along("b", low, 2)
    red.along("a", low, 0)
    meeting.start(1, meeting.total(0))
    red.along("z", high, 0)
    red.along("z", high, 1)
    red.along("a", low, 1)
    red.along("z", low, 0)
    meeting.start(2, meeting.total(1))
    red.along("z", high, 2)
    red.along("a", low, 2)
    red.along("z", low, 1)
    meeting.start(3, meeting.total(2))
    red.along("z", low, 2)
    for part in range(3):
        red.last(part)
    me = g.chip(g.z, g.a, g.b)
    d = 1 - c
    half = ud_out.shape[1]
    at = lambda k: pl.ds(pl.multiple_of(me * 2 * half + k * half, half), half)
    fin_send_buf[...] = gud[c, at(d), :]
    swap = remote(fin_send_buf, fin, fin_send, fin_recv, g.sibling())
    swap.start()
    ud_out[c] = gud[c, at(c), :].astype(F32)
    sq_out[...] = gsq[me, c].astype(F32)
    small_out[...] = meeting.total(3)
    for planes in (high, low):
        for part in range(3):
            for axis in "baz":
                red.along(axis, planes, part, True)
        for kind in range(2):
            for q in planes:
                red.sibling_copy(q, kind).wait_send()
    for copy in sends + meeting.sends:
        copy.wait_send()

    @pl.when(away)
    def _():
        home.wait()
        gx_ref[...] = gx_in[...].astype(F32)

    @pl.when(g.at_home())
    def _():
        gx_ref[...] = gx_buf[...].astype(F32)

    swap.wait()
    ud_out[d] = fin[...].astype(F32)


def back(qkv, pos, grad_out, prob, head_size, coarse, fine, gains, signal, resid1, grad2, first, second, squares, some, gtaps, ud_full, sq_full):
    rows, width = signal.shape
    nz, nf = lax.axis_size("seq"), lax.axis_size("fsdp")
    chips = nz * nf // 2
    plane = nf // 2
    side = math.isqrt(plane)
    na, nb = (side, side) if side * side == plane else (plane, 1)
    cols = width // nz
    units = ud_full.shape[1] // 2
    own = ud_full.shape[1] // (2 * chips)
    block = 3 * own
    most = max(nz, na, nb, 2)
    tall = -(-(14 + gtaps.shape[0]) // 8) * 8
    vmem = pl.BlockSpec(memory_space=pltpu.VMEM)
    hbm = pl.BlockSpec(memory_space=pl.ANY)
    shape = jax.ShapeDtypeStruct
    dma = pltpu.SemaphoreType.DMA
    frames = rows * nz
    heads = cols // head_size
    operands = (qkv, pos, grad_out, coarse, fine, gains, signal, resid1, grad2, *first, *second, *squares, some, gtaps)
    places = lambda n: n + 1 if n > 2 else 1
    slots = {"b": places(nb) * na * nz, "a": places(na) * nz, "z": places(nz)}
    return pl.pallas_call(
        lambda *refs: back_kernel(head_size, *refs),
        name="back",
        out_shape=(
            shape((rows, width), F32),
            shape((2, own, width), F32),
            shape((own, width), F32),
            shape((tall, width), F32),
        ),
        in_specs=[vmem] * len(operands) + [hbm] * 3,
        out_specs=[vmem] * 4,
        scratch_shapes=[
            pltpu.VMEM((2, heads, rows, frames), BF),
            pltpu.VMEM((cols, frames), F32),
            pltpu.VMEM((cols, frames), F32),
            pltpu.VMEM((cols, 2 * frames), F32),
            pltpu.VMEM((2, cols), F32),
            pltpu.VMEM((3, nz, rows, cols), BF),
            dma((2,)),
            pltpu.VMEM((3 * width, width), BF),
            pltpu.VMEM((3, nz, rows, cols), BF),
            pltpu.VMEM((3, rows, width), BF),
            pltpu.VMEM((rows, units), BF),
            pltpu.VMEM((tall, width), F32),
            pltpu.VMEM((2, 2 * units, width), BF),
            pltpu.VMEM((chips, 2, own, width), BF),
            pltpu.VMEM((2 * units, width), BF),
            pltpu.VMEM((chips, own, width), BF),
            pltpu.VMEM((slots["b"], block, width), BF),
            pltpu.VMEM((slots["a"], block, width), BF),
            pltpu.VMEM((slots["z"], block, width), BF),
            pltpu.VMEM((4, most, tall, width), F32),
            pltpu.VMEM((own, width), BF),
            pltpu.VMEM((own, width), BF),
            pltpu.VMEM((rows, width), BF),
            pltpu.VMEM((rows, width), BF),
            dma((2,)),
            dma((3,)),
            dma((3, nz)),
            dma((3, nz)),
            dma((2, nz)),
            dma((2, nz)),
            dma((2, 3, slots["b"])),
            dma((3, slots["b"])),
            dma((2, 3, slots["a"])),
            dma((3, slots["a"])),
            dma((2, 3, slots["z"])),
            dma((3, slots["z"])),
            dma((4, most)),
            dma((4, most)),
            dma,
            dma,
        ],
        compiler_params=pltpu.CompilerParams(
            collective_id=7, has_side_effects=True, vmem_limit_bytes=61000 * 1024
        ),
    )(*operands, prob, ud_full, sq_full)


def when(*conditions):
    holds = 1
    for condition in conditions:
        holds = holds * jnp.asarray(condition).astype(jnp.int32)
    return pl.when(holds == 1) if conditions else lambda act: act()


class Gather:
    WAYS = {"z+": 0, "z-": 1, "a+": 2, "a-": 3, "b+": 4, "b-": 5, "s": 6}
    PARTS = (0, 1, 2)
    SPREAD = ("a+", "a-", "b+", "b-", "s")

    def __init__(self, g, ud, sq, recv_sem, sib_recv, send_sem):
        self.g, self.ud, self.sq = g, ud, sq
        self.recv_sem, self.sib_recv, self.send_sem = recv_sem, sib_recv, send_sem
        self.rows = sq.shape[2]
        half = g.nz // 2
        if half == 2:
            first = jnp.minimum(g.z, 1)
            second = jnp.maximum(g.z, 2)
            self.low, self.high = [first, 1 - first], [second, 5 - second]
        else:
            self.low, self.high = list(range(half)), list(range(half, g.nz))
        self.below = g.z < half

    def piece(self, part, t, color):
        if part == 0:
            return self.sq.at[t, color]
        return self.ud.at[color, pl.ds(t * 2 * self.rows + (part - 1) * self.rows, self.rows)]

    def onward(self, part, t, ways, finish, *only):
        g = self.g
        ref = self.piece(part, t, g.core)
        for way in ways:
            p, n = (0, 2) if way == "s" else g.place(way[0])

            def act():
                if way == "s":
                    target, arrive = g.sibling(), self.sib_recv
                else:
                    target, arrive = g.up(way[0]) if way[1] == "+" else g.down(way[0]), self.recv_sem
                copy = remote(ref, ref, self.send_sem.at[self.WAYS[way], part, t], arrive.at[part, t], target)
                copy.wait_send() if finish else copy.start()

            if way == "s":
                when(*only)(act)
            elif n > 1:
                when(*only, p < n - 1 if way[1] == "+" else p > 0)(act)

    def wait(self, part, t, finish):
        if not finish:
            arrived(self.piece(part, t, self.g.core), self.recv_sem.at[part, t])

    def column(self, q, spread, finish, *only):
        g = self.g
        t = g.chip(q, g.a, g.b)
        for part in self.PARTS:
            when(*only, q != g.z)(lambda: self.wait(part, t, finish))
            self.onward(part, t, ("z+",), finish, *only, q <= g.z)
            self.onward(part, t, ("z-",), finish, *only, q >= g.z)
            if spread:
                self.onward(part, t, self.SPREAD, finish, *only)

    def spread(self, q, finish, *only):
        g = self.g
        for part in self.PARTS:
            self.onward(part, g.chip(q, g.a, g.b), self.SPREAD, finish, *only)

    def both(self, axis, k, act):
        p, n = self.g.place(axis)
        pl.when(p >= k)(lambda: act(p - k, axis + "+"))
        pl.when(p + k < n)(lambda: act(p + k, axis + "-"))

    def along_a(self, q, finish=False):
        g = self.g

        def take(a, way):
            t = g.chip(q, a, g.b)
            for part in self.PARTS:
                self.wait(part, t, finish)
                self.onward(part, t, (way, "b+", "b-", "s"), finish)

        for k in range(1, g.na):
            self.both("a", k, take)

    def along_b(self, q, finish=False):
        g = self.g

        def row(b, way):
            def body(i, _):
                t = g.chip(q, lax.rem(g.a + i, g.na), b)
                for part in self.PARTS:
                    self.wait(part, t, finish)
                    self.onward(part, t, (way, "s"), finish)
                return 0

            lax.fori_loop(0, g.na, body, 0)

        for k in range(1, g.nb):
            self.both("b", k, row)

    def first(self, finish=False):
        below, above = self.below, jnp.logical_not(self.below)
        self.column(self.high[0], False, finish, above)
        for q in self.low:
            self.column(q, True, finish)
        self.spread(self.high[0], finish, above)
        self.column(self.high[0], False, finish, below)
        for q in self.low:
            self.along_a(q, finish)
        for q in self.high[1:]:
            self.column(q, False, finish)
        for q in self.low:
            self.along_b(q, finish)
        self.spread(self.high[0], finish, below)
        for q in self.high[1:]:
            self.spread(q, finish)

    def from_sibling(self, upper):
        g = self.g
        count = g.chips // 2

        def body(i, _):
            for part in self.PARTS:
                t = upper * count + i
                arrived(self.piece(part, t, 1 - g.core), self.sib_recv.at[part, t])
            return 0

        lax.fori_loop(0, count, body, 0)


def head_kernel(head_size, up_own, down_own, sq_own, small_in, x_in, cot_in, len_in, coarse_ref, fine_ref,
                ud_full, sq_full, small_ref, x_ref, cot_ref, len_ref,
                x1_ref, a1_ref, h1_ref, s1_ref, a2_ref, heads_ref, pos_ref, att_ref, prob_hbm,
                own, sbuf, up, down, wqkv, wpos, mine, prob_buf,
                move_send, move_recv, local_sem, swap_sem, recv_sem, sib_recv, gather_send, s_send, s_recv,
                load_sem, send_sem, heads_recv, prob_sem):
    g = Grid()
    z, nz, c = g.t, g.nz, g.core
    rows, width = x_in.shape
    cols = width // nz
    units = up.shape[0]
    half = up_own.shape[0]
    me = g.chip(g.z, g.a, g.b)
    own[0] = up_own[...].astype(BF)
    own[1] = down_own[...].astype(BF)
    own[2] = sq_own[...].astype(BF)
    here = pl.ds(me * 2 * half + c * half, half)
    local = [
        pltpu.make_async_copy(own.at[c], ud_full.at[c, here], local_sem.at[0]),
        pltpu.make_async_copy(own.at[2], sq_full.at[me, c], local_sem.at[1]),
    ]
    for copy in local:
        copy.start()
    greet_lines(g, "cabz", g.owner())
    swap = remote(own.at[1 - c], ud_full.at[1 - c, here], swap_sem.at[0], swap_sem.at[1], g.sibling())
    swap.start()
    moves = [
        remote(src, dst, move_send.at[k], move_recv.at[k], g.worker())
        for k, (src, dst) in enumerate(((x_in, x_ref), (len_in, len_ref), (cot_in, cot_ref)))
    ]

    @pl.when(jnp.logical_not(g.at_home()))
    def _():
        for copy in moves[:2]:
            copy.start()

    @pl.when(g.at_home())
    def _():
        x_ref[...] = x_in[...]
        len_ref[...] = len_in[...]
        cot_ref[...] = cot_in[...]

    meeting = Meeting(g, sbuf, s_send, s_recv)
    meeting.start(0, small_in[...].astype(BF))
    gather = Gather(g, ud_full, sq_full, recv_sem, sib_recv, gather_send)
    for copy in local:
        copy.wait()
    swap.wait_recv()
    meeting.start(1, meeting.total(0))
    meeting.start(2, meeting.total(1))
    gather.first()
    meeting.start(3, meeting.total(2))

    @pl.when(jnp.logical_not(g.at_home()))
    def _():
        moves[2].start()
        for copy in moves[:2]:
            copy.wait()

    gather.from_sibling(0)
    loads = [
        pltpu.make_async_copy(ud_full.at[0, pl.ds(0, units)], up, load_sem.at[0]),
        pltpu.make_async_copy(ud_full.at[1, pl.ds(0, units)], down, load_sem.at[1]),
    ]
    per = width // (2 * half)
    squares = pltpu.make_async_copy(sq_full.at[pl.ds(0, 3 * per)], wqkv, load_sem.at[2])
    pieces = cols // half
    positions = [
        pltpu.make_async_copy(
            sq_full.at[3 * per + (z * pieces + i) // 2, (z * pieces + i) % 2],
            wpos.at[pl.ds(i * half, half)],
            load_sem.at[3],
        )
        for i in range(pieces)
    ]
    for load in loads + [squares]:
        load.start()
    for load in positions:
        load.start()
        load.wait()
    small_ref[...] = meeting.total(3).astype(F32)
    gains = small_ref[...]
    signal = x_ref[...].astype(F32)
    normed1 = norm_forward(signal, gains, 0)
    a1_ref[...] = normed1
    for load in loads:
        load.wait()
    resid1 = signal + 0.5 * module_forward(normed1, up, down, h1_ref, s1_ref)
    x1_ref[...] = resid1
    gather.along_a(gather.high[0])
    normed2 = norm_forward(resid1, gains, 1)
    a2_ref[...] = normed2
    squares.wait()
    for k in range(3):
        weight = wqkv[pl.ds(k * per, per)].reshape(width, width)
        out = dot(normed2, weight, NT).astype(BF)
        for q in range(nz):
            mine[q, k] = out[:, q * cols : (q + 1) * cols]
    sends = []
    for k in range(1, nz):
        q = lax.rem(z + k, nz)
        copy = remote(mine.at[q], heads_ref.at[:, pl.ds(z * rows, rows)], send_sem.at[k], heads_recv.at[z], g.time(q))
        copy.start()
        sends.append(copy)
    slot = pl.ds(pl.multiple_of(z * rows, rows), rows)
    for k in range(3):
        heads_ref[k, slot, :] = mine[z, k]
    for q in gather.high[1:]:
        gather.along_a(q)
    fine = fine_ref.shape[1]
    weight = wpos[...]

    def position(i, _):
        table = coarse_ref[0, pl.ds(i, 1), :] * fine_ref[0] + coarse_ref[1, pl.ds(i, 1), :] * fine_ref[1]
        there = pl.ds(pl.multiple_of(i * fine, fine), fine)
        pos_ref[there, :] = dot(table.astype(BF), weight, NT).astype(BF)
        return 0

    lax.fori_loop(0, coarse_ref.shape[1], position, 0)
    for k in range(1, nz):
        q = lax.rem(z + k, nz)
        arrived(heads_ref.at[:, pl.ds(q * rows, rows)], heads_recv.at[q])
    bias = small_ref[10:12, pl.ds(pl.multiple_of(z * cols, cols), cols)]

    def keep(i):
        return pltpu.make_async_copy(
            prob_buf.at[i % 2], prob_hbm.at[:, pl.ds(i * rows, rows)], prob_sem.at[i % 2]
        )

    def attend(i, _):
        pl.when(i >= 2)(lambda: keep(i - 2).wait())
        there = pl.ds(pl.multiple_of(i * rows, rows), rows)
        att_ref[there, :] = attend_block(
            head_size, i, heads_ref[0, there, :], heads_ref.at[1], heads_ref.at[2], pos_ref, bias, len_ref, prob_buf.at[i % 2]
        )
        keep(i).start()
        for k, q in enumerate(gather.high):
            pl.when(i == min(2 * k + 1, nz - 1))(lambda: gather.along_b(q))
        return 0

    lax.fori_loop(0, nz, attend, 0)
    gather.from_sibling(1)
    keep(nz - 2).wait()
    keep(nz - 1).wait()
    swap.wait_send()
    for copy in sends + meeting.sends:
        copy.wait_send()
    gather.first(True)
    for q in gather.high:
        gather.along_a(q, True)
        gather.along_b(q, True)

    @pl.when(jnp.logical_not(g.at_home()))
    def _():
        moves[2].wait()


def head(upward, downward, square, small, signal, cotangent, length, coarse, fine, head_size):
    rows, width = signal.shape
    nz, nf = lax.axis_size("seq"), lax.axis_size("fsdp")
    devices = nz * nf
    chips, plane = devices // 2, nf // 2
    own = upward.shape[0]
    frames, cols = rows * nz, width // nz
    units = own * devices // 2
    heads = cols // head_size
    side = math.isqrt(plane)
    most = max(nz, side if side * side == plane else plane, 2)
    vmem = pl.BlockSpec(memory_space=pltpu.VMEM)
    hbm = pl.BlockSpec(memory_space=pl.ANY)
    shape = jax.ShapeDtypeStruct
    dma = pltpu.SemaphoreType.DMA
    return pl.pallas_call(
        lambda *refs: head_kernel(head_size, *refs),
        name="head",
        out_shape=(
            shape((2, devices * own, width), BF),
            shape((chips, 2, own, width), BF),
            shape(small.shape, F32),
            shape(signal.shape, signal.dtype),
            shape(cotangent.shape, cotangent.dtype),
            shape(length.shape, length.dtype),
            shape((rows, width), F32),
            shape((rows, width), BF),
            shape((rows, units), BF),
            shape((rows, units), BF),
            shape((rows, width), BF),
            shape((3, frames, cols), BF),
            shape((2 * frames, cols), BF),
            shape((frames, cols), BF),
            shape((heads, frames, frames), BF),
        ),
        in_specs=[vmem] * 9,
        out_specs=[hbm] * 2 + [vmem] * 12 + [hbm],
        scratch_shapes=[
            pltpu.VMEM((3, own, width), BF),
            pltpu.VMEM((4, most) + small.shape, BF),
            pltpu.VMEM((units, width), BF),
            pltpu.VMEM((units, width), BF),
            pltpu.VMEM((3 * width // (2 * own), 2, own, width), BF),
            pltpu.VMEM((cols, width), BF),
            pltpu.VMEM((nz, 3, rows, cols), BF),
            pltpu.VMEM((2, heads, rows, frames), BF),
            dma((3,)),
            dma((3,)),
            dma((2,)),
            dma((2,)),
            dma((3, chips)),
            dma((3, chips)),
            dma((7, 3, chips)),
            dma((4, most)),
            dma((4, most)),
            dma((4,)),
            dma((nz,)),
            dma((nz,)),
            dma((2,)),
        ],
        compiler_params=pltpu.CompilerParams(
            collective_id=5, has_side_effects=True, vmem_limit_bytes=56 * 1024 * 1024
        ),
    )(upward, downward, square, small, signal, cotangent, length, coarse, fine)


def per_device(
    inputs,
    cotangent,
    lengths,
    square,
    upward,
    downward,
    vectors,
    kernel,
    square_momentum,
    square_variance,
    upward_momentum,
    upward_variance,
    downward_momentum,
    downward_variance,
    vectors_momentum,
    vectors_variance,
    kernel_momentum,
    kernel_variance,
):
    model_width = inputs.shape[2]
    seq_place = lax.axis_index("seq")
    seq_frames = inputs.shape[1] * lax.axis_size("seq")
    head_size = D // H
    coarse, fine = position_tables(seq_frames, model_width)
    place = seq_place * lax.axis_size("fsdp") + lax.axis_index("fsdp")
    share = vectors.shape[1]
    tall = -(-(vectors.shape[0] + kernel.shape[0]) // 16) * 16
    small = jnp.concatenate([vectors, kernel], axis=0)
    small = lax.dynamic_update_slice(jnp.zeros((tall, model_width), F32), small, (0, place * share))
    length = jnp.broadcast_to(lengths.astype(F32)[:, None], (8, LANES))
    (
        full_ud, full_sq, small, signal, cotangent_here, length,
        resid1, normed1, hidden1, active1, normed2, heads, pos_heads, attended, prob,
    ) = head(upward, downward, square, small, inputs[0], cotangent[0], length, coarse, fine, head_size)
    full_sq = full_sq.reshape(model_width * 8, model_width)
    (
        layer_output, grad_res2, grad_out_head, out_time, grad_att_b, normed3, grad_pair, grad_conv_b, swish_b, normed4,
        active4, grad_hidden4, half4, small_grads, grad_taps,
    ) = middle(length, attended, resid1, cotangent_here, small, kernel.shape[0], full_ud, full_sq)
    layer_output = layer_output[None]
    input_grad, matrix_grads, square_grad, small_sums = back(
        heads, pos_heads, grad_out_head, prob, head_size, coarse, fine, small,
        signal, resid1, grad_res2, (normed1, hidden1, active1, normed2), (normed4, active4, grad_hidden4, half4),
        (out_time, grad_att_b, normed3, grad_pair, grad_conv_b, swish_b), small_grads, grad_taps, full_ud, full_sq,
    )
    input_grad = input_grad[None]
    upward_grad, downward_grad = matrix_grads[0], matrix_grads[1]
    small_own = lax.dynamic_slice_in_dim(small_sums, place * share, share, 1)
    vectors_grad = small_own[: vectors.shape[0]]
    kernel_grad = small_own[vectors.shape[0] : vectors.shape[0] + kernel.shape[0]]
    square_next, momentum_square, variance_square = adam_step(
        square, square_grad, square_momentum, square_variance, DECAY_RATE
    )
    upward_next, momentum_upward, variance_upward = adam_step(
        upward, upward_grad, upward_momentum, upward_variance, DECAY_RATE
    )
    downward_next, momentum_downward, variance_downward = adam_step(
        downward, downward_grad, downward_momentum, downward_variance, DECAY_RATE
    )
    vectors_next, momentum_vectors, variance_vectors = adam_step(
        vectors, vectors_grad, vectors_momentum, vectors_variance, 0.0
    )
    kernel_next, momentum_kernel, variance_kernel = adam_step(
        kernel, kernel_grad, kernel_momentum, kernel_variance, DECAY_RATE
    )
    return (
        layer_output,
        input_grad,
        square_grad,
        upward_grad,
        downward_grad,
        vectors_grad,
        kernel_grad,
        square_next,
        upward_next,
        downward_next,
        vectors_next,
        kernel_next,
        momentum_square,
        variance_square,
        momentum_upward,
        variance_upward,
        momentum_downward,
        variance_downward,
        momentum_vectors,
        variance_vectors,
        momentum_kernel,
        variance_kernel,
    )


def solution(mesh):
    return jax.shard_map(
        per_device,
        mesh=mesh,
        in_specs=(
            P("fsdp", "seq", None),
            P("fsdp", "seq", None),
            P("fsdp"),
            P(("seq", "fsdp"), None),
            P(("seq", "fsdp"), None),
            P(("seq", "fsdp"), None),
            P(None, ("seq", "fsdp")),
            P(None, ("seq", "fsdp")),
            P(("seq", "fsdp"), None),
            P(("seq", "fsdp"), None),
            P(("seq", "fsdp"), None),
            P(("seq", "fsdp"), None),
            P(("seq", "fsdp"), None),
            P(("seq", "fsdp"), None),
            P(None, ("seq", "fsdp")),
            P(None, ("seq", "fsdp")),
            P(None, ("seq", "fsdp")),
            P(None, ("seq", "fsdp")),
        ),
        out_specs=(
            P("fsdp", "seq", None),
            P("fsdp", "seq", None),
            P(("seq", "fsdp"), None),
            P(("seq", "fsdp"), None),
            P(("seq", "fsdp"), None),
            P(None, ("seq", "fsdp")),
            P(None, ("seq", "fsdp")),
            P(("seq", "fsdp"), None),
            P(("seq", "fsdp"), None),
            P(("seq", "fsdp"), None),
            P(None, ("seq", "fsdp")),
            P(None, ("seq", "fsdp")),
            P(("seq", "fsdp"), None),
            P(("seq", "fsdp"), None),
            P(("seq", "fsdp"), None),
            P(("seq", "fsdp"), None),
            P(("seq", "fsdp"), None),
            P(("seq", "fsdp"), None),
            P(None, ("seq", "fsdp")),
            P(None, ("seq", "fsdp")),
            P(None, ("seq", "fsdp")),
            P(None, ("seq", "fsdp")),
        ),
        check_vma=False,
    )
```

```python
import math

import jax
import jax.numpy as jnp
from jax import lax
from jax.experimental import pallas as pl
from jax.experimental.pallas import tpu as pltpu
from jax.sharding import PartitionSpec as P

D = 512
H = 8
FF = 2048
ADAM_STEP = 4

LN_EPS = 1e-05
BN_EPS = 1e-05
BETA_ONE = 0.9
BETA_TWO = 0.98
ADAM_EPS = 1e-08
LEARN_RATE = 0.005
DECAY_RATE = 0.01


def position_tables(seq_frames, model_width):
    fine = math.gcd(2 * seq_frames, 64)
    column = jnp.arange(model_width)
    frequency = jnp.exp(-math.log(10000.0) * 2.0 * (column // 2).astype(jnp.float32) / model_width)
    coarse_at = (seq_frames - 1 - fine * jnp.arange(2 * seq_frames // fine)).astype(jnp.float32)
    coarse_phase = coarse_at[:, None] * frequency[None, :]
    fine_phase = jnp.arange(fine).astype(jnp.float32)[:, None] * frequency[None, :]
    even = (column % 2 == 0)[None, :]
    sine, cosine = jnp.sin(coarse_phase), jnp.cos(coarse_phase)
    with_cosine = jnp.where(even, sine, cosine)
    with_sine = jnp.where(even, -cosine, sine)
    return jnp.stack([with_cosine, with_sine]), jnp.stack([jnp.cos(fine_phase), jnp.sin(fine_phase)])


MESH = pl.DeviceIdType.MESH
BF = jnp.bfloat16
F32 = jnp.float32
LANES = 128


class Grid:
    def __init__(self):
        self.nz = lax.axis_size("seq")
        self.nf = lax.axis_size("fsdp")
        plane = self.nf // 2
        side = math.isqrt(plane)
        self.z = lax.axis_index("seq")
        f = lax.axis_index("fsdp")
        self.core = f % 2
        if side * side == plane:
            self.na = self.nb = side
            self.step_a = 2 + self.core * (2 * side - 2)
            self.step_b = 2 * side - self.core * (2 * side - 2)
        else:
            self.na, self.nb = plane, 1
            self.step_a, self.step_b = 2, self.nf
        self.f = f
        self.a = (f // self.step_a) % self.na
        self.b = (f // self.step_b) % self.nb
        self.plane = plane
        self.chips = plane * self.nz

        self.half = self.nz // 2
        self.t = (self.z % self.half) * 2 + self.core
        self.column = f - self.core

    def time(self, q):
        return (self.z - self.z % self.half + q // 2, self.column + q % 2)

    def owner(self):
        return (self.t, self.column + self.z // self.half)

    def worker(self):
        return (self.core * self.half + self.z // 2, self.column + self.z % 2)

    def at_home(self):
        return jnp.logical_and(self.t == self.z, self.z // self.half == self.core)

    def chip(self, z, a, b):
        return z * self.plane + (a * self.step_a + b * self.step_b) // 2

    def device(self, z, a, b):
        return (z, a * self.step_a + b * self.step_b + self.core)

    def sibling(self):
        return (self.z, self.f + 1 - 2 * self.core)

    def up(self, axis):
        return self.device(self.z + (axis == "z"), self.a + (axis == "a"), self.b + (axis == "b"))

    def down(self, axis):
        return self.device(self.z - (axis == "z"), self.a - (axis == "a"), self.b - (axis == "b"))

    def line(self, axis):
        return {
            "c": (self.core, 2, lambda q: (self.z, self.f - self.core + q)),
            "a": (self.a, self.na, lambda q: self.device(self.z, q, self.b)),
            "b": (self.b, self.nb, lambda q: self.device(self.z, self.a, q)),
            "z": (self.z, self.nz, lambda q: self.device(q, self.a, self.b)),
        }[axis]

    def place(self, axis):
        return {"z": (self.z, self.nz), "a": (self.a, self.na), "b": (self.b, self.nb)}[axis]


def greet_mover(g, barrier, source):
    @pl.when(jnp.logical_not(g.at_home()))
    def _():
        pl.semaphore_signal(barrier, inc=1, device_id=source, device_id_type=MESH)

    return 1 - g.at_home().astype(jnp.int32)


def merge_moments(first_op, second_op):
    count = first_op[0:1] + second_op[0:1]
    share = second_op[0:1] / jnp.maximum(count, 1.0)
    gap = second_op[1:2] - first_op[1:2]
    mean = first_op[1:2] + gap * share
    squares = first_op[2:3] + second_op[2:3] + gap * gap * (first_op[0:1] * share)
    return jnp.concatenate([count, mean, squares, first_op[3:]], axis=0)


NT = (((1,), (1,)), ((), ()))
TN = (((0,), (0,)), ((), ()))
NN = (((1,), (0,)), ((), ()))


def dot(first_op, second_op, dims):
    return lax.dot_general(first_op, second_op, dims, preferred_element_type=F32)


def keep_head(value, h, head_size):
    lane = lax.broadcasted_iota(jnp.int32, value.shape, 1)
    return jnp.where(lane // head_size == h, value, jnp.zeros_like(value))


def attend_block(head_size, i, query_b, k_ref, v_ref, pos_ref, bias, len_ref, prob_ref):
    rows, cols = query_b.shape
    frames = k_ref.shape[0]
    width = rows + frames
    query = query_b.astype(F32)
    content = (query + bias[0:1, :]).astype(BF)
    positional = (query + bias[1:2, :]).astype(BF)
    window = pos_ref[pl.ds(pl.multiple_of(frames - rows - i * rows, rows), width), :]
    live = lax.broadcasted_iota(jnp.int32, (rows, frames), 1).astype(F32) < len_ref[0:1, 0:1]
    out = jnp.zeros((rows, cols), F32)
    for h in range(cols // head_size):
        direct = dot(keep_head(content, h, head_size), k_ref[...], NT)
        spread = dot(keep_head(positional, h, head_size), window, NT)
        shifted = pltpu.roll(spread, width - rows + 1, 1, stride=1, stride_axis=0)[:, :frames]
        score = jnp.where(live, (direct + shifted) * (1.0 / math.sqrt(head_size)), -1e30)
        top = jnp.max(score, axis=-1, keepdims=True)
        power = jnp.exp(score - top)
        prob_b = (power * (1.0 / jnp.sum(power, axis=-1, keepdims=True))).astype(BF)
        prob_ref[h] = prob_b
        out = out + keep_head(dot(prob_b, v_ref[...], NN), h, head_size)
    return out.astype(BF)


def attend_back_block(head_size, i, query_b, k_ref, v_ref, pos_ref, bias, prob_ref, grad_heads, gk_acc, gv_acc, gpos_acc, gbias):
    rows, cols = query_b.shape
    frames = k_ref.shape[0]
    width = rows + frames
    query = query_b.astype(F32)
    content = (query + bias[0:1, :]).astype(BF)
    positional = (query + bias[1:2, :]).astype(BF)
    down = lax.broadcasted_iota(jnp.int32, (rows, rows), 0)
    across = lax.broadcasted_iota(jnp.int32, (rows, rows), 1)
    turn = jnp.where(down + across == rows - 1, 1.0, 0.0).astype(BF)
    positional_turned = dot(turn, positional, NN).astype(BF)
    here = pl.ds(pl.multiple_of(frames - rows - i * rows, rows), width)
    window = pos_ref[here, :]
    grad_content = jnp.zeros((rows, cols), F32)
    grad_position = jnp.zeros((rows, cols), F32)
    for h in range(cols // head_size):
        grad_out = keep_head(grad_heads, h, head_size)
        prob_b = prob_ref[h]
        prob = prob_b.astype(F32)
        grad_prob = dot(grad_out, v_ref[...], NT)
        delta = jnp.sum(prob * grad_prob, axis=-1, keepdims=True)
        score_b = (prob * (grad_prob - delta) * (1.0 / math.sqrt(head_size))).astype(BF)
        grad_content = grad_content + keep_head(dot(score_b, k_ref[...], NN), h, head_size)
        gk_acc[...] += dot(keep_head(content, h, head_size), score_b, TN)
        gv_acc[...] += dot(grad_out, prob_b, TN)
        wide = jnp.concatenate([dot(turn, score_b, NN), jnp.zeros((rows, width - frames), F32)], axis=1)
        spread = pltpu.roll(wide, 0, 1, stride=1, stride_axis=0).astype(BF)
        grad_position = grad_position + keep_head(dot(spread, window, NN), h, head_size)
        gpos_acc[:, here] += dot(keep_head(positional_turned, h, head_size), spread, TN)
    high = grad_position.astype(BF)
    low = (grad_position - high.astype(F32)).astype(BF)
    grad_position = dot(turn, high, NN) + dot(turn, low, NN)
    gbias[0:1, :] += jnp.sum(grad_content, axis=0, keepdims=True)
    gbias[1:2, :] += jnp.sum(grad_position, axis=0, keepdims=True)
    return (grad_content + grad_position).astype(BF)

def normalize(value):
    mean = jnp.mean(value, axis=-1, keepdims=True)
    centred = value - mean
    spread = lax.rsqrt(jnp.mean(centred * centred, axis=-1, keepdims=True) + LN_EPS)
    return centred * spread, spread


def norm_forward(value, gains, k):
    unit, _ = normalize(value)
    return (unit * gains[2 * k : 2 * k + 1] + gains[2 * k + 1 : 2 * k + 2]).astype(BF)


def norm_backward(value, gains, k, upstream):
    unit, spread = normalize(value)
    inner = upstream * gains[2 * k : 2 * k + 1]
    along = jnp.mean(inner * unit, axis=-1, keepdims=True)
    grad = spread * (inner - jnp.mean(inner, axis=-1, keepdims=True) - unit * along)
    gain = jnp.sum(upstream * unit, axis=0, keepdims=True)
    return grad, gain, jnp.sum(upstream, axis=0, keepdims=True)


def sigmoid(value):
    return 1.0 / (1.0 + jnp.exp(-value))


def module_forward(normed, up_ref, down_ref, hidden_ref, active_ref):
    units, width = up_ref.shape
    step = min(512, units)

    def chunk(j, total):
        here = pl.ds(pl.multiple_of(j * step, step), step)
        hidden = dot(normed, up_ref[here, :], NT)
        active = (hidden * sigmoid(hidden)).astype(BF)
        hidden_ref[:, here] = hidden.astype(hidden_ref.dtype)
        active_ref[:, here] = active
        return total + dot(active, down_ref[here, :], NN)

    return lax.fori_loop(0, units // step, chunk, jnp.zeros((normed.shape[0], width), F32))


def module_backward(upstream_b, up_ref, down_ref, hidden_ref, grad_ref):
    units, width = up_ref.shape
    step = min(512, units)

    def chunk(j, total):
        here = pl.ds(pl.multiple_of(j * step, step), step)
        hidden = hidden_ref[:, here].astype(F32)
        sigma = sigmoid(hidden)
        slope = sigma * (1.0 + hidden * (1.0 - sigma))
        grad = (dot(upstream_b, down_ref[here, :], NT) * slope).astype(BF)
        grad_ref[:, here] = grad
        return total + dot(grad, up_ref[here, :], NN)

    return lax.fori_loop(0, units // step, chunk, jnp.zeros((upstream_b.shape[0], width), F32))


def greet_lines(g, axes, source=None):
    barrier = pltpu.get_barrier_semaphore()
    total = g.nz - 1
    for k in range(1, g.nz):
        pl.semaphore_signal(barrier, inc=1, device_id=g.time(lax.rem(g.t + k, g.nz)), device_id_type=MESH)
    if source is not None:
        total = total + greet_mover(g, barrier, source)
    for axis in axes:
        p, n, device = g.line(axis)
        for k in range(1, n):
            pl.semaphore_signal(barrier, inc=1, device_id=device(lax.rem(p + k, n)), device_id_type=MESH)
            total += 1
    pl.semaphore_wait(barrier, total)


def remote(src, dst, send, recv, device):
    return pltpu.make_async_remote_copy(
        src_ref=src, dst_ref=dst, send_sem=send, recv_sem=recv, device_id=device, device_id_type=MESH
    )


def arrived(ref, sem):
    pltpu.make_async_copy(ref, ref, sem).wait()


def meet_levels(g, value, merge, buf, send_sem, recv_sem):
    sends = []
    for level, axis in enumerate("cabz"):
        p, n, device = g.line(axis)
        if n == 1:
            continue
        buf[level, p] = value
        for k in range(1, n):
            copy = remote(buf.at[level, p], buf.at[level, p], send_sem.at[level, k], recv_sem.at[level, p], device(lax.rem(p + k, n)))
            copy.start()
            sends.append(copy)
        for k in range(1, n):
            q = lax.rem(p + k, n)
            arrived(buf.at[level, q], recv_sem.at[level, q])
        value = buf[level, 0]
        for q in range(1, n):
            value = merge(value, buf[level, q])
    return value, sends


HALO = 16


def swap_edges(g, body, low, high, send_sem, recv_sem, pad):
    rows = body.shape[0]
    p, n = g.t, g.nz
    up = remote(body.at[pl.ds(rows - HALO, HALO)], low, send_sem.at[0], recv_sem.at[0], g.time(p + 1))
    down = remote(body.at[pl.ds(0, HALO)], high, send_sem.at[1], recv_sem.at[1], g.time(p - 1))
    pl.when(p < n - 1)(lambda: up.start())
    pl.when(p > 0)(lambda: down.start())
    pad[pl.ds(HALO, rows), :] = body[...].astype(F32)

    def fill(at, ref, sem, there):
        @pl.when(there)
        def _():
            arrived(ref, sem)
            pad[pl.ds(at, HALO), :] = ref[...].astype(F32)

        @pl.when(jnp.logical_not(there))
        def _():
            pad[pl.ds(at, HALO), :] = jnp.zeros((HALO, pad.shape[1]), F32)

    fill(0, low, recv_sem.at[0], p > 0)
    fill(HALO + rows, high, recv_sem.at[1], p < n - 1)

    def finish():
        pl.when(p < n - 1)(lambda: up.wait_send())
        pl.when(p > 0)(lambda: down.wait_send())

    return finish


def middle_kernel(taps, len_ref, att_ref, x1_ref, cot_ref, gains_ref, ud_hbm, sq_hbm,
                  y_ref, g2_ref, go_ref, o_ref, e2_ref, a3_ref, gpair_ref, e3_ref, sw_ref, a4_ref, s4_ref, gh4_ref, e4_ref,
                  small_ref, gtaps_ref,
                  up, down, wsq, o_buf, go_buf, glu_b, gc_b, low1, high1, low2, high2, pad_glu, pad_gc, h4, c_ref, y_buf, y_sem,
                  buf1, buf2, load_sem, a_send, a_recv, b_send, b_recv, h_send, h_recv, m_send, m_recv):
    g = Grid()
    z, nz = g.t, g.nz
    rows, width = x1_ref.shape
    cols = width // nz
    units = up.shape[0]
    rim = (taps - 1) // 2
    loads = [
        pltpu.make_async_copy(sq_hbm.at[pl.ds(4 * width, 4 * width)], wsq, load_sem.at[0]),
        pltpu.make_async_copy(ud_hbm.at[0, pl.ds(units, units)], up, load_sem.at[1]),
        pltpu.make_async_copy(ud_hbm.at[1, pl.ds(units, units)], down, load_sem.at[2]),
    ]
    for load in loads:
        load.start()
    greet_lines(g, "cabz", g.worker())
    sends = []
    for k in range(1, nz):
        q = lax.rem(z + k, nz)
        copy = remote(att_ref.at[pl.ds(q * rows, rows)], o_buf.at[z], a_send.at[k], a_recv.at[z], g.time(q))
        copy.start()
        sends.append(copy)
    o_buf[z] = att_ref[pl.ds(pl.multiple_of(z * rows, rows), rows), :]
    gains = gains_ref[...]
    frame = z * rows + lax.broadcasted_iota(jnp.int32, (rows, 1), 0)
    live = jnp.where(frame.astype(F32) < len_ref[0:1, 0:1], 1.0, 0.0)
    loads[0].wait()
    weight = lambda k: wsq[pl.ds((k - 4) * width, width), :]
    for k in range(1, nz):
        q = lax.rem(z + k, nz)
        arrived(o_buf.at[q], a_recv.at[q])
    out = jnp.concatenate([o_buf[q] for q in range(nz)], axis=1)
    o_ref[...] = out
    resid2 = x1_ref[...] + dot(out, weight(4), NT)
    normed3 = norm_forward(resid2, gains, 2)
    a3_ref[...] = normed3
    value = dot(normed3, weight(5), NT)
    gate = sigmoid(dot(normed3, weight(6), NT))
    glu_b[...] = (value * gate * live).astype(BF)
    done1 = swap_edges(g, glu_b, low1, high1, h_send.at[0], h_recv.at[0], pad_glu)
    for at in range(0, width, LANES):
        lanes = pl.ds(at, LANES)
        total = jnp.zeros((rows, LANES), F32)
        for m in range(taps):
            total = total + gains_ref[14 + m : 15 + m, lanes] * pad_glu[pl.ds(HALO - rim + m, rows), lanes]
        c_ref[:, lanes] = total
    conv = c_ref[...]
    count = jnp.sum(live, axis=0, keepdims=True)
    mean = jnp.sum(live * conv, axis=0, keepdims=True) / jnp.maximum(count, 1.0)
    squares = jnp.sum(live * (conv - mean) * (conv - mean), axis=0, keepdims=True)
    moments = jnp.concatenate([jnp.broadcast_to(count, mean.shape), mean, squares, jnp.zeros((5, width), F32)], axis=0)
    moments, more = meet_levels(g, moments, merge_moments, buf1, m_send.at[0], m_recv.at[0])
    sends += more
    total_frames = moments[0:1]
    inv_std = lax.rsqrt(moments[2:3] / total_frames + BN_EPS)
    centre = moments[1:2]
    centred = c_ref[...] - centre
    zed = centred * inv_std
    bn_val = gains[12:13] * zed + gains[13:14]
    swish = (bn_val * sigmoid(bn_val)).astype(BF)
    sw_ref[...] = swish
    resid3 = resid2 + dot(swish, weight(7), NT)
    normed4 = norm_forward(resid3, gains, 3)
    a4_ref[...] = normed4
    loads[1].wait()
    loads[2].wait()
    resid4 = resid3 + 0.5 * module_forward(normed4, up, down, h4, s4_ref)
    y_buf[...] = norm_forward(resid4, gains, 4)
    away = jnp.logical_not(g.at_home())
    home = remote(y_buf, y_ref, y_sem.at[0], y_sem.at[1], g.owner())
    pl.when(away)(lambda: home.start())

    @pl.when(g.at_home())
    def _():
        y_ref[...] = y_buf[...]

    grad4, gain4, shift4 = norm_backward(resid4, gains, 4, cot_ref[...].astype(F32))
    half4 = (0.5 * grad4).astype(BF)
    e4_ref[...] = half4
    grad_norm, gain3, shift3 = norm_backward(resid3, gains, 3, module_backward(half4, up, down, h4, gh4_ref))
    grad3 = grad4 + grad_norm
    e3 = grad3.astype(BF)
    e3_ref[...] = e3
    sigma = sigmoid(bn_val)
    grad_bn = dot(e3, weight(7), NN) * (sigma * (1.0 + bn_val * (1.0 - sigma)))
    gamma = jnp.sum(grad_bn * zed, axis=0, keepdims=True)
    beta = jnp.sum(grad_bn, axis=0, keepdims=True)
    grad_zed = grad_bn * gains[12:13]
    sum_one = jnp.sum(grad_zed, axis=0, keepdims=True)
    sum_two = jnp.sum(grad_zed * centred, axis=0, keepdims=True)
    sums = jnp.concatenate([sum_one, sum_two, jnp.zeros((6, width), F32)], axis=0)
    sums, more = meet_levels(g, sums, lambda x, y: x + y, buf2, m_send.at[1], m_recv.at[1])
    sends += more
    offset = inv_std * sums[0:1] + inv_std * inv_std * inv_std * sums[1:2] * centred
    gc_b[...] = (inv_std * grad_zed - live / total_frames * offset).astype(BF)
    done2 = swap_edges(g, gc_b, low2, high2, h_send.at[1], h_recv.at[1], pad_gc)
    for at in range(0, width, LANES):
        lanes = pl.ds(at, LANES)
        total = jnp.zeros((rows, LANES), F32)
        upstream = pad_gc[pl.ds(HALO, rows), lanes]
        for m in range(taps):
            total = total + gains_ref[14 + m : 15 + m, lanes] * pad_gc[pl.ds(HALO + rim - m, rows), lanes]
            gtaps_ref[m : m + 1, lanes] = jnp.sum(
                upstream * pad_glu[pl.ds(HALO - rim + m, rows), lanes], axis=0, keepdims=True
            )
        c_ref[:, lanes] = total
    grad_glu = c_ref[...] * live
    gv5 = (grad_glu * gate).astype(BF)
    gv6 = (grad_glu * value * gate * (1.0 - gate)).astype(BF)
    gpair_ref[0] = gv5
    gpair_ref[1] = gv6
    grad_norm, gain2, shift2 = norm_backward(
        resid2, gains, 2, dot(gv5, weight(5), NN) + dot(gv6, weight(6), NN)
    )
    grad2 = grad3 + grad_norm
    g2_ref[...] = grad2
    e2 = grad2.astype(BF)
    e2_ref[...] = e2
    grad_out = dot(e2, weight(4), NN).astype(BF)
    for q in range(nz):
        go_buf[q] = grad_out[:, q * cols : (q + 1) * cols]
    for k in range(1, nz):
        q = lax.rem(z + k, nz)
        copy = remote(go_buf.at[q], go_ref.at[pl.ds(z * rows, rows)], b_send.at[k], b_recv.at[z], g.time(q))
        copy.start()
        sends.append(copy)
    go_ref[pl.ds(pl.multiple_of(z * rows, rows), rows), :] = go_buf[z]
    small_ref[...] = jnp.concatenate([gain2, shift2, gain3, shift3, gain4, shift4, gamma, beta], axis=0)
    for k in range(1, nz):
        q = lax.rem(z + k, nz)
        arrived(go_ref.at[pl.ds(q * rows, rows)], b_recv.at[q])
    pl.when(away)(lambda: home.wait())
    done1()
    done2()
    for copy in sends:
        copy.wait_send()


def middle(length, attended, resid1, cotangent, gains, taps, ud_full, sq_full):
    rows, width = resid1.shape
    nz, nf = lax.axis_size("seq"), lax.axis_size("fsdp")
    frames, cols = rows * nz, width // nz
    units = ud_full.shape[1] // 2
    most = max(nz, nf // 2)
    vmem = pl.BlockSpec(memory_space=pltpu.VMEM)
    hbm = pl.BlockSpec(memory_space=pl.ANY)
    shape = jax.ShapeDtypeStruct
    dma = pltpu.SemaphoreType.DMA
    row = shape((rows, width), BF)
    return pl.pallas_call(
        lambda *refs: middle_kernel(taps, *refs),
        name="middle",
        out_shape=(
            row,
            shape((rows, width), F32),
            shape((frames, cols), BF),
            row,
            row,
            row,
            shape((2, rows, width), BF),
            row,
            row,
            row,
            shape((rows, units), BF),
            shape((rows, units), BF),
            row,
            shape((8, width), F32),
            shape((taps, width), F32),
        ),
        in_specs=[vmem] * 5 + [hbm] * 2,
        out_specs=[vmem] * 15,
        scratch_shapes=[
            pltpu.VMEM((units, width), BF),
            pltpu.VMEM((units, width), BF),
            pltpu.VMEM((4 * width, width), BF),
            pltpu.VMEM((nz, rows, cols), BF),
            pltpu.VMEM((nz, rows, cols), BF),
            pltpu.VMEM((rows, width), BF),
            pltpu.VMEM((rows, width), BF),
        ]
        + [pltpu.VMEM((HALO, width), BF)] * 4
        + [
            pltpu.VMEM((rows + 2 * HALO, width), F32),
            pltpu.VMEM((rows + 2 * HALO, width), F32),
            pltpu.VMEM((rows, units), F32),
            pltpu.VMEM((rows, width), F32),
            pltpu.VMEM((rows, width), BF),
            dma((2,)),
            pltpu.VMEM((4, most, 8, width), F32),
            pltpu.VMEM((4, most, 8, width), F32),
            dma((3,)),
            dma((nz,)),
            dma((nz,)),
            dma((nz,)),
            dma((nz,)),
            dma((2, 2)),
            dma((2, 2)),
            dma((2, 4, most)),
            dma((2, 4, most)),
        ],
        compiler_params=pltpu.CompilerParams(
            collective_id=6, has_side_effects=True, vmem_limit_bytes=56 * 1024 * 1024
        ),
    )(length, attended, resid1, cotangent, gains, ud_full, sq_full)


class Meeting:
    def __init__(self, g, buf, send_sem, recv_sem, order="cabz"):
        self.g, self.buf, self.send_sem, self.recv_sem, self.order = g, buf, send_sem, recv_sem, order

    def copies(self, level):
        p, n, device = self.g.line(self.order[level])
        here = self.buf.at[level, p]
        return [
            remote(here, here, self.send_sem.at[level, k], self.recv_sem.at[level, p], device(lax.rem(p + k, n)))
            for k in range(1, n)
        ]

    def start(self, level, value):
        self.buf[level, self.g.line(self.order[level])[0]] = value
        for copy in self.copies(level):
            copy.start()

    def finish(self):
        for level in range(len(self.order)):
            for copy in self.copies(level):
                copy.wait_send()

    def total(self, level):
        p, n, _ = self.g.line(self.order[level])
        for k in range(1, n):
            q = lax.rem(p + k, n)
            arrived(self.buf.at[level, q], self.recv_sem.at[level, q])
        value = self.buf[level, 0]
        for q in range(1, n):
            value = value + self.buf[level, q]
        return value


class Reduction:
    def __init__(self, g, gud, gsq, sib_ud, sib_sq, sib_sem, rb, ra, rz, sems):
        self.g, self.gud, self.gsq, self.sib_ud, self.sib_sq = g, gud, gsq, sib_ud, sib_sq
        self.sib_send, self.sib_recv = sib_sem
        self.bufs = {"b": rb, "a": ra, "z": rz}
        self.sems = sems
        self.sq_rows = gsq.shape[2]
        self.pair = 2 * self.sq_rows
        self.height = g.plane * self.pair

    def rows(self, t, part):
        return pl.ds(pl.multiple_of(t * self.pair + (part - 1) * self.sq_rows, self.sq_rows), self.sq_rows)

    def own(self, t, part):
        c = self.g.core
        return self.gsq.at[t, c] if part == 0 else self.gud.at[c, self.rows(t, part)]

    def sibling_copy(self, z, kind):
        g = self.g
        d = 1 - g.core
        if kind == 0:
            chips = pl.ds(z * g.plane, g.plane)
            src, dst = self.gsq.at[chips, d], self.sib_sq.at[chips]
        else:
            tall = pl.ds(z * self.height, self.height)
            src, dst = self.gud.at[d, tall], self.sib_ud.at[tall]
        return remote(src, dst, self.sib_send.at[kind, z], self.sib_recv.at[kind, z], g.sibling())

    def to_sibling(self, planes, kind):
        for z in planes:
            self.sibling_copy(z, kind).start()

    def from_sibling(self, planes, kind):
        for z in planes:
            self.sibling_copy(z, kind).wait_recv()

    def add_sibling(self, t, part):
        ref = self.own(t, part)
        ref[...] = ref[...] + (self.sib_sq[t] if part == 0 else self.sib_ud[self.rows(t, part), :])

    def landing(self, axis, slot, part):
        return self.bufs[axis].at[slot, pl.ds(part * self.sq_rows, self.sq_rows)]

    def slot(self, axis, upward, z, a, b, there):
        g = self.g
        p, n = g.place(axis)
        q = {"z": z, "a": a, "b": b}[axis]
        if there:
            p = p + 1 if upward else p - 1
        if upward:
            q = q + 1 - n * (p == n - 1)
        return {"b": (q * g.na + a) * g.nz + z, "a": q * g.nz + z, "z": q}[axis]

    def hop(self, axis, upward, z, a, b, part):
        g = self.g
        slot = self.slot(axis, upward, z, a, b, True)
        sends, recvs = self.sems[axis]
        device = g.up(axis) if upward else g.down(axis)
        src, dst = self.own(g.chip(z, a, b), part), self.landing(axis, slot, part)
        return remote(src, dst, sends.at[1 if upward else 0, part, slot], recvs.at[part, slot], device)

    def take(self, axis, upward, z, a, b, part):
        slot = self.slot(axis, upward, z, a, b, False)
        src, dst = self.landing(axis, slot, part), self.own(self.g.chip(z, a, b), part)
        arrived(src, self.sems[axis][1].at[part, slot])
        dst[...] = dst[...] + src[...]

    def settle(self, axis, z, a, b, part):
        p, n = self.g.place(axis)
        if n > 1:
            pl.when(p > 0)(lambda: self.take(axis, True, z, a, b, part))
            pl.when(p < n - 1)(lambda: self.take(axis, False, z, a, b, part))

    def ready(self, axis, z, a, b, part):
        if axis == "b":
            self.add_sibling(self.g.chip(z, a, b), part)
        else:
            before = {"a": "b", "z": "a"}[axis]
            self.ready(before, z, a, b, part)
            self.settle(before, z, a, b, part)

    def pass_on(self, axis, upward, z, a, b, part, finish):
        p, n = self.g.place(axis)
        if finish:
            self.hop(axis, upward, z, a, b, part).wait_send()
            return
        self.ready(axis, z, a, b, part)
        behind = p > 0 if upward else p < n - 1
        pl.when(behind)(lambda: self.take(axis, upward, z, a, b, part))
        self.hop(axis, upward, z, a, b, part).start()

    def along(self, axis, planes, part, finish=False):
        g = self.g
        p, n = g.place(axis)
        if axis == "z":
            for q in planes:
                pl.when(p < q)(lambda: self.pass_on("z", True, q, g.a, g.b, part, finish))
                pl.when(p > q)(lambda: self.pass_on("z", False, q, g.a, g.b, part, finish))
            return
        step = planes[1] - planes[0] if len(planes) > 1 else 1
        count = len(planes)
        for k in range(n - 1, 0, -1):
            for upward in (True, False):
                q = p + k if upward else p - k

                def act():
                    def body(i, _):
                        plane = planes[0] + step * lax.rem(i, count)
                        if axis == "b":
                            a = lax.rem(g.a + 1 + i // count, g.na)
                            self.pass_on("b", upward, plane, a, q, part, finish)
                        else:
                            self.pass_on("a", upward, plane, q, g.b, part, finish)
                        return 0

                    lax.fori_loop(0, (g.na if axis == "b" else 1) * count, body, 0)

                pl.when(p + k < n if upward else p >= k)(act)

    def last(self, part):
        g = self.g
        self.ready("z", g.z, g.a, g.b, part)
        self.settle("z", g.z, g.a, g.b, part)


def back_kernel(head_size, qkv_ref, pos_ref, go_ref, coarse_ref, fine_ref, gains_ref,
                x_ref, x1_ref, g2_ref, a1_ref, h1_ref, s1_ref, a2_ref,
                a4_ref, s4_ref, gh4_ref, e4_ref, o_ref, e2_ref, a3_ref, gpair_ref, e3_ref, sw_ref, some_ref, gtaps_ref,
                prob_hbm, ud_hbm, sq_hbm,
                gx_ref, ud_out, sq_out, small_out,
                prob_buf, gk_acc, gv_acc, gpos_acc, gbias, grads, prob_sem, wqkv, heads, gqkv, gh1, small, few, fbuf, f_send, f_recv, gud, gsq, sib_ud, sib_sq, rb, ra, rz, sbuf, fin_send_buf, fin, gx_buf, gx_in, gx_sem,
                load_sem, h_send, h_recv, sib_send, sib_recv, b_send, b_recv, a_send, a_recv, z_send, z_recv, s_send, s_recv,
                fin_send, fin_recv):
    g = Grid()
    z, nz, c = g.t, g.nz, g.core
    rows, width = x_ref.shape
    cols = width // nz
    units = h1_ref.shape[1]
    frames = qkv_ref.shape[1]
    up, down = gud.at[0, pl.ds(0, units)], gud.at[1, pl.ds(0, units)]
    loads = [
        pltpu.make_async_copy(sq_hbm.at[pl.ds(0, 3 * width)], wqkv, load_sem.at[0]),
        pltpu.make_async_copy(ud_hbm.at[0, pl.ds(0, units)], up, load_sem.at[1]),
        pltpu.make_async_copy(ud_hbm.at[1, pl.ds(0, units)], down, load_sem.at[2]),
    ]

    def probabilities(i):
        return pltpu.make_async_copy(prob_hbm.at[:, pl.ds(i * rows, rows)], prob_buf.at[i % 2], prob_sem.at[i % 2])

    probabilities(0).start()
    for load in loads:
        load.start()
    greet_lines(g, "cabz", g.worker())
    sends = []
    small[...] = jnp.zeros_like(small)
    small[0:8, :] = some_ref[...]
    small[8 : 8 + gtaps_ref.shape[0], :] = gtaps_ref[...]
    early = Meeting(g, sbuf, s_send, s_recv)
    early.start(0, small[...])
    red = Reduction(
        g, gud, gsq, sib_ud, sib_sq, (sib_send, sib_recv), rb, ra, rz,
        {"b": (b_send, b_recv), "a": (a_send, a_recv), "z": (z_send, z_recv)},
    )
    total_rows = gud.shape[1]
    sq_rows = gsq.shape[2]
    high = list(range(nz - 1, nz // 2 - 1, -1))
    low = list(range(0, nz // 2))
    part = 256

    def matrix_terms(color, left_ref, right, first_row, count):
        def body(i, _):
            here = pl.ds(pl.multiple_of(i * part, part), part)
            there = pl.ds(pl.multiple_of(first_row + i * part, part), part)
            gud[color, there, :] = dot(left_ref[:, here], right, TN).astype(BF)
            return 0

        lax.fori_loop(0, count // part, body, 0)

    per = width // sq_rows // 2

    def square_terms(block, left, right):
        sums = dot(left, right, TN).astype(BF).reshape(per, 2, sq_rows, width)
        gsq[pl.ds(block * per, per)] = sums

    square_terms(7, e3_ref[...], sw_ref[...])
    square_terms(6, gpair_ref[1], a3_ref[...])
    square_terms(5, gpair_ref[0], a3_ref[...])
    square_terms(4, e2_ref[...], o_ref[...])
    red.to_sibling(high, 0)
    early.start(1, early.total(0))
    matrix_terms(0, gh4_ref, a4_ref[...], units, units)
    matrix_terms(1, s4_ref, e4_ref[...], units, units)
    red.to_sibling(high, 1)
    early.start(2, early.total(1))
    gk_acc[...] = jnp.zeros_like(gk_acc)
    gv_acc[...] = jnp.zeros_like(gv_acc)
    gpos_acc[...] = jnp.zeros_like(gpos_acc)
    gbias[...] = jnp.zeros_like(gbias)
    to_time = lambda j, q, k: remote(grads.at[j, q], heads.at[j, z], h_send.at[j, k], h_recv.at[j, z], g.time(q))
    bias = gains_ref[10:12, pl.ds(pl.multiple_of(z * cols, cols), cols)]

    def attend(i, _):
        pl.when(i + 1 < nz)(lambda: probabilities(i + 1).start())
        probabilities(i).wait()
        here = pl.ds(pl.multiple_of(i * rows, rows), rows)
        grads[0, i] = attend_back_block(
            head_size, i, qkv_ref[0, here, :], qkv_ref.at[1], qkv_ref.at[2], pos_ref, bias, prob_buf.at[i % 2],
            go_ref[here, :], gk_acc, gv_acc, gpos_acc, gbias,
        )

        @pl.when(i == 0)
        def _():
            early.start(3, early.total(2))
            red.from_sibling(high, 0)
            red.along("b", high, 0)

        @pl.when(i == 1)
        def _():
            red.from_sibling(high, 1)
            red.along("b", high, 1)
            red.along("b", high, 2)

        return 0

    lax.fori_loop(0, nz, attend, 0)
    small[...] = early.total(3)
    grads_k = gk_acc[...].T.astype(BF)
    grads_v = gv_acc[...].T.astype(BF)
    for q in range(nz):
        grads[1, q] = grads_k[q * rows : (q + 1) * rows]
        grads[2, q] = grads_v[q * rows : (q + 1) * rows]
    for k in range(1, nz):
        q = lax.rem(z + k, nz)
        for j in range(3):
            copy = to_time(j, q, k)
            copy.start()
            sends.append(copy)
    for j in range(3):
        heads[j, z] = grads[j, z]
    red.along("a", high, 0)
    fine = fine_ref.shape[1]

    def position(i, total):
        table = coarse_ref[0, pl.ds(2 * i, 1), :] * fine_ref[0] + coarse_ref[1, pl.ds(2 * i, 1), :] * fine_ref[1]
        after = coarse_ref[0, pl.ds(2 * i + 1, 1), :] * fine_ref[0] + coarse_ref[1, pl.ds(2 * i + 1, 1), :] * fine_ref[1]
        both = jnp.concatenate([table, after], axis=0).astype(BF)
        return total + dot(gpos_acc[:, pl.ds(pl.multiple_of(i * 2 * fine, 2 * fine), 2 * fine)].astype(BF), both, NN)

    gpos = lax.fori_loop(0, coarse_ref.shape[1] // 2, position, jnp.zeros((cols, width), F32)).astype(BF)
    gsq[pl.ds(3 * per, per)] = jnp.zeros((per, 2, sq_rows, width), BF)
    pieces = cols // sq_rows
    for i in range(pieces):
        piece = z * pieces + i
        gsq[3 * per + piece // 2, piece % 2] = gpos[i * sq_rows : (i + 1) * sq_rows]
    gains = gains_ref[...]
    loads[0].wait()
    grad_norm = jnp.zeros((rows, width), F32)
    for j in range(3):
        for k in range(1, nz):
            q = lax.rem(z + k, nz)
            arrived(heads.at[j, q], h_recv.at[j, q])
        full = jnp.concatenate([heads[j, q] for q in range(nz)], axis=1)
        gqkv[j] = full
        grad_norm = grad_norm + dot(full, wqkv[pl.ds(j * width, width), :], NN)
    for j in range(3):
        square_terms(j, gqkv[j], a2_ref[...])
    red.to_sibling(low, 0)
    resid1 = x1_ref[...]
    grad_add, gain1, shift1 = norm_backward(resid1, gains, 1, grad_norm)
    grad1 = g2_ref[...] + grad_add
    half1 = (0.5 * grad1).astype(BF)
    loads[1].wait()
    loads[2].wait()
    red.along("a", high, 1)
    grad_norm = module_backward(half1, up, down, h1_ref, gh1)
    red.from_sibling(low, 0)
    red.along("b", low, 0)
    matrix_terms(0, gh1, a1_ref[...], 0, units)
    matrix_terms(1, s1_ref, half1, 0, units)
    red.to_sibling(low, 1)
    red.along("a", high, 2)
    grad_add, gain0, shift0 = norm_backward(x_ref[...].astype(F32), gains, 0, grad_norm)
    away = jnp.logical_not(g.at_home())
    gx_buf[...] = (grad1 + grad_add).astype(BF)
    home = remote(gx_buf, gx_in, gx_sem.at[0], gx_sem.at[1], g.owner())
    pl.when(away)(lambda: home.start())
    few[...] = jnp.zeros_like(few)
    few[0:1, :] = gain0
    few[1:2, :] = shift0
    few[2:3, :] = gain1
    few[3:4, :] = shift1
    few[4:6, pl.ds(pl.multiple_of(z * cols, cols), cols)] = gbias[...]
    meeting = Meeting(g, fbuf, f_send, f_recv)
    meeting.start(0, few[...])
    red.from_sibling(low, 1)
    red.along("b", low, 1)
    red.along("b", low, 2)
    red.along("a", low, 0)
    meeting.start(1, meeting.total(0))
    red.along("z", high, 0)
    red.along("z", high, 1)
    red.along("a", low, 1)
    red.along("z", low, 0)
    meeting.start(2, meeting.total(1))
    red.along("z", high, 2)
    red.along("a", low, 2)
    red.along("z", low, 1)
    meeting.start(3, meeting.total(2))
    red.along("z", low, 2)
    for part in range(3):
        red.last(part)
    me = g.chip(g.z, g.a, g.b)
    d = 1 - c
    half = ud_out.shape[1]
    at = lambda k: pl.ds(pl.multiple_of(me * 2 * half + k * half, half), half)
    fin_send_buf[...] = gud[c, at(d), :]
    swap = remote(fin_send_buf, fin, fin_send, fin_recv, g.sibling())
    swap.start()
    ud_out[c] = gud[c, at(c), :].astype(F32)
    sq_out[...] = gsq[me, c].astype(F32)
    total = meeting.total(3)
    small_out[0:4, :] = total[0:4]
    small_out[4:10, :] = small[0:6, :]
    small_out[10:12, :] = total[4:6]
    small_out[12 : small.shape[0] + 6, :] = small[6:, :]
    for planes in (high, low):
        for part in range(3):
            for axis in "baz":
                red.along(axis, planes, part, True)
        for kind in range(2):
            for q in planes:
                red.sibling_copy(q, kind).wait_send()
    for copy in sends:
        copy.wait_send()
    early.finish()
    meeting.finish()

    @pl.when(away)
    def _():
        home.wait()
        gx_ref[...] = gx_in[...].astype(F32)

    @pl.when(g.at_home())
    def _():
        gx_ref[...] = gx_buf[...].astype(F32)

    swap.wait()
    ud_out[d] = fin[...].astype(F32)


def back(qkv, pos, grad_out, prob, head_size, coarse, fine, gains, signal, resid1, grad2, first, second, squares, some, gtaps, ud_full, sq_full):
    rows, width = signal.shape
    nz, nf = lax.axis_size("seq"), lax.axis_size("fsdp")
    chips = nz * nf // 2
    plane = nf // 2
    side = math.isqrt(plane)
    na, nb = (side, side) if side * side == plane else (plane, 1)
    cols = width // nz
    units = ud_full.shape[1] // 2
    own = ud_full.shape[1] // (2 * chips)
    block = 3 * own
    most = max(nz, na, nb, 2)
    tall = -(-(8 + gtaps.shape[0]) // 8) * 8
    vmem = pl.BlockSpec(memory_space=pltpu.VMEM)
    hbm = pl.BlockSpec(memory_space=pl.ANY)
    shape = jax.ShapeDtypeStruct
    dma = pltpu.SemaphoreType.DMA
    frames = rows * nz
    heads = cols // head_size
    operands = (qkv, pos, grad_out, coarse, fine, gains, signal, resid1, grad2, *first, *second, *squares, some, gtaps)
    places = lambda n: n + 1 if n > 2 else 1
    slots = {"b": places(nb) * na * nz, "a": places(na) * nz, "z": places(nz)}
    return pl.pallas_call(
        lambda *refs: back_kernel(head_size, *refs),
        name="back",
        out_shape=(
            shape((rows, width), F32),
            shape((2, own, width), F32),
            shape((own, width), F32),
            shape((tall + 6, width), F32),
        ),
        in_specs=[vmem] * len(operands) + [hbm] * 3,
        out_specs=[vmem] * 4,
        scratch_shapes=[
            pltpu.VMEM((2, heads, rows, frames), BF),
            pltpu.VMEM((cols, frames), F32),
            pltpu.VMEM((cols, frames), F32),
            pltpu.VMEM((cols, 2 * frames), F32),
            pltpu.VMEM((2, cols), F32),
            pltpu.VMEM((3, nz, rows, cols), BF),
            dma((2,)),
            pltpu.VMEM((3 * width, width), BF),
            pltpu.VMEM((3, nz, rows, cols), BF),
            pltpu.VMEM((3, rows, width), BF),
            pltpu.VMEM((rows, units), BF),
            pltpu.VMEM((tall, width), F32),
            pltpu.VMEM((8, width), F32),
            pltpu.VMEM((4, most, 8, width), F32),
            dma((4, most)),
            dma((4, most)),
            pltpu.VMEM((2, 2 * units, width), BF),
            pltpu.VMEM((chips, 2, own, width), BF),
            pltpu.VMEM((2 * units, width), BF),
            pltpu.VMEM((chips, own, width), BF),
            pltpu.VMEM((slots["b"], block, width), BF),
            pltpu.VMEM((slots["a"], block, width), BF),
            pltpu.VMEM((slots["z"], block, width), BF),
            pltpu.VMEM((4, most, tall, width), F32),
            pltpu.VMEM((own, width), BF),
            pltpu.VMEM((own, width), BF),
            pltpu.VMEM((rows, width), BF),
            pltpu.VMEM((rows, width), BF),
            dma((2,)),
            dma((3,)),
            dma((3, nz)),
            dma((3, nz)),
            dma((2, nz)),
            dma((2, nz)),
            dma((2, 3, slots["b"])),
            dma((3, slots["b"])),
            dma((2, 3, slots["a"])),
            dma((3, slots["a"])),
            dma((2, 3, slots["z"])),
            dma((3, slots["z"])),
            dma((4, most)),
            dma((4, most)),
            dma,
            dma,
        ],
        compiler_params=pltpu.CompilerParams(
            collective_id=7, has_side_effects=True, vmem_limit_bytes=61000 * 1024
        ),
    )(*operands, prob, ud_full, sq_full)


def finish_kernel(rows, y_ref, gx_ref, matrices_ref, square_ref, small_ref, *refs):
    states, outs = refs[:15], refs[15:]
    outs[0][...] = y_ref[...]
    outs[1][...] = gx_ref[...]
    count, share = rows, states[9].shape[1]
    taps = states[12].shape[1]
    width = small_ref.shape[1]
    place = lax.axis_index("seq") * lax.axis_size("fsdp") + lax.axis_index("fsdp")
    own = pltpu.roll(small_ref[...], lax.rem(width - place * share, width), 1)[:, :LANES]
    below = jnp.concatenate([own[count : count + taps], jnp.zeros((-taps % 8, LANES), F32)], axis=0)
    gradients = (
        square_ref[...],
        matrices_ref[0],
        matrices_ref[1],
        own[:count, :share],
        below.T[:share, :taps],
    )
    fix_one = 1.0 - BETA_ONE**ADAM_STEP
    fix_two = 1.0 - BETA_TWO**ADAM_STEP
    for k, gradient in enumerate(gradients):
        weight, first_mom, second_mom = (ref[...] for ref in states[3 * k : 3 * k + 3])
        decay = 0.0 if k == 3 else DECAY_RATE
        first_new = BETA_ONE * first_mom + (1.0 - BETA_ONE) * gradient
        second_new = BETA_TWO * second_mom + (1.0 - BETA_TWO) * gradient * gradient
        update = first_new / fix_one / (jnp.sqrt(second_new / fix_two) + ADAM_EPS)
        there = outs[2 + 4 * k : 6 + 4 * k]
        there[0][...] = gradient
        there[1][...] = weight - LEARN_RATE * (update + decay * weight)
        there[2][...] = first_new
        there[3][...] = second_new


def finish(layer_output, input_grad, matrices, square, small, states):
    flat = [array for state in states for array in state]
    results = [layer_output, input_grad] + [array for state in states for array in (state[0],) * 4]
    vmem = pl.BlockSpec(memory_space=pltpu.VMEM)
    return pl.pallas_call(
        lambda *refs: finish_kernel(states[3][0].shape[0], *refs),
        name="finish",
        out_shape=[jax.ShapeDtypeStruct(array.shape, array.dtype) for array in results],
        in_specs=[vmem] * (5 + len(flat)),
        out_specs=[vmem] * len(results),
    )(layer_output, input_grad, matrices, square, small, *flat)


def when(*conditions):
    holds = 1
    for condition in conditions:
        holds = holds * jnp.asarray(condition).astype(jnp.int32)
    return pl.when(holds == 1) if conditions else lambda act: act()


class Gather:
    WAYS = {"z+": 0, "z-": 1, "a+": 2, "a-": 3, "b+": 4, "b-": 5, "s": 6}
    PARTS = (0, 1, 2)
    SPREAD = ("a+", "a-", "b+", "b-", "s")

    def __init__(self, g, ud, sq, recv_sem, sib_recv, send_sem):
        self.g, self.ud, self.sq = g, ud, sq
        self.recv_sem, self.sib_recv, self.send_sem = recv_sem, sib_recv, send_sem
        self.rows = sq.shape[2]
        half = g.nz // 2
        if half == 2:
            first = jnp.minimum(g.z, 1)
            second = jnp.maximum(g.z, 2)
            self.low, self.high = [first, 1 - first], [second, 5 - second]
        else:
            self.low, self.high = list(range(half)), list(range(half, g.nz))
        self.below = g.z < half

    def piece(self, part, t, color):
        if part == 0:
            return self.sq.at[t, color]
        return self.ud.at[color, pl.ds(t * 2 * self.rows + (part - 1) * self.rows, self.rows)]

    def onward(self, part, t, ways, finish, *only):
        g = self.g
        ref = self.piece(part, t, g.core)
        for way in ways:
            p, n = (0, 2) if way == "s" else g.place(way[0])

            def act():
                if way == "s":
                    target, arrive = g.sibling(), self.sib_recv
                else:
                    target, arrive = g.up(way[0]) if way[1] == "+" else g.down(way[0]), self.recv_sem
                copy = remote(ref, ref, self.send_sem.at[self.WAYS[way], part, t], arrive.at[part, t], target)
                copy.wait_send() if finish else copy.start()

            if way == "s":
                when(*only)(act)
            elif n > 1:
                when(*only, p < n - 1 if way[1] == "+" else p > 0)(act)

    def wait(self, part, t, finish):
        if not finish:
            arrived(self.piece(part, t, self.g.core), self.recv_sem.at[part, t])

    def column(self, q, spread, finish, *only):
        g = self.g
        t = g.chip(q, g.a, g.b)
        for part in self.PARTS:
            when(*only, q != g.z)(lambda: self.wait(part, t, finish))
            self.onward(part, t, ("z+",), finish, *only, q <= g.z)
            self.onward(part, t, ("z-",), finish, *only, q >= g.z)
            if spread:
                self.onward(part, t, self.SPREAD, finish, *only)

    def spread(self, q, finish, *only):
        g = self.g
        for part in self.PARTS:
            self.onward(part, g.chip(q, g.a, g.b), self.SPREAD, finish, *only)

    def both(self, axis, k, act):
        p, n = self.g.place(axis)
        pl.when(p >= k)(lambda: act(p - k, axis + "+"))
        pl.when(p + k < n)(lambda: act(p + k, axis + "-"))

    def along_a(self, q, finish=False):
        g = self.g

        def take(a, way):
            t = g.chip(q, a, g.b)
            for part in self.PARTS:
                self.wait(part, t, finish)
                self.onward(part, t, (way, "b+", "b-", "s"), finish)

        for k in range(1, g.na):
            self.both("a", k, take)

    def along_b(self, q, finish=False):
        g = self.g

        def row(b, way):
            def body(i, _):
                t = g.chip(q, lax.rem(g.a + i, g.na), b)
                for part in self.PARTS:
                    self.wait(part, t, finish)
                    self.onward(part, t, (way, "s"), finish)
                return 0

            lax.fori_loop(0, g.na, body, 0)

        for k in range(1, g.nb):
            self.both("b", k, row)

    def own(self, finish=False):
        if len(self.low) == 2:
            self.column(self.low[0], True, finish, self.below)
        self.column(self.high[0], False, finish, jnp.logical_not(self.below))

    def first(self, finish=False):
        below, above = self.below, jnp.logical_not(self.below)
        if len(self.low) == 2:
            self.column(self.low[0], True, finish, above)
        else:
            self.column(self.low[0], True, finish)
        for q in self.high[1:]:
            self.column(q, False, finish, above)
        self.along_a(self.low[0], finish)
        for q in self.low[1:]:
            self.column(q, True, finish)
            self.along_a(q, finish)
        self.spread(self.high[0], finish, above)
        self.column(self.high[0], False, finish, below)
        for q in self.low:
            self.along_b(q, finish)
        for q in self.high[1:]:
            self.column(q, False, finish, below)
        self.spread(self.high[0], finish, below)
        for q in self.high[1:]:
            self.spread(q, finish)

    def from_sibling(self, upper):
        g = self.g
        count = g.chips // 2

        def body(i, _):
            for part in self.PARTS:
                t = upper * count + i
                arrived(self.piece(part, t, 1 - g.core), self.sib_recv.at[part, t])
            return 0

        lax.fori_loop(0, count, body, 0)


def head_kernel(head_size, up_own, down_own, sq_own, vec_in, taps_in, x_in, cot_in, len_smem, coarse_ref, fine_ref,
                ud_full, sq_full, small_ref, x_ref, cot_ref, len_ref,
                x1_ref, a1_ref, h1_ref, s1_ref, a2_ref, heads_ref, pos_ref, att_ref, prob_hbm,
                own, len_in, columns, sbuf, up, down, wqkv, wpos, mine, prob_buf,
                move_send, move_recv, local_sem, swap_sem, recv_sem, sib_recv, gather_send, s_send, s_recv,
                load_sem, send_sem, heads_recv, prob_sem):
    g = Grid()
    z, nz, c = g.t, g.nz, g.core
    rows, width = x_in.shape
    cols = width // nz
    units = up.shape[0]
    half = up_own.shape[0]
    me = g.chip(g.z, g.a, g.b)
    own[0] = up_own[...].astype(BF)
    own[1] = down_own[...].astype(BF)
    own[2] = sq_own[...].astype(BF)
    here = pl.ds(me * 2 * half + c * half, half)
    local = [
        pltpu.make_async_copy(own.at[c], ud_full.at[c, here], local_sem.at[0]),
        pltpu.make_async_copy(own.at[2], sq_full.at[me, c], local_sem.at[1]),
    ]
    for copy in local:
        copy.start()
    len_in[...] = jnp.full(len_in.shape, len_smem[0].astype(F32))
    share = vec_in.shape[1]
    count = vec_in.shape[0]
    taps = taps_in.shape[1]
    lane = lax.broadcasted_iota(jnp.int32, (share, width), 1)
    column = lax.broadcasted_iota(jnp.int32, (share, width), 0)
    place = jnp.where(lane - (g.z * g.nf + g.f) * share == column, 1.0, 0.0).astype(BF)
    columns[...] = jnp.zeros_like(columns)
    columns[0:count, :] = dot(vec_in[...].astype(BF), place, NN)
    columns[count : count + taps, :] = dot(taps_in[...].astype(BF), place, TN)
    greet_lines(g, "cabz", g.owner())
    swap = remote(own.at[1 - c], ud_full.at[1 - c, here], swap_sem.at[0], swap_sem.at[1], g.sibling())
    swap.start()
    moves = [
        remote(src, dst, move_send.at[k], move_recv.at[k], g.worker())
        for k, (src, dst) in enumerate(((x_in, x_ref), (len_in, len_ref), (cot_in, cot_ref)))
    ]

    @pl.when(jnp.logical_not(g.at_home()))
    def _():
        for copy in moves[:2]:
            copy.start()

    @pl.when(g.at_home())
    def _():
        x_ref[...] = x_in[...]
        len_ref[...] = len_in[...]
        cot_ref[...] = cot_in[...]

    meeting = Meeting(g, sbuf, s_send, s_recv)
    meeting.start(0, columns[...].astype(BF))
    gather = Gather(g, ud_full, sq_full, recv_sem, sib_recv, gather_send)
    for copy in local:
        copy.wait()
    swap.wait_recv()
    gather.own()
    meeting.start(1, meeting.total(0))
    meeting.start(2, meeting.total(1))
    gather.first()
    meeting.start(3, meeting.total(2))

    @pl.when(jnp.logical_not(g.at_home()))
    def _():
        moves[2].start()
        for copy in moves[:2]:
            copy.wait()

    gather.from_sibling(0)
    loads = [
        pltpu.make_async_copy(ud_full.at[0, pl.ds(0, units)], up, load_sem.at[0]),
        pltpu.make_async_copy(ud_full.at[1, pl.ds(0, units)], down, load_sem.at[1]),
    ]
    per = width // (2 * half)
    squares = pltpu.make_async_copy(sq_full.at[pl.ds(0, 3 * per)], wqkv, load_sem.at[2])
    pieces = cols // half
    positions = [
        pltpu.make_async_copy(
            sq_full.at[3 * per + (z * pieces + i) // 2, (z * pieces + i) % 2],
            wpos.at[pl.ds(i * half, half)],
            load_sem.at[3],
        )
        for i in range(pieces)
    ]
    for load in loads + [squares]:
        load.start()
    for load in positions:
        load.start()
        load.wait()
    small_ref[...] = meeting.total(3).astype(F32)
    gains = small_ref[...]
    signal = x_ref[...].astype(F32)
    normed1 = norm_forward(signal, gains, 0)
    a1_ref[...] = normed1
    for load in loads:
        load.wait()
    resid1 = signal + 0.5 * module_forward(normed1, up, down, h1_ref, s1_ref)
    x1_ref[...] = resid1
    gather.along_a(gather.high[0])
    normed2 = norm_forward(resid1, gains, 1)
    a2_ref[...] = normed2
    squares.wait()
    for k in range(3):
        weight = wqkv[pl.ds(k * per, per)].reshape(width, width)
        out = dot(normed2, weight, NT).astype(BF)
        for q in range(nz):
            mine[q, k] = out[:, q * cols : (q + 1) * cols]
    sends = []
    for k in range(1, nz):
        q = lax.rem(z + k, nz)
        copy = remote(mine.at[q], heads_ref.at[:, pl.ds(z * rows, rows)], send_sem.at[k], heads_recv.at[z], g.time(q))
        copy.start()
        sends.append(copy)
    slot = pl.ds(pl.multiple_of(z * rows, rows), rows)
    for k in range(3):
        heads_ref[k, slot, :] = mine[z, k]
    for q in gather.high[1:]:
        gather.along_a(q)
    fine = fine_ref.shape[1]
    weight = wpos[...]

    def position(i, _):
        table = coarse_ref[0, pl.ds(i, 1), :] * fine_ref[0] + coarse_ref[1, pl.ds(i, 1), :] * fine_ref[1]
        there = pl.ds(pl.multiple_of(i * fine, fine), fine)
        pos_ref[there, :] = dot(table.astype(BF), weight, NT).astype(BF)
        return 0

    lax.fori_loop(0, coarse_ref.shape[1], position, 0)
    for k in range(1, nz):
        q = lax.rem(z + k, nz)
        arrived(heads_ref.at[:, pl.ds(q * rows, rows)], heads_recv.at[q])
    bias = small_ref[10:12, pl.ds(pl.multiple_of(z * cols, cols), cols)]

    def keep(i):
        return pltpu.make_async_copy(
            prob_buf.at[i % 2], prob_hbm.at[:, pl.ds(i * rows, rows)], prob_sem.at[i % 2]
        )

    def attend(i, _):
        pl.when(i >= 2)(lambda: keep(i - 2).wait())
        there = pl.ds(pl.multiple_of(i * rows, rows), rows)
        att_ref[there, :] = attend_block(
            head_size, i, heads_ref[0, there, :], heads_ref.at[1], heads_ref.at[2], pos_ref, bias, len_ref, prob_buf.at[i % 2]
        )
        keep(i).start()
        for k, q in enumerate(gather.high):
            pl.when(i == min(2 * k + 1, nz - 1))(lambda: gather.along_b(q))
        return 0

    lax.fori_loop(0, nz, attend, 0)
    gather.from_sibling(1)
    keep(nz - 2).wait()
    keep(nz - 1).wait()
    swap.wait_send()
    for copy in sends:
        copy.wait_send()
    meeting.finish()
    gather.own(True)
    gather.first(True)
    for q in gather.high:
        gather.along_a(q, True)
        gather.along_b(q, True)

    @pl.when(jnp.logical_not(g.at_home()))
    def _():
        moves[2].wait()


def head(upward, downward, square, vectors, kernel, signal, cotangent, lengths, coarse, fine, head_size):
    rows, width = signal.shape
    nz, nf = lax.axis_size("seq"), lax.axis_size("fsdp")
    devices = nz * nf
    chips, plane = devices // 2, nf // 2
    own = upward.shape[0]
    frames, cols = rows * nz, width // nz
    units = own * devices // 2
    heads = cols // head_size
    tall = -(-(vectors.shape[0] + kernel.shape[1]) // 16) * 16
    side = math.isqrt(plane)
    most = max(nz, side if side * side == plane else plane, 2)
    vmem = pl.BlockSpec(memory_space=pltpu.VMEM)
    hbm = pl.BlockSpec(memory_space=pl.ANY)
    shape = jax.ShapeDtypeStruct
    dma = pltpu.SemaphoreType.DMA
    return pl.pallas_call(
        lambda *refs: head_kernel(head_size, *refs),
        name="head",
        out_shape=(
            shape((2, devices * own, width), BF),
            shape((chips, 2, own, width), BF),
            shape((tall, width), F32),
            shape(signal.shape, signal.dtype),
            shape(cotangent.shape, cotangent.dtype),
            shape((8, LANES), F32),
            shape((rows, width), F32),
            shape((rows, width), BF),
            shape((rows, units), BF),
            shape((rows, units), BF),
            shape((rows, width), BF),
            shape((3, frames, cols), BF),
            shape((2 * frames, cols), BF),
            shape((frames, cols), BF),
            shape((heads, frames, frames), BF),
        ),
        in_specs=[vmem] * 7 + [pl.BlockSpec(memory_space=pltpu.SMEM)] + [vmem] * 2,
        out_specs=[hbm] * 2 + [vmem] * 12 + [hbm],
        scratch_shapes=[
            pltpu.VMEM((3, own, width), BF),
            pltpu.VMEM((8, LANES), F32),
            pltpu.VMEM((tall, width), F32),
            pltpu.VMEM((4, most, tall, width), BF),
            pltpu.VMEM((units, width), BF),
            pltpu.VMEM((units, width), BF),
            pltpu.VMEM((3 * width // (2 * own), 2, own, width), BF),
            pltpu.VMEM((cols, width), BF),
            pltpu.VMEM((nz, 3, rows, cols), BF),
            pltpu.VMEM((2, heads, rows, frames), BF),
            dma((3,)),
            dma((3,)),
            dma((2,)),
            dma((2,)),
            dma((3, chips)),
            dma((3, chips)),
            dma((7, 3, chips)),
            dma((4, most)),
            dma((4, most)),
            dma((4,)),
            dma((nz,)),
            dma((nz,)),
            dma((2,)),
        ],
        compiler_params=pltpu.CompilerParams(
            collective_id=5, has_side_effects=True, vmem_limit_bytes=56 * 1024 * 1024
        ),
    )(upward, downward, square, vectors, kernel, signal, cotangent, lengths, coarse, fine)


def per_device(
    inputs,
    cotangent,
    lengths,
    square,
    upward,
    downward,
    vectors,
    kernel,
    square_momentum,
    square_variance,
    upward_momentum,
    upward_variance,
    downward_momentum,
    downward_variance,
    vectors_momentum,
    vectors_variance,
    kernel_momentum,
    kernel_variance,
):
    model_width = inputs.shape[2]
    seq_frames = inputs.shape[1] * lax.axis_size("seq")
    head_size = D // H
    coarse, fine = position_tables(seq_frames, model_width)
    (
        full_ud, full_sq, small, signal, cotangent_here, length,
        resid1, normed1, hidden1, active1, normed2, heads, pos_heads, attended, prob,
    ) = head(upward, downward, square, vectors, kernel.T, inputs[0], cotangent[0], lengths, coarse, fine, head_size)
    full_sq = full_sq.reshape(model_width * 8, model_width)
    (
        layer_output, grad_res2, grad_out_head, out_time, grad_att_b, normed3, grad_pair, grad_conv_b, swish_b, normed4,
        active4, grad_hidden4, half4, small_grads, grad_taps,
    ) = middle(length, attended, resid1, cotangent_here, small, kernel.shape[0], full_ud, full_sq)
    input_grad, matrix_grads, square_grad, small_sums = back(
        heads, pos_heads, grad_out_head, prob, head_size, coarse, fine, small,
        signal, resid1, grad_res2, (normed1, hidden1, active1, normed2), (normed4, active4, grad_hidden4, half4),
        (out_time, grad_att_b, normed3, grad_pair, grad_conv_b, swish_b), small_grads, grad_taps, full_ud, full_sq,
    )
    (
        layer_output, input_grad,
        square_grad, square_next, momentum_square, variance_square,
        upward_grad, upward_next, momentum_upward, variance_upward,
        downward_grad, downward_next, momentum_downward, variance_downward,
        vectors_grad, vectors_next, momentum_vectors, variance_vectors,
        kernel_grad, kernel_next, momentum_kernel, variance_kernel,
    ) = finish(
        layer_output, input_grad, matrix_grads, square_grad, small_sums,
        (
            (square, square_momentum, square_variance),
            (upward, upward_momentum, upward_variance),
            (downward, downward_momentum, downward_variance),
            (vectors, vectors_momentum, vectors_variance),
            (kernel.T, kernel_momentum.T, kernel_variance.T),
        ),
    )
    return (
        layer_output[None],
        input_grad[None],
        square_grad,
        upward_grad,
        downward_grad,
        vectors_grad,
        kernel_grad.T,
        square_next,
        upward_next,
        downward_next,
        vectors_next,
        kernel_next.T,
        momentum_square,
        variance_square,
        momentum_upward,
        variance_upward,
        momentum_downward,
        variance_downward,
        momentum_vectors,
        variance_vectors,
        momentum_kernel.T,
        variance_kernel.T,
    )


def solution(mesh):
    return jax.shard_map(
        per_device,
        mesh=mesh,
        in_specs=(
            P("fsdp", "seq", None),
            P("fsdp", "seq", None),
            P("fsdp"),
            P(("seq", "fsdp"), None),
            P(("seq", "fsdp"), None),
            P(("seq", "fsdp"), None),
            P(None, ("seq", "fsdp")),
            P(None, ("seq", "fsdp")),
            P(("seq", "fsdp"), None),
            P(("seq", "fsdp"), None),
            P(("seq", "fsdp"), None),
            P(("seq", "fsdp"), None),
            P(("seq", "fsdp"), None),
            P(("seq", "fsdp"), None),
            P(None, ("seq", "fsdp")),
            P(None, ("seq", "fsdp")),
            P(None, ("seq", "fsdp")),
            P(None, ("seq", "fsdp")),
        ),
        out_specs=(
            P("fsdp", "seq", None),
            P("fsdp", "seq", None),
            P(("seq", "fsdp"), None),
            P(("seq", "fsdp"), None),
            P(("seq", "fsdp"), None),
            P(None, ("seq", "fsdp")),
            P(None, ("seq", "fsdp")),
            P(("seq", "fsdp"), None),
            P(("seq", "fsdp"), None),
            P(("seq", "fsdp"), None),
            P(None, ("seq", "fsdp")),
            P(None, ("seq", "fsdp")),
            P(("seq", "fsdp"), None),
            P(("seq", "fsdp"), None),
            P(("seq", "fsdp"), None),
            P(("seq", "fsdp"), None),
            P(("seq", "fsdp"), None),
            P(("seq", "fsdp"), None),
            P(None, ("seq", "fsdp")),
            P(None, ("seq", "fsdp")),
            P(None, ("seq", "fsdp")),
            P(None, ("seq", "fsdp")),
        ),
        check_vma=False,
    )
```

```python
import math

import jax
import jax.numpy as jnp
from jax import lax
from jax.experimental import pallas as pl
from jax.experimental.pallas import tpu as pltpu
from jax.sharding import PartitionSpec as P

D = 512
H = 8
FF = 2048
ADAM_STEP = 4

LN_EPS = 1e-05
BN_EPS = 1e-05
BETA_ONE = 0.9
BETA_TWO = 0.98
ADAM_EPS = 1e-08
LEARN_RATE = 0.005
DECAY_RATE = 0.01


def position_tables(seq_frames, model_width):
    fine = math.gcd(2 * seq_frames, 64)
    column = jnp.arange(model_width)
    frequency = jnp.exp(-math.log(10000.0) * 2.0 * (column // 2).astype(jnp.float32) / model_width)
    coarse_at = (seq_frames - 1 - fine * jnp.arange(2 * seq_frames // fine)).astype(jnp.float32)
    coarse_phase = coarse_at[:, None] * frequency[None, :]
    fine_phase = jnp.arange(fine).astype(jnp.float32)[:, None] * frequency[None, :]
    even = (column % 2 == 0)[None, :]
    sine, cosine = jnp.sin(coarse_phase), jnp.cos(coarse_phase)
    with_cosine = jnp.where(even, sine, cosine)
    with_sine = jnp.where(even, -cosine, sine)
    return jnp.stack([with_cosine, with_sine]), jnp.stack([jnp.cos(fine_phase), jnp.sin(fine_phase)])


MESH = pl.DeviceIdType.MESH
BF = jnp.bfloat16
F32 = jnp.float32
LANES = 128


class Grid:
    def __init__(self):
        self.nz = lax.axis_size("seq")
        self.nf = lax.axis_size("fsdp")
        plane = self.nf // 2
        side = math.isqrt(plane)
        self.z = lax.axis_index("seq")
        f = lax.axis_index("fsdp")
        self.core = f % 2
        if side * side == plane:
            self.na = self.nb = side
            self.step_a = 2 + self.core * (2 * side - 2)
            self.step_b = 2 * side - self.core * (2 * side - 2)
        else:
            self.na, self.nb = plane, 1
            self.step_a, self.step_b = 2, self.nf
        self.f = f
        self.a = (f // self.step_a) % self.na
        self.b = (f // self.step_b) % self.nb
        self.plane = plane
        self.chips = plane * self.nz

        self.half = self.nz // 2
        self.t = (self.z % self.half) * 2 + self.core
        self.column = f - self.core

    def time(self, q):
        return (self.z - self.z % self.half + q // 2, self.column + q % 2)

    def owner(self):
        return (self.t, self.column + self.z // self.half)

    def worker(self):
        return (self.core * self.half + self.z // 2, self.column + self.z % 2)

    def at_home(self):
        return jnp.logical_and(self.t == self.z, self.z // self.half == self.core)

    def chip(self, z, a, b):
        return z * self.plane + (a * self.step_a + b * self.step_b) // 2

    def device(self, z, a, b):
        return (z, a * self.step_a + b * self.step_b + self.core)

    def sibling(self):
        return (self.z, self.f + 1 - 2 * self.core)

    def up(self, axis):
        return self.device(self.z + (axis == "z"), self.a + (axis == "a"), self.b + (axis == "b"))

    def down(self, axis):
        return self.device(self.z - (axis == "z"), self.a - (axis == "a"), self.b - (axis == "b"))

    def line(self, axis):
        return {
            "c": (self.core, 2, lambda q: (self.z, self.f - self.core + q)),
            "a": (self.a, self.na, lambda q: self.device(self.z, q, self.b)),
            "b": (self.b, self.nb, lambda q: self.device(self.z, self.a, q)),
            "z": (self.z, self.nz, lambda q: self.device(q, self.a, self.b)),
        }[axis]

    def place(self, axis):
        return {"z": (self.z, self.nz), "a": (self.a, self.na), "b": (self.b, self.nb)}[axis]


def greet_mover(g, barrier, source):
    @pl.when(jnp.logical_not(g.at_home()))
    def _():
        pl.semaphore_signal(barrier, inc=1, device_id=source, device_id_type=MESH)

    return 1 - g.at_home().astype(jnp.int32)


def merge_moments(first_op, second_op):
    count = first_op[0:1] + second_op[0:1]
    share = second_op[0:1] / jnp.maximum(count, 1.0)
    gap = second_op[1:2] - first_op[1:2]
    mean = first_op[1:2] + gap * share
    squares = first_op[2:3] + second_op[2:3] + gap * gap * (first_op[0:1] * share)
    return jnp.concatenate([count, mean, squares, first_op[3:]], axis=0)


NT = (((1,), (1,)), ((), ()))
TN = (((0,), (0,)), ((), ()))
NN = (((1,), (0,)), ((), ()))


def dot(first_op, second_op, dims):
    return lax.dot_general(first_op, second_op, dims, preferred_element_type=F32)


def keep_head(value, h, head_size):
    lane = lax.broadcasted_iota(jnp.int32, value.shape, 1)
    return jnp.where(lane // head_size == h, value, jnp.zeros_like(value))


def attend_block(head_size, i, query_b, k_ref, v_ref, pos_ref, bias, len_ref, prob_ref):
    rows, cols = query_b.shape
    frames = k_ref.shape[0]
    width = rows + frames
    query = query_b.astype(F32)
    content = (query + bias[0:1, :]).astype(BF)
    positional = (query + bias[1:2, :]).astype(BF)
    window = pos_ref[pl.ds(pl.multiple_of(frames - rows - i * rows, rows), width), :]
    live = lax.broadcasted_iota(jnp.int32, (rows, frames), 1).astype(F32) < len_ref[0:1, 0:1]
    out = jnp.zeros((rows, cols), F32)
    for h in range(cols // head_size):
        direct = dot(keep_head(content, h, head_size), k_ref[...], NT)
        spread = dot(keep_head(positional, h, head_size), window, NT)
        shifted = pltpu.roll(spread, width - rows + 1, 1, stride=1, stride_axis=0)[:, :frames]
        score = jnp.where(live, (direct + shifted) * (1.0 / math.sqrt(head_size)), -1e30)
        top = jnp.max(score, axis=-1, keepdims=True)
        power = jnp.exp(score - top)
        prob_b = (power * (1.0 / jnp.sum(power, axis=-1, keepdims=True))).astype(BF)
        prob_ref[h] = prob_b
        out = out + keep_head(dot(prob_b, v_ref[...], NN), h, head_size)
    return out.astype(BF)


def attend_back_block(head_size, i, query_b, k_ref, v_ref, pos_ref, bias, prob_ref, grad_heads, gk_acc, gv_acc, gpos_acc, gbias):
    rows, cols = query_b.shape
    frames = k_ref.shape[0]
    width = rows + frames
    query = query_b.astype(F32)
    content = (query + bias[0:1, :]).astype(BF)
    positional = (query + bias[1:2, :]).astype(BF)
    down = lax.broadcasted_iota(jnp.int32, (rows, rows), 0)
    across = lax.broadcasted_iota(jnp.int32, (rows, rows), 1)
    turn = jnp.where(down + across == rows - 1, 1.0, 0.0).astype(BF)
    positional_turned = dot(turn, positional, NN).astype(BF)
    here = pl.ds(pl.multiple_of(frames - rows - i * rows, rows), width)
    window = pos_ref[here, :]
    grad_content = jnp.zeros((rows, cols), F32)
    grad_position = jnp.zeros((rows, cols), F32)
    for h in range(cols // head_size):
        grad_out = keep_head(grad_heads, h, head_size)
        prob_b = prob_ref[h]
        prob = prob_b.astype(F32)
        grad_prob = dot(grad_out, v_ref[...], NT)
        delta = jnp.sum(prob * grad_prob, axis=-1, keepdims=True)
        score_b = (prob * (grad_prob - delta) * (1.0 / math.sqrt(head_size))).astype(BF)
        grad_content = grad_content + keep_head(dot(score_b, k_ref[...], NN), h, head_size)
        gk_acc[...] += dot(keep_head(content, h, head_size), score_b, TN)
        gv_acc[...] += dot(grad_out, prob_b, TN)
        wide = jnp.concatenate([dot(turn, score_b, NN), jnp.zeros((rows, width - frames), F32)], axis=1)
        spread = pltpu.roll(wide, 0, 1, stride=1, stride_axis=0).astype(BF)
        grad_position = grad_position + keep_head(dot(spread, window, NN), h, head_size)
        gpos_acc[:, here] += dot(keep_head(positional_turned, h, head_size), spread, TN)
    high = grad_position.astype(BF)
    low = (grad_position - high.astype(F32)).astype(BF)
    grad_position = dot(turn, high, NN) + dot(turn, low, NN)
    gbias[0:1, :] += jnp.sum(grad_content, axis=0, keepdims=True)
    gbias[1:2, :] += jnp.sum(grad_position, axis=0, keepdims=True)
    return (grad_content + grad_position).astype(BF)

def normalize(value):
    mean = jnp.mean(value, axis=-1, keepdims=True)
    centred = value - mean
    spread = lax.rsqrt(jnp.mean(centred * centred, axis=-1, keepdims=True) + LN_EPS)
    return centred * spread, spread


def norm_forward(value, gains, k):
    unit, _ = normalize(value)
    return (unit * gains[2 * k : 2 * k + 1] + gains[2 * k + 1 : 2 * k + 2]).astype(BF)


def norm_backward(value, gains, k, upstream):
    unit, spread = normalize(value)
    inner = upstream * gains[2 * k : 2 * k + 1]
    along = jnp.mean(inner * unit, axis=-1, keepdims=True)
    grad = spread * (inner - jnp.mean(inner, axis=-1, keepdims=True) - unit * along)
    gain = jnp.sum(upstream * unit, axis=0, keepdims=True)
    return grad, gain, jnp.sum(upstream, axis=0, keepdims=True)


def sigmoid(value):
    return 1.0 / (1.0 + jnp.exp(-value))


def module_forward(normed, up_ref, down_ref, hidden_ref, active_ref):
    units, width = up_ref.shape
    step = min(512, units)

    def chunk(j, total):
        here = pl.ds(pl.multiple_of(j * step, step), step)
        hidden = dot(normed, up_ref[here, :], NT)
        active = (hidden * sigmoid(hidden)).astype(BF)
        hidden_ref[:, here] = hidden.astype(hidden_ref.dtype)
        active_ref[:, here] = active
        return total + dot(active, down_ref[here, :], NN)

    return lax.fori_loop(0, units // step, chunk, jnp.zeros((normed.shape[0], width), F32))


def module_backward(upstream_b, up_ref, down_ref, hidden_ref, grad_ref):
    units, width = up_ref.shape
    step = min(512, units)

    def chunk(j, total):
        here = pl.ds(pl.multiple_of(j * step, step), step)
        hidden = hidden_ref[:, here].astype(F32)
        sigma = sigmoid(hidden)
        slope = sigma * (1.0 + hidden * (1.0 - sigma))
        grad = (dot(upstream_b, down_ref[here, :], NT) * slope).astype(BF)
        grad_ref[:, here] = grad
        return total + dot(grad, up_ref[here, :], NN)

    return lax.fori_loop(0, units // step, chunk, jnp.zeros((upstream_b.shape[0], width), F32))


def greet_lines(g, axes, source=None):
    barrier = pltpu.get_barrier_semaphore()
    total = g.nz - 1
    for k in range(1, g.nz):
        pl.semaphore_signal(barrier, inc=1, device_id=g.time(lax.rem(g.t + k, g.nz)), device_id_type=MESH)
    if source is not None:
        total = total + greet_mover(g, barrier, source)
    for axis in axes:
        p, n, device = g.line(axis)
        for k in range(1, n):
            pl.semaphore_signal(barrier, inc=1, device_id=device(lax.rem(p + k, n)), device_id_type=MESH)
            total += 1
    pl.semaphore_wait(barrier, total)


def remote(src, dst, send, recv, device):
    return pltpu.make_async_remote_copy(
        src_ref=src, dst_ref=dst, send_sem=send, recv_sem=recv, device_id=device, device_id_type=MESH
    )


def arrived(ref, sem):
    pltpu.make_async_copy(ref, ref, sem).wait()


def meet_levels(g, value, merge, buf, send_sem, recv_sem):
    sends = []
    for level, axis in enumerate("cabz"):
        p, n, device = g.line(axis)
        if n == 1:
            continue
        buf[level, p] = value
        for k in range(1, n):
            copy = remote(buf.at[level, p], buf.at[level, p], send_sem.at[level, k], recv_sem.at[level, p], device(lax.rem(p + k, n)))
            copy.start()
            sends.append(copy)
        for k in range(1, n):
            q = lax.rem(p + k, n)
            arrived(buf.at[level, q], recv_sem.at[level, q])
        value = buf[level, 0]
        for q in range(1, n):
            value = merge(value, buf[level, q])
    return value, sends


HALO = 16


def swap_edges(g, body, low, high, send_sem, recv_sem, pad):
    rows = body.shape[0]
    p, n = g.t, g.nz
    up = remote(body.at[pl.ds(rows - HALO, HALO)], low, send_sem.at[0], recv_sem.at[0], g.time(p + 1))
    down = remote(body.at[pl.ds(0, HALO)], high, send_sem.at[1], recv_sem.at[1], g.time(p - 1))
    pl.when(p < n - 1)(lambda: up.start())
    pl.when(p > 0)(lambda: down.start())
    pad[pl.ds(HALO, rows), :] = body[...].astype(F32)

    def fill(at, ref, sem, there):
        @pl.when(there)
        def _():
            arrived(ref, sem)
            pad[pl.ds(at, HALO), :] = ref[...].astype(F32)

        @pl.when(jnp.logical_not(there))
        def _():
            pad[pl.ds(at, HALO), :] = jnp.zeros((HALO, pad.shape[1]), F32)

    fill(0, low, recv_sem.at[0], p > 0)
    fill(HALO + rows, high, recv_sem.at[1], p < n - 1)

    def finish():
        pl.when(p < n - 1)(lambda: up.wait_send())
        pl.when(p > 0)(lambda: down.wait_send())

    return finish


def middle_kernel(taps, len_ref, att_ref, x1_ref, cot_ref, gains_ref, ud_hbm, sq_hbm,
                  y_ref, g2_ref, go_ref, o_ref, e2_ref, a3_ref, gpair_ref, e3_ref, sw_ref, a4_ref, s4_ref, gh4_ref, e4_ref,
                  small_ref, gtaps_ref,
                  up, down, wsq, o_buf, go_buf, glu_b, gc_b, low1, high1, low2, high2, pad_glu, pad_gc, h4, c_ref, y_buf, y_sem,
                  buf1, buf2, load_sem, a_send, a_recv, b_send, b_recv, h_send, h_recv, m_send, m_recv):
    g = Grid()
    z, nz = g.t, g.nz
    rows, width = x1_ref.shape
    cols = width // nz
    units = up.shape[0]
    rim = (taps - 1) // 2
    loads = [
        pltpu.make_async_copy(sq_hbm.at[pl.ds(4 * width, 4 * width)], wsq, load_sem.at[0]),
        pltpu.make_async_copy(ud_hbm.at[0, pl.ds(units, units)], up, load_sem.at[1]),
        pltpu.make_async_copy(ud_hbm.at[1, pl.ds(units, units)], down, load_sem.at[2]),
    ]
    for load in loads:
        load.start()
    greet_lines(g, "cabz", g.worker())
    sends = []
    for k in range(1, nz):
        q = lax.rem(z + k, nz)
        copy = remote(att_ref.at[pl.ds(q * rows, rows)], o_buf.at[z], a_send.at[k], a_recv.at[z], g.time(q))
        copy.start()
        sends.append(copy)
    o_buf[z] = att_ref[pl.ds(pl.multiple_of(z * rows, rows), rows), :]
    gains = gains_ref[...]
    frame = z * rows + lax.broadcasted_iota(jnp.int32, (rows, 1), 0)
    live = jnp.where(frame.astype(F32) < len_ref[0:1, 0:1], 1.0, 0.0)
    loads[0].wait()
    weight = lambda k: wsq[pl.ds((k - 4) * width, width), :]
    for k in range(1, nz):
        q = lax.rem(z + k, nz)
        arrived(o_buf.at[q], a_recv.at[q])
    out = jnp.concatenate([o_buf[q] for q in range(nz)], axis=1)
    o_ref[...] = out
    resid2 = x1_ref[...] + dot(out, weight(4), NT)
    normed3 = norm_forward(resid2, gains, 2)
    a3_ref[...] = normed3
    value = dot(normed3, weight(5), NT)
    gate = sigmoid(dot(normed3, weight(6), NT))
    glu_b[...] = (value * gate * live).astype(BF)
    done1 = swap_edges(g, glu_b, low1, high1, h_send.at[0], h_recv.at[0], pad_glu)
    for at in range(0, width, LANES):
        lanes = pl.ds(at, LANES)
        total = jnp.zeros((rows, LANES), F32)
        for m in range(taps):
            total = total + gains_ref[14 + m : 15 + m, lanes] * pad_glu[pl.ds(HALO - rim + m, rows), lanes]
        c_ref[:, lanes] = total
    conv = c_ref[...]
    count = jnp.sum(live, axis=0, keepdims=True)
    mean = jnp.sum(live * conv, axis=0, keepdims=True) / jnp.maximum(count, 1.0)
    squares = jnp.sum(live * (conv - mean) * (conv - mean), axis=0, keepdims=True)
    moments = jnp.concatenate([jnp.broadcast_to(count, mean.shape), mean, squares, jnp.zeros((5, width), F32)], axis=0)
    moments, more = meet_levels(g, moments, merge_moments, buf1, m_send.at[0], m_recv.at[0])
    sends += more
    total_frames = moments[0:1]
    inv_std = lax.rsqrt(moments[2:3] / total_frames + BN_EPS)
    centre = moments[1:2]
    centred = c_ref[...] - centre
    zed = centred * inv_std
    bn_val = gains[12:13] * zed + gains[13:14]
    swish = (bn_val * sigmoid(bn_val)).astype(BF)
    sw_ref[...] = swish
    resid3 = resid2 + dot(swish, weight(7), NT)
    normed4 = norm_forward(resid3, gains, 3)
    a4_ref[...] = normed4
    loads[1].wait()
    loads[2].wait()
    resid4 = resid3 + 0.5 * module_forward(normed4, up, down, h4, s4_ref)
    y_buf[...] = norm_forward(resid4, gains, 4)
    away = jnp.logical_not(g.at_home())
    home = remote(y_buf, y_ref, y_sem.at[0], y_sem.at[1], g.owner())
    pl.when(away)(lambda: home.start())

    @pl.when(g.at_home())
    def _():
        y_ref[...] = y_buf[...]

    grad4, gain4, shift4 = norm_backward(resid4, gains, 4, cot_ref[...].astype(F32))
    half4 = (0.5 * grad4).astype(BF)
    e4_ref[...] = half4
    grad_norm, gain3, shift3 = norm_backward(resid3, gains, 3, module_backward(half4, up, down, h4, gh4_ref))
    grad3 = grad4 + grad_norm
    e3 = grad3.astype(BF)
    e3_ref[...] = e3
    sigma = sigmoid(bn_val)
    grad_bn = dot(e3, weight(7), NN) * (sigma * (1.0 + bn_val * (1.0 - sigma)))
    gamma = jnp.sum(grad_bn * zed, axis=0, keepdims=True)
    beta = jnp.sum(grad_bn, axis=0, keepdims=True)
    grad_zed = grad_bn * gains[12:13]
    sum_one = jnp.sum(grad_zed, axis=0, keepdims=True)
    sum_two = jnp.sum(grad_zed * centred, axis=0, keepdims=True)
    sums = jnp.concatenate([sum_one, sum_two, jnp.zeros((6, width), F32)], axis=0)
    sums, more = meet_levels(g, sums, lambda x, y: x + y, buf2, m_send.at[1], m_recv.at[1])
    sends += more
    offset = inv_std * sums[0:1] + inv_std * inv_std * inv_std * sums[1:2] * centred
    gc_b[...] = (inv_std * grad_zed - live / total_frames * offset).astype(BF)
    done2 = swap_edges(g, gc_b, low2, high2, h_send.at[1], h_recv.at[1], pad_gc)
    for at in range(0, width, LANES):
        lanes = pl.ds(at, LANES)
        total = jnp.zeros((rows, LANES), F32)
        upstream = pad_gc[pl.ds(HALO, rows), lanes]
        for m in range(taps):
            total = total + gains_ref[14 + m : 15 + m, lanes] * pad_gc[pl.ds(HALO + rim - m, rows), lanes]
            gtaps_ref[m : m + 1, lanes] = jnp.sum(
                upstream * pad_glu[pl.ds(HALO - rim + m, rows), lanes], axis=0, keepdims=True
            )
        c_ref[:, lanes] = total
    grad_glu = c_ref[...] * live
    gv5 = (grad_glu * gate).astype(BF)
    gv6 = (grad_glu * value * gate * (1.0 - gate)).astype(BF)
    gpair_ref[0] = gv5
    gpair_ref[1] = gv6
    grad_norm, gain2, shift2 = norm_backward(
        resid2, gains, 2, dot(gv5, weight(5), NN) + dot(gv6, weight(6), NN)
    )
    grad2 = grad3 + grad_norm
    g2_ref[...] = grad2
    e2 = grad2.astype(BF)
    e2_ref[...] = e2
    grad_out = dot(e2, weight(4), NN).astype(BF)
    for q in range(nz):
        go_buf[q] = grad_out[:, q * cols : (q + 1) * cols]
    for k in range(1, nz):
        q = lax.rem(z + k, nz)
        copy = remote(go_buf.at[q], go_ref.at[pl.ds(z * rows, rows)], b_send.at[k], b_recv.at[z], g.time(q))
        copy.start()
        sends.append(copy)
    go_ref[pl.ds(pl.multiple_of(z * rows, rows), rows), :] = go_buf[z]
    small_ref[...] = jnp.concatenate([gain2, shift2, gain3, shift3, gain4, shift4, gamma, beta], axis=0)
    for k in range(1, nz):
        q = lax.rem(z + k, nz)
        arrived(go_ref.at[pl.ds(q * rows, rows)], b_recv.at[q])
    pl.when(away)(lambda: home.wait())
    done1()
    done2()
    for copy in sends:
        copy.wait_send()


def middle(length, attended, resid1, cotangent, gains, taps, ud_full, sq_full):
    rows, width = resid1.shape
    nz, nf = lax.axis_size("seq"), lax.axis_size("fsdp")
    frames, cols = rows * nz, width // nz
    units = ud_full.shape[1] // 2
    most = max(nz, nf // 2)
    vmem = pl.BlockSpec(memory_space=pltpu.VMEM)
    hbm = pl.BlockSpec(memory_space=pl.ANY)
    shape = jax.ShapeDtypeStruct
    dma = pltpu.SemaphoreType.DMA
    row = shape((rows, width), BF)
    return pl.pallas_call(
        lambda *refs: middle_kernel(taps, *refs),
        name="middle",
        out_shape=(
            row,
            shape((rows, width), F32),
            shape((frames, cols), BF),
            row,
            row,
            row,
            shape((2, rows, width), BF),
            row,
            row,
            row,
            shape((rows, units), BF),
            shape((rows, units), BF),
            row,
            shape((8, width), F32),
            shape((taps, width), F32),
        ),
        in_specs=[vmem] * 5 + [hbm] * 2,
        out_specs=[vmem] * 15,
        scratch_shapes=[
            pltpu.VMEM((units, width), BF),
            pltpu.VMEM((units, width), BF),
            pltpu.VMEM((4 * width, width), BF),
            pltpu.VMEM((nz, rows, cols), BF),
            pltpu.VMEM((nz, rows, cols), BF),
            pltpu.VMEM((rows, width), BF),
            pltpu.VMEM((rows, width), BF),
        ]
        + [pltpu.VMEM((HALO, width), BF)] * 4
        + [
            pltpu.VMEM((rows + 2 * HALO, width), F32),
            pltpu.VMEM((rows + 2 * HALO, width), F32),
            pltpu.VMEM((rows, units), F32),
            pltpu.VMEM((rows, width), F32),
            pltpu.VMEM((rows, width), BF),
            dma((2,)),
            pltpu.VMEM((4, most, 8, width), F32),
            pltpu.VMEM((4, most, 8, width), F32),
            dma((3,)),
            dma((nz,)),
            dma((nz,)),
            dma((nz,)),
            dma((nz,)),
            dma((2, 2)),
            dma((2, 2)),
            dma((2, 4, most)),
            dma((2, 4, most)),
        ],
        compiler_params=pltpu.CompilerParams(
            collective_id=6, has_side_effects=True, vmem_limit_bytes=56 * 1024 * 1024
        ),
    )(length, attended, resid1, cotangent, gains, ud_full, sq_full)


class Meeting:
    def __init__(self, g, buf, send_sem, recv_sem, order="cabz"):
        self.g, self.buf, self.send_sem, self.recv_sem, self.order = g, buf, send_sem, recv_sem, order

    def copies(self, level):
        p, n, device = self.g.line(self.order[level])
        here = self.buf.at[level, p]
        return [
            remote(here, here, self.send_sem.at[level, k], self.recv_sem.at[level, p], device(lax.rem(p + k, n)))
            for k in range(1, n)
        ]

    def start(self, level, value):
        self.buf[level, self.g.line(self.order[level])[0]] = value
        for copy in self.copies(level):
            copy.start()

    def finish(self):
        for level in range(len(self.order)):
            for copy in self.copies(level):
                copy.wait_send()

    def total(self, level):
        p, n, _ = self.g.line(self.order[level])
        for k in range(1, n):
            q = lax.rem(p + k, n)
            arrived(self.buf.at[level, q], self.recv_sem.at[level, q])
        value = self.buf[level, 0]
        for q in range(1, n):
            value = value + self.buf[level, q]
        return value


class Reduction:
    def __init__(self, g, gud, gsq, sib_ud, sib_sq, sib_sem, rb, ra, rz, sems):
        self.g, self.gud, self.gsq, self.sib_ud, self.sib_sq = g, gud, gsq, sib_ud, sib_sq
        self.sib_send, self.sib_recv = sib_sem
        self.bufs = {"b": rb, "a": ra, "z": rz}
        self.sems = sems
        self.sq_rows = gsq.shape[2]
        self.pair = 2 * self.sq_rows
        self.height = g.plane * self.pair

    def rows(self, t, part):
        return pl.ds(pl.multiple_of(t * self.pair + (part - 1) * self.sq_rows, self.sq_rows), self.sq_rows)

    def own(self, t, part):
        c = self.g.core
        return self.gsq.at[t, c] if part == 0 else self.gud.at[c, self.rows(t, part)]

    def sibling_copy(self, z, kind):
        g = self.g
        d = 1 - g.core
        if kind == 0:
            chips = pl.ds(z * g.plane, g.plane)
            src, dst = self.gsq.at[chips, d], self.sib_sq.at[chips]
        else:
            tall = pl.ds(z * self.height, self.height)
            src, dst = self.gud.at[d, tall], self.sib_ud.at[tall]
        return remote(src, dst, self.sib_send.at[kind, z], self.sib_recv.at[kind, z], g.sibling())

    def to_sibling(self, planes, kind):
        for z in planes:
            self.sibling_copy(z, kind).start()

    def from_sibling(self, planes, kind):
        for z in planes:
            self.sibling_copy(z, kind).wait_recv()

    def add_sibling(self, t, part):
        ref = self.own(t, part)
        ref[...] = ref[...] + (self.sib_sq[t] if part == 0 else self.sib_ud[self.rows(t, part), :])

    def landing(self, axis, slot, part):
        return self.bufs[axis].at[slot, pl.ds(part * self.sq_rows, self.sq_rows)]

    def slot(self, axis, upward, z, a, b, there):
        g = self.g
        p, n = g.place(axis)
        q = {"z": z, "a": a, "b": b}[axis]
        if there:
            p = p + 1 if upward else p - 1
        if upward:
            q = q + 1 - n * (p == n - 1)
        return {"b": (q * g.na + a) * g.nz + z, "a": q * g.nz + z, "z": q}[axis]

    def hop(self, axis, upward, z, a, b, part):
        g = self.g
        slot = self.slot(axis, upward, z, a, b, True)
        sends, recvs = self.sems[axis]
        device = g.up(axis) if upward else g.down(axis)
        src, dst = self.own(g.chip(z, a, b), part), self.landing(axis, slot, part)
        return remote(src, dst, sends.at[1 if upward else 0, part, slot], recvs.at[part, slot], device)

    def take(self, axis, upward, z, a, b, part):
        slot = self.slot(axis, upward, z, a, b, False)
        src, dst = self.landing(axis, slot, part), self.own(self.g.chip(z, a, b), part)
        arrived(src, self.sems[axis][1].at[part, slot])
        dst[...] = dst[...] + src[...]

    def settle(self, axis, z, a, b, part):
        p, n = self.g.place(axis)
        if n > 1:
            pl.when(p > 0)(lambda: self.take(axis, True, z, a, b, part))
            pl.when(p < n - 1)(lambda: self.take(axis, False, z, a, b, part))

    def ready(self, axis, z, a, b, part):
        if axis == "b":
            self.add_sibling(self.g.chip(z, a, b), part)
        else:
            before = {"a": "b", "z": "a"}[axis]
            self.ready(before, z, a, b, part)
            self.settle(before, z, a, b, part)

    def pass_on(self, axis, upward, z, a, b, part, finish):
        p, n = self.g.place(axis)
        if finish:
            self.hop(axis, upward, z, a, b, part).wait_send()
            return
        self.ready(axis, z, a, b, part)
        behind = p > 0 if upward else p < n - 1
        pl.when(behind)(lambda: self.take(axis, upward, z, a, b, part))
        self.hop(axis, upward, z, a, b, part).start()

    def along(self, axis, planes, part, finish=False):
        g = self.g
        p, n = g.place(axis)
        if axis == "z":
            for q in planes:
                pl.when(p < q)(lambda: self.pass_on("z", True, q, g.a, g.b, part, finish))
                pl.when(p > q)(lambda: self.pass_on("z", False, q, g.a, g.b, part, finish))
            return
        step = planes[1] - planes[0] if len(planes) > 1 else 1
        count = len(planes)
        for k in range(n - 1, 0, -1):
            for upward in (True, False):
                q = p + k if upward else p - k

                def act():
                    def body(i, _):
                        plane = planes[0] + step * lax.rem(i, count)
                        if axis == "b":
                            a = lax.rem(g.a + 1 + i // count, g.na)
                            self.pass_on("b", upward, plane, a, q, part, finish)
                        else:
                            self.pass_on("a", upward, plane, q, g.b, part, finish)
                        return 0

                    lax.fori_loop(0, (g.na if axis == "b" else 1) * count, body, 0)

                pl.when(p + k < n if upward else p >= k)(act)

    def last(self, part):
        g = self.g
        self.ready("z", g.z, g.a, g.b, part)
        self.settle("z", g.z, g.a, g.b, part)


def back_kernel(head_size, qkv_ref, pos_ref, go_ref, coarse_ref, fine_ref, gains_ref,
                x_ref, x1_ref, g2_ref, a1_ref, h1_ref, s1_ref, a2_ref,
                a4_ref, s4_ref, gh4_ref, e4_ref, o_ref, e2_ref, a3_ref, gpair_ref, e3_ref, sw_ref, some_ref, gtaps_ref,
                prob_hbm, ud_hbm, sq_hbm,
                gx_ref, ud_out, sq_out, small_out,
                prob_buf, gk_acc, gv_acc, gpos_acc, gbias, grads, prob_sem, wqkv, heads, gqkv, gh1, small, few, fbuf, f_send, f_recv, gud, gsq, sib_ud, sib_sq, rb, ra, rz, sbuf, fin_send_buf, fin, gx_buf, gx_in, gx_sem,
                load_sem, h_send, h_recv, sib_send, sib_recv, b_send, b_recv, a_send, a_recv, z_send, z_recv, s_send, s_recv,
                fin_send, fin_recv):
    g = Grid()
    z, nz, c = g.t, g.nz, g.core
    rows, width = x_ref.shape
    cols = width // nz
    units = h1_ref.shape[1]
    frames = qkv_ref.shape[1]
    up, down = gud.at[0, pl.ds(0, units)], gud.at[1, pl.ds(0, units)]
    loads = [
        pltpu.make_async_copy(sq_hbm.at[pl.ds(0, 3 * width)], wqkv, load_sem.at[0]),
        pltpu.make_async_copy(ud_hbm.at[0, pl.ds(0, units)], up, load_sem.at[1]),
        pltpu.make_async_copy(ud_hbm.at[1, pl.ds(0, units)], down, load_sem.at[2]),
    ]

    def probabilities(i):
        return pltpu.make_async_copy(prob_hbm.at[:, pl.ds(i * rows, rows)], prob_buf.at[i % 2], prob_sem.at[i % 2])

    probabilities(0).start()
    for load in loads:
        load.start()
    greet_lines(g, "cabz", g.worker())
    sends = []
    small[...] = jnp.zeros_like(small)
    small[0:8, :] = some_ref[...]
    small[8 : 8 + gtaps_ref.shape[0], :] = gtaps_ref[...]
    early = Meeting(g, sbuf, s_send, s_recv)
    early.start(0, small[...])
    red = Reduction(
        g, gud, gsq, sib_ud, sib_sq, (sib_send, sib_recv), rb, ra, rz,
        {"b": (b_send, b_recv), "a": (a_send, a_recv), "z": (z_send, z_recv)},
    )
    total_rows = gud.shape[1]
    sq_rows = gsq.shape[2]
    high = list(range(nz - 1, nz // 2 - 1, -1))
    low = list(range(0, nz // 2))
    part = 256

    def matrix_terms(color, left_ref, right, first_row, count):
        def body(i, _):
            here = pl.ds(pl.multiple_of(i * part, part), part)
            there = pl.ds(pl.multiple_of(first_row + i * part, part), part)
            gud[color, there, :] = dot(left_ref[:, here], right, TN).astype(BF)
            return 0

        lax.fori_loop(0, count // part, body, 0)

    per = width // sq_rows // 2

    def square_terms(block, left, right):
        sums = dot(left, right, TN).astype(BF).reshape(per, 2, sq_rows, width)
        gsq[pl.ds(block * per, per)] = sums

    square_terms(7, e3_ref[...], sw_ref[...])
    square_terms(6, gpair_ref[1], a3_ref[...])
    square_terms(5, gpair_ref[0], a3_ref[...])
    square_terms(4, e2_ref[...], o_ref[...])
    red.to_sibling(high, 0)
    early.start(1, early.total(0))
    matrix_terms(0, gh4_ref, a4_ref[...], units, units)
    matrix_terms(1, s4_ref, e4_ref[...], units, units)
    red.to_sibling(high, 1)
    early.start(2, early.total(1))
    gk_acc[...] = jnp.zeros_like(gk_acc)
    gv_acc[...] = jnp.zeros_like(gv_acc)
    gpos_acc[...] = jnp.zeros_like(gpos_acc)
    gbias[...] = jnp.zeros_like(gbias)
    to_time = lambda j, q, k: remote(grads.at[j, q], heads.at[j, z], h_send.at[j, k], h_recv.at[j, z], g.time(q))
    bias = gains_ref[10:12, pl.ds(pl.multiple_of(z * cols, cols), cols)]

    def attend(i, _):
        pl.when(i + 1 < nz)(lambda: probabilities(i + 1).start())
        probabilities(i).wait()
        here = pl.ds(pl.multiple_of(i * rows, rows), rows)
        grads[0, i] = attend_back_block(
            head_size, i, qkv_ref[0, here, :], qkv_ref.at[1], qkv_ref.at[2], pos_ref, bias, prob_buf.at[i % 2],
            go_ref[here, :], gk_acc, gv_acc, gpos_acc, gbias,
        )

        @pl.when(i == 0)
        def _():
            early.start(3, early.total(2))
            red.from_sibling(high, 0)
            red.along("b", high, 0)

        @pl.when(i == 1)
        def _():
            red.from_sibling(high, 1)
            red.along("b", high, 1)
            red.along("b", high, 2)

        return 0

    lax.fori_loop(0, nz, attend, 0)
    small[...] = early.total(3)
    grads_k = gk_acc[...].T.astype(BF)
    grads_v = gv_acc[...].T.astype(BF)
    for q in range(nz):
        grads[1, q] = grads_k[q * rows : (q + 1) * rows]
        grads[2, q] = grads_v[q * rows : (q + 1) * rows]
    for k in range(1, nz):
        q = lax.rem(z + k, nz)
        for j in range(3):
            copy = to_time(j, q, k)
            copy.start()
            sends.append(copy)
    for j in range(3):
        heads[j, z] = grads[j, z]
    red.along("a", high, 0)
    fine = fine_ref.shape[1]

    def position(i, total):
        table = coarse_ref[0, pl.ds(2 * i, 1), :] * fine_ref[0] + coarse_ref[1, pl.ds(2 * i, 1), :] * fine_ref[1]
        after = coarse_ref[0, pl.ds(2 * i + 1, 1), :] * fine_ref[0] + coarse_ref[1, pl.ds(2 * i + 1, 1), :] * fine_ref[1]
        both = jnp.concatenate([table, after], axis=0).astype(BF)
        return total + dot(gpos_acc[:, pl.ds(pl.multiple_of(i * 2 * fine, 2 * fine), 2 * fine)].astype(BF), both, NN)

    gpos = lax.fori_loop(0, coarse_ref.shape[1] // 2, position, jnp.zeros((cols, width), F32)).astype(BF)
    gsq[pl.ds(3 * per, per)] = jnp.zeros((per, 2, sq_rows, width), BF)
    pieces = cols // sq_rows
    for i in range(pieces):
        piece = z * pieces + i
        gsq[3 * per + piece // 2, piece % 2] = gpos[i * sq_rows : (i + 1) * sq_rows]
    gains = gains_ref[...]
    loads[0].wait()
    grad_norm = jnp.zeros((rows, width), F32)
    for j in range(3):
        for k in range(1, nz):
            q = lax.rem(z + k, nz)
            arrived(heads.at[j, q], h_recv.at[j, q])
        full = jnp.concatenate([heads[j, q] for q in range(nz)], axis=1)
        gqkv[j] = full
        grad_norm = grad_norm + dot(full, wqkv[pl.ds(j * width, width), :], NN)
    for j in range(3):
        square_terms(j, gqkv[j], a2_ref[...])
    red.to_sibling(low, 0)
    resid1 = x1_ref[...]
    grad_add, gain1, shift1 = norm_backward(resid1, gains, 1, grad_norm)
    grad1 = g2_ref[...] + grad_add
    half1 = (0.5 * grad1).astype(BF)
    loads[1].wait()
    loads[2].wait()
    red.along("a", high, 1)
    grad_norm = module_backward(half1, up, down, h1_ref, gh1)
    red.from_sibling(low, 0)
    red.along("b", low, 0)
    matrix_terms(0, gh1, a1_ref[...], 0, units)
    matrix_terms(1, s1_ref, half1, 0, units)
    red.to_sibling(low, 1)
    red.along("a", high, 2)
    grad_add, gain0, shift0 = norm_backward(x_ref[...].astype(F32), gains, 0, grad_norm)
    away = jnp.logical_not(g.at_home())
    gx_buf[...] = (grad1 + grad_add).astype(BF)
    home = remote(gx_buf, gx_in, gx_sem.at[0], gx_sem.at[1], g.owner())
    pl.when(away)(lambda: home.start())
    few[...] = jnp.zeros_like(few)
    few[0:1, :] = gain0
    few[1:2, :] = shift0
    few[2:3, :] = gain1
    few[3:4, :] = shift1
    few[4:6, pl.ds(pl.multiple_of(z * cols, cols), cols)] = gbias[...]
    meeting = Meeting(g, fbuf, f_send, f_recv)
    meeting.start(0, few[...])
    red.from_sibling(low, 1)
    red.along("b", low, 1)
    red.along("b", low, 2)
    red.along("a", low, 0)
    meeting.start(1, meeting.total(0))
    red.along("z", high, 0)
    red.along("z", high, 1)
    red.along("a", low, 1)
    red.along("z", low, 0)
    meeting.start(2, meeting.total(1))
    red.along("z", high, 2)
    red.along("a", low, 2)
    red.along("z", low, 1)
    meeting.start(3, meeting.total(2))
    red.along("z", low, 2)
    for part in range(3):
        red.last(part)
    me = g.chip(g.z, g.a, g.b)
    d = 1 - c
    half = ud_out.shape[1]
    at = lambda k: pl.ds(pl.multiple_of(me * 2 * half + k * half, half), half)
    fin_send_buf[...] = gud[c, at(d), :]
    swap = remote(fin_send_buf, fin, fin_send, fin_recv, g.sibling())
    swap.start()
    ud_out[c] = gud[c, at(c), :].astype(F32)
    sq_out[...] = gsq[me, c].astype(F32)
    total = meeting.total(3)
    small_out[0:4, :] = total[0:4]
    small_out[4:10, :] = small[0:6, :]
    small_out[10:12, :] = total[4:6]
    small_out[12 : small.shape[0] + 6, :] = small[6:, :]
    for planes in (high, low):
        for part in range(3):
            for axis in "baz":
                red.along(axis, planes, part, True)
        for kind in range(2):
            for q in planes:
                red.sibling_copy(q, kind).wait_send()
    for copy in sends:
        copy.wait_send()
    early.finish()
    meeting.finish()

    @pl.when(away)
    def _():
        home.wait()
        gx_ref[...] = gx_in[...].astype(F32)

    @pl.when(g.at_home())
    def _():
        gx_ref[...] = gx_buf[...].astype(F32)

    swap.wait()
    ud_out[d] = fin[...].astype(F32)


def back(qkv, pos, grad_out, prob, head_size, coarse, fine, gains, signal, resid1, grad2, first, second, squares, some, gtaps, ud_full, sq_full):
    rows, width = signal.shape
    nz, nf = lax.axis_size("seq"), lax.axis_size("fsdp")
    chips = nz * nf // 2
    plane = nf // 2
    side = math.isqrt(plane)
    na, nb = (side, side) if side * side == plane else (plane, 1)
    cols = width // nz
    units = ud_full.shape[1] // 2
    own = ud_full.shape[1] // (2 * chips)
    block = 3 * own
    most = max(nz, na, nb, 2)
    tall = -(-(8 + gtaps.shape[0]) // 8) * 8
    vmem = pl.BlockSpec(memory_space=pltpu.VMEM)
    hbm = pl.BlockSpec(memory_space=pl.ANY)
    shape = jax.ShapeDtypeStruct
    dma = pltpu.SemaphoreType.DMA
    frames = rows * nz
    heads = cols // head_size
    operands = (qkv, pos, grad_out, coarse, fine, gains, signal, resid1, grad2, *first, *second, *squares, some, gtaps)
    places = lambda n: n + 1 if n > 2 else 1
    slots = {"b": places(nb) * na * nz, "a": places(na) * nz, "z": places(nz)}
    return pl.pallas_call(
        lambda *refs: back_kernel(head_size, *refs),
        name="back",
        out_shape=(
            shape((rows, width), F32),
            shape((2, own, width), F32),
            shape((own, width), F32),
            shape((tall + 6, width), F32),
        ),
        in_specs=[vmem] * len(operands) + [hbm] * 3,
        out_specs=[vmem] * 4,
        scratch_shapes=[
            pltpu.VMEM((2, heads, rows, frames), BF),
            pltpu.VMEM((cols, frames), F32),
            pltpu.VMEM((cols, frames), F32),
            pltpu.VMEM((cols, 2 * frames), F32),
            pltpu.VMEM((2, cols), F32),
            pltpu.VMEM((3, nz, rows, cols), BF),
            dma((2,)),
            pltpu.VMEM((3 * width, width), BF),
            pltpu.VMEM((3, nz, rows, cols), BF),
            pltpu.VMEM((3, rows, width), BF),
            pltpu.VMEM((rows, units), BF),
            pltpu.VMEM((tall, width), F32),
            pltpu.VMEM((8, width), F32),
            pltpu.VMEM((4, most, 8, width), F32),
            dma((4, most)),
            dma((4, most)),
            pltpu.VMEM((2, 2 * units, width), BF),
            pltpu.VMEM((chips, 2, own, width), BF),
            pltpu.VMEM((2 * units, width), BF),
            pltpu.VMEM((chips, own, width), BF),
            pltpu.VMEM((slots["b"], block, width), BF),
            pltpu.VMEM((slots["a"], block, width), BF),
            pltpu.VMEM((slots["z"], block, width), BF),
            pltpu.VMEM((4, most, tall, width), F32),
            pltpu.VMEM((own, width), BF),
            pltpu.VMEM((own, width), BF),
            pltpu.VMEM((rows, width), BF),
            pltpu.VMEM((rows, width), BF),
            dma((2,)),
            dma((3,)),
            dma((3, nz)),
            dma((3, nz)),
            dma((2, nz)),
            dma((2, nz)),
            dma((2, 3, slots["b"])),
            dma((3, slots["b"])),
            dma((2, 3, slots["a"])),
            dma((3, slots["a"])),
            dma((2, 3, slots["z"])),
            dma((3, slots["z"])),
            dma((4, most)),
            dma((4, most)),
            dma,
            dma,
        ],
        compiler_params=pltpu.CompilerParams(
            collective_id=7, has_side_effects=True, vmem_limit_bytes=61000 * 1024
        ),
    )(*operands, prob, ud_full, sq_full)


def finish_kernel(rows, y_ref, gx_ref, matrices_ref, square_ref, small_ref, *refs):
    states, outs = refs[:15], refs[15:]
    outs[0][...] = y_ref[...]
    outs[1][...] = gx_ref[...]
    count, share = rows, states[9].shape[1]
    taps = states[12].shape[1]
    width = small_ref.shape[1]
    place = lax.axis_index("seq") * lax.axis_size("fsdp") + lax.axis_index("fsdp")
    own = pltpu.roll(small_ref[...], lax.rem(width - place * share, width), 1)[:, :LANES]
    below = jnp.concatenate([own[count : count + taps], jnp.zeros((-taps % 8, LANES), F32)], axis=0)
    gradients = (
        square_ref[...],
        matrices_ref[0],
        matrices_ref[1],
        own[:count, :share],
        below.T[:share, :taps],
    )
    fix_one = 1.0 - BETA_ONE**ADAM_STEP
    fix_two = 1.0 - BETA_TWO**ADAM_STEP
    for k, gradient in enumerate(gradients):
        weight, first_mom, second_mom = (ref[...] for ref in states[3 * k : 3 * k + 3])
        decay = 0.0 if k == 3 else DECAY_RATE
        first_new = BETA_ONE * first_mom + (1.0 - BETA_ONE) * gradient
        second_new = BETA_TWO * second_mom + (1.0 - BETA_TWO) * gradient * gradient
        update = first_new / fix_one / (jnp.sqrt(second_new / fix_two) + ADAM_EPS)
        there = outs[2 + 4 * k : 6 + 4 * k]
        there[0][...] = gradient
        there[1][...] = weight - LEARN_RATE * (update + decay * weight)
        there[2][...] = first_new
        there[3][...] = second_new


def finish(layer_output, input_grad, matrices, square, small, states):
    flat = [array for state in states for array in state]
    results = [layer_output, input_grad] + [array for state in states for array in (state[0],) * 4]
    vmem = pl.BlockSpec(memory_space=pltpu.VMEM)
    return pl.pallas_call(
        lambda *refs: finish_kernel(states[3][0].shape[0], *refs),
        name="finish",
        out_shape=[jax.ShapeDtypeStruct(array.shape, array.dtype) for array in results],
        in_specs=[vmem] * (5 + len(flat)),
        out_specs=[vmem] * len(results),
    )(layer_output, input_grad, matrices, square, small, *flat)


def when(*conditions):
    holds = 1
    for condition in conditions:
        holds = holds * jnp.asarray(condition).astype(jnp.int32)
    return pl.when(holds == 1) if conditions else lambda act: act()


class Gather:
    WAYS = {"z+": 0, "z-": 1, "a+": 2, "a-": 3, "b+": 4, "b-": 5, "s": 6}
    PARTS = (0, 1, 2)
    SPREAD = ("a+", "a-", "b+", "b-", "s")

    def __init__(self, g, ud, sq, recv_sem, sib_recv, send_sem):
        self.g, self.ud, self.sq = g, ud, sq
        self.recv_sem, self.sib_recv, self.send_sem = recv_sem, sib_recv, send_sem
        self.rows = sq.shape[2]
        half = g.nz // 2
        if half == 2:
            first = jnp.minimum(g.z, 1)
            second = jnp.maximum(g.z, 2)
            self.low, self.high = [first, 1 - first], [second, 5 - second]
        else:
            self.low, self.high = list(range(half)), list(range(half, g.nz))
        self.below = g.z < half

    def piece(self, part, t, color):
        if part == 0:
            return self.sq.at[t, color]
        return self.ud.at[color, pl.ds(t * 2 * self.rows + (part - 1) * self.rows, self.rows)]

    def onward(self, part, t, ways, finish, *only):
        g = self.g
        ref = self.piece(part, t, g.core)
        for way in ways:
            p, n = (0, 2) if way == "s" else g.place(way[0])

            def act():
                if way == "s":
                    target, arrive = g.sibling(), self.sib_recv
                else:
                    target, arrive = g.up(way[0]) if way[1] == "+" else g.down(way[0]), self.recv_sem
                copy = remote(ref, ref, self.send_sem.at[self.WAYS[way], part, t], arrive.at[part, t], target)
                copy.wait_send() if finish else copy.start()

            if way == "s":
                when(*only)(act)
            elif n > 1:
                when(*only, p < n - 1 if way[1] == "+" else p > 0)(act)

    def wait(self, part, t, finish):
        if not finish:
            arrived(self.piece(part, t, self.g.core), self.recv_sem.at[part, t])

    def column(self, q, spread, finish, *only):
        g = self.g
        t = g.chip(q, g.a, g.b)
        for part in self.PARTS:
            when(*only, q != g.z)(lambda: self.wait(part, t, finish))
            self.onward(part, t, ("z+",), finish, *only, q <= g.z)
            self.onward(part, t, ("z-",), finish, *only, q >= g.z)
            if spread:
                self.onward(part, t, self.SPREAD, finish, *only)

    def spread(self, q, finish, *only):
        g = self.g
        for part in self.PARTS:
            self.onward(part, g.chip(q, g.a, g.b), self.SPREAD, finish, *only)

    def both(self, axis, k, act):
        p, n = self.g.place(axis)
        pl.when(p >= k)(lambda: act(p - k, axis + "+"))
        pl.when(p + k < n)(lambda: act(p + k, axis + "-"))

    def along_a(self, q, finish=False):
        g = self.g

        def take(a, way):
            t = g.chip(q, a, g.b)
            for part in self.PARTS:
                self.wait(part, t, finish)
                self.onward(part, t, (way, "b+", "b-", "s"), finish)

        for k in range(1, g.na):
            self.both("a", k, take)

    def along_b(self, q, finish=False):
        g = self.g

        def row(b, way):
            def body(i, _):
                t = g.chip(q, lax.rem(g.a + i, g.na), b)
                for part in self.PARTS:
                    self.wait(part, t, finish)
                    self.onward(part, t, (way, "s"), finish)
                return 0

            lax.fori_loop(0, g.na, body, 0)

        for k in range(1, g.nb):
            self.both("b", k, row)

    def own(self, finish=False):
        if len(self.low) == 2:
            self.column(self.low[0], True, finish, self.below)
        self.column(self.high[0], False, finish, jnp.logical_not(self.below))

    def first(self, finish=False):
        below, above = self.below, jnp.logical_not(self.below)
        if len(self.low) == 2:
            self.column(self.low[0], True, finish, above)
        else:
            self.column(self.low[0], True, finish)
        for q in self.high[1:]:
            self.column(q, False, finish, above)
        self.along_a(self.low[0], finish)
        for q in self.low[1:]:
            self.column(q, True, finish)
            self.along_a(q, finish)
        self.spread(self.high[0], finish, above)
        self.column(self.high[0], True, finish, below)
        for q in self.low:
            self.along_b(q, finish)
        for q in self.high[1:]:
            self.column(q, False, finish, below)
        for q in self.high[1:]:
            self.spread(q, finish)

    def from_sibling(self, upper):
        g = self.g
        count = g.chips // 2

        def body(i, _):
            for part in self.PARTS:
                t = upper * count + i
                arrived(self.piece(part, t, 1 - g.core), self.sib_recv.at[part, t])
            return 0

        lax.fori_loop(0, count, body, 0)


def head_kernel(head_size, up_own, down_own, sq_own, vec_in, taps_in, x_in, cot_in, len_smem, coarse_ref, fine_ref,
                ud_full, sq_full, small_ref, x_ref, cot_ref, len_ref,
                x1_ref, a1_ref, h1_ref, s1_ref, a2_ref, heads_ref, pos_ref, att_ref, prob_hbm,
                own, len_in, columns, sbuf, up, down, wqkv, wpos, mine, prob_buf,
                move_send, move_recv, local_sem, swap_sem, recv_sem, sib_recv, gather_send, s_send, s_recv,
                load_sem, send_sem, heads_recv, prob_sem):
    g = Grid()
    z, nz, c = g.t, g.nz, g.core
    rows, width = x_in.shape
    cols = width // nz
    units = up.shape[0]
    half = up_own.shape[0]
    me = g.chip(g.z, g.a, g.b)
    own[0] = up_own[...].astype(BF)
    own[1] = down_own[...].astype(BF)
    own[2] = sq_own[...].astype(BF)
    here = pl.ds(me * 2 * half + c * half, half)
    local = [
        pltpu.make_async_copy(own.at[c], ud_full.at[c, here], local_sem.at[0]),
        pltpu.make_async_copy(own.at[2], sq_full.at[me, c], local_sem.at[1]),
    ]
    for copy in local:
        copy.start()
    len_in[...] = jnp.full(len_in.shape, len_smem[0].astype(F32))
    share = vec_in.shape[1]
    count = vec_in.shape[0]
    taps = taps_in.shape[1]
    lane = lax.broadcasted_iota(jnp.int32, (share, width), 1)
    column = lax.broadcasted_iota(jnp.int32, (share, width), 0)
    place = jnp.where(lane - (g.z * g.nf + g.f) * share == column, 1.0, 0.0).astype(BF)
    columns[...] = jnp.zeros_like(columns)
    columns[0:count, :] = dot(vec_in[...].astype(BF), place, NN)
    columns[count : count + taps, :] = dot(taps_in[...].astype(BF), place, TN)
    greet_lines(g, "cabz", g.owner())
    swap = remote(own.at[1 - c], ud_full.at[1 - c, here], swap_sem.at[0], swap_sem.at[1], g.sibling())
    swap.start()
    moves = [
        remote(src, dst, move_send.at[k], move_recv.at[k], g.worker())
        for k, (src, dst) in enumerate(((x_in, x_ref), (len_in, len_ref), (cot_in, cot_ref)))
    ]

    @pl.when(jnp.logical_not(g.at_home()))
    def _():
        for copy in moves[:2]:
            copy.start()

    @pl.when(g.at_home())
    def _():
        x_ref[...] = x_in[...]
        len_ref[...] = len_in[...]
        cot_ref[...] = cot_in[...]

    meeting = Meeting(g, sbuf, s_send, s_recv)
    meeting.start(0, columns[...].astype(BF))
    gather = Gather(g, ud_full, sq_full, recv_sem, sib_recv, gather_send)
    for copy in local:
        copy.wait()
    swap.wait_recv()
    gather.own()
    meeting.start(1, meeting.total(0))
    meeting.start(2, meeting.total(1))
    gather.first()
    meeting.start(3, meeting.total(2))

    @pl.when(jnp.logical_not(g.at_home()))
    def _():
        moves[2].start()
        for copy in moves[:2]:
            copy.wait()

    gather.from_sibling(0)
    loads = [
        pltpu.make_async_copy(ud_full.at[0, pl.ds(0, units)], up, load_sem.at[0]),
        pltpu.make_async_copy(ud_full.at[1, pl.ds(0, units)], down, load_sem.at[1]),
    ]
    per = width // (2 * half)
    squares = pltpu.make_async_copy(sq_full.at[pl.ds(0, 3 * per)], wqkv, load_sem.at[2])
    pieces = cols // half
    positions = [
        pltpu.make_async_copy(
            sq_full.at[3 * per + (z * pieces + i) // 2, (z * pieces + i) % 2],
            wpos.at[pl.ds(i * half, half)],
            load_sem.at[3],
        )
        for i in range(pieces)
    ]
    for load in loads + [squares]:
        load.start()
    for load in positions:
        load.start()
        load.wait()
    small_ref[...] = meeting.total(3).astype(F32)
    gains = small_ref[...]
    signal = x_ref[...].astype(F32)
    normed1 = norm_forward(signal, gains, 0)
    a1_ref[...] = normed1
    for load in loads:
        load.wait()
    resid1 = signal + 0.5 * module_forward(normed1, up, down, h1_ref, s1_ref)
    x1_ref[...] = resid1
    gather.along_a(gather.high[0])
    normed2 = norm_forward(resid1, gains, 1)
    a2_ref[...] = normed2
    squares.wait()
    for k in range(3):
        weight = wqkv[pl.ds(k * per, per)].reshape(width, width)
        out = dot(normed2, weight, NT).astype(BF)
        for q in range(nz):
            mine[q, k] = out[:, q * cols : (q + 1) * cols]
    sends = []
    for k in range(1, nz):
        q = lax.rem(z + k, nz)
        copy = remote(mine.at[q], heads_ref.at[:, pl.ds(z * rows, rows)], send_sem.at[k], heads_recv.at[z], g.time(q))
        copy.start()
        sends.append(copy)
    slot = pl.ds(pl.multiple_of(z * rows, rows), rows)
    for k in range(3):
        heads_ref[k, slot, :] = mine[z, k]
    for q in gather.high[1:]:
        gather.along_a(q)
    fine = fine_ref.shape[1]
    weight = wpos[...]

    def position(i, _):
        table = coarse_ref[0, pl.ds(i, 1), :] * fine_ref[0] + coarse_ref[1, pl.ds(i, 1), :] * fine_ref[1]
        there = pl.ds(pl.multiple_of(i * fine, fine), fine)
        pos_ref[there, :] = dot(table.astype(BF), weight, NT).astype(BF)
        return 0

    lax.fori_loop(0, coarse_ref.shape[1], position, 0)
    for k in range(1, nz):
        q = lax.rem(z + k, nz)
        arrived(heads_ref.at[:, pl.ds(q * rows, rows)], heads_recv.at[q])
    bias = small_ref[10:12, pl.ds(pl.multiple_of(z * cols, cols), cols)]

    def keep(i):
        return pltpu.make_async_copy(
            prob_buf.at[i % 2], prob_hbm.at[:, pl.ds(i * rows, rows)], prob_sem.at[i % 2]
        )

    def attend(i, _):
        pl.when(i >= 2)(lambda: keep(i - 2).wait())
        there = pl.ds(pl.multiple_of(i * rows, rows), rows)
        att_ref[there, :] = attend_block(
            head_size, i, heads_ref[0, there, :], heads_ref.at[1], heads_ref.at[2], pos_ref, bias, len_ref, prob_buf.at[i % 2]
        )
        keep(i).start()
        for k, q in enumerate(gather.high):
            pl.when(i == min(k + 1, nz - 1))(lambda: gather.along_b(q))
        return 0

    lax.fori_loop(0, nz, attend, 0)
    gather.from_sibling(1)
    keep(nz - 2).wait()
    keep(nz - 1).wait()
    swap.wait_send()
    for copy in sends:
        copy.wait_send()
    meeting.finish()
    gather.own(True)
    gather.first(True)
    for q in gather.high:
        gather.along_a(q, True)
        gather.along_b(q, True)

    @pl.when(jnp.logical_not(g.at_home()))
    def _():
        moves[2].wait()


def head(upward, downward, square, vectors, kernel, signal, cotangent, lengths, coarse, fine, head_size):
    rows, width = signal.shape
    nz, nf = lax.axis_size("seq"), lax.axis_size("fsdp")
    devices = nz * nf
    chips, plane = devices // 2, nf // 2
    own = upward.shape[0]
    frames, cols = rows * nz, width // nz
    units = own * devices // 2
    heads = cols // head_size
    tall = -(-(vectors.shape[0] + kernel.shape[1]) // 16) * 16
    side = math.isqrt(plane)
    most = max(nz, side if side * side == plane else plane, 2)
    vmem = pl.BlockSpec(memory_space=pltpu.VMEM)
    hbm = pl.BlockSpec(memory_space=pl.ANY)
    shape = jax.ShapeDtypeStruct
    dma = pltpu.SemaphoreType.DMA
    return pl.pallas_call(
        lambda *refs: head_kernel(head_size, *refs),
        name="head",
        out_shape=(
            shape((2, devices * own, width), BF),
            shape((chips, 2, own, width), BF),
            shape((tall, width), F32),
            shape(signal.shape, signal.dtype),
            shape(cotangent.shape, cotangent.dtype),
            shape((8, LANES), F32),
            shape((rows, width), F32),
            shape((rows, width), BF),
            shape((rows, units), BF),
            shape((rows, units), BF),
            shape((rows, width), BF),
            shape((3, frames, cols), BF),
            shape((2 * frames, cols), BF),
            shape((frames, cols), BF),
            shape((heads, frames, frames), BF),
        ),
        in_specs=[vmem] * 7 + [pl.BlockSpec(memory_space=pltpu.SMEM)] + [vmem] * 2,
        out_specs=[hbm] * 2 + [vmem] * 12 + [hbm],
        scratch_shapes=[
            pltpu.VMEM((3, own, width), BF),
            pltpu.VMEM((8, LANES), F32),
            pltpu.VMEM((tall, width), F32),
            pltpu.VMEM((4, most, tall, width), BF),
            pltpu.VMEM((units, width), BF),
            pltpu.VMEM((units, width), BF),
            pltpu.VMEM((3 * width // (2 * own), 2, own, width), BF),
            pltpu.VMEM((cols, width), BF),
            pltpu.VMEM((nz, 3, rows, cols), BF),
            pltpu.VMEM((2, heads, rows, frames), BF),
            dma((3,)),
            dma((3,)),
            dma((2,)),
            dma((2,)),
            dma((3, chips)),
            dma((3, chips)),
            dma((7, 3, chips)),
            dma((4, most)),
            dma((4, most)),
            dma((4,)),
            dma((nz,)),
            dma((nz,)),
            dma((2,)),
        ],
        compiler_params=pltpu.CompilerParams(
            collective_id=5, has_side_effects=True, vmem_limit_bytes=56 * 1024 * 1024
        ),
    )(upward, downward, square, vectors, kernel, signal, cotangent, lengths, coarse, fine)


def per_device(
    inputs,
    cotangent,
    lengths,
    square,
    upward,
    downward,
    vectors,
    kernel,
    square_momentum,
    square_variance,
    upward_momentum,
    upward_variance,
    downward_momentum,
    downward_variance,
    vectors_momentum,
    vectors_variance,
    kernel_momentum,
    kernel_variance,
):
    model_width = inputs.shape[2]
    seq_frames = inputs.shape[1] * lax.axis_size("seq")
    head_size = D // H
    coarse, fine = position_tables(seq_frames, model_width)
    (
        full_ud, full_sq, small, signal, cotangent_here, length,
        resid1, normed1, hidden1, active1, normed2, heads, pos_heads, attended, prob,
    ) = head(upward, downward, square, vectors, kernel.T, inputs[0], cotangent[0], lengths, coarse, fine, head_size)
    full_sq = full_sq.reshape(model_width * 8, model_width)
    (
        layer_output, grad_res2, grad_out_head, out_time, grad_att_b, normed3, grad_pair, grad_conv_b, swish_b, normed4,
        active4, grad_hidden4, half4, small_grads, grad_taps,
    ) = middle(length, attended, resid1, cotangent_here, small, kernel.shape[0], full_ud, full_sq)
    input_grad, matrix_grads, square_grad, small_sums = back(
        heads, pos_heads, grad_out_head, prob, head_size, coarse, fine, small,
        signal, resid1, grad_res2, (normed1, hidden1, active1, normed2), (normed4, active4, grad_hidden4, half4),
        (out_time, grad_att_b, normed3, grad_pair, grad_conv_b, swish_b), small_grads, grad_taps, full_ud, full_sq,
    )
    (
        layer_output, input_grad,
        square_grad, square_next, momentum_square, variance_square,
        upward_grad, upward_next, momentum_upward, variance_upward,
        downward_grad, downward_next, momentum_downward, variance_downward,
        vectors_grad, vectors_next, momentum_vectors, variance_vectors,
        kernel_grad, kernel_next, momentum_kernel, variance_kernel,
    ) = finish(
        layer_output, input_grad, matrix_grads, square_grad, small_sums,
        (
            (square, square_momentum, square_variance),
            (upward, upward_momentum, upward_variance),
            (downward, downward_momentum, downward_variance),
            (vectors, vectors_momentum, vectors_variance),
            (kernel.T, kernel_momentum.T, kernel_variance.T),
        ),
    )
    return (
        layer_output[None],
        input_grad[None],
        square_grad,
        upward_grad,
        downward_grad,
        vectors_grad,
        kernel_grad.T,
        square_next,
        upward_next,
        downward_next,
        vectors_next,
        kernel_next.T,
        momentum_square,
        variance_square,
        momentum_upward,
        variance_upward,
        momentum_downward,
        variance_downward,
        momentum_vectors,
        variance_vectors,
        momentum_kernel.T,
        variance_kernel.T,
    )


def solution(mesh):
    return jax.shard_map(
        per_device,
        mesh=mesh,
        in_specs=(
            P("fsdp", "seq", None),
            P("fsdp", "seq", None),
            P("fsdp"),
            P(("seq", "fsdp"), None),
            P(("seq", "fsdp"), None),
            P(("seq", "fsdp"), None),
            P(None, ("seq", "fsdp")),
            P(None, ("seq", "fsdp")),
            P(("seq", "fsdp"), None),
            P(("seq", "fsdp"), None),
            P(("seq", "fsdp"), None),
            P(("seq", "fsdp"), None),
            P(("seq", "fsdp"), None),
            P(("seq", "fsdp"), None),
            P(None, ("seq", "fsdp")),
            P(None, ("seq", "fsdp")),
            P(None, ("seq", "fsdp")),
            P(None, ("seq", "fsdp")),
        ),
        out_specs=(
            P("fsdp", "seq", None),
            P("fsdp", "seq", None),
            P(("seq", "fsdp"), None),
            P(("seq", "fsdp"), None),
            P(("seq", "fsdp"), None),
            P(None, ("seq", "fsdp")),
            P(None, ("seq", "fsdp")),
            P(("seq", "fsdp"), None),
            P(("seq", "fsdp"), None),
            P(("seq", "fsdp"), None),
            P(None, ("seq", "fsdp")),
            P(None, ("seq", "fsdp")),
            P(("seq", "fsdp"), None),
            P(("seq", "fsdp"), None),
            P(("seq", "fsdp"), None),
            P(("seq", "fsdp"), None),
            P(("seq", "fsdp"), None),
            P(("seq", "fsdp"), None),
            P(None, ("seq", "fsdp")),
            P(None, ("seq", "fsdp")),
            P(None, ("seq", "fsdp")),
            P(None, ("seq", "fsdp")),
        ),
        check_vma=False,
    )
```

```python
import math

import jax
import jax.numpy as jnp
from jax import lax
from jax.experimental import pallas as pl
from jax.experimental.pallas import tpu as pltpu
from jax.sharding import PartitionSpec as P

D = 512
H = 8
FF = 2048
ADAM_STEP = 4

LN_EPS = 1e-05
BN_EPS = 1e-05
BETA_ONE = 0.9
BETA_TWO = 0.98
ADAM_EPS = 1e-08
LEARN_RATE = 0.005
DECAY_RATE = 0.01


def position_tables(seq_frames, model_width):
    fine = math.gcd(2 * seq_frames, 64)
    column = jnp.arange(model_width)
    frequency = jnp.exp(-math.log(10000.0) * 2.0 * (column // 2).astype(jnp.float32) / model_width)
    coarse_at = (seq_frames - 1 - fine * jnp.arange(2 * seq_frames // fine)).astype(jnp.float32)
    coarse_phase = coarse_at[:, None] * frequency[None, :]
    fine_phase = jnp.arange(fine).astype(jnp.float32)[:, None] * frequency[None, :]
    even = (column % 2 == 0)[None, :]
    sine, cosine = jnp.sin(coarse_phase), jnp.cos(coarse_phase)
    with_cosine = jnp.where(even, sine, cosine)
    with_sine = jnp.where(even, -cosine, sine)
    return jnp.stack([with_cosine, with_sine]), jnp.stack([jnp.cos(fine_phase), jnp.sin(fine_phase)])


MESH = pl.DeviceIdType.MESH
BF = jnp.bfloat16
F32 = jnp.float32
LANES = 128


class Grid:
    def __init__(self):
        self.nz = lax.axis_size("seq")
        self.nf = lax.axis_size("fsdp")
        plane = self.nf // 2
        side = math.isqrt(plane)
        self.z = lax.axis_index("seq")
        f = lax.axis_index("fsdp")
        self.core = f % 2
        if side * side == plane:
            self.na = self.nb = side
            self.step_a = 2 + self.core * (2 * side - 2)
            self.step_b = 2 * side - self.core * (2 * side - 2)
        else:
            self.na, self.nb = plane, 1
            self.step_a, self.step_b = 2, self.nf
        self.f = f
        self.a = (f // self.step_a) % self.na
        self.b = (f // self.step_b) % self.nb
        self.plane = plane
        self.chips = plane * self.nz

        self.half = self.nz // 2
        self.t = (self.z % self.half) * 2 + self.core
        self.column = f - self.core

    def time(self, q):
        return (self.z - self.z % self.half + q // 2, self.column + q % 2)

    def owner(self):
        return (self.t, self.column + self.z // self.half)

    def worker(self):
        return (self.core * self.half + self.z // 2, self.column + self.z % 2)

    def at_home(self):
        return jnp.logical_and(self.t == self.z, self.z // self.half == self.core)

    def chip(self, z, a, b):
        return z * self.plane + (a * self.step_a + b * self.step_b) // 2

    def device(self, z, a, b):
        return (z, a * self.step_a + b * self.step_b + self.core)

    def sibling(self):
        return (self.z, self.f + 1 - 2 * self.core)

    def up(self, axis):
        return self.device(self.z + (axis == "z"), self.a + (axis == "a"), self.b + (axis == "b"))

    def down(self, axis):
        return self.device(self.z - (axis == "z"), self.a - (axis == "a"), self.b - (axis == "b"))

    def line(self, axis):
        return {
            "c": (self.core, 2, lambda q: (self.z, self.f - self.core + q)),
            "a": (self.a, self.na, lambda q: self.device(self.z, q, self.b)),
            "b": (self.b, self.nb, lambda q: self.device(self.z, self.a, q)),
            "z": (self.z, self.nz, lambda q: self.device(q, self.a, self.b)),
        }[axis]

    def place(self, axis):
        return {"z": (self.z, self.nz), "a": (self.a, self.na), "b": (self.b, self.nb)}[axis]


def greet_mover(g, barrier, source):
    @pl.when(jnp.logical_not(g.at_home()))
    def _():
        pl.semaphore_signal(barrier, inc=1, device_id=source, device_id_type=MESH)

    return 1 - g.at_home().astype(jnp.int32)


def merge_moments(first_op, second_op):
    count = first_op[0:1] + second_op[0:1]
    share = second_op[0:1] / jnp.maximum(count, 1.0)
    gap = second_op[1:2] - first_op[1:2]
    mean = first_op[1:2] + gap * share
    squares = first_op[2:3] + second_op[2:3] + gap * gap * (first_op[0:1] * share)
    return jnp.concatenate([count, mean, squares, first_op[3:]], axis=0)


NT = (((1,), (1,)), ((), ()))
TN = (((0,), (0,)), ((), ()))
NN = (((1,), (0,)), ((), ()))


def dot(first_op, second_op, dims):
    return lax.dot_general(first_op, second_op, dims, preferred_element_type=F32)


def keep_head(value, h, head_size):
    lane = lax.broadcasted_iota(jnp.int32, value.shape, 1)
    return jnp.where(lane // head_size == h, value, jnp.zeros_like(value))


def attend_block(head_size, i, query_b, k_ref, v_ref, pos_ref, bias, len_ref, prob_ref):
    rows, cols = query_b.shape
    frames = k_ref.shape[0]
    width = rows + frames
    query = query_b.astype(F32)
    content = (query + bias[0:1, :]).astype(BF)
    positional = (query + bias[1:2, :]).astype(BF)
    window = pos_ref[pl.ds(pl.multiple_of(frames - rows - i * rows, rows), width), :]
    live = lax.broadcasted_iota(jnp.int32, (rows, frames), 1).astype(F32) < len_ref[0:1, 0:1]
    out = jnp.zeros((rows, cols), F32)
    for h in range(cols // head_size):
        direct = dot(keep_head(content, h, head_size), k_ref[...], NT)
        spread = dot(keep_head(positional, h, head_size), window, NT)
        shifted = pltpu.roll(spread, width - rows + 1, 1, stride=1, stride_axis=0)[:, :frames]
        score = jnp.where(live, (direct + shifted) * (1.0 / math.sqrt(head_size)), -1e30)
        top = jnp.max(score, axis=-1, keepdims=True)
        power = jnp.exp(score - top)
        prob_b = (power * (1.0 / jnp.sum(power, axis=-1, keepdims=True))).astype(BF)
        prob_ref[h] = prob_b
        out = out + keep_head(dot(prob_b, v_ref[...], NN), h, head_size)
    return out.astype(BF)


def attend_back_block(head_size, i, query_b, k_ref, v_ref, pos_ref, bias, prob_ref, grad_heads, gk_acc, gv_acc, gpos_acc, gbias):
    rows, cols = query_b.shape
    frames = k_ref.shape[0]
    width = rows + frames
    query = query_b.astype(F32)
    content = (query + bias[0:1, :]).astype(BF)
    positional = (query + bias[1:2, :]).astype(BF)
    down = lax.broadcasted_iota(jnp.int32, (rows, rows), 0)
    across = lax.broadcasted_iota(jnp.int32, (rows, rows), 1)
    turn = jnp.where(down + across == rows - 1, 1.0, 0.0).astype(BF)
    positional_turned = dot(turn, positional, NN).astype(BF)
    here = pl.ds(pl.multiple_of(frames - rows - i * rows, rows), width)
    window = pos_ref[here, :]
    grad_content = jnp.zeros((rows, cols), F32)
    grad_position = jnp.zeros((rows, cols), F32)
    for h in range(cols // head_size):
        grad_out = keep_head(grad_heads, h, head_size)
        prob_b = prob_ref[h]
        prob = prob_b.astype(F32)
        grad_prob = dot(grad_out, v_ref[...], NT)
        delta = jnp.sum(prob * grad_prob, axis=-1, keepdims=True)
        score_b = (prob * (grad_prob - delta) * (1.0 / math.sqrt(head_size))).astype(BF)
        grad_content = grad_content + keep_head(dot(score_b, k_ref[...], NN), h, head_size)
        gk_acc[...] += dot(keep_head(content, h, head_size), score_b, TN)
        gv_acc[...] += dot(grad_out, prob_b, TN)
        wide = jnp.concatenate([dot(turn, score_b, NN), jnp.zeros((rows, width - frames), F32)], axis=1)
        spread = pltpu.roll(wide, 0, 1, stride=1, stride_axis=0).astype(BF)
        grad_position = grad_position + keep_head(dot(spread, window, NN), h, head_size)
        gpos_acc[:, here] += dot(keep_head(positional_turned, h, head_size), spread, TN)
    high = grad_position.astype(BF)
    low = (grad_position - high.astype(F32)).astype(BF)
    grad_position = dot(turn, high, NN) + dot(turn, low, NN)
    gbias[0:1, :] += jnp.sum(grad_content, axis=0, keepdims=True)
    gbias[1:2, :] += jnp.sum(grad_position, axis=0, keepdims=True)
    return (grad_content + grad_position).astype(BF)

def normalize(value):
    mean = jnp.mean(value, axis=-1, keepdims=True)
    centred = value - mean
    spread = lax.rsqrt(jnp.mean(centred * centred, axis=-1, keepdims=True) + LN_EPS)
    return centred * spread, spread


def norm_forward(value, gains, k):
    unit, _ = normalize(value)
    return (unit * gains[2 * k : 2 * k + 1] + gains[2 * k + 1 : 2 * k + 2]).astype(BF)


def norm_backward(value, gains, k, upstream):
    unit, spread = normalize(value)
    inner = upstream * gains[2 * k : 2 * k + 1]
    along = jnp.mean(inner * unit, axis=-1, keepdims=True)
    grad = spread * (inner - jnp.mean(inner, axis=-1, keepdims=True) - unit * along)
    gain = jnp.sum(upstream * unit, axis=0, keepdims=True)
    return grad, gain, jnp.sum(upstream, axis=0, keepdims=True)


def sigmoid(value):
    return 1.0 / (1.0 + jnp.exp(-value))


def module_forward(normed, up_ref, down_ref, hidden_ref, active_ref):
    units, width = up_ref.shape
    step = min(512, units)

    def chunk(j, total):
        here = pl.ds(pl.multiple_of(j * step, step), step)
        hidden = dot(normed, up_ref[here, :], NT)
        active = (hidden * sigmoid(hidden)).astype(BF)
        hidden_ref[:, here] = hidden.astype(hidden_ref.dtype)
        active_ref[:, here] = active
        return total + dot(active, down_ref[here, :], NN)

    return lax.fori_loop(0, units // step, chunk, jnp.zeros((normed.shape[0], width), F32))


def module_backward(upstream_b, up_ref, down_ref, hidden_ref, grad_ref):
    units, width = up_ref.shape
    step = min(512, units)

    def chunk(j, total):
        here = pl.ds(pl.multiple_of(j * step, step), step)
        hidden = hidden_ref[:, here].astype(F32)
        sigma = sigmoid(hidden)
        slope = sigma * (1.0 + hidden * (1.0 - sigma))
        grad = (dot(upstream_b, down_ref[here, :], NT) * slope).astype(BF)
        grad_ref[:, here] = grad
        return total + dot(grad, up_ref[here, :], NN)

    return lax.fori_loop(0, units // step, chunk, jnp.zeros((upstream_b.shape[0], width), F32))


def greet_lines(g, axes, source=None):
    barrier = pltpu.get_barrier_semaphore()
    total = g.nz - 1
    for k in range(1, g.nz):
        pl.semaphore_signal(barrier, inc=1, device_id=g.time(lax.rem(g.t + k, g.nz)), device_id_type=MESH)
    if source is not None:
        total = total + greet_mover(g, barrier, source)
    for axis in axes:
        p, n, device = g.line(axis)
        for k in range(1, n):
            pl.semaphore_signal(barrier, inc=1, device_id=device(lax.rem(p + k, n)), device_id_type=MESH)
            total += 1
    pl.semaphore_wait(barrier, total)


def remote(src, dst, send, recv, device):
    return pltpu.make_async_remote_copy(
        src_ref=src, dst_ref=dst, send_sem=send, recv_sem=recv, device_id=device, device_id_type=MESH
    )


def arrived(ref, sem):
    pltpu.make_async_copy(ref, ref, sem).wait()


def meet_levels(g, value, merge, buf, send_sem, recv_sem):
    sends = []
    for level, axis in enumerate("cabz"):
        p, n, device = g.line(axis)
        if n == 1:
            continue
        buf[level, p] = value
        for k in range(1, n):
            copy = remote(buf.at[level, p], buf.at[level, p], send_sem.at[level, k], recv_sem.at[level, p], device(lax.rem(p + k, n)))
            copy.start()
            sends.append(copy)
        for k in range(1, n):
            q = lax.rem(p + k, n)
            arrived(buf.at[level, q], recv_sem.at[level, q])
        value = buf[level, 0]
        for q in range(1, n):
            value = merge(value, buf[level, q])
    return value, sends


HALO = 16


def swap_edges(g, body, low, high, send_sem, recv_sem, pad):
    rows = body.shape[0]
    p, n = g.t, g.nz
    up = remote(body.at[pl.ds(rows - HALO, HALO)], low, send_sem.at[0], recv_sem.at[0], g.time(p + 1))
    down = remote(body.at[pl.ds(0, HALO)], high, send_sem.at[1], recv_sem.at[1], g.time(p - 1))
    pl.when(p < n - 1)(lambda: up.start())
    pl.when(p > 0)(lambda: down.start())
    pad[pl.ds(HALO, rows), :] = body[...].astype(F32)

    def fill(at, ref, sem, there):
        @pl.when(there)
        def _():
            arrived(ref, sem)
            pad[pl.ds(at, HALO), :] = ref[...].astype(F32)

        @pl.when(jnp.logical_not(there))
        def _():
            pad[pl.ds(at, HALO), :] = jnp.zeros((HALO, pad.shape[1]), F32)

    fill(0, low, recv_sem.at[0], p > 0)
    fill(HALO + rows, high, recv_sem.at[1], p < n - 1)

    def finish():
        pl.when(p < n - 1)(lambda: up.wait_send())
        pl.when(p > 0)(lambda: down.wait_send())

    return finish


def middle_kernel(taps, len_ref, att_ref, x1_ref, cot_ref, gains_ref, ud_hbm, sq_hbm,
                  y_ref, g2_ref, go_ref, o_ref, e2_ref, a3_ref, gpair_ref, e3_ref, sw_ref, a4_ref, s4_ref, gh4_ref, e4_ref,
                  small_ref, gtaps_ref,
                  up, down, wsq, o_buf, go_buf, glu_b, gc_b, low1, high1, low2, high2, pad_glu, pad_gc, h4, c_ref, y_buf, y_sem,
                  buf1, buf2, load_sem, a_send, a_recv, b_send, b_recv, h_send, h_recv, m_send, m_recv):
    g = Grid()
    z, nz = g.t, g.nz
    rows, width = x1_ref.shape
    cols = width // nz
    units = up.shape[0]
    rim = (taps - 1) // 2
    loads = [
        pltpu.make_async_copy(sq_hbm.at[pl.ds(4 * width, 4 * width)], wsq, load_sem.at[0]),
        pltpu.make_async_copy(ud_hbm.at[0, pl.ds(units, units)], up, load_sem.at[1]),
        pltpu.make_async_copy(ud_hbm.at[1, pl.ds(units, units)], down, load_sem.at[2]),
    ]
    for load in loads:
        load.start()
    greet_lines(g, "cabz", g.worker())
    sends = []
    for k in range(1, nz):
        q = lax.rem(z + k, nz)
        copy = remote(att_ref.at[pl.ds(q * rows, rows)], o_buf.at[z], a_send.at[k], a_recv.at[z], g.time(q))
        copy.start()
        sends.append(copy)
    o_buf[z] = att_ref[pl.ds(pl.multiple_of(z * rows, rows), rows), :]
    gains = gains_ref[...]
    frame = z * rows + lax.broadcasted_iota(jnp.int32, (rows, 1), 0)
    live = jnp.where(frame.astype(F32) < len_ref[0:1, 0:1], 1.0, 0.0)
    loads[0].wait()
    weight = lambda k: wsq[pl.ds((k - 4) * width, width), :]
    for k in range(1, nz):
        q = lax.rem(z + k, nz)
        arrived(o_buf.at[q], a_recv.at[q])
    out = jnp.concatenate([o_buf[q] for q in range(nz)], axis=1)
    o_ref[...] = out
    resid2 = x1_ref[...] + dot(out, weight(4), NT)
    normed3 = norm_forward(resid2, gains, 2)
    a3_ref[...] = normed3
    value = dot(normed3, weight(5), NT)
    gate = sigmoid(dot(normed3, weight(6), NT))
    glu_b[...] = (value * gate * live).astype(BF)
    done1 = swap_edges(g, glu_b, low1, high1, h_send.at[0], h_recv.at[0], pad_glu)
    for at in range(0, width, LANES):
        lanes = pl.ds(at, LANES)
        total = jnp.zeros((rows, LANES), F32)
        for m in range(taps):
            total = total + gains_ref[14 + m : 15 + m, lanes] * pad_glu[pl.ds(HALO - rim + m, rows), lanes]
        c_ref[:, lanes] = total
    conv = c_ref[...]
    count = jnp.sum(live, axis=0, keepdims=True)
    mean = jnp.sum(live * conv, axis=0, keepdims=True) / jnp.maximum(count, 1.0)
    squares = jnp.sum(live * (conv - mean) * (conv - mean), axis=0, keepdims=True)
    moments = jnp.concatenate([jnp.broadcast_to(count, mean.shape), mean, squares, jnp.zeros((5, width), F32)], axis=0)
    moments, more = meet_levels(g, moments, merge_moments, buf1, m_send.at[0], m_recv.at[0])
    sends += more
    total_frames = moments[0:1]
    inv_std = lax.rsqrt(moments[2:3] / total_frames + BN_EPS)
    centre = moments[1:2]
    centred = c_ref[...] - centre
    zed = centred * inv_std
    bn_val = gains[12:13] * zed + gains[13:14]
    swish = (bn_val * sigmoid(bn_val)).astype(BF)
    sw_ref[...] = swish
    resid3 = resid2 + dot(swish, weight(7), NT)
    normed4 = norm_forward(resid3, gains, 3)
    a4_ref[...] = normed4
    loads[1].wait()
    loads[2].wait()
    resid4 = resid3 + 0.5 * module_forward(normed4, up, down, h4, s4_ref)
    y_buf[...] = norm_forward(resid4, gains, 4)
    away = jnp.logical_not(g.at_home())
    home = remote(y_buf, y_ref, y_sem.at[0], y_sem.at[1], g.owner())
    pl.when(away)(lambda: home.start())

    @pl.when(g.at_home())
    def _():
        y_ref[...] = y_buf[...]

    grad4, gain4, shift4 = norm_backward(resid4, gains, 4, cot_ref[...].astype(F32))
    half4 = (0.5 * grad4).astype(BF)
    e4_ref[...] = half4
    grad_norm, gain3, shift3 = norm_backward(resid3, gains, 3, module_backward(half4, up, down, h4, gh4_ref))
    grad3 = grad4 + grad_norm
    e3 = grad3.astype(BF)
    e3_ref[...] = e3
    sigma = sigmoid(bn_val)
    grad_bn = dot(e3, weight(7), NN) * (sigma * (1.0 + bn_val * (1.0 - sigma)))
    gamma = jnp.sum(grad_bn * zed, axis=0, keepdims=True)
    beta = jnp.sum(grad_bn, axis=0, keepdims=True)
    grad_zed = grad_bn * gains[12:13]
    sum_one = jnp.sum(grad_zed, axis=0, keepdims=True)
    sum_two = jnp.sum(grad_zed * centred, axis=0, keepdims=True)
    sums = jnp.concatenate([sum_one, sum_two, jnp.zeros((6, width), F32)], axis=0)
    sums, more = meet_levels(g, sums, lambda x, y: x + y, buf2, m_send.at[1], m_recv.at[1])
    sends += more
    offset = inv_std * sums[0:1] + inv_std * inv_std * inv_std * sums[1:2] * centred
    gc_b[...] = (inv_std * grad_zed - live / total_frames * offset).astype(BF)
    done2 = swap_edges(g, gc_b, low2, high2, h_send.at[1], h_recv.at[1], pad_gc)
    for at in range(0, width, LANES):
        lanes = pl.ds(at, LANES)
        total = jnp.zeros((rows, LANES), F32)
        upstream = pad_gc[pl.ds(HALO, rows), lanes]
        for m in range(taps):
            total = total + gains_ref[14 + m : 15 + m, lanes] * pad_gc[pl.ds(HALO + rim - m, rows), lanes]
            gtaps_ref[m : m + 1, lanes] = jnp.sum(
                upstream * pad_glu[pl.ds(HALO - rim + m, rows), lanes], axis=0, keepdims=True
            )
        c_ref[:, lanes] = total
    grad_glu = c_ref[...] * live
    gv5 = (grad_glu * gate).astype(BF)
    gv6 = (grad_glu * value * gate * (1.0 - gate)).astype(BF)
    gpair_ref[0] = gv5
    gpair_ref[1] = gv6
    grad_norm, gain2, shift2 = norm_backward(
        resid2, gains, 2, dot(gv5, weight(5), NN) + dot(gv6, weight(6), NN)
    )
    grad2 = grad3 + grad_norm
    g2_ref[...] = grad2
    e2 = grad2.astype(BF)
    e2_ref[...] = e2
    grad_out = dot(e2, weight(4), NN).astype(BF)
    for q in range(nz):
        go_buf[q] = grad_out[:, q * cols : (q + 1) * cols]
    for k in range(1, nz):
        q = lax.rem(z + k, nz)
        copy = remote(go_buf.at[q], go_ref.at[pl.ds(z * rows, rows)], b_send.at[k], b_recv.at[z], g.time(q))
        copy.start()
        sends.append(copy)
    go_ref[pl.ds(pl.multiple_of(z * rows, rows), rows), :] = go_buf[z]
    small_ref[...] = jnp.concatenate([gain2, shift2, gain3, shift3, gain4, shift4, gamma, beta], axis=0)
    for k in range(1, nz):
        q = lax.rem(z + k, nz)
        arrived(go_ref.at[pl.ds(q * rows, rows)], b_recv.at[q])
    pl.when(away)(lambda: home.wait())
    done1()
    done2()
    for copy in sends:
        copy.wait_send()


def middle(length, attended, resid1, cotangent, gains, taps, ud_full, sq_full):
    rows, width = resid1.shape
    nz, nf = lax.axis_size("seq"), lax.axis_size("fsdp")
    frames, cols = rows * nz, width // nz
    units = ud_full.shape[1] // 2
    most = max(nz, nf // 2)
    vmem = pl.BlockSpec(memory_space=pltpu.VMEM)
    hbm = pl.BlockSpec(memory_space=pl.ANY)
    shape = jax.ShapeDtypeStruct
    dma = pltpu.SemaphoreType.DMA
    row = shape((rows, width), BF)
    return pl.pallas_call(
        lambda *refs: middle_kernel(taps, *refs),
        name="middle",
        out_shape=(
            row,
            shape((rows, width), F32),
            shape((frames, cols), BF),
            row,
            row,
            row,
            shape((2, rows, width), BF),
            row,
            row,
            row,
            shape((rows, units), BF),
            shape((rows, units), BF),
            row,
            shape((8, width), F32),
            shape((taps, width), F32),
        ),
        in_specs=[vmem] * 5 + [hbm] * 2,
        out_specs=[vmem] * 15,
        scratch_shapes=[
            pltpu.VMEM((units, width), BF),
            pltpu.VMEM((units, width), BF),
            pltpu.VMEM((4 * width, width), BF),
            pltpu.VMEM((nz, rows, cols), BF),
            pltpu.VMEM((nz, rows, cols), BF),
            pltpu.VMEM((rows, width), BF),
            pltpu.VMEM((rows, width), BF),
        ]
        + [pltpu.VMEM((HALO, width), BF)] * 4
        + [
            pltpu.VMEM((rows + 2 * HALO, width), F32),
            pltpu.VMEM((rows + 2 * HALO, width), F32),
            pltpu.VMEM((rows, units), F32),
            pltpu.VMEM((rows, width), F32),
            pltpu.VMEM((rows, width), BF),
            dma((2,)),
            pltpu.VMEM((4, most, 8, width), F32),
            pltpu.VMEM((4, most, 8, width), F32),
            dma((3,)),
            dma((nz,)),
            dma((nz,)),
            dma((nz,)),
            dma((nz,)),
            dma((2, 2)),
            dma((2, 2)),
            dma((2, 4, most)),
            dma((2, 4, most)),
        ],
        compiler_params=pltpu.CompilerParams(
            collective_id=6, has_side_effects=True, vmem_limit_bytes=56 * 1024 * 1024
        ),
    )(length, attended, resid1, cotangent, gains, ud_full, sq_full)


class Meeting:
    def __init__(self, g, buf, send_sem, recv_sem, order="cabz"):
        self.g, self.buf, self.send_sem, self.recv_sem, self.order = g, buf, send_sem, recv_sem, order

    def copies(self, level):
        p, n, device = self.g.line(self.order[level])
        here = self.buf.at[level, p]
        return [
            remote(here, here, self.send_sem.at[level, k], self.recv_sem.at[level, p], device(lax.rem(p + k, n)))
            for k in range(1, n)
        ]

    def start(self, level, value):
        self.buf[level, self.g.line(self.order[level])[0]] = value
        for copy in self.copies(level):
            copy.start()

    def finish(self):
        for level in range(len(self.order)):
            for copy in self.copies(level):
                copy.wait_send()

    def total(self, level):
        p, n, _ = self.g.line(self.order[level])
        for k in range(1, n):
            q = lax.rem(p + k, n)
            arrived(self.buf.at[level, q], self.recv_sem.at[level, q])
        value = self.buf[level, 0]
        for q in range(1, n):
            value = value + self.buf[level, q]
        return value


class Reduction:
    def __init__(self, g, gud, gsq, sib_ud, sib_sq, sib_sem, rb, ra, rz, sems):
        self.g, self.gud, self.gsq, self.sib_ud, self.sib_sq = g, gud, gsq, sib_ud, sib_sq
        self.sib_send, self.sib_recv = sib_sem
        self.bufs = {"b": rb, "a": ra, "z": rz}
        self.sems = sems
        self.sq_rows = gsq.shape[2]
        self.pair = 2 * self.sq_rows
        self.height = g.plane * self.pair

    def rows(self, t, part):
        return pl.ds(pl.multiple_of(t * self.pair + (part - 1) * self.sq_rows, self.sq_rows), self.sq_rows)

    def own(self, t, part):
        c = self.g.core
        return self.gsq.at[t, c] if part == 0 else self.gud.at[c, self.rows(t, part)]

    def sibling_copy(self, z, kind):
        g = self.g
        d = 1 - g.core
        if kind == 0:
            chips = pl.ds(z * g.plane, g.plane)
            src, dst = self.gsq.at[chips, d], self.sib_sq.at[chips]
        else:
            tall = pl.ds(z * self.height, self.height)
            src, dst = self.gud.at[d, tall], self.sib_ud.at[tall]
        return remote(src, dst, self.sib_send.at[kind, z], self.sib_recv.at[kind, z], g.sibling())

    def to_sibling(self, planes, kind):
        for z in planes:
            self.sibling_copy(z, kind).start()

    def from_sibling(self, planes, kind):
        for z in planes:
            self.sibling_copy(z, kind).wait_recv()

    def add_sibling(self, t, part):
        ref = self.own(t, part)
        ref[...] = ref[...] + (self.sib_sq[t] if part == 0 else self.sib_ud[self.rows(t, part), :])

    def landing(self, axis, slot, part):
        return self.bufs[axis].at[slot, pl.ds(part * self.sq_rows, self.sq_rows)]

    def slot(self, axis, upward, z, a, b, there):
        g = self.g
        p, n = g.place(axis)
        q = {"z": z, "a": a, "b": b}[axis]
        if there:
            p = p + 1 if upward else p - 1
        if upward:
            q = q + 1 - n * (p == n - 1)
        return {"b": (q * g.na + a) * g.nz + z, "a": q * g.nz + z, "z": q}[axis]

    def hop(self, axis, upward, z, a, b, part):
        g = self.g
        slot = self.slot(axis, upward, z, a, b, True)
        sends, recvs = self.sems[axis]
        device = g.up(axis) if upward else g.down(axis)
        src, dst = self.own(g.chip(z, a, b), part), self.landing(axis, slot, part)
        return remote(src, dst, sends.at[1 if upward else 0, part, slot], recvs.at[part, slot], device)

    def take(self, axis, upward, z, a, b, part):
        slot = self.slot(axis, upward, z, a, b, False)
        src, dst = self.landing(axis, slot, part), self.own(self.g.chip(z, a, b), part)
        arrived(src, self.sems[axis][1].at[part, slot])
        dst[...] = dst[...] + src[...]

    def settle(self, axis, z, a, b, part):
        p, n = self.g.place(axis)
        if n > 1:
            pl.when(p > 0)(lambda: self.take(axis, True, z, a, b, part))
            pl.when(p < n - 1)(lambda: self.take(axis, False, z, a, b, part))

    def ready(self, axis, z, a, b, part):
        if axis == "b":
            self.add_sibling(self.g.chip(z, a, b), part)
        else:
            before = {"a": "b", "z": "a"}[axis]
            self.ready(before, z, a, b, part)
            self.settle(before, z, a, b, part)

    def pass_on(self, axis, upward, z, a, b, part, finish):
        p, n = self.g.place(axis)
        if finish:
            self.hop(axis, upward, z, a, b, part).wait_send()
            return
        self.ready(axis, z, a, b, part)
        behind = p > 0 if upward else p < n - 1
        pl.when(behind)(lambda: self.take(axis, upward, z, a, b, part))
        self.hop(axis, upward, z, a, b, part).start()

    def along(self, axis, planes, part, finish=False):
        g = self.g
        p, n = g.place(axis)
        if axis == "z":
            for q in planes:
                pl.when(p < q)(lambda: self.pass_on("z", True, q, g.a, g.b, part, finish))
                pl.when(p > q)(lambda: self.pass_on("z", False, q, g.a, g.b, part, finish))
            return
        step = planes[1] - planes[0] if len(planes) > 1 else 1
        count = len(planes)
        for k in range(n - 1, 0, -1):
            for upward in (True, False):
                q = p + k if upward else p - k

                def act():
                    def body(i, _):
                        plane = planes[0] + step * lax.rem(i, count)
                        if axis == "b":
                            a = lax.rem(g.a + 1 + i // count, g.na)
                            self.pass_on("b", upward, plane, a, q, part, finish)
                        else:
                            self.pass_on("a", upward, plane, q, g.b, part, finish)
                        return 0

                    lax.fori_loop(0, (g.na if axis == "b" else 1) * count, body, 0)

                pl.when(p + k < n if upward else p >= k)(act)

    def last(self, part):
        g = self.g
        self.ready("z", g.z, g.a, g.b, part)
        self.settle("z", g.z, g.a, g.b, part)


def back_kernel(head_size, qkv_ref, pos_ref, go_ref, coarse_ref, fine_ref, gains_ref,
                x_ref, x1_ref, g2_ref, a1_ref, h1_ref, s1_ref, a2_ref,
                a4_ref, s4_ref, gh4_ref, e4_ref, o_ref, e2_ref, a3_ref, gpair_ref, e3_ref, sw_ref, some_ref, gtaps_ref,
                prob_hbm, ud_hbm, sq_hbm,
                gx_ref, ud_out, sq_out, small_out,
                prob_buf, gk_acc, gv_acc, gpos_acc, gbias, grads, prob_sem, wqkv, heads, gqkv, gh1, small, few, fbuf, f_send, f_recv, gud, gsq, sib_ud, sib_sq, rb, ra, rz, sbuf, fin_send_buf, fin, gx_buf, gx_in, gx_sem,
                load_sem, h_send, h_recv, sib_send, sib_recv, b_send, b_recv, a_send, a_recv, z_send, z_recv, s_send, s_recv,
                fin_send, fin_recv):
    g = Grid()
    z, nz, c = g.t, g.nz, g.core
    rows, width = x_ref.shape
    cols = width // nz
    units = h1_ref.shape[1]
    frames = qkv_ref.shape[1]
    up, down = gud.at[0, pl.ds(0, units)], gud.at[1, pl.ds(0, units)]
    loads = [
        pltpu.make_async_copy(sq_hbm.at[pl.ds(0, 3 * width)], wqkv, load_sem.at[0]),
        pltpu.make_async_copy(ud_hbm.at[0, pl.ds(0, units)], up, load_sem.at[1]),
        pltpu.make_async_copy(ud_hbm.at[1, pl.ds(0, units)], down, load_sem.at[2]),
    ]

    def probabilities(i):
        return pltpu.make_async_copy(prob_hbm.at[:, pl.ds(i * rows, rows)], prob_buf.at[i % 2], prob_sem.at[i % 2])

    probabilities(0).start()
    for load in loads:
        load.start()
    greet_lines(g, "cabz", g.worker())
    sends = []
    small[...] = jnp.zeros_like(small)
    small[0:8, :] = some_ref[...]
    small[8 : 8 + gtaps_ref.shape[0], :] = gtaps_ref[...]
    early = Meeting(g, sbuf, s_send, s_recv)
    early.start(0, small[...])
    red = Reduction(
        g, gud, gsq, sib_ud, sib_sq, (sib_send, sib_recv), rb, ra, rz,
        {"b": (b_send, b_recv), "a": (a_send, a_recv), "z": (z_send, z_recv)},
    )
    total_rows = gud.shape[1]
    sq_rows = gsq.shape[2]
    high = list(range(nz - 1, nz // 2 - 1, -1))
    low = list(range(0, nz // 2))
    part = 256

    def matrix_terms(color, left_ref, right, first_row, count):
        def body(i, _):
            here = pl.ds(pl.multiple_of(i * part, part), part)
            there = pl.ds(pl.multiple_of(first_row + i * part, part), part)
            gud[color, there, :] = dot(left_ref[:, here], right, TN).astype(BF)
            return 0

        lax.fori_loop(0, count // part, body, 0)

    per = width // sq_rows // 2

    def square_terms(block, left, right):
        sums = dot(left, right, TN).astype(BF).reshape(per, 2, sq_rows, width)
        gsq[pl.ds(block * per, per)] = sums

    square_terms(7, e3_ref[...], sw_ref[...])
    square_terms(6, gpair_ref[1], a3_ref[...])
    square_terms(5, gpair_ref[0], a3_ref[...])
    square_terms(4, e2_ref[...], o_ref[...])
    red.to_sibling(high, 0)
    early.start(1, early.total(0))
    matrix_terms(0, gh4_ref, a4_ref[...], units, units)
    matrix_terms(1, s4_ref, e4_ref[...], units, units)
    red.to_sibling(high, 1)
    early.start(2, early.total(1))
    gk_acc[...] = jnp.zeros_like(gk_acc)
    gv_acc[...] = jnp.zeros_like(gv_acc)
    gpos_acc[...] = jnp.zeros_like(gpos_acc)
    gbias[...] = jnp.zeros_like(gbias)
    to_time = lambda j, q, k: remote(grads.at[j, q], heads.at[j, z], h_send.at[j, k], h_recv.at[j, z], g.time(q))
    bias = gains_ref[10:12, pl.ds(pl.multiple_of(z * cols, cols), cols)]

    def attend(i, _):
        pl.when(i + 1 < nz)(lambda: probabilities(i + 1).start())
        probabilities(i).wait()
        here = pl.ds(pl.multiple_of(i * rows, rows), rows)
        grads[0, i] = attend_back_block(
            head_size, i, qkv_ref[0, here, :], qkv_ref.at[1], qkv_ref.at[2], pos_ref, bias, prob_buf.at[i % 2],
            go_ref[here, :], gk_acc, gv_acc, gpos_acc, gbias,
        )

        @pl.when(i == 0)
        def _():
            early.start(3, early.total(2))
            red.from_sibling(high, 0)
            red.along("b", high, 0)

        @pl.when(i == 1)
        def _():
            red.from_sibling(high, 1)
            red.along("b", high, 1)
            red.along("b", high, 2)

        return 0

    lax.fori_loop(0, nz, attend, 0)
    small[...] = early.total(3)
    grads_k = gk_acc[...].T.astype(BF)
    grads_v = gv_acc[...].T.astype(BF)
    for q in range(nz):
        grads[1, q] = grads_k[q * rows : (q + 1) * rows]
        grads[2, q] = grads_v[q * rows : (q + 1) * rows]
    for k in range(1, nz):
        q = lax.rem(z + k, nz)
        for j in range(3):
            copy = to_time(j, q, k)
            copy.start()
            sends.append(copy)
    for j in range(3):
        heads[j, z] = grads[j, z]
    red.along("a", high, 0)
    fine = fine_ref.shape[1]

    def position(i, total):
        table = coarse_ref[0, pl.ds(2 * i, 1), :] * fine_ref[0] + coarse_ref[1, pl.ds(2 * i, 1), :] * fine_ref[1]
        after = coarse_ref[0, pl.ds(2 * i + 1, 1), :] * fine_ref[0] + coarse_ref[1, pl.ds(2 * i + 1, 1), :] * fine_ref[1]
        both = jnp.concatenate([table, after], axis=0).astype(BF)
        return total + dot(gpos_acc[:, pl.ds(pl.multiple_of(i * 2 * fine, 2 * fine), 2 * fine)].astype(BF), both, NN)

    gpos = lax.fori_loop(0, coarse_ref.shape[1] // 2, position, jnp.zeros((cols, width), F32)).astype(BF)
    gsq[pl.ds(3 * per, per)] = jnp.zeros((per, 2, sq_rows, width), BF)
    pieces = cols // sq_rows
    for i in range(pieces):
        piece = z * pieces + i
        gsq[3 * per + piece // 2, piece % 2] = gpos[i * sq_rows : (i + 1) * sq_rows]
    gains = gains_ref[...]
    loads[0].wait()
    grad_norm = jnp.zeros((rows, width), F32)
    for j in range(3):
        for k in range(1, nz):
            q = lax.rem(z + k, nz)
            arrived(heads.at[j, q], h_recv.at[j, q])
        full = jnp.concatenate([heads[j, q] for q in range(nz)], axis=1)
        gqkv[j] = full
        grad_norm = grad_norm + dot(full, wqkv[pl.ds(j * width, width), :], NN)
    for j in range(3):
        square_terms(j, gqkv[j], a2_ref[...])
    red.to_sibling(low, 0)
    resid1 = x1_ref[...]
    grad_add, gain1, shift1 = norm_backward(resid1, gains, 1, grad_norm)
    grad1 = g2_ref[...] + grad_add
    half1 = (0.5 * grad1).astype(BF)
    loads[1].wait()
    loads[2].wait()
    red.along("a", high, 1)
    grad_norm = module_backward(half1, up, down, h1_ref, gh1)
    red.from_sibling(low, 0)
    red.along("b", low, 0)
    matrix_terms(0, gh1, a1_ref[...], 0, units)
    matrix_terms(1, s1_ref, half1, 0, units)
    red.to_sibling(low, 1)
    red.along("a", high, 2)
    red.along("a", low, 0)
    grad_add, gain0, shift0 = norm_backward(x_ref[...].astype(F32), gains, 0, grad_norm)
    away = jnp.logical_not(g.at_home())
    gx_buf[...] = (grad1 + grad_add).astype(BF)
    home = remote(gx_buf, gx_in, gx_sem.at[0], gx_sem.at[1], g.owner())
    pl.when(away)(lambda: home.start())
    few[...] = jnp.zeros_like(few)
    few[0:1, :] = gain0
    few[1:2, :] = shift0
    few[2:3, :] = gain1
    few[3:4, :] = shift1
    few[4:6, pl.ds(pl.multiple_of(z * cols, cols), cols)] = gbias[...]
    meeting = Meeting(g, fbuf, f_send, f_recv)
    meeting.start(0, few[...])
    red.from_sibling(low, 1)
    red.along("b", low, 1)
    red.along("b", low, 2)
    meeting.start(1, meeting.total(0))
    red.along("z", high, 0)
    red.along("z", high, 1)
    red.along("a", low, 1)
    red.along("z", low, 0)
    meeting.start(2, meeting.total(1))
    red.along("z", high, 2)
    red.along("a", low, 2)
    red.along("z", low, 1)
    meeting.start(3, meeting.total(2))
    red.along("z", low, 2)
    for part in range(3):
        red.last(part)
    me = g.chip(g.z, g.a, g.b)
    d = 1 - c
    half = ud_out.shape[1]
    at = lambda k: pl.ds(pl.multiple_of(me * 2 * half + k * half, half), half)
    fin_send_buf[...] = gud[c, at(d), :]
    swap = remote(fin_send_buf, fin, fin_send, fin_recv, g.sibling())
    swap.start()
    ud_out[c] = gud[c, at(c), :].astype(F32)
    sq_out[...] = gsq[me, c].astype(F32)
    total = meeting.total(3)
    small_out[0:4, :] = total[0:4]
    small_out[4:10, :] = small[0:6, :]
    small_out[10:12, :] = total[4:6]
    small_out[12 : small.shape[0] + 6, :] = small[6:, :]
    for planes in (high, low):
        for part in range(3):
            for axis in "baz":
                red.along(axis, planes, part, True)
        for kind in range(2):
            for q in planes:
                red.sibling_copy(q, kind).wait_send()
    for copy in sends:
        copy.wait_send()
    early.finish()
    meeting.finish()

    @pl.when(away)
    def _():
        home.wait()
        gx_ref[...] = gx_in[...].astype(F32)

    @pl.when(g.at_home())
    def _():
        gx_ref[...] = gx_buf[...].astype(F32)

    swap.wait()
    ud_out[d] = fin[...].astype(F32)


def back(qkv, pos, grad_out, prob, head_size, coarse, fine, gains, signal, resid1, grad2, first, second, squares, some, gtaps, ud_full, sq_full):
    rows, width = signal.shape
    nz, nf = lax.axis_size("seq"), lax.axis_size("fsdp")
    chips = nz * nf // 2
    plane = nf // 2
    side = math.isqrt(plane)
    na, nb = (side, side) if side * side == plane else (plane, 1)
    cols = width // nz
    units = ud_full.shape[1] // 2
    own = ud_full.shape[1] // (2 * chips)
    block = 3 * own
    most = max(nz, na, nb, 2)
    tall = -(-(8 + gtaps.shape[0]) // 8) * 8
    vmem = pl.BlockSpec(memory_space=pltpu.VMEM)
    hbm = pl.BlockSpec(memory_space=pl.ANY)
    shape = jax.ShapeDtypeStruct
    dma = pltpu.SemaphoreType.DMA
    frames = rows * nz
    heads = cols // head_size
    operands = (qkv, pos, grad_out, coarse, fine, gains, signal, resid1, grad2, *first, *second, *squares, some, gtaps)
    places = lambda n: n + 1 if n > 2 else 1
    slots = {"b": places(nb) * na * nz, "a": places(na) * nz, "z": places(nz)}
    return pl.pallas_call(
        lambda *refs: back_kernel(head_size, *refs),
        name="back",
        out_shape=(
            shape((rows, width), F32),
            shape((2, own, width), F32),
            shape((own, width), F32),
            shape((tall + 6, width), F32),
        ),
        in_specs=[vmem] * len(operands) + [hbm] * 3,
        out_specs=[vmem] * 4,
        scratch_shapes=[
            pltpu.VMEM((2, heads, rows, frames), BF),
            pltpu.VMEM((cols, frames), F32),
            pltpu.VMEM((cols, frames), F32),
            pltpu.VMEM((cols, 2 * frames), F32),
            pltpu.VMEM((2, cols), F32),
            pltpu.VMEM((3, nz, rows, cols), BF),
            dma((2,)),
            pltpu.VMEM((3 * width, width), BF),
            pltpu.VMEM((3, nz, rows, cols), BF),
            pltpu.VMEM((3, rows, width), BF),
            pltpu.VMEM((rows, units), BF),
            pltpu.VMEM((tall, width), F32),
            pltpu.VMEM((8, width), F32),
            pltpu.VMEM((4, most, 8, width), F32),
            dma((4, most)),
            dma((4, most)),
            pltpu.VMEM((2, 2 * units, width), BF),
            pltpu.VMEM((chips, 2, own, width), BF),
            pltpu.VMEM((2 * units, width), BF),
            pltpu.VMEM((chips, own, width), BF),
            pltpu.VMEM((slots["b"], block, width), BF),
            pltpu.VMEM((slots["a"], block, width), BF),
            pltpu.VMEM((slots["z"], block, width), BF),
            pltpu.VMEM((4, most, tall, width), F32),
            pltpu.VMEM((own, width), BF),
            pltpu.VMEM((own, width), BF),
            pltpu.VMEM((rows, width), BF),
            pltpu.VMEM((rows, width), BF),
            dma((2,)),
            dma((3,)),
            dma((3, nz)),
            dma((3, nz)),
            dma((2, nz)),
            dma((2, nz)),
            dma((2, 3, slots["b"])),
            dma((3, slots["b"])),
            dma((2, 3, slots["a"])),
            dma((3, slots["a"])),
            dma((2, 3, slots["z"])),
            dma((3, slots["z"])),
            dma((4, most)),
            dma((4, most)),
            dma,
            dma,
        ],
        compiler_params=pltpu.CompilerParams(
            collective_id=7, has_side_effects=True, vmem_limit_bytes=61000 * 1024
        ),
    )(*operands, prob, ud_full, sq_full)


def finish_kernel(rows, y_ref, gx_ref, matrices_ref, square_ref, small_ref, *refs):
    states, outs = refs[:15], refs[15:]
    outs[0][...] = y_ref[...]
    outs[1][...] = gx_ref[...]
    count, share = rows, states[9].shape[1]
    taps = states[12].shape[1]
    width = small_ref.shape[1]
    place = lax.axis_index("seq") * lax.axis_size("fsdp") + lax.axis_index("fsdp")
    own = pltpu.roll(small_ref[...], lax.rem(width - place * share, width), 1)[:, :LANES]
    below = jnp.concatenate([own[count : count + taps], jnp.zeros((-taps % 8, LANES), F32)], axis=0)
    gradients = (
        square_ref[...],
        matrices_ref[0],
        matrices_ref[1],
        own[:count, :share],
        below.T[:share, :taps],
    )
    fix_one = 1.0 - BETA_ONE**ADAM_STEP
    fix_two = 1.0 - BETA_TWO**ADAM_STEP
    for k, gradient in enumerate(gradients):
        weight, first_mom, second_mom = (ref[...] for ref in states[3 * k : 3 * k + 3])
        decay = 0.0 if k == 3 else DECAY_RATE
        first_new = BETA_ONE * first_mom + (1.0 - BETA_ONE) * gradient
        second_new = BETA_TWO * second_mom + (1.0 - BETA_TWO) * gradient * gradient
        update = first_new / fix_one / (jnp.sqrt(second_new / fix_two) + ADAM_EPS)
        there = outs[2 + 4 * k : 6 + 4 * k]
        there[0][...] = gradient
        there[1][...] = weight - LEARN_RATE * (update + decay * weight)
        there[2][...] = first_new
        there[3][...] = second_new


def finish(layer_output, input_grad, matrices, square, small, states):
    flat = [array for state in states for array in state]
    results = [layer_output, input_grad] + [array for state in states for array in (state[0],) * 4]
    vmem = pl.BlockSpec(memory_space=pltpu.VMEM)
    return pl.pallas_call(
        lambda *refs: finish_kernel(states[3][0].shape[0], *refs),
        name="finish",
        out_shape=[jax.ShapeDtypeStruct(array.shape, array.dtype) for array in results],
        in_specs=[vmem] * (5 + len(flat)),
        out_specs=[vmem] * len(results),
    )(layer_output, input_grad, matrices, square, small, *flat)


def when(*conditions):
    holds = 1
    for condition in conditions:
        holds = holds * jnp.asarray(condition).astype(jnp.int32)
    return pl.when(holds == 1) if conditions else lambda act: act()


class Gather:
    WAYS = {"z+": 0, "z-": 1, "a+": 2, "a-": 3, "b+": 4, "b-": 5, "s": 6}
    PARTS = (0, 1, 2)
    SPREAD = ("a+", "a-", "b+", "b-", "s")

    def __init__(self, g, ud, sq, recv_sem, sib_recv, send_sem):
        self.g, self.ud, self.sq = g, ud, sq
        self.recv_sem, self.sib_recv, self.send_sem = recv_sem, sib_recv, send_sem
        self.rows = sq.shape[2]
        half = g.nz // 2
        if half == 2:
            first = jnp.minimum(g.z, 1)
            second = jnp.maximum(g.z, 2)
            self.low, self.high = [first, 1 - first], [second, 5 - second]
        else:
            self.low, self.high = list(range(half)), list(range(half, g.nz))
        self.below = g.z < half

    def piece(self, part, t, color):
        if part == 0:
            return self.sq.at[t, color]
        return self.ud.at[color, pl.ds(t * 2 * self.rows + (part - 1) * self.rows, self.rows)]

    def onward(self, part, t, ways, finish, *only):
        g = self.g
        ref = self.piece(part, t, g.core)
        for way in ways:
            p, n = (0, 2) if way == "s" else g.place(way[0])

            def act():
                if way == "s":
                    target, arrive = g.sibling(), self.sib_recv
                else:
                    target, arrive = g.up(way[0]) if way[1] == "+" else g.down(way[0]), self.recv_sem
                copy = remote(ref, ref, self.send_sem.at[self.WAYS[way], part, t], arrive.at[part, t], target)
                copy.wait_send() if finish else copy.start()

            if way == "s":
                when(*only)(act)
            elif n > 1:
                when(*only, p < n - 1 if way[1] == "+" else p > 0)(act)

    def wait(self, part, t, finish):
        if not finish:
            arrived(self.piece(part, t, self.g.core), self.recv_sem.at[part, t])

    def column(self, q, spread, finish, *only):
        g = self.g
        t = g.chip(q, g.a, g.b)
        for part in self.PARTS:
            when(*only, q != g.z)(lambda: self.wait(part, t, finish))
            self.onward(part, t, ("z+",), finish, *only, q <= g.z)
            self.onward(part, t, ("z-",), finish, *only, q >= g.z)
            if spread:
                self.onward(part, t, self.SPREAD, finish, *only)

    def spread(self, q, finish, *only):
        g = self.g
        for part in self.PARTS:
            self.onward(part, g.chip(q, g.a, g.b), self.SPREAD, finish, *only)

    def both(self, axis, k, act):
        p, n = self.g.place(axis)
        pl.when(p >= k)(lambda: act(p - k, axis + "+"))
        pl.when(p + k < n)(lambda: act(p + k, axis + "-"))

    def along_a(self, q, finish=False):
        g = self.g

        def take(a, way):
            t = g.chip(q, a, g.b)
            for part in self.PARTS:
                self.wait(part, t, finish)
                self.onward(part, t, (way, "b+", "b-", "s"), finish)

        for k in range(1, g.na):
            self.both("a", k, take)

    def along_b(self, q, finish=False):
        g = self.g

        def row(b, way):
            def body(i, _):
                t = g.chip(q, lax.rem(g.a + i, g.na), b)
                for part in self.PARTS:
                    self.wait(part, t, finish)
                    self.onward(part, t, (way, "s"), finish)
                return 0

            lax.fori_loop(0, g.na, body, 0)

        for k in range(1, g.nb):
            self.both("b", k, row)

    def own(self, finish=False):
        if len(self.low) == 2:
            self.column(self.low[0], True, finish, self.below)
        self.column(self.high[0], False, finish, jnp.logical_not(self.below))

    def first(self, finish=False):
        below, above = self.below, jnp.logical_not(self.below)
        if len(self.low) == 2:
            self.column(self.low[0], True, finish, above)
        else:
            self.column(self.low[0], True, finish)
        for q in self.high[1:]:
            self.column(q, False, finish, above)
        self.along_a(self.low[0], finish)
        for q in self.low[1:]:
            self.column(q, True, finish)
            self.along_a(q, finish)
        self.spread(self.high[0], finish, above)
        self.column(self.high[0], True, finish, below)
        for q in self.low:
            self.along_b(q, finish)
        for q in self.high[1:]:
            self.column(q, False, finish, below)
        for q in self.high[1:]:
            self.spread(q, finish)

    def from_sibling(self, upper):
        g = self.g
        count = g.chips // 2

        def body(i, _):
            for part in self.PARTS:
                t = upper * count + i
                arrived(self.piece(part, t, 1 - g.core), self.sib_recv.at[part, t])
            return 0

        lax.fori_loop(0, count, body, 0)


def head_kernel(head_size, up_own, down_own, sq_own, vec_in, taps_in, x_in, cot_in, len_smem, coarse_ref, fine_ref,
                ud_full, sq_full, small_ref, x_ref, cot_ref, len_ref,
                x1_ref, a1_ref, h1_ref, s1_ref, a2_ref, heads_ref, pos_ref, att_ref, prob_hbm,
                own, len_in, columns, sbuf, up, down, wqkv, wpos, mine, prob_buf,
                move_send, move_recv, local_sem, swap_sem, recv_sem, sib_recv, gather_send, s_send, s_recv,
                load_sem, send_sem, heads_recv, prob_sem):
    g = Grid()
    z, nz, c = g.t, g.nz, g.core
    rows, width = x_in.shape
    cols = width // nz
    units = up.shape[0]
    half = up_own.shape[0]
    me = g.chip(g.z, g.a, g.b)
    own[0] = up_own[...].astype(BF)
    own[1] = down_own[...].astype(BF)
    own[2] = sq_own[...].astype(BF)
    here = pl.ds(me * 2 * half + c * half, half)
    local = [
        pltpu.make_async_copy(own.at[c], ud_full.at[c, here], local_sem.at[0]),
        pltpu.make_async_copy(own.at[2], sq_full.at[me, c], local_sem.at[1]),
    ]
    for copy in local:
        copy.start()
    len_in[...] = jnp.full(len_in.shape, len_smem[0].astype(F32))
    share = vec_in.shape[1]
    count = vec_in.shape[0]
    taps = taps_in.shape[1]
    lane = lax.broadcasted_iota(jnp.int32, (share, width), 1)
    column = lax.broadcasted_iota(jnp.int32, (share, width), 0)
    place = jnp.where(lane - (g.z * g.nf + g.f) * share == column, 1.0, 0.0).astype(BF)
    columns[...] = jnp.zeros_like(columns)
    columns[0:count, :] = dot(vec_in[...].astype(BF), place, NN)
    columns[count : count + taps, :] = dot(taps_in[...].astype(BF), place, TN)
    greet_lines(g, "cabz", g.owner())
    swap = remote(own.at[1 - c], ud_full.at[1 - c, here], swap_sem.at[0], swap_sem.at[1], g.sibling())
    swap.start()
    moves = [
        remote(src, dst, move_send.at[k], move_recv.at[k], g.worker())
        for k, (src, dst) in enumerate(((x_in, x_ref), (len_in, len_ref), (cot_in, cot_ref)))
    ]

    @pl.when(jnp.logical_not(g.at_home()))
    def _():
        for copy in moves[:2]:
            copy.start()

    @pl.when(g.at_home())
    def _():
        x_ref[...] = x_in[...]
        len_ref[...] = len_in[...]
        cot_ref[...] = cot_in[...]

    meeting = Meeting(g, sbuf, s_send, s_recv)
    meeting.start(0, columns[...].astype(BF))
    gather = Gather(g, ud_full, sq_full, recv_sem, sib_recv, gather_send)
    for copy in local:
        copy.wait()
    swap.wait_recv()
    gather.own()
    meeting.start(1, meeting.total(0))
    meeting.start(2, meeting.total(1))
    gather.first()
    meeting.start(3, meeting.total(2))

    @pl.when(jnp.logical_not(g.at_home()))
    def _():
        moves[2].start()
        for copy in moves[:2]:
            copy.wait()

    gather.from_sibling(0)
    loads = [
        pltpu.make_async_copy(ud_full.at[0, pl.ds(0, units)], up, load_sem.at[0]),
        pltpu.make_async_copy(ud_full.at[1, pl.ds(0, units)], down, load_sem.at[1]),
    ]
    per = width // (2 * half)
    squares = pltpu.make_async_copy(sq_full.at[pl.ds(0, 3 * per)], wqkv, load_sem.at[2])
    pieces = cols // half
    positions = [
        pltpu.make_async_copy(
            sq_full.at[3 * per + (z * pieces + i) // 2, (z * pieces + i) % 2],
            wpos.at[pl.ds(i * half, half)],
            load_sem.at[3],
        )
        for i in range(pieces)
    ]
    for load in loads + [squares]:
        load.start()
    for load in positions:
        load.start()
        load.wait()
    small_ref[...] = meeting.total(3).astype(F32)
    gains = small_ref[...]
    signal = x_ref[...].astype(F32)
    normed1 = norm_forward(signal, gains, 0)
    a1_ref[...] = normed1
    for load in loads:
        load.wait()
    resid1 = signal + 0.5 * module_forward(normed1, up, down, h1_ref, s1_ref)
    x1_ref[...] = resid1
    gather.along_a(gather.high[0])
    normed2 = norm_forward(resid1, gains, 1)
    a2_ref[...] = normed2
    squares.wait()
    for k in range(3):
        weight = wqkv[pl.ds(k * per, per)].reshape(width, width)
        out = dot(normed2, weight, NT).astype(BF)
        for q in range(nz):
            mine[q, k] = out[:, q * cols : (q + 1) * cols]
    sends = []
    for k in range(1, nz):
        q = lax.rem(z + k, nz)
        copy = remote(mine.at[q], heads_ref.at[:, pl.ds(z * rows, rows)], send_sem.at[k], heads_recv.at[z], g.time(q))
        copy.start()
        sends.append(copy)
    slot = pl.ds(pl.multiple_of(z * rows, rows), rows)
    for k in range(3):
        heads_ref[k, slot, :] = mine[z, k]
    for q in gather.high[1:]:
        gather.along_a(q)
    fine = fine_ref.shape[1]
    weight = wpos[...]

    def position(i, _):
        table = coarse_ref[0, pl.ds(i, 1), :] * fine_ref[0] + coarse_ref[1, pl.ds(i, 1), :] * fine_ref[1]
        there = pl.ds(pl.multiple_of(i * fine, fine), fine)
        pos_ref[there, :] = dot(table.astype(BF), weight, NT).astype(BF)
        return 0

    lax.fori_loop(0, coarse_ref.shape[1], position, 0)
    for k in range(1, nz):
        q = lax.rem(z + k, nz)
        arrived(heads_ref.at[:, pl.ds(q * rows, rows)], heads_recv.at[q])
    bias = small_ref[10:12, pl.ds(pl.multiple_of(z * cols, cols), cols)]

    def keep(i):
        return pltpu.make_async_copy(
            prob_buf.at[i % 2], prob_hbm.at[:, pl.ds(i * rows, rows)], prob_sem.at[i % 2]
        )

    def attend(i, _):
        pl.when(i >= 2)(lambda: keep(i - 2).wait())
        there = pl.ds(pl.multiple_of(i * rows, rows), rows)
        att_ref[there, :] = attend_block(
            head_size, i, heads_ref[0, there, :], heads_ref.at[1], heads_ref.at[2], pos_ref, bias, len_ref, prob_buf.at[i % 2]
        )
        keep(i).start()
        for k, q in enumerate(gather.high):
            pl.when(i == min(k, nz - 1))(lambda: gather.along_b(q))
        return 0

    lax.fori_loop(0, nz, attend, 0)
    gather.from_sibling(1)
    keep(nz - 2).wait()
    keep(nz - 1).wait()
    swap.wait_send()
    for copy in sends:
        copy.wait_send()
    meeting.finish()
    gather.own(True)
    gather.first(True)
    for q in gather.high:
        gather.along_a(q, True)
        gather.along_b(q, True)

    @pl.when(jnp.logical_not(g.at_home()))
    def _():
        moves[2].wait()


def head(upward, downward, square, vectors, kernel, signal, cotangent, lengths, coarse, fine, head_size):
    rows, width = signal.shape
    nz, nf = lax.axis_size("seq"), lax.axis_size("fsdp")
    devices = nz * nf
    chips, plane = devices // 2, nf // 2
    own = upward.shape[0]
    frames, cols = rows * nz, width // nz
    units = own * devices // 2
    heads = cols // head_size
    tall = -(-(vectors.shape[0] + kernel.shape[1]) // 16) * 16
    side = math.isqrt(plane)
    most = max(nz, side if side * side == plane else plane, 2)
    vmem = pl.BlockSpec(memory_space=pltpu.VMEM)
    hbm = pl.BlockSpec(memory_space=pl.ANY)
    shape = jax.ShapeDtypeStruct
    dma = pltpu.SemaphoreType.DMA
    return pl.pallas_call(
        lambda *refs: head_kernel(head_size, *refs),
        name="head",
        out_shape=(
            shape((2, devices * own, width), BF),
            shape((chips, 2, own, width), BF),
            shape((tall, width), F32),
            shape(signal.shape, signal.dtype),
            shape(cotangent.shape, cotangent.dtype),
            shape((8, LANES), F32),
            shape((rows, width), F32),
            shape((rows, width), BF),
            shape((rows, units), BF),
            shape((rows, units), BF),
            shape((rows, width), BF),
            shape((3, frames, cols), BF),
            shape((2 * frames, cols), BF),
            shape((frames, cols), BF),
            shape((heads, frames, frames), BF),
        ),
        in_specs=[vmem] * 7 + [pl.BlockSpec(memory_space=pltpu.SMEM)] + [vmem] * 2,
        out_specs=[hbm] * 2 + [vmem] * 12 + [hbm],
        scratch_shapes=[
            pltpu.VMEM((3, own, width), BF),
            pltpu.VMEM((8, LANES), F32),
            pltpu.VMEM((tall, width), F32),
            pltpu.VMEM((4, most, tall, width), BF),
            pltpu.VMEM((units, width), BF),
            pltpu.VMEM((units, width), BF),
            pltpu.VMEM((3 * width // (2 * own), 2, own, width), BF),
            pltpu.VMEM((cols, width), BF),
            pltpu.VMEM((nz, 3, rows, cols), BF),
            pltpu.VMEM((2, heads, rows, frames), BF),
            dma((3,)),
            dma((3,)),
            dma((2,)),
            dma((2,)),
            dma((3, chips)),
            dma((3, chips)),
            dma((7, 3, chips)),
            dma((4, most)),
            dma((4, most)),
            dma((4,)),
            dma((nz,)),
            dma((nz,)),
            dma((2,)),
        ],
        compiler_params=pltpu.CompilerParams(
            collective_id=5, has_side_effects=True, vmem_limit_bytes=56 * 1024 * 1024
        ),
    )(upward, downward, square, vectors, kernel, signal, cotangent, lengths, coarse, fine)


def per_device(
    inputs,
    cotangent,
    lengths,
    square,
    upward,
    downward,
    vectors,
    kernel,
    square_momentum,
    square_variance,
    upward_momentum,
    upward_variance,
    downward_momentum,
    downward_variance,
    vectors_momentum,
    vectors_variance,
    kernel_momentum,
    kernel_variance,
):
    model_width = inputs.shape[2]
    seq_frames = inputs.shape[1] * lax.axis_size("seq")
    head_size = D // H
    coarse, fine = position_tables(seq_frames, model_width)
    (
        full_ud, full_sq, small, signal, cotangent_here, length,
        resid1, normed1, hidden1, active1, normed2, heads, pos_heads, attended, prob,
    ) = head(upward, downward, square, vectors, kernel.T, inputs[0], cotangent[0], lengths, coarse, fine, head_size)
    full_sq = full_sq.reshape(model_width * 8, model_width)
    (
        layer_output, grad_res2, grad_out_head, out_time, grad_att_b, normed3, grad_pair, grad_conv_b, swish_b, normed4,
        active4, grad_hidden4, half4, small_grads, grad_taps,
    ) = middle(length, attended, resid1, cotangent_here, small, kernel.shape[0], full_ud, full_sq)
    input_grad, matrix_grads, square_grad, small_sums = back(
        heads, pos_heads, grad_out_head, prob, head_size, coarse, fine, small,
        signal, resid1, grad_res2, (normed1, hidden1, active1, normed2), (normed4, active4, grad_hidden4, half4),
        (out_time, grad_att_b, normed3, grad_pair, grad_conv_b, swish_b), small_grads, grad_taps, full_ud, full_sq,
    )
    (
        layer_output, input_grad,
        square_grad, square_next, momentum_square, variance_square,
        upward_grad, upward_next, momentum_upward, variance_upward,
        downward_grad, downward_next, momentum_downward, variance_downward,
        vectors_grad, vectors_next, momentum_vectors, variance_vectors,
        kernel_grad, kernel_next, momentum_kernel, variance_kernel,
    ) = finish(
        layer_output, input_grad, matrix_grads, square_grad, small_sums,
        (
            (square, square_momentum, square_variance),
            (upward, upward_momentum, upward_variance),
            (downward, downward_momentum, downward_variance),
            (vectors, vectors_momentum, vectors_variance),
            (kernel.T, kernel_momentum.T, kernel_variance.T),
        ),
    )
    return (
        layer_output[None],
        input_grad[None],
        square_grad,
        upward_grad,
        downward_grad,
        vectors_grad,
        kernel_grad.T,
        square_next,
        upward_next,
        downward_next,
        vectors_next,
        kernel_next.T,
        momentum_square,
        variance_square,
        momentum_upward,
        variance_upward,
        momentum_downward,
        variance_downward,
        momentum_vectors,
        variance_vectors,
        momentum_kernel.T,
        variance_kernel.T,
    )


def solution(mesh):
    return jax.shard_map(
        per_device,
        mesh=mesh,
        in_specs=(
            P("fsdp", "seq", None),
            P("fsdp", "seq", None),
            P("fsdp"),
            P(("seq", "fsdp"), None),
            P(("seq", "fsdp"), None),
            P(("seq", "fsdp"), None),
            P(None, ("seq", "fsdp")),
            P(None, ("seq", "fsdp")),
            P(("seq", "fsdp"), None),
            P(("seq", "fsdp"), None),
            P(("seq", "fsdp"), None),
            P(("seq", "fsdp"), None),
            P(("seq", "fsdp"), None),
            P(("seq", "fsdp"), None),
            P(None, ("seq", "fsdp")),
            P(None, ("seq", "fsdp")),
            P(None, ("seq", "fsdp")),
            P(None, ("seq", "fsdp")),
        ),
        out_specs=(
            P("fsdp", "seq", None),
            P("fsdp", "seq", None),
            P(("seq", "fsdp"), None),
            P(("seq", "fsdp"), None),
            P(("seq", "fsdp"), None),
            P(None, ("seq", "fsdp")),
            P(None, ("seq", "fsdp")),
            P(("seq", "fsdp"), None),
            P(("seq", "fsdp"), None),
            P(("seq", "fsdp"), None),
            P(None, ("seq", "fsdp")),
            P(None, ("seq", "fsdp")),
            P(("seq", "fsdp"), None),
            P(("seq", "fsdp"), None),
            P(("seq", "fsdp"), None),
            P(("seq", "fsdp"), None),
            P(("seq", "fsdp"), None),
            P(("seq", "fsdp"), None),
            P(None, ("seq", "fsdp")),
            P(None, ("seq", "fsdp")),
            P(None, ("seq", "fsdp")),
            P(None, ("seq", "fsdp")),
        ),
        check_vma=False,
    )
```
